8 devices in a mesh: col: 2 (over z, y), row: 4 (over x, core).
Axes of the slice: x: 2, y: 2, z: 1, core: 2. Of those that a mesh axis runs over, the one named last changes fastest.
Arguments:
- vel_x: float32 [20, 2, 512, 512], P(None, None, 'row', 'col')
- vel_y: float32 [20, 2, 512, 512], P(None, None, 'row', 'col')
- pot_temp: float32 [20, 2, 512, 512], P(None, None, 'row', 'col')
- salinity: float32 [20, 2, 512, 512], P(None, None, 'row', 'col')
- surf_eta: float32 [2, 512, 512], P(None, 'row', 'col')
- trans_x: float32 [2, 512, 512], P(None, 'row', 'col')
- trans_y: float32 [2, 512, 512], P(None, 'row', 'col')
- col_depth: float32 [512, 512], P('row', 'col')
- wet_levels: int32 [512, 512], P('row', 'col')
- avg_weights: float32 [20], replicated
Outputs:
- output 1: float32 [2, 512, 512], P(None, 'row', 'col')
- output 2: float32 [2, 512, 512], P(None, 'row', 'col')
- output 3: float32 [2, 512, 512], P(None, 'row', 'col')
- output 4: float32 [20, 2, 512, 512], P(None, None, 'row', 'col')
- output 5: float32 [20, 2, 512, 512], P(None, None, 'row', 'col')
- output 6: float32 [20, 2, 512, 512], P(None, None, 'row', 'col')
- output 7: float32 [20, 2, 512, 512], P(None, None, 'row', 'col')
All inputs are finite; a program needn't handle non-finite values.
Results may differ from the reference program's by a relative error of at most 0.001.
Values sent between devices are 32-bit elements.
A program may use at most 1 GiB of HBM per device.

```python
import jax
import jax.numpy as jnp
from jax import lax

MEMBERS = 2
LEVELS = 20
SUBCYCLES = 20
GRID_Y = 512
GRID_X = 512

WAVE_COURANT = 0.4
THERM_EXP = 0.2
HALINE_CON = 0.15
PRESS_SCALE = 0.5
VISC_NUMBER = 1.0
DIFF_NUMBER = 0.5


def east_of(field_in):
    return jnp.roll(field_in, -1, axis=-1)


def west_of(field_in):
    return jnp.roll(field_in, 1, axis=-1)


def north_of(field_in):
    return jnp.concatenate([field_in[..., 1:, :], jnp.zeros_like(field_in[..., :1, :])], axis=-2)


def south_of(field_in):
    return jnp.concatenate([jnp.zeros_like(field_in[..., :1, :]), field_in[..., :-1, :]], axis=-2)


def wet_masks(wet_levels, level_total):
    levels = jnp.arange(level_total).reshape(level_total, 1, 1, 1)
    cell_mask = (levels < wet_levels).astype(jnp.float32)
    xface_mask = cell_mask * (levels < east_of(wet_levels)).astype(jnp.float32)
    yface_mask = cell_mask * (levels < north_of(wet_levels)).astype(jnp.float32)
    return cell_mask, xface_mask, yface_mask


def setup_inputs(seed: int = 0) -> dict:
    key_list = jax.random.split(jax.random.key(seed), 12)
    shape_3d = (LEVELS, MEMBERS, GRID_Y, GRID_X)
    shape_2d = (MEMBERS, GRID_Y, GRID_X)
    land_draw = jax.random.randint(key_list[0], (GRID_Y, GRID_X), 0, 10)
    depth_draw = jax.random.randint(key_list[1], (GRID_Y, GRID_X), 1, LEVELS + 1)
    wet_levels = jnp.where(land_draw == 0, 0, jnp.where(land_draw < 5, LEVELS, depth_draw)).astype(jnp.int32)
    cell_mask, xface_mask, yface_mask = wet_masks(wet_levels, LEVELS)
    profile = jnp.cos(jnp.pi * (jnp.arange(LEVELS) + 0.5) / LEVELS).reshape(LEVELS, 1, 1, 1)

    def tracer_field(key_pair):
        key_a, key_b, key_c = jax.random.split(key_pair, 3)
        base_field = jax.random.normal(key_a, shape_2d, jnp.float32)
        mode_field = jax.random.normal(key_b, shape_2d, jnp.float32)
        noise_3d = jax.random.normal(key_c, shape_3d, jnp.float32)
        return cell_mask * (base_field + mode_field * profile + 0.3 * noise_3d)

    vel_x = xface_mask * 0.3 * jax.random.normal(key_list[2], shape_3d, jnp.float32)
    vel_y = yface_mask * 0.3 * jax.random.normal(key_list[3], shape_3d, jnp.float32)
    pot_temp = tracer_field(key_list[4])
    salinity = tracer_field(key_list[5])
    surf_eta = cell_mask[0] * 0.3 * jax.random.normal(key_list[6], shape_2d, jnp.float32)
    trans_x = xface_mask[0] * 0.3 * jax.random.normal(key_list[7], shape_2d, jnp.float32)
    trans_y = yface_mask[0] * 0.3 * jax.random.normal(key_list[8], shape_2d, jnp.float32)
    col_depth = 0.5 + 1.5 * jax.random.uniform(key_list[9], (GRID_Y, GRID_X), jnp.float32)
    step_frac = (jnp.arange(SUBCYCLES) + 1.0) / SUBCYCLES
    raw_weights = step_frac * step_frac * (2.0 - step_frac * step_frac) * (0.3 + 1.4 * jax.random.uniform(key_list[10], (SUBCYCLES,), jnp.float32))
    avg_weights = raw_weights / jnp.sum(raw_weights)
    return {"vel_x": vel_x, "vel_y": vel_y, "pot_temp": pot_temp, "salinity": salinity, "surf_eta": surf_eta, "trans_x": trans_x, "trans_y": trans_y, "col_depth": col_depth, "wet_levels": wet_levels, "avg_weights": avg_weights}


def vertical_solve(right_side, face_mask, strength):
    mask_below = jnp.concatenate([face_mask[1:], jnp.zeros_like(face_mask[:1])], axis=0)
    face_up = face_mask * mask_below
    face_down = jnp.concatenate([jnp.zeros_like(face_up[:1]), face_up[:-1]], axis=0)
    lower_diag = -strength * face_down
    upper_diag = -strength * face_up
    main_diag = 1.0 + strength * (face_down + face_up)

    def forward(state_prev, level_row):
        upper_prev, side_prev = state_prev
        low_k, diag_k, up_k, side_k = level_row
        divisor = diag_k - low_k * upper_prev
        upper_new = up_k / divisor
        side_new = (side_k - low_k * side_prev) / divisor
        return (upper_new, side_new), (upper_new, side_new)

    zero_level = jnp.zeros_like(right_side[0])
    upper_all, side_all = lax.scan(forward, (zero_level, zero_level), (lower_diag, main_diag, upper_diag, right_side))[1]

    def backward(sol_next, level_row):
        up_k, side_k = level_row
        sol_k = side_k - up_k * sol_next
        return sol_k, sol_k

    return lax.scan(backward, zero_level, (upper_all, side_all), reverse=True)[1]


def tracer_step(tracer, vel_x, vel_y, cell_mask):
    flux_x = vel_x * 0.5 * (tracer + east_of(tracer))
    flux_y = vel_y * 0.5 * (tracer + north_of(tracer))
    advected = cell_mask * (tracer - (flux_x - west_of(flux_x) + flux_y - south_of(flux_y)))
    return vertical_solve(advected, cell_mask, DIFF_NUMBER)


def barotropic(surf_eta, trans_x, trans_y, force_x, force_y, depth_x, depth_y, wet_top, xface_top, yface_top, avg_weights):
    sub_count = avg_weights.shape[0]
    step_x = force_x / sub_count
    step_y = force_y / sub_count

    def subcycle(sub_state, weight):
        eta_now, tx_now, ty_now, eta_avg, tx_avg, ty_avg = sub_state
        eta_now = wet_top * (eta_now - WAVE_COURANT * (tx_now - west_of(tx_now) + ty_now - south_of(ty_now)))
        tx_now = xface_top * (tx_now + step_x - WAVE_COURANT * depth_x * (east_of(eta_now) - eta_now))
        ty_now = yface_top * (ty_now + step_y - WAVE_COURANT * depth_y * (north_of(eta_now) - eta_now))
        return (eta_now, tx_now, ty_now, eta_avg + weight * eta_now, tx_avg + weight * tx_now, ty_avg + weight * ty_now), None

    zero_field = jnp.zeros_like(surf_eta)
    end_state = lax.scan(subcycle, (surf_eta, trans_x, trans_y, zero_field, zero_field, zero_field), avg_weights)[0]
    return end_state[3], end_state[4], end_state[5]


def reference(vel_x, vel_y, pot_temp, salinity, surf_eta, trans_x, trans_y, col_depth, wet_levels, avg_weights):
    level_count = vel_x.shape[0]
    cell_mask, xface_mask, yface_mask = wet_masks(wet_levels, level_count)
    density = HALINE_CON * salinity - THERM_EXP * pot_temp
    pressure = (PRESS_SCALE / level_count) * (jnp.cumsum(density, axis=0) - 0.5 * density)
    vy_south = south_of(vel_y)
    vx_north = north_of(vel_x)
    vy_at_x = 0.25 * (vel_y + vy_south + east_of(vel_y) + east_of(vy_south))
    vx_at_y = 0.25 * (vel_x + west_of(vel_x) + vx_north + west_of(vx_north))
    tend_x = xface_mask * (pressure - east_of(pressure) - 0.5 * vel_x * (east_of(vel_x) - west_of(vel_x)) - 0.5 * vy_at_x * (vx_north - south_of(vel_x)))
    tend_y = yface_mask * (pressure - north_of(pressure) - 0.5 * vx_at_y * (east_of(vel_y) - west_of(vel_y)) - 0.5 * vel_y * (north_of(vel_y) - vy_south))
    count_x = jnp.maximum(jnp.sum(xface_mask, axis=0), 1.0)
    count_y = jnp.maximum(jnp.sum(yface_mask, axis=0), 1.0)
    depth_x = 0.5 * (col_depth + east_of(col_depth)) * xface_mask[0]
    depth_y = 0.5 * (col_depth + north_of(col_depth)) * yface_mask[0]
    force_x = depth_x * jnp.sum(tend_x, axis=0) / count_x
    force_y = depth_y * jnp.sum(tend_y, axis=0) / count_y
    pred_x = vertical_solve(vel_x + tend_x, xface_mask, VISC_NUMBER)
    pred_y = vertical_solve(vel_y + tend_y, yface_mask, VISC_NUMBER)
    temp_new = tracer_step(pot_temp, vel_x, vel_y, cell_mask)
    salt_new = tracer_step(salinity, vel_x, vel_y, cell_mask)
    eta_new, trans_x_new, trans_y_new = barotropic(surf_eta, trans_x, trans_y, force_x, force_y, depth_x, depth_y, cell_mask[0], xface_mask[0], yface_mask[0], avg_weights)
    vel_x_new = xface_mask * (pred_x - jnp.sum(pred_x, axis=0) / count_x + trans_x_new / (depth_x + 1.0 - xface_mask[0]))
    vel_y_new = yface_mask * (pred_y - jnp.sum(pred_y, axis=0) / count_y + trans_y_new / (depth_y + 1.0 - yface_mask[0]))
    return eta_new, trans_x_new, trans_y_new, vel_x_new, vel_y_new, temp_new, salt_new
```

```python
import functools
import numpy as np
import jax
import jax.numpy as jnp
from jax import lax
from jax.experimental import pallas as pl
from jax.experimental.pallas import tpu as pltpu
from jax.sharding import PartitionSpec as P

WAVE_COURANT = 0.4
THERM_EXP = 0.2
HALINE_CON = 0.15
PRESS_SCALE = 0.5
VISC_NUMBER = 1.0
DIFF_NUMBER = 0.5

LEVELS = 20
SUBS = 20
CHUNK = 4
NCH = LEVELS // CHUNK
PAIRS = 2 * CHUNK
ROWS = 128
LN = 128
PR = 144
EXT = 192
F32 = jnp.float32
PK = 32
UP = 32
MESH_ID = pl.DeviceIdType.MESH


def solve_table(strength):
    inner = np.zeros(LEVELS)
    last = np.zeros(LEVELS)
    inner[0] = 1.0 + strength
    last[0] = 1.0
    for k in range(1, LEVELS):
        inner[k] = 1.0 + 2.0 * strength - strength**2 / inner[k - 1]
        last[k] = 1.0 + strength - strength**2 / inner[k - 1]
    ratio = strength / inner
    before = np.concatenate([[0.0], ratio[:-1]])
    return np.stack([before, ratio, 1.0 / inner, 1.0 / last]).astype(np.float32)


def lanes(rows):
    return lax.broadcasted_iota(jnp.int32, (rows, LN), 1)


def east(tile, following):
    return pltpu.roll(jnp.where(lanes(tile.shape[0]) == 0, following, tile), LN - 1, 1)


def west(tile, previous):
    return pltpu.roll(jnp.where(lanes(tile.shape[0]) == LN - 1, previous, tile), 1, 1)


NEXT = (1, 2, 0)
PREV = (2, 0, 1)


def unpack_columns(packed, buf, chunk, fields, index_of):
    def block(i, carry):
        r = pl.multiple_of(i * 16, 16)
        tile = packed[pl.ds(r, 16), :]
        for f in fields:
            for kk in range(CHUNK):
                for m in range(2):
                    j = f * PAIRS + kk * 2 + m
                    buf[index_of[f], chunk * CHUNK + kk, m, 2, pl.ds(8 + r, 16), :] = pltpu.roll(tile, LN - 1 - 2 * j, 1)
        return carry
    lax.fori_loop(0, ROWS // 16, block, 0)


def momentum_kernel(u_hbm, v_hbm, t_hbm, s_hbm, eta_hbm, tx_hbm, ty_hbm, h_hbm, kmt_ref, weights, table,
                    us_hbm, vs_hbm, eta_out, tx_out, ty_out, corr_out, kmask_out, col_out, rows_out,
                    buf, tu, tv, pbuf, pacc, gsum, xsum, ku, kv,
                    send_col, recv_col, send_row, recv_row, send_dia, recv_dia,
                    xb, sp, rp, xf, sf, rf, hux, huy, ae, aw, an, as_, cc, ebuf, dbuf, gbuf, eacc, bacc,
                    ld_sem, xl_sem, cs_sem, cr_sem, xs_sem, xr_sem, fs_sem, fr_sem, st_sem, ot_sem):
    me_c = lax.axis_index("col")
    me_r = lax.axis_index("row")
    peer = 1 - me_c
    has_n = me_r < 3
    has_s = me_r > 0
    hbm = (u_hbm, v_hbm, t_hbm, s_hbm)

    def loads(c):
        out = []
        for f in range(4):
            for t in range(2):
                out.append(pltpu.make_async_copy(
                    hbm[f].at[pl.ds(c * CHUNK, CHUNK), :, :, pl.ds(t * LN, LN)],
                    buf.at[f, pl.ds(c * CHUNK, CHUNK), :, t, pl.ds(8, ROWS), :], ld_sem.at[c, f * 2 + t]))
        return out

    def ext_loads():
        out = []
        for t in range(2):
            lane = pl.ds(t * LN, LN)
            out.append(pltpu.make_async_copy(h_hbm.at[:, lane], xb.at[1, t, pl.ds(32, ROWS), :], xl_sem.at[t]))
            for i, ref in enumerate((eta_hbm, tx_hbm, ty_hbm)):
                out.append(pltpu.make_async_copy(ref.at[:, :, lane], xb.at[pl.ds(2 + 2 * i, 2), t, pl.ds(32, ROWS), :], xl_sem.at[2 + 2 * i + t]))
        return out

    for copy in ext_loads() + loads(0) + loads(1):
        copy.start()

    barrier = pltpu.get_barrier_semaphore()

    def greet(col, row):
        pl.semaphore_signal(barrier, inc=1, device_id={"col": col, "row": row}, device_id_type=MESH_ID)

    greet(peer, me_r)

    @pl.when(has_n)
    def _():
        greet(me_c, me_r + 1)
        greet(peer, me_r + 1)

    @pl.when(has_s)
    def _():
        greet(me_c, me_r - 1)
        greet(peer, me_r - 1)

    zrow = jnp.zeros((8, LN), F32)
    for ref, count in ((xb, 8), (xf, 4)):
        for f in range(count):
            for t in range(3):
                ref[f, t, 0:8, :] = zrow
                ref[f, t, EXT - 8:EXT, :] = zrow
    for ref, count in ((rp, 4), (rf, 2)):
        for f in range(count):
            ref[f, 0:8, :] = zrow
            ref[f, EXT - 8:EXT, :] = zrow

    def zero_side(side, lo):
        z24 = jnp.zeros((24, LN), F32)
        for f in range(8):
            for t in range(2):
                xb[f, t, lo:lo + 24, :] = z24
        for f in range(4):
            rp[f, lo:lo + 24, :] = z24
            for t in range(2):
                xf[f, t, lo:lo + 24, :] = z24
        for f in range(2):
            rf[f, lo:lo + 24, :] = z24
        for c in range(NCH):
            recv_dia[side, c, :, :] = zrow
            for f in range(4):
                for t in range(2):
                    recv_row[side, c, t, f, :, :] = zrow

    @pl.when(me_r == 0)
    def _():
        zero_side(0, 8)

    @pl.when(me_r == 3)
    def _():
        zero_side(1, 160)

    def zero_planes(i, carry):
        r = pl.multiple_of(i * 16, 16)
        z = jnp.zeros((16, LN), F32)
        for m in range(2):
            for t in range(3):
                pacc[m, t, pl.ds(r, 16), :] = z
        return carry
    lax.fori_loop(0, PR // 16, zero_planes, 0)

    def zero_planes2(i, carry):
        r = pl.multiple_of(i * 16, 16)
        z = jnp.zeros((16, LN), F32)
        for m in range(2):
            for t in range(2):
                for f in range(2):
                    gsum[f, m, t, pl.ds(r, 16), :] = z
                    xsum[f, m, t, pl.ds(r, 16), :] = z
                for ref in (tu, tv):
                    ref[0, m, t, pl.ds(r, 16), :] = z
                    ref[LEVELS + 1, m, t, pl.ds(r, 16), :] = z
        return carry
    lax.fori_loop(0, ROWS // 16, zero_planes2, 0)

    for t in range(2):
        for r in range(0, ROWS, 32):
            xb[0, t, 32 + r:64 + r, :] = kmt_ref[r:r + 32, t * LN:(t + 1) * LN].astype(F32)
    for copy in ext_loads():
        copy.wait()

    def pack_pair(first, second, send, slot, rows):
        lane = lanes(rows)

        def block(i, carry):
            r = pl.multiple_of(i * rows, rows)
            a = jnp.where(lane < 64, first(0, r), first(1, r))
            b = jnp.where(lane < 64, second(0, r), second(1, r))
            outer = (lane < 32) | (lane >= 96)
            send[slot, pl.ds(r, rows), :] = jnp.where(outer, a, pltpu.roll(b, 64, 1))
            return carry
        lax.fori_loop(0, ROWS // rows, block, 0)

    for pair in range(4):
        pack_pair(lambda t, r, p=pair: xb[2 * p, t, pl.ds(32 + r, 64), :],
                  lambda t, r, p=pair: xb[2 * p + 1, t, pl.ds(32 + r, 64), :], sp, pair, 64)

    @pl.when((me_r == 0) | (me_r == 3))
    def _():
        pl.semaphore_wait(barrier, 3)

    @pl.when((me_r != 0) & (me_r != 3))
    def _():
        pl.semaphore_wait(barrier, 5)

    def remote(src, dst, ssem, rsem, col, row):
        return pltpu.make_async_remote_copy(src_ref=src, dst_ref=dst, send_sem=ssem, recv_sem=rsem,
                                            device_id={"col": col, "row": row}, device_id_type=MESH_ID)

    def wide_copies(own, packed, landing, ssem, rsem):
        north, south = me_r + 1, me_r - 1
        side = remote(packed, landing.at[:, pl.ds(32, ROWS), :], ssem.at[0], rsem.at[0], peer, me_r)
        up = (remote(own.at[:, pl.ds(0, 2), pl.ds(136, 24), :], own.at[:, pl.ds(0, 2), pl.ds(8, 24), :], ssem.at[1], rsem.at[1], me_c, north),
              remote(packed.at[:, pl.ds(104, 24), :], landing.at[:, pl.ds(8, 24), :], ssem.at[2], rsem.at[2], peer, north))
        down = (remote(own.at[:, pl.ds(0, 2), pl.ds(32, 24), :], own.at[:, pl.ds(0, 2), pl.ds(160, 24), :], ssem.at[3], rsem.at[3], me_c, south),
                remote(packed.at[:, pl.ds(0, 24), :], landing.at[:, pl.ds(160, 24), :], ssem.at[4], rsem.at[4], peer, south))
        return side, up, down

    def edge_copies(c):
        north, south = me_r + 1, me_r - 1
        side = remote(send_col.at[c], recv_col.at[c], cs_sem.at[c, 0], cr_sem.at[c, 0], peer, me_r)
        up = (remote(send_row.at[0, c], recv_row.at[0, c], cs_sem.at[c, 1], cr_sem.at[c, 1], me_c, north),
              remote(send_dia.at[0, c], recv_dia.at[0, c], cs_sem.at[c, 2], cr_sem.at[c, 2], peer, north))
        down = (remote(send_row.at[1, c], recv_row.at[1, c], cs_sem.at[c, 3], cr_sem.at[c, 3], me_c, south),
                remote(send_dia.at[1, c], recv_dia.at[1, c], cs_sem.at[c, 4], cr_sem.at[c, 4], peer, south))
        return side, up, down

    def start_all(copies):
        side, up, down = copies
        side.start()

        @pl.when(has_n)
        def _():
            for copy in up:
                copy.start()

        @pl.when(has_s)
        def _():
            for copy in down:
                copy.start()

    def wait_recv_all(copies):
        side, up, down = copies
        side.wait_recv()

        @pl.when(has_s)
        def _():
            for copy in up:
                copy.wait_recv()

        @pl.when(has_n)
        def _():
            for copy in down:
                copy.wait_recv()

    def wait_send_all(copies):
        side, up, down = copies
        side.wait_send()

        @pl.when(has_n)
        def _():
            for copy in up:
                copy.wait_send()

        @pl.when(has_s)
        def _():
            for copy in down:
                copy.wait_send()

    start_all(wide_copies(xb, sp, rp, xs_sem, xr_sem))

    def pack_and_send(c):
        for copy in loads(c):
            copy.wait()
        lane = lanes(PK)

        def block(i, carry):
            r = pl.multiple_of(i * PK, PK)
            packed = jnp.zeros((PK, LN), F32)
            for f in range(4):
                for kk in range(CHUNK):
                    for m in range(2):
                        j = f * PAIRS + kk * 2 + m
                        k = c * CHUNK + kk
                        edge = jnp.where(lane == 0, buf[f, k, m, 0, pl.ds(8 + r, PK), :], buf[f, k, m, 1, pl.ds(8 + r, PK), :])
                        packed = jnp.where(lane >= 2 * j, pltpu.roll(edge, 2 * j + 1, 1), packed)
            send_col[c, pl.ds(r, PK), :] = packed
            return carry
        lane1 = lanes(1)
        for kk in range(CHUNK):
            for m in range(2):
                jj = kk * 2 + m
                k = c * CHUNK + kk
                for side, row, dia in ((0, 8 + ROWS - 1, 1), (1, 8, 0)):
                    for f in range(4):
                        a = buf[f, k, m, 0, row:row + 1, :]
                        b = buf[f, k, m, 1, row:row + 1, :]
                        send_row[side, c, 0, f, jj:jj + 1, :] = a
                        send_row[side, c, 1, f, jj:jj + 1, :] = b
                        if f == dia:
                            send_dia[side, c, jj:jj + 1, :] = jnp.where(lane1 == 0, a, b)
        lax.fori_loop(0, ROWS // PK, block, 0)
        start_all(edge_copies(c))

    pack_and_send(0)
    for copy in loads(2):
        copy.start()
    pack_and_send(1)

    wait_recv_all(wide_copies(xb, sp, rp, xs_sem, xr_sem))

    def unpack_wide(i, carry):
        r = pl.multiple_of(i * 32, 32)
        for pair in range(4):
            tile = rp[pair, pl.ds(r, 32), :]
            xb[2 * pair, 2, pl.ds(r, 32), :] = tile
            xb[2 * pair + 1, 2, pl.ds(r, 32), :] = pltpu.roll(tile, 64, 1)
        return carry
    lax.fori_loop(0, EXT // 32, unpack_wide, 0)

    XR = 88

    def depths(i, carry):
        r = pl.multiple_of(8 + i * XR, 8)
        kt = [xb[0, t, pl.ds(r, XR), :] for t in range(3)]
        ht = [xb[1, t, pl.ds(r, XR), :] for t in range(3)]
        for t in range(3):
            kx = jnp.minimum(kt[t], east(kt[t], kt[NEXT[t]]))
            ky = jnp.minimum(kt[t], xb[0, t, pl.ds(r + 1, XR), :])
            hux[t, pl.ds(r, XR), :] = jnp.where(kx > 0.0, 0.5 * (ht[t] + east(ht[t], ht[NEXT[t]])), 0.0)
            huy[t, pl.ds(r, XR), :] = jnp.where(ky > 0.0, 0.5 * (ht[t] + xb[1, t, pl.ds(r + 1, XR), :]), 0.0)
            cc[t, pl.ds(r, XR), :] = jnp.where(kt[t] > 0.0, WAVE_COURANT, 0.0)
        return carry
    for t in range(3):
        for ref in (hux, huy):
            ref[t, 0:8, :] = zrow
        for p in range(2):
            for m in range(2):
                ebuf[p, m, t, 0:8, :] = zrow
                ebuf[p, m, t, EXT - 8:EXT, :] = zrow
    lax.fori_loop(0, 2, depths, 0)

    def face_levels(i, carry):
        r = pl.multiple_of(i * 64, 64)
        kt = [xb[0, t, pl.ds(32 + r, 64), :] for t in range(3)]
        for t in range(2):
            ku[t, pl.ds(r, 64), :] = jnp.minimum(kt[t], east(kt[t], kt[NEXT[t]]))
            kv[t, pl.ds(r, 64), :] = jnp.minimum(kt[t], xb[0, t, pl.ds(33 + r, 64), :])
            kmask_out[0, t, pl.ds(r, 64), :] = kt[t]
        return carry
    lax.fori_loop(0, 2, face_levels, 0)

    def coefficients(i, carry):
        r = pl.multiple_of(8 + i * XR, 8)
        hx = [hux[t, pl.ds(r, XR), :] for t in range(3)]
        for t in range(3):
            c0 = cc[t, pl.ds(r, XR), :]
            cw = WAVE_COURANT * c0
            ae[t, pl.ds(r, XR), :] = cw * hx[t]
            aw[t, pl.ds(r, XR), :] = cw * west(hx[t], hx[PREV[t]])
            an[t, pl.ds(r, XR), :] = cw * huy[t, pl.ds(r, XR), :]
            as_[t, pl.ds(r, XR), :] = cw * huy[t, pl.ds(r - 1, XR), :]
        return carry
    lax.fori_loop(0, 2, coefficients, 0)

    def first_subcycle(m, base, rows):
        tx = [xb[4 + m, t, pl.ds(base, rows), :] for t in range(3)]
        for t in range(3):
            c0 = cc[t, pl.ds(base, rows), :]
            ty = xb[6 + m, t, pl.ds(base, rows), :]
            div = tx[t] - west(tx[t], tx[PREV[t]]) + ty - xb[6 + m, t, pl.ds(base - 1, rows), :]
            change = -c0 * div
            dbuf[m, t, pl.ds(base, rows), :] = change
            eta = jnp.where(c0 > 0.0, xb[2 + m, t, pl.ds(base, rows), :], 0.0) + change
            ebuf[1, m, t, pl.ds(base, rows), :] = eta

    def first_block(i, carry):
        for m in range(2):
            first_subcycle(m, pl.multiple_of(8 + i * XR, 8), XR)
        return carry
    lax.fori_loop(0, 2, first_block, 0)

    RHO_T = np.float32(-THERM_EXP * PRESS_SCALE / LEVELS / 2)
    RHO_S = np.float32(HALINE_CON * PRESS_SCALE / LEVELS / 2)
    BR = 64

    def pressure_rows(k, base, rows, tiles):
        for m in range(2):
            for t in tiles:
                half = RHO_T * buf[2, k, m, t, pl.ds(base, rows), :] + RHO_S * buf[3, k, m, t, pl.ds(base, rows), :]
                p = pacc[m, t, pl.ds(base, rows), :] + half
                pbuf[m, t, pl.ds(base, rows), :] = p
                pacc[m, t, pl.ds(base, rows), :] = p + half

    def level(k):
        def pressure_block(i, carry):
            pressure_rows(k, pl.multiple_of(8 + i * 64, 8), 64, range(3))
            return carry
        lax.fori_loop(0, 2, pressure_block, 0)
        pressure_rows(k, 8 + ROWS, 8, range(2))
        level_no = k.astype(F32)
        before = table[0, k]

        def block(i, carry):
            r = pl.multiple_of(i * BR, BR)
            b = pl.multiple_of(8 + i * BR, 8)
            wet_x = [ku[t, pl.ds(r, BR), :] > level_no for t in range(2)]
            wet_y = [kv[t, pl.ds(r, BR), :] > level_no for t in range(2)]
            for m in range(2):
                u = [buf[0, k, m, t, pl.ds(b, BR), :] for t in range(3)]
                v = [buf[1, k, m, t, pl.ds(b, BR), :] for t in range(3)]
                un = [buf[0, k, m, t, pl.ds(b + 1, BR), :] for t in range(3)]
                vs = [buf[1, k, m, t, pl.ds(b - 1, BR), :] for t in range(3)]
                p = [pbuf[m, t, pl.ds(b, BR), :] for t in range(3)]
                w = [v[t] + vs[t] for t in range(3)]
                z = [u[t] + un[t] for t in range(3)]
                for t in range(2):
                    nx, pv = NEXT[t], PREV[t]
                    us = buf[0, k, m, t, pl.ds(b - 1, BR), :]
                    gu = (p[t] - east(p[t], p[nx])) - (0.5 * u[t]) * (east(u[t], u[nx]) - west(u[t], u[pv])) \
                        - (0.125 * (w[t] + east(w[t], w[nx]))) * (un[t] - us)
                    gu = jnp.where(wet_x[t], gu, 0.0)
                    gsum[0, m, t, pl.ds(r, BR), :] += gu
                    tu[k + 1, m, t, pl.ds(r, BR), :] = u[t] + gu + before * tu[k, m, t, pl.ds(r, BR), :]
                    vn = buf[1, k, m, t, pl.ds(b + 1, BR), :]
                    pn = pbuf[m, t, pl.ds(b + 1, BR), :]
                    gv = (p[t] - pn) - (0.125 * (z[t] + west(z[t], z[pv]))) * (east(v[t], v[nx]) - west(v[t], v[pv])) \
                        - (0.5 * v[t]) * (vn - vs[t])
                    gv = jnp.where(wet_y[t], gv, 0.0)
                    gsum[1, m, t, pl.ds(r, BR), :] += gv
                    tv[k + 1, m, t, pl.ds(r, BR), :] = v[t] + gv + before * tv[k, m, t, pl.ds(r, BR), :]
            return carry
        lax.fori_loop(0, ROWS // BR, block, 0)

    def chunk_step(c, carry):
        @pl.when(c + 3 < NCH)
        def _():
            for copy in loads(c + 3):
                copy.start()

        @pl.when(c + 2 < NCH)
        def _():
            pack_and_send(c + 2)

        wait_recv_all(edge_copies(c))
        unpack_columns(recv_col.at[c], buf, c, range(4), range(4))
        for kk in range(CHUNK):
            k = c * CHUNK + kk
            for m in range(2):
                jj = kk * 2 + m
                for side, row, dia in ((0, 7, 1), (1, 8 + ROWS, 0)):
                    for f in range(4):
                        for t in range(2):
                            buf[f, k, m, t, row:row + 1, :] = recv_row[side, c, t, f, jj:jj + 1, :]
                    buf[dia, k, m, 2, row:row + 1, :] = recv_dia[side, c, jj:jj + 1, :]

        def one_level(kk, carry2):
            level(c * CHUNK + kk)
            return carry2
        lax.fori_loop(0, CHUNK, one_level, 0)
        return carry
    lax.fori_loop(0, NCH, chunk_step, 0)

    packet_copies = [pltpu.make_async_copy(recv_col, col_out, ot_sem.at[0]),
                     pltpu.make_async_copy(recv_row, rows_out, ot_sem.at[1])]
    for copy in packet_copies:
        copy.start()

    def forcing(i, carry):
        r = pl.multiple_of(i * 32, 32)
        for t in range(2):
            nx = jnp.maximum(ku[t, pl.ds(r, 32), :], 1.0)
            ny = jnp.maximum(kv[t, pl.ds(r, 32), :], 1.0)
            fx = hux[t, pl.ds(32 + r, 32), :] / nx / SUBS
            fy = huy[t, pl.ds(32 + r, 32), :] / ny / SUBS
            for m in range(2):
                xf[m, t, pl.ds(32 + r, 32), :] = fx * gsum[0, m, t, pl.ds(r, 32), :]
                xf[2 + m, t, pl.ds(32 + r, 32), :] = fy * gsum[1, m, t, pl.ds(r, 32), :]
        return carry
    lax.fori_loop(0, ROWS // 32, forcing, 0)
    for m in range(2):
        pack_pair(lambda t, r, m=m: xf[m, t, pl.ds(32 + r, 64), :],
                  lambda t, r, m=m: xf[2 + m, t, pl.ds(32 + r, 64), :], sf, m, 64)
    start_all(wide_copies(xf, sf, rf, fs_sem, fr_sem))

    def stores(c):
        out = []
        for f, (ref, dst) in enumerate(((tu, us_hbm), (tv, vs_hbm))):
            for t in range(2):
                out.append(pltpu.make_async_copy(ref.at[pl.ds(c * CHUNK + 1, CHUNK), :, t, :, :],
                                                 dst.at[pl.ds(c * CHUNK, CHUNK), :, :, pl.ds(t * LN, LN)], st_sem.at[c, f * 2 + t]))
        return out

    def upward(step, carry):
        c = NCH - 1 - step

        def block(i, carry2):
            r = pl.multiple_of(i * UP, UP)
            for f, (ref, kp) in enumerate(((tu, ku), (tv, kv))):
                for t in range(2):
                    depth = kp[t, pl.ds(r, UP), :]
                    below = [ref[c * CHUNK + CHUNK + 1, m, t, pl.ds(r, UP), :] for m in range(2)]
                    total = [xsum[f, m, t, pl.ds(r, UP), :] for m in range(2)]
                    for kk in range(CHUNK - 1, -1, -1):
                        k = c * CHUNK + kk
                        level_no = k.astype(F32)
                        inv = jnp.where(depth > level_no + 1.0, table[2, k], jnp.where(depth > level_no, table[3, k], 0.0))
                        for m in range(2):
                            below[m] = ref[k + 1, m, t, pl.ds(r, UP), :] * inv + table[1, k] * below[m]
                            ref[k + 1, m, t, pl.ds(r, UP), :] = below[m]
                            total[m] = total[m] + below[m]
                    for m in range(2):
                        xsum[f, m, t, pl.ds(r, UP), :] = total[m]
            return carry2
        lax.fori_loop(0, ROWS // UP, block, 0)
        for copy in stores(c):
            copy.start()
        return carry
    lax.fori_loop(0, NCH, upward, 0)

    wait_recv_all(wide_copies(xf, sf, rf, fs_sem, fr_sem))

    def unpack_force(i, carry):
        r = pl.multiple_of(i * 32, 32)
        for m in range(2):
            tile = rf[m, pl.ds(r, 32), :]
            xf[m, 2, pl.ds(r, 32), :] = tile
            xf[2 + m, 2, pl.ds(r, 32), :] = pltpu.roll(tile, 64, 1)
        return carry
    lax.fori_loop(0, EXT // 32, unpack_force, 0)

    def forcing_divergence(i, carry):
        r = pl.multiple_of(8 + i * XR, 8)
        for m in range(2):
            fx = [xf[m, t, pl.ds(r, XR), :] for t in range(3)]
            for t in range(3):
                div = fx[t] - west(fx[t], fx[PREV[t]]) + xf[2 + m, t, pl.ds(r, XR), :] - xf[2 + m, t, pl.ds(r - 1, XR), :]
                gbuf[m, t, pl.ds(r, XR), :] = cc[t, pl.ds(r, XR), :] * div
        return carry
    lax.fori_loop(0, 2, forcing_divergence, 0)

    whole = weights[SUBS - 1]
    moment = weights[SUBS - 1]
    for n in range(SUBS - 2, -1, -1):
        whole = whole + weights[n]
        moment = moment + whole

    def first_sums(i, carry):
        r = pl.multiple_of(i * 8, 8)
        for m in range(2):
            for t in range(3):
                eta = ebuf[1, m, t, pl.ds(32 + r, 8), :]
                bacc[m, t, pl.ds(r, 8), :] = whole * eta
                if t < 2:
                    eacc[m, t, pl.ds(r, 8), :] = weights[0] * eta
        return carry
    lax.fori_loop(0, 17, first_sums, 0)

    def subcycle(n, tail, lo, hi):
        old, new = lax.rem(n - 1, 2), lax.rem(n, 2)
        weight = weights[n - 1]
        for r, end in ((lo, 96), (96, hi)):
            first = max(r, 32)
            for t in range(3):
                c_e, c_w = ae[t, r:end, :], aw[t, r:end, :]
                c_n, c_s = an[t, r:end, :], as_[t, r:end, :]
                for m in range(2):
                    e = ebuf[old, m, t, r:end, :]
                    to_e = east(e, ebuf[old, m, NEXT[t], r:end, :])
                    to_w = west(e, ebuf[old, m, PREV[t], r:end, :])
                    to_n = ebuf[old, m, t, r + 1:end + 1, :]
                    to_s = ebuf[old, m, t, r - 1:end - 1, :]
                    d = dbuf[m, t, r:end, :] - gbuf[m, t, r:end, :]
                    d = d + (c_e * (to_e - e) + c_w * (to_w - e)) + (c_n * (to_n - e) + c_s * (to_s - e))
                    dbuf[m, t, r:end, :] = d
                    e = e + d
                    ebuf[new, m, t, r:end, :] = e
                    last = min(end, 168)
                    bacc[m, t, first - 32:last - 32, :] += tail * e[first - r:last - r]
                    if t < 2:
                        last = min(end, 160)
                        eacc[m, t, first - 32:last - 32, :] += weight * e[first - r:last - r]

    tail = whole
    for first_n, last_n, lo, hi in ((2, 5, 8, 184), (5, 13, 16, 176), (13, 21, 24, 168)):
        def body(n, carry, lo=lo, hi=hi):
            carry = carry - weights[n - 2]
            subcycle(n, carry, lo, hi)
            return carry
        tail = lax.fori_loop(first_n, last_n, body, tail)

    def averages(i, carry):
        r = pl.multiple_of(i * 16, 16)
        g = pl.multiple_of(32 + i * 16, 16)
        for t in range(2):
            depth_x = hux[t, pl.ds(g, 16), :]
            depth_y = huy[t, pl.ds(g, 16), :]
            kx = ku[t, pl.ds(r, 16), :]
            ky = kv[t, pl.ds(r, 16), :]
            inv_x = 1.0 / (depth_x + jnp.where(kx > 0.0, 0.0, 1.0))
            inv_y = 1.0 / (depth_y + jnp.where(ky > 0.0, 0.0, 1.0))
            mean_x = 1.0 / jnp.maximum(kx, 1.0)
            mean_y = 1.0 / jnp.maximum(ky, 1.0)
            kmask_out[1, t, pl.ds(r, 16), :] = kx
            kmask_out[2, t, pl.ds(r, 16), :] = ky
            for m in range(2):
                lane = slice(t * LN, (t + 1) * LN)
                acc = bacc[m, t, pl.ds(r, 16), :]
                eta_out[m, pl.ds(r, 16), lane] = eacc[m, t, pl.ds(r, 16), :]
                tx = whole * xb[4 + m, t, pl.ds(g, 16), :] + moment * xf[m, t, pl.ds(g, 16), :] \
                    - WAVE_COURANT * depth_x * (east(acc, bacc[m, NEXT[t], pl.ds(r, 16), :]) - acc)
                ty = whole * xb[6 + m, t, pl.ds(g, 16), :] + moment * xf[2 + m, t, pl.ds(g, 16), :] \
                    - WAVE_COURANT * depth_y * (bacc[m, t, pl.ds(r + 1, 16), :] - acc)
                tx = jnp.where(kx > 0.0, tx, 0.0)
                ty = jnp.where(ky > 0.0, ty, 0.0)
                tx_out[m, pl.ds(r, 16), lane] = tx
                ty_out[m, pl.ds(r, 16), lane] = ty
                corr_out[0, m, t, pl.ds(r, 16), :] = tx * inv_x - xsum[0, m, t, pl.ds(r, 16), :] * mean_x
                corr_out[1, m, t, pl.ds(r, 16), :] = ty * inv_y - xsum[1, m, t, pl.ds(r, 16), :] * mean_y
        return carry
    lax.fori_loop(0, ROWS // 16, averages, 0)

    wait_send_all(wide_copies(xb, sp, rp, xs_sem, xr_sem))
    wait_send_all(wide_copies(xf, sf, rf, fs_sem, fr_sem))
    for copy in packet_copies:
        copy.wait()

    def drain(c, carry):
        wait_send_all(edge_copies(c))
        for copy in stores(c):
            copy.wait()
        return carry
    lax.fori_loop(0, NCH, drain, 0)


def tracer_kernel(u_hbm, v_hbm, t_hbm, s_hbm, us_hbm, vs_hbm, eta_in, tx_in, ty_in, corr, kmask, col_in, rows_in, table,
                  eta_hbm, tx_hbm, ty_hbm, un_hbm, vn_hbm, tn_hbm, sn_hbm,
                  buf, tt, ts, su, sv, small, cols, rows, ld_sem, ed_sem, st_sem, in_sem, out_sem):
    hbm = (u_hbm, v_hbm, t_hbm, s_hbm)
    sources = (eta_in, tx_in, ty_in)
    sinks = (eta_hbm, tx_hbm, ty_hbm)

    def loads(c):
        out = []
        for f in range(4):
            for t in range(2):
                out.append(pltpu.make_async_copy(
                    hbm[f].at[pl.ds(c * CHUNK, CHUNK), :, :, pl.ds(t * LN, LN)],
                    buf.at[f, pl.ds(c * CHUNK, CHUNK), :, t, pl.ds(8, ROWS), :], ld_sem.at[c, f * 2 + t]))
        for f, (src, dst) in enumerate(((us_hbm, su), (vs_hbm, sv))):
            out.append(pltpu.make_async_copy(src.at[pl.ds(c * CHUNK, CHUNK)], dst.at[pl.ds(c * CHUNK, CHUNK)], ld_sem.at[c, 8 + f]))
        return out

    def stores_v(c):
        return [pltpu.make_async_copy(src.at[pl.ds(c * CHUNK, CHUNK)], dst.at[pl.ds(c * CHUNK, CHUNK)], st_sem.at[c, f])
                for f, (src, dst) in enumerate(((su, un_hbm), (sv, vn_hbm)))]

    def stores_t(c):
        return [pltpu.make_async_copy(src.at[pl.ds(c * CHUNK + 1, CHUNK)], dst.at[pl.ds(c * CHUNK, CHUNK)], st_sem.at[c, 2 + f])
                for f, (src, dst) in enumerate(((tt, tn_hbm), (ts, sn_hbm)))]

    edges = [pltpu.make_async_copy(col_in, cols, ed_sem.at[0]), pltpu.make_async_copy(rows_in, rows, ed_sem.at[1])]
    for copy in edges:
        copy.start()
    for c in range(NCH):
        for copy in loads(c):
            copy.start()
    small_in = [pltpu.make_async_copy(sources[i], small.at[i], in_sem.at[i]) for i in range(3)]
    small_out = [pltpu.make_async_copy(small.at[i], sinks[i], out_sem.at[i]) for i in range(3)]
    for copy in small_in:
        copy.start()

    def zero_planes(i, carry):
        r = pl.multiple_of(i * 16, 16)
        z = jnp.zeros((16, 2 * LN), F32)
        for m in range(2):
            for ref in (tt, ts):
                ref[0, m, pl.ds(r, 16), :] = z
                ref[LEVELS + 1, m, pl.ds(r, 16), :] = z
        return carry
    lax.fori_loop(0, ROWS // 16, zero_planes, 0)
    for copy in edges:
        copy.wait()

    BR = 32

    def level(k):
        level_no = k.astype(F32)
        before = table[0, k]

        def block(i, carry):
            r = pl.multiple_of(i * BR, BR)
            b = pl.multiple_of(8 + i * BR, 8)
            for t in range(2):
                lane = slice(t * LN, (t + 1) * LN)
                wet_x = kmask[1, t, pl.ds(r, BR), :] > level_no
                wet_y = kmask[2, t, pl.ds(r, BR), :] > level_no
                for m in range(2):
                    su[k, m, pl.ds(r, BR), lane] = jnp.where(wet_x, su[k, m, pl.ds(r, BR), lane] + corr[0, m, t, pl.ds(r, BR), :], 0.0)
                    sv[k, m, pl.ds(r, BR), lane] = jnp.where(wet_y, sv[k, m, pl.ds(r, BR), lane] + corr[1, m, t, pl.ds(r, BR), :], 0.0)
            wet = [kmask[0, t, pl.ds(r, BR), :] > level_no for t in range(2)]
            for m in range(2):
                hu = [0.5 * buf[0, k, m, t, pl.ds(b, BR), :] for t in range(3)]
                hv = [0.5 * buf[1, k, m, t, pl.ds(b, BR), :] for t in range(2)]
                hs = [0.5 * buf[1, k, m, t, pl.ds(b - 1, BR), :] for t in range(2)]
                for f, ref in ((2, tt), (3, ts)):
                    q = [buf[f, k, m, t, pl.ds(b, BR), :] for t in range(3)]
                    fx = [hu[t] * (q[t] + east(q[t], q[NEXT[t]])) for t in range(3)]
                    for t in range(2):
                        lane = slice(t * LN, (t + 1) * LN)
                        fy = hv[t] * (q[t] + buf[f, k, m, t, pl.ds(b + 1, BR), :])
                        fs = hs[t] * (q[t] + buf[f, k, m, t, pl.ds(b - 1, BR), :])
                        adv = q[t] - ((fx[t] - west(fx[t], fx[PREV[t]])) + (fy - fs))
                        adv = jnp.where(wet[t], adv, 0.0)
                        ref[k + 1, m, pl.ds(r, BR), lane] = adv + before * ref[k, m, pl.ds(r, BR), lane]
            return carry
        lax.fori_loop(0, ROWS // BR, block, 0)

    def chunk_step(c, carry):
        for copy in loads(c):
            copy.wait()
        unpack_columns(cols.at[c], buf, c, (0, 2, 3), range(4))
        for kk in range(CHUNK):
            k = c * CHUNK + kk
            for m in range(2):
                jj = kk * 2 + m
                for f in (1, 2, 3):
                    for t in range(2):
                        buf[f, k, m, t, 7:8, :] = rows[0, c, t, f, jj:jj + 1, :]
                for f in (2, 3):
                    for t in range(2):
                        buf[f, k, m, t, 8 + ROWS:9 + ROWS, :] = rows[1, c, t, f, jj:jj + 1, :]

        def one_level(kk, carry2):
            level(c * CHUNK + kk)
            return carry2
        lax.fori_loop(0, CHUNK, one_level, 0)
        for copy in stores_v(c):
            copy.start()
        return carry
    lax.fori_loop(0, NCH, chunk_step, 0)

    for copy in small_in:
        copy.wait()
    for copy in small_out:
        copy.start()

    def upward(step, carry):
        c = NCH - 1 - step

        def block(i, carry2):
            r = pl.multiple_of(i * 16, 16)
            for t in range(2):
                lane = slice(t * LN, (t + 1) * LN)
                depth = kmask[0, t, pl.ds(r, 16), :]
                below = [[ref[c * CHUNK + CHUNK + 1, m, pl.ds(r, 16), lane] for m in range(2)] for ref in (tt, ts)]
                for kk in range(CHUNK - 1, -1, -1):
                    k = c * CHUNK + kk
                    level_no = k.astype(F32)
                    inv = jnp.where(depth > level_no + 1.0, table[2, k], jnp.where(depth > level_no, table[3, k], 0.0))
                    for f, ref in enumerate((tt, ts)):
                        for m in range(2):
                            below[f][m] = ref[k + 1, m, pl.ds(r, 16), lane] * inv + table[1, k] * below[f][m]
                            ref[k + 1, m, pl.ds(r, 16), lane] = below[f][m]
            return carry2
        lax.fori_loop(0, ROWS // 16, block, 0)
        for copy in stores_t(c):
            copy.start()
        return carry
    lax.fori_loop(0, NCH, upward, 0)

    for copy in small_out:
        copy.wait()

    def drain(c, carry):
        for copy in stores_v(c) + stores_t(c):
            copy.wait()
        return carry
    lax.fori_loop(0, NCH, drain, 0)


def solution(mesh):
    assert mesh.shape["col"] == 2 and mesh.shape["row"] == 4
    any_spec = pl.BlockSpec(memory_space=pl.ANY)
    vmem_spec = pl.BlockSpec(memory_space=pltpu.VMEM)
    smem_spec = pl.BlockSpec(memory_space=pltpu.SMEM)
    shape = lambda *dims: jax.ShapeDtypeStruct(dims, F32)
    dma = lambda *dims: pltpu.SemaphoreType.DMA(dims)
    vm = lambda *dims: pltpu.VMEM(dims, F32)
    visc = solve_table(VISC_NUMBER)
    diff = solve_table(DIFF_NUMBER)
    full = (LEVELS, 2, ROWS, 2 * LN)
    flat = (2, ROWS, 2 * LN)

    momentum = pl.pallas_call(
        momentum_kernel,
        name="momentum",
        out_shape=(shape(*full), shape(*full), shape(*flat), shape(*flat), shape(*flat), shape(2, 2, 2, ROWS, LN),
                   shape(3, 2, ROWS, LN), shape(NCH, ROWS, LN), shape(2, NCH, 2, 4, PAIRS, LN)),
        in_specs=[any_spec] * 8 + [vmem_spec, smem_spec, smem_spec],
        out_specs=(any_spec, any_spec, vmem_spec, vmem_spec, vmem_spec, vmem_spec, vmem_spec, any_spec, any_spec),
        scratch_shapes=[
            vm(4, LEVELS, 2, 3, PR, LN), vm(LEVELS + 2, 2, 2, ROWS, LN), vm(LEVELS + 2, 2, 2, ROWS, LN),
            vm(2, 3, PR, LN), vm(2, 3, PR, LN), vm(2, 2, 2, ROWS, LN), vm(2, 2, 2, ROWS, LN), vm(2, ROWS, LN), vm(2, ROWS, LN),
            vm(NCH, ROWS, LN), vm(NCH, ROWS, LN), vm(2, NCH, 2, 4, PAIRS, LN), vm(2, NCH, 2, 4, PAIRS, LN),
            vm(2, NCH, PAIRS, LN), vm(2, NCH, PAIRS, LN),
            vm(8, 3, EXT, LN), vm(4, ROWS, LN), vm(4, EXT, LN), vm(4, 3, EXT, LN), vm(2, ROWS, LN), vm(2, EXT, LN),
            vm(3, EXT, LN), vm(3, EXT, LN), vm(3, EXT, LN), vm(3, EXT, LN), vm(3, EXT, LN), vm(3, EXT, LN), vm(3, EXT, LN),
            vm(2, 2, 3, EXT, LN), vm(2, 3, EXT, LN), vm(2, 3, EXT, LN), vm(2, 2, ROWS + 8, LN), vm(2, 3, ROWS + 8, LN),
            dma(NCH, 8), dma(8), dma(NCH, 5), dma(NCH, 5), dma(5), dma(5), dma(5), dma(5), dma(NCH, 4), dma(2),
        ],
        compiler_params=pltpu.CompilerParams(collective_id=0, has_side_effects=True, vmem_limit_bytes=67043328),
    )

    tracers = pl.pallas_call(
        tracer_kernel,
        name="tracers",
        out_shape=(shape(*flat), shape(*flat), shape(*flat), shape(*full), shape(*full), shape(*full), shape(*full)),
        in_specs=[any_spec] * 9 + [vmem_spec, vmem_spec, any_spec, any_spec, smem_spec],
        out_specs=(any_spec,) * 7,
        scratch_shapes=[
            vm(4, LEVELS, 2, 3, PR, LN), vm(LEVELS + 2, 2, ROWS, 2 * LN), vm(LEVELS + 2, 2, ROWS, 2 * LN),
            vm(*full), vm(*full), vm(3, 2, ROWS, 2 * LN), vm(NCH, ROWS, LN), vm(2, NCH, 2, 4, PAIRS, LN),
            dma(NCH, 10), dma(2), dma(NCH, 4), dma(3), dma(3),
        ],
        compiler_params=pltpu.CompilerParams(vmem_limit_bytes=67043328),
    )

    def local_step(vel_x, vel_y, pot_temp, salinity, surf_eta, trans_x, trans_y, col_depth, wet_levels, avg_weights):
        star_x, star_y, eta, tx, ty, corr, kmask, cols, rows = momentum(
            vel_x, vel_y, pot_temp, salinity, surf_eta, trans_x, trans_y, col_depth, wet_levels, avg_weights, jnp.asarray(visc))
        return tracers(vel_x, vel_y, pot_temp, salinity, star_x, star_y, eta, tx, ty, corr, kmask, cols, rows, jnp.asarray(diff))

    spec_3d = P(None, None, "row", "col")
    spec_2d = P(None, "row", "col")
    spec_map = P("row", "col")
    return jax.shard_map(local_step, mesh=mesh, in_specs=(spec_3d, spec_3d, spec_3d, spec_3d, spec_2d, spec_2d, spec_2d, spec_map, spec_map, P()),
                         out_specs=(spec_2d, spec_2d, spec_2d, spec_3d, spec_3d, spec_3d, spec_3d), check_vma=False)
```

```python
import functools
import numpy as np
import jax
import jax.numpy as jnp
from jax import lax
from jax.experimental import pallas as pl
from jax.experimental.pallas import tpu as pltpu
from jax.sharding import PartitionSpec as P

WAVE_COURANT = 0.4
THERM_EXP = 0.2
HALINE_CON = 0.15
PRESS_SCALE = 0.5
VISC_NUMBER = 1.0
DIFF_NUMBER = 0.5

LEVELS = 20
SUBS = 20
CHUNK = 4
NCH = LEVELS // CHUNK
PAIRS = 2 * CHUNK
ROWS = 128
LN = 128
PR = 144
EXT = 192
F32 = jnp.float32
PK = 64
UP = 32
MESH_ID = pl.DeviceIdType.MESH


def solve_table(strength):
    inner = np.zeros(LEVELS)
    last = np.zeros(LEVELS)
    inner[0] = 1.0 + strength
    last[0] = 1.0
    for k in range(1, LEVELS):
        inner[k] = 1.0 + 2.0 * strength - strength**2 / inner[k - 1]
        last[k] = 1.0 + strength - strength**2 / inner[k - 1]
    ratio = strength / inner
    before = np.concatenate([[0.0], ratio[:-1]])
    return np.stack([before, ratio, 1.0 / inner, 1.0 / last]).astype(np.float32)


def lanes(rows):
    return lax.broadcasted_iota(jnp.int32, (rows, LN), 1)


def east(tile, following):
    return pltpu.roll(jnp.where(lanes(tile.shape[0]) == 0, following, tile), LN - 1, 1)


def west(tile, previous):
    return pltpu.roll(jnp.where(lanes(tile.shape[0]) == LN - 1, previous, tile), 1, 1)


NEXT = (1, 2, 0)
PREV = (2, 0, 1)


def halo(packed, j):
    return pltpu.roll(packed, LN - 1 - 2 * j, 1)


def east_pair(first, second, edge):
    last = lanes(first.shape[0]) == LN - 1
    a, b = pltpu.roll(first, LN - 1, 1), pltpu.roll(second, LN - 1, 1)
    return jnp.where(last, b, a), jnp.where(last, edge, b)


def west_pair(first, second, edge):
    origin = lanes(first.shape[0]) == 0
    a, b = pltpu.roll(first, 1, 1), pltpu.roll(second, 1, 1)
    return jnp.where(origin, edge, a), jnp.where(origin, a, b)


def momentum_kernel(u_hbm, v_hbm, t_hbm, s_hbm, eta_hbm, tx_hbm, ty_hbm, h_hbm, kmt_ref, weights, table,
                    us_hbm, vs_hbm, eta_out, tx_out, ty_out, corr_out, kmask_out, col_out, rows_out,
                    buf, tu, tv, cu, cv, pbuf, pacc, phal, rhoc, gsum, xsum, ku, kv,
                    send_col, recv_col, send_row, recv_row,
                    xb, sp, rp, xf, sf, rf, hux, huy, ae, aw, an, as_, cc, ebufa, ebufb, dbuf, gbuf, eacc, bacc,
                    ld_sem, xl_sem, cs_sem, cr_sem, xs_sem, xr_sem, fs_sem, fr_sem, st_sem, ot_sem):
    me_c = lax.axis_index("col")
    me_r = lax.axis_index("row")
    peer = 1 - me_c
    has_n = me_r < 3
    has_s = me_r > 0
    hbm = (u_hbm, v_hbm, t_hbm, s_hbm)

    def loads(c):
        out = []
        for f in range(4):
            for t in range(2):
                out.append(pltpu.make_async_copy(
                    hbm[f].at[pl.ds(c * CHUNK, CHUNK), :, :, pl.ds(t * LN, LN)],
                    buf.at[f, pl.ds(c * CHUNK, CHUNK), :, t, pl.ds(8, ROWS), :], ld_sem.at[c, f * 2 + t]))
        return out

    def ext_loads():
        out = []
        for t in range(2):
            lane = pl.ds(t * LN, LN)
            out.append(pltpu.make_async_copy(h_hbm.at[:, lane], xb.at[1, t, pl.ds(32, ROWS), :], xl_sem.at[t]))
            for i, ref in enumerate((eta_hbm, tx_hbm, ty_hbm)):
                out.append(pltpu.make_async_copy(ref.at[:, :, lane], xb.at[pl.ds(2 + 2 * i, 2), t, pl.ds(32, ROWS), :], xl_sem.at[2 + 2 * i + t]))
        return out

    for copy in loads(0) + ext_loads() + loads(1):
        copy.start()

    barrier = pltpu.get_barrier_semaphore()

    def greet(col, row):
        pl.semaphore_signal(barrier, inc=1, device_id={"col": col, "row": row}, device_id_type=MESH_ID)

    greet(peer, me_r)

    @pl.when(has_n)
    def _():
        greet(me_c, me_r + 1)
        greet(peer, me_r + 1)

    @pl.when(has_s)
    def _():
        greet(me_c, me_r - 1)
        greet(peer, me_r - 1)

    zrow = jnp.zeros((8, LN), F32)
    for ref, count in ((xb, 8), (xf, 4)):
        for f in range(count):
            for t in range(3):
                ref[f, t, 0:8, :] = zrow
                ref[f, t, EXT - 8:EXT, :] = zrow
    for ref, count in ((rp, 4), (rf, 2)):
        for f in range(count):
            ref[f, 0:8, :] = zrow
            ref[f, EXT - 8:EXT, :] = zrow

    def zero_side(side, lo):
        z24 = jnp.zeros((24, LN), F32)
        for f in range(8):
            for t in range(2):
                xb[f, t, lo:lo + 24, :] = z24
        for f in range(4):
            rp[f, lo:lo + 24, :] = z24
            for t in range(2):
                xf[f, t, lo:lo + 24, :] = z24
        for f in range(2):
            rf[f, lo:lo + 24, :] = z24
        for c in range(NCH):
            recv_col[c, 136 * side:136 * side + 8, :] = zrow
            for f in range(4):
                for t in range(2):
                    recv_row[side, c, t, f, :, :] = zrow

    @pl.when(me_r == 0)
    def _():
        zero_side(0, 8)

    @pl.when(me_r == 3)
    def _():
        zero_side(1, 160)

    def zero_planes(i, carry):
        r = pl.multiple_of(i * 16, 16)
        z = jnp.zeros((16, LN), F32)
        for m in range(2):
            for t in range(2):
                pacc[m, t, pl.ds(r, 16), :] = z
            phal[m, pl.ds(r, 16), :] = z
        return carry
    lax.fori_loop(0, PR // 16, zero_planes, 0)

    def zero_planes2(i, carry):
        r = pl.multiple_of(i * 16, 16)
        z = jnp.zeros((16, LN), F32)
        for m in range(2):
            for t in range(2):
                for f in range(2):
                    gsum[f, m, t, pl.ds(r, 16), :] = z
                    xsum[f, m, t, pl.ds(r, 16), :] = z
                for ref in (cu, cv):
                    ref[m, t, pl.ds(r, 16), :] = z
                for ref in (tu, tv):
                    ref[LEVELS, m, t, pl.ds(r, 16), :] = z
        return carry
    lax.fori_loop(0, ROWS // 16, zero_planes2, 0)

    for t in range(2):
        for r in range(0, ROWS, 32):
            xb[0, t, 32 + r:64 + r, :] = kmt_ref[r:r + 32, t * LN:(t + 1) * LN].astype(F32)
    for copy in ext_loads():
        copy.wait()

    @pl.when((me_r == 0) | (me_r == 3))
    def _():
        pl.semaphore_wait(barrier, 3)

    @pl.when((me_r != 0) & (me_r != 3))
    def _():
        pl.semaphore_wait(barrier, 5)

    def remote(src, dst, ssem, rsem, col, row):
        return pltpu.make_async_remote_copy(src_ref=src, dst_ref=dst, send_sem=ssem, recv_sem=rsem,
                                            device_id={"col": col, "row": row}, device_id_type=MESH_ID)

    def wide_copies(own, packed, landing, ssem, rsem):
        north, south = me_r + 1, me_r - 1
        side = remote(packed, landing.at[:, pl.ds(32, ROWS), :], ssem.at[0], rsem.at[0], peer, me_r)
        up = (remote(own.at[:, pl.ds(0, 2), pl.ds(136, 24), :], own.at[:, pl.ds(0, 2), pl.ds(8, 24), :], ssem.at[1], rsem.at[1], me_c, north),
              remote(packed.at[:, pl.ds(104, 24), :], landing.at[:, pl.ds(8, 24), :], ssem.at[2], rsem.at[2], peer, north))
        down = (remote(own.at[:, pl.ds(0, 2), pl.ds(32, 24), :], own.at[:, pl.ds(0, 2), pl.ds(160, 24), :], ssem.at[3], rsem.at[3], me_c, south),
                remote(packed.at[:, pl.ds(0, 24), :], landing.at[:, pl.ds(160, 24), :], ssem.at[4], rsem.at[4], peer, south))
        return side, up, down

    def edge_copies(c):
        north, south = me_r + 1, me_r - 1
        side = remote(send_col.at[c], recv_col.at[c, pl.ds(8, ROWS), :], cs_sem.at[c, 0], cr_sem.at[c, 0], peer, me_r)
        up = (remote(send_row.at[0, c], recv_row.at[0, c], cs_sem.at[c, 1], cr_sem.at[c, 1], me_c, north),
              remote(send_col.at[c, pl.ds(ROWS - 8, 8), :], recv_col.at[c, pl.ds(0, 8), :], cs_sem.at[c, 2], cr_sem.at[c, 2], peer, north))
        down = (remote(send_row.at[1, c], recv_row.at[1, c], cs_sem.at[c, 3], cr_sem.at[c, 3], me_c, south),
                remote(send_col.at[c, pl.ds(0, 8), :], recv_col.at[c, pl.ds(8 + ROWS, 8), :], cs_sem.at[c, 4], cr_sem.at[c, 4], peer, south))
        return side, up, down

    def start_all(copies):
        side, up, down = copies
        if side is not None:
            side.start()

        @pl.when(has_n)
        def _():
            for copy in up:
                copy.start()

        @pl.when(has_s)
        def _():
            for copy in down:
                copy.start()

    def wait_recv_all(copies):
        side, up, down = copies
        if side is not None:
            side.wait_recv()

        @pl.when(has_s)
        def _():
            for copy in up:
                copy.wait_recv()

        @pl.when(has_n)
        def _():
            for copy in down:
                copy.wait_recv()

    def wait_send_all(copies):
        side, up, down = copies
        side.wait_send()

        @pl.when(has_n)
        def _():
            for copy in up:
                copy.wait_send()

        @pl.when(has_s)
        def _():
            for copy in down:
                copy.wait_send()

    def rows_only(copies):
        return None, copies[1][:1], copies[2][:1]

    def columns_only(copies):
        return copies[0], copies[1][1:], copies[2][1:]

    start_all(rows_only(wide_copies(xb, sp, rp, xs_sem, xr_sem)))

    def pack_and_send(c, with_maps=False):
        for copy in loads(c):
            copy.wait()
        lane = lanes(PK)

        def block(i, carry):
            r = pl.multiple_of(i * PK, PK)
            pairs = [(f, c * CHUNK + kk, m) for f in range(4) for kk in range(CHUNK) for m in range(2)]
            column = [[buf[f, k, m, t, pl.ds(8 + r, PK), :] for f, k, m in pairs] for t in range(2)]
            if with_maps:
                for t in range(2):
                    column[t] += [xb[0, t, pl.ds(32 + r, PK), :], xb[1, t, pl.ds(32 + r, PK), :]]
            packed = jnp.zeros((PK, LN), F32)
            count = len(column[0])
            for i in range(count + 1):
                edge = jnp.where(lane == 0, column[0][min(i, count - 1)], column[1][max(i - 1, 0)])
                edge = pltpu.roll(edge, 2 * i, 1) if i else edge
                packed = jnp.where(lane >= 2 * i - 1, edge, packed) if i else edge
            send_col[c, pl.ds(r, PK), :] = packed
            return carry
        for kk in range(CHUNK):
            for m in range(2):
                jj = kk * 2 + m
                k = c * CHUNK + kk
                for side, row in ((0, 8 + ROWS - 1), (1, 8)):
                    for f in range(4):
                        for t in range(2):
                            send_row[side, c, t, f, jj:jj + 1, :] = buf[f, k, m, t, row:row + 1, :]
        lax.fori_loop(0, ROWS // PK, block, 0)
        start_all(edge_copies(c))

    pack_and_send(0, with_maps=True)
    for copy in loads(2):
        copy.start()
    pack_and_send(1)

    RHO_T = np.float32(-THERM_EXP * PRESS_SCALE / LEVELS / 2)
    RHO_S = np.float32(HALINE_CON * PRESS_SCALE / LEVELS / 2)
    BR = 64

    def pressure_rows(k, slot, base, rows):
        for m in range(2):
            for t in range(2):
                half = RHO_T * buf[2, k, m, t, pl.ds(base, rows), :] + RHO_S * buf[3, k, m, t, pl.ds(base, rows), :]
                p = pacc[m, t, pl.ds(base, rows), :] + half
                slot[m, t, pl.ds(base, rows), :] = p
                pacc[m, t, pl.ds(base, rows), :] = p + half

    def level(c, kk, now, later):
        k = c * CHUNK + kk
        pressure_rows(k, now, 8 + ROWS, 8)
        level_no = k.astype(F32)
        before = table[0, k]
        following = jnp.minimum(k + 1, LEVELS - 1)

        def block(i, carry):
            r = pl.multiple_of(i * BR, BR)
            b = pl.multiple_of(8 + i * BR, 8)
            wet_x = [ku[t, pl.ds(r, BR), :] > level_no for t in range(2)]
            wet_y = [kv[t, pl.ds(r, BR), :] > level_no for t in range(2)]
            packed = recv_col[c, pl.ds(b, BR), :]
            packed_w = packed + recv_col[c, pl.ds(b - 1, BR), :]
            packed_z = packed + recv_col[c, pl.ds(b + 1, BR), :]
            packed_r = rhoc[pl.ds(r, BR), :]
            for m in range(2):
                j = kk * 2 + m
                half = halo(packed_r, j)
                p_edge = phal[m, pl.ds(r, BR), :] + half
                phal[m, pl.ds(r, BR), :] = p_edge + half
                u_edge, v_edge = halo(packed, j), halo(packed, PAIRS + j)
                w_edge, z_edge = halo(packed_w, PAIRS + j), halo(packed_z, j)
                u = [buf[0, k, m, t, pl.ds(b, BR), :] for t in range(2)]
                v = [buf[1, k, m, t, pl.ds(b, BR), :] for t in range(2)]
                un = [buf[0, k, m, t, pl.ds(b + 1, BR), :] for t in range(2)]
                vs = [buf[1, k, m, t, pl.ds(b - 1, BR), :] for t in range(2)]
                p = [now[m, t, pl.ds(b, BR), :] for t in range(2)]
                w = [v[t] + vs[t] for t in range(2)]
                z = [u[t] + un[t] for t in range(2)]
                ue, uw = east_pair(*u, u_edge), west_pair(*u, u_edge)
                ve, vw = east_pair(*v, v_edge), west_pair(*v, v_edge)
                pe, we, zw = east_pair(*p, p_edge), east_pair(*w, w_edge), west_pair(*z, z_edge)
                for t in range(2):
                    us = buf[0, k, m, t, pl.ds(b - 1, BR), :]
                    gu = (p[t] - pe[t]) - (0.5 * u[t]) * (ue[t] - uw[t]) - (0.125 * (w[t] + we[t])) * (un[t] - us)
                    gu = jnp.where(wet_x[t], gu, 0.0)
                    gsum[0, m, t, pl.ds(r, BR), :] += gu
                    new = u[t] + gu + before * cu[m, t, pl.ds(r, BR), :]
                    cu[m, t, pl.ds(r, BR), :] = new
                    tu[k, m, t, pl.ds(r, BR), :] = new
                    vn = buf[1, k, m, t, pl.ds(b + 1, BR), :]
                    pn = now[m, t, pl.ds(b + 1, BR), :]
                    gv = (p[t] - pn) - (0.125 * (z[t] + zw[t])) * (ve[t] - vw[t]) - (0.5 * v[t]) * (vn - vs[t])
                    gv = jnp.where(wet_y[t], gv, 0.0)
                    gsum[1, m, t, pl.ds(r, BR), :] += gv
                    new = v[t] + gv + before * cv[m, t, pl.ds(r, BR), :]
                    cv[m, t, pl.ds(r, BR), :] = new
                    tv[k, m, t, pl.ds(r, BR), :] = new
            pressure_rows(following, later, b, BR)
            return carry
        lax.fori_loop(0, ROWS // BR, block, 0)

    def first_pressure(i, carry):
        pressure_rows(0, pbuf.at[0], pl.multiple_of(8 + i * 64, 8), 64)
        return carry
    lax.fori_loop(0, 2, first_pressure, 0)

    def chunk_step(c, carry):
        @pl.when(c + 3 < NCH)
        def _():
            for copy in loads(c + 3):
                copy.start()

        @pl.when(c + 2 < NCH)
        def _():
            pack_and_send(c + 2)

        @pl.when(c == 2)
        def _():
            pack_wide()

        wait_recv_all(edge_copies(c))

        @pl.when(c == 0)
        def _():
            face_maps()

        for kk in range(CHUNK):
            k = c * CHUNK + kk
            for m in range(2):
                jj = kk * 2 + m
                for side, row in ((0, 7), (1, 8 + ROWS)):
                    for f in range(4):
                        for t in range(2):
                            buf[f, k, m, t, row:row + 1, :] = recv_row[side, c, t, f, jj:jj + 1, :]
        packed = recv_col[c, 8:8 + ROWS, :]
        rhoc[...] = RHO_T * pltpu.roll(packed, LN - 4 * PAIRS, 1) + RHO_S * pltpu.roll(packed, LN - 6 * PAIRS, 1)

        def two_levels(h, carry2):
            level(c, 2 * h, pbuf.at[0], pbuf.at[1])
            level(c, 2 * h + 1, pbuf.at[1], pbuf.at[0])
            return carry2
        lax.fori_loop(0, CHUNK // 2, two_levels, 0)
        return carry

    def pack_wide():
        for pair in range(4):
            pack_pair(lambda t, r, p=pair: xb[2 * p, t, pl.ds(32 + r, 64), :],
                      lambda t, r, p=pair: xb[2 * p + 1, t, pl.ds(32 + r, 64), :], sp, pair, 64)
        start_all(columns_only(wide_copies(xb, sp, rp, xs_sem, xr_sem)))

    def face_maps():
        wait_recv_all(rows_only(wide_copies(xb, sp, rp, xs_sem, xr_sem)))

        def maps(i, carry):
            r = pl.multiple_of(i * 64, 64)
            packed = recv_col[0, pl.ds(8 + r, 64), :]
            kt = [xb[0, t, pl.ds(32 + r, 64), :] for t in range(2)]
            ht = [xb[1, t, pl.ds(32 + r, 64), :] for t in range(2)]
            ke = east_pair(*kt, halo(packed, 4 * PAIRS))
            he = east_pair(*ht, halo(packed, 4 * PAIRS + 1))
            for t in range(2):
                kx = jnp.minimum(kt[t], ke[t])
                ky = jnp.minimum(kt[t], xb[0, t, pl.ds(33 + r, 64), :])
                ku[t, pl.ds(r, 64), :] = kx
                kv[t, pl.ds(r, 64), :] = ky
                kmask_out[0, t, pl.ds(r, 64), :] = kt[t]
                kmask_out[1, t, pl.ds(r, 64), :] = kx
                kmask_out[2, t, pl.ds(r, 64), :] = ky
                hux[t, pl.ds(32 + r, 64), :] = jnp.where(kx > 0.0, 0.5 * (ht[t] + he[t]), 0.0)
                huy[t, pl.ds(32 + r, 64), :] = jnp.where(ky > 0.0, 0.5 * (ht[t] + xb[1, t, pl.ds(33 + r, 64), :]), 0.0)
            return carry
        lax.fori_loop(0, 2, maps, 0)

    def pack_pair(first, second, send, slot, rows):
        lane = lanes(rows)

        def block(i, carry):
            r = pl.multiple_of(i * rows, rows)
            a = jnp.where(lane < 64, first(0, r), first(1, r))
            b = jnp.where(lane < 64, second(0, r), second(1, r))
            outer = (lane < 32) | (lane >= 96)
            send[slot, pl.ds(r, rows), :] = jnp.where(outer, a, pltpu.roll(b, 64, 1))
            return carry
        lax.fori_loop(0, ROWS // rows, block, 0)

    lax.fori_loop(0, NCH, chunk_step, 0)

    packet_copies = [pltpu.make_async_copy(recv_col, col_out, ot_sem.at[0]),
                     pltpu.make_async_copy(recv_row, rows_out, ot_sem.at[1])]
    for copy in packet_copies:
        copy.start()

    def forcing(i, carry):
        r = pl.multiple_of(i * 32, 32)
        for t in range(2):
            nx = jnp.maximum(ku[t, pl.ds(r, 32), :], 1.0)
            ny = jnp.maximum(kv[t, pl.ds(r, 32), :], 1.0)
            fx = hux[t, pl.ds(32 + r, 32), :] / nx / SUBS
            fy = huy[t, pl.ds(32 + r, 32), :] / ny / SUBS
            for m in range(2):
                xf[m, t, pl.ds(32 + r, 32), :] = fx * gsum[0, m, t, pl.ds(r, 32), :]
                xf[2 + m, t, pl.ds(32 + r, 32), :] = fy * gsum[1, m, t, pl.ds(r, 32), :]
        return carry
    lax.fori_loop(0, ROWS // 32, forcing, 0)
    for m in range(2):
        pack_pair(lambda t, r, m=m: xf[m, t, pl.ds(32 + r, 64), :],
                  lambda t, r, m=m: xf[2 + m, t, pl.ds(32 + r, 64), :], sf, m, 64)
    start_all(wide_copies(xf, sf, rf, fs_sem, fr_sem))

    def stores(c):
        out = []
        for f, (ref, dst) in enumerate(((tu, us_hbm), (tv, vs_hbm))):
            for t in range(2):
                out.append(pltpu.make_async_copy(ref.at[pl.ds(c * CHUNK, CHUNK), :, t, :, :],
                                                 dst.at[pl.ds(c * CHUNK, CHUNK), :, :, pl.ds(t * LN, LN)], st_sem.at[c, f * 2 + t]))
        return out

    def upward(step, carry):
        c = NCH - 1 - step

        def block(i, carry2):
            r = pl.multiple_of(i * UP, UP)
            for f, (ref, kp) in enumerate(((tu, ku), (tv, kv))):
                for t in range(2):
                    depth = kp[t, pl.ds(r, UP), :]
                    below = [ref[c * CHUNK + CHUNK, m, t, pl.ds(r, UP), :] for m in range(2)]
                    total = [xsum[f, m, t, pl.ds(r, UP), :] for m in range(2)]
                    for kk in range(CHUNK - 1, -1, -1):
                        k = c * CHUNK + kk
                        level_no = k.astype(F32)
                        inv = jnp.where(depth > level_no + 1.0, table[2, k], jnp.where(depth > level_no, table[3, k], 0.0))
                        for m in range(2):
                            below[m] = ref[k, m, t, pl.ds(r, UP), :] * inv + table[1, k] * below[m]
                            ref[k, m, t, pl.ds(r, UP), :] = below[m]
                            total[m] = total[m] + below[m]
                    for m in range(2):
                        xsum[f, m, t, pl.ds(r, UP), :] = total[m]
            return carry2
        lax.fori_loop(0, ROWS // UP, block, 0)
        for copy in stores(c):
            copy.start()
        return carry
    lax.fori_loop(0, NCH, upward, 0)

    wait_recv_all(columns_only(wide_copies(xb, sp, rp, xs_sem, xr_sem)))

    def unpack_wide(i, carry):
        r = pl.multiple_of(i * 32, 32)
        for pair in range(4):
            tile = rp[pair, pl.ds(r, 32), :]
            xb[2 * pair, 2, pl.ds(r, 32), :] = tile
            xb[2 * pair + 1, 2, pl.ds(r, 32), :] = pltpu.roll(tile, 64, 1)
        return carry
    lax.fori_loop(0, EXT // 32, unpack_wide, 0)

    XR = 88

    def depths(i, carry):
        r = pl.multiple_of(8 + i * XR, 8)
        kt = [xb[0, t, pl.ds(r, XR), :] for t in range(3)]
        ht = [xb[1, t, pl.ds(r, XR), :] for t in range(3)]
        for t in range(3):
            kx = jnp.minimum(kt[t], east(kt[t], kt[NEXT[t]]))
            ky = jnp.minimum(kt[t], xb[0, t, pl.ds(r + 1, XR), :])
            hux[t, pl.ds(r, XR), :] = jnp.where(kx > 0.0, 0.5 * (ht[t] + east(ht[t], ht[NEXT[t]])), 0.0)
            huy[t, pl.ds(r, XR), :] = jnp.where(ky > 0.0, 0.5 * (ht[t] + xb[1, t, pl.ds(r + 1, XR), :]), 0.0)
            cc[t, pl.ds(r, XR), :] = jnp.where(kt[t] > 0.0, WAVE_COURANT, 0.0)
        return carry
    for t in range(3):
        for ref in (hux, huy):
            ref[t, 0:8, :] = zrow
        for ref in (ebufa, ebufb):
            for m in range(2):
                ref[m, t, 0:8, :] = zrow
                ref[m, t, EXT - 8:EXT, :] = zrow
    lax.fori_loop(0, 2, depths, 0)

    def coefficients(i, carry):
        r = pl.multiple_of(8 + i * XR, 8)
        hx = [hux[t, pl.ds(r, XR), :] for t in range(3)]
        for t in range(3):
            c0 = cc[t, pl.ds(r, XR), :]
            cw = WAVE_COURANT * c0
            ae[t, pl.ds(r, XR), :] = cw * hx[t]
            aw[t, pl.ds(r, XR), :] = cw * west(hx[t], hx[PREV[t]])
            an[t, pl.ds(r, XR), :] = cw * huy[t, pl.ds(r, XR), :]
            as_[t, pl.ds(r, XR), :] = cw * huy[t, pl.ds(r - 1, XR), :]
        return carry
    lax.fori_loop(0, 2, coefficients, 0)

    def first_subcycle(m, base, rows):
        tx = [xb[4 + m, t, pl.ds(base, rows), :] for t in range(3)]
        for t in range(3):
            c0 = cc[t, pl.ds(base, rows), :]
            ty = xb[6 + m, t, pl.ds(base, rows), :]
            div = tx[t] - west(tx[t], tx[PREV[t]]) + ty - xb[6 + m, t, pl.ds(base - 1, rows), :]
            change = -c0 * div
            dbuf[m, t, pl.ds(base, rows), :] = change
            eta = jnp.where(c0 > 0.0, xb[2 + m, t, pl.ds(base, rows), :], 0.0) + change
            ebufa[m, t, pl.ds(base, rows), :] = eta

    def first_block(i, carry):
        for m in range(2):
            first_subcycle(m, pl.multiple_of(8 + i * XR, 8), XR)
        return carry
    lax.fori_loop(0, 2, first_block, 0)

    wait_recv_all(wide_copies(xf, sf, rf, fs_sem, fr_sem))

    def unpack_force(i, carry):
        r = pl.multiple_of(i * 32, 32)
        for m in range(2):
            tile = rf[m, pl.ds(r, 32), :]
            xf[m, 2, pl.ds(r, 32), :] = tile
            xf[2 + m, 2, pl.ds(r, 32), :] = pltpu.roll(tile, 64, 1)
        return carry
    lax.fori_loop(0, EXT // 32, unpack_force, 0)

    def forcing_divergence(i, carry):
        r = pl.multiple_of(8 + i * XR, 8)
        for m in range(2):
            fx = [xf[m, t, pl.ds(r, XR), :] for t in range(3)]
            for t in range(3):
                div = fx[t] - west(fx[t], fx[PREV[t]]) + xf[2 + m, t, pl.ds(r, XR), :] - xf[2 + m, t, pl.ds(r - 1, XR), :]
                gbuf[m, t, pl.ds(r, XR), :] = cc[t, pl.ds(r, XR), :] * div
        return carry
    lax.fori_loop(0, 2, forcing_divergence, 0)

    whole = weights[SUBS - 1]
    moment = weights[SUBS - 1]
    for n in range(SUBS - 2, -1, -1):
        whole = whole + weights[n]
        moment = moment + whole

    def first_sums(i, carry):
        r = pl.multiple_of(i * 8, 8)
        for m in range(2):
            for t in range(3):
                eta = ebufa[m, t, pl.ds(32 + r, 8), :]
                bacc[m, t, pl.ds(r, 8), :] = whole * eta
                if t < 2:
                    eacc[m, t, pl.ds(r, 8), :] = weights[0] * eta
        return carry
    lax.fori_loop(0, 17, first_sums, 0)

    def subcycle(n, tail, lo, hi, old, new):
        tail = tail - weights[n - 2]
        weight = weights[n - 1]
        for r, end in ((lo, 96), (96, hi)):
            first = max(r, 32)
            for t in range(3):
                c_e, c_w = ae[t, r:end, :], aw[t, r:end, :]
                c_n, c_s = an[t, r:end, :], as_[t, r:end, :]
                for m in range(2):
                    e = old[m, t, r:end, :]
                    to_e = east(e, old[m, NEXT[t], r:end, :])
                    to_w = west(e, old[m, PREV[t], r:end, :])
                    to_n = old[m, t, r + 1:end + 1, :]
                    to_s = old[m, t, r - 1:end - 1, :]
                    d = dbuf[m, t, r:end, :] - gbuf[m, t, r:end, :]
                    d = d + (c_e * (to_e - e) + c_w * (to_w - e)) + (c_n * (to_n - e) + c_s * (to_s - e))
                    dbuf[m, t, r:end, :] = d
                    e = e + d
                    new[m, t, r:end, :] = e
                    last = min(end, 168)
                    bacc[m, t, first - 32:last - 32, :] += tail * e[first - r:last - r]
                    if t < 2:
                        last = min(end, 160)
                        eacc[m, t, first - 32:last - 32, :] += weight * e[first - r:last - r]
        return tail

    tail = subcycle(2, whole, 8, 184, ebufa, ebufb)
    for first_n, steps, lo, hi in ((3, 1, 8, 184), (5, 4, 16, 176), (13, 4, 24, 168)):
        def two_cycles(h, carry, first_n=first_n, lo=lo, hi=hi):
            n = first_n + 2 * h
            carry = subcycle(n, carry, lo, hi, ebufb, ebufa)
            return subcycle(n + 1, carry, lo, hi, ebufa, ebufb)
        tail = lax.fori_loop(0, steps, two_cycles, tail)

    def averages(i, carry):
        r = pl.multiple_of(i * 16, 16)
        g = pl.multiple_of(32 + i * 16, 16)
        for t in range(2):
            depth_x = hux[t, pl.ds(g, 16), :]
            depth_y = huy[t, pl.ds(g, 16), :]
            kx = ku[t, pl.ds(r, 16), :]
            ky = kv[t, pl.ds(r, 16), :]
            inv_x = 1.0 / (depth_x + jnp.where(kx > 0.0, 0.0, 1.0))
            inv_y = 1.0 / (depth_y + jnp.where(ky > 0.0, 0.0, 1.0))
            mean_x = 1.0 / jnp.maximum(kx, 1.0)
            mean_y = 1.0 / jnp.maximum(ky, 1.0)
            for m in range(2):
                lane = slice(t * LN, (t + 1) * LN)
                acc = bacc[m, t, pl.ds(r, 16), :]
                eta_out[m, pl.ds(r, 16), lane] = eacc[m, t, pl.ds(r, 16), :]
                tx = whole * xb[4 + m, t, pl.ds(g, 16), :] + moment * xf[m, t, pl.ds(g, 16), :] \
                    - WAVE_COURANT * depth_x * (east(acc, bacc[m, NEXT[t], pl.ds(r, 16), :]) - acc)
                ty = whole * xb[6 + m, t, pl.ds(g, 16), :] + moment * xf[2 + m, t, pl.ds(g, 16), :] \
                    - WAVE_COURANT * depth_y * (bacc[m, t, pl.ds(r + 1, 16), :] - acc)
                tx = jnp.where(kx > 0.0, tx, 0.0)
                ty = jnp.where(ky > 0.0, ty, 0.0)
                tx_out[m, pl.ds(r, 16), lane] = tx
                ty_out[m, pl.ds(r, 16), lane] = ty
                corr_out[0, m, t, pl.ds(r, 16), :] = tx * inv_x - xsum[0, m, t, pl.ds(r, 16), :] * mean_x
                corr_out[1, m, t, pl.ds(r, 16), :] = ty * inv_y - xsum[1, m, t, pl.ds(r, 16), :] * mean_y
        return carry
    lax.fori_loop(0, ROWS // 16, averages, 0)

    wait_send_all(wide_copies(xb, sp, rp, xs_sem, xr_sem))
    wait_send_all(wide_copies(xf, sf, rf, fs_sem, fr_sem))
    for copy in packet_copies:
        copy.wait()

    def drain(c, carry):
        wait_send_all(edge_copies(c))
        for copy in stores(c):
            copy.wait()
        return carry
    lax.fori_loop(0, NCH, drain, 0)


def tracer_kernel(u_hbm, v_hbm, t_hbm, s_hbm, us_hbm, vs_hbm, eta_in, tx_in, ty_in, corr_in, kmask_in, col_in, rows_in, table,
                  eta_hbm, tx_hbm, ty_hbm, un_hbm, vn_hbm, tn_hbm, sn_hbm,
                  buf, tt, ts, ct, su, sv, small, corr, kmask, cols, rows, ld_sem, ed_sem, st_sem, in_sem, out_sem):
    hbm = (u_hbm, v_hbm, t_hbm, s_hbm)
    sources = (eta_in, tx_in, ty_in)
    sinks = (eta_hbm, tx_hbm, ty_hbm)

    def loads(c):
        out = []
        for f in range(4):
            for t in range(2):
                out.append(pltpu.make_async_copy(
                    hbm[f].at[pl.ds(c * CHUNK, CHUNK), :, :, pl.ds(t * LN, LN)],
                    buf.at[f, pl.ds(c * CHUNK, CHUNK), :, t, pl.ds(8, ROWS), :], ld_sem.at[c, f * 2 + t]))
        for f, (src, dst) in enumerate(((us_hbm, su), (vs_hbm, sv))):
            out.append(pltpu.make_async_copy(src.at[pl.ds(c * CHUNK, CHUNK)], dst.at[pl.ds(c * CHUNK, CHUNK)], ld_sem.at[c, 8 + f]))
        return out

    def stores_v(c):
        return [pltpu.make_async_copy(src.at[pl.ds(c * CHUNK, CHUNK)], dst.at[pl.ds(c * CHUNK, CHUNK)], st_sem.at[c, f])
                for f, (src, dst) in enumerate(((su, un_hbm), (sv, vn_hbm)))]

    def stores_t(c):
        return [pltpu.make_async_copy(src.at[pl.ds(c * CHUNK, CHUNK)], dst.at[pl.ds(c * CHUNK, CHUNK)], st_sem.at[c, 2 + f])
                for f, (src, dst) in enumerate(((tt, tn_hbm), (ts, sn_hbm)))]

    edges = [pltpu.make_async_copy(src, dst, ed_sem.at[i])
             for i, (src, dst) in enumerate(((col_in, cols), (rows_in, rows), (corr_in, corr), (kmask_in, kmask)))]
    for copy in edges:
        copy.start()
    for c in range(NCH):
        for copy in loads(c):
            copy.start()
    small_in = [pltpu.make_async_copy(sources[i], small.at[i], in_sem.at[i]) for i in range(3)]
    small_out = [pltpu.make_async_copy(small.at[i], sinks[i], out_sem.at[i]) for i in range(3)]
    for copy in small_in:
        copy.start()

    def zero_planes(i, carry):
        r = pl.multiple_of(i * 16, 16)
        z = jnp.zeros((16, 2 * LN), F32)
        for f in range(2):
            for m in range(2):
                for t in range(2):
                    ct[f, m, t, pl.ds(r, 16), :] = z[:, :LN]
        for m in range(2):
            for ref in (tt, ts):
                ref[LEVELS, m, pl.ds(r, 16), :] = z
        return carry
    lax.fori_loop(0, ROWS // 16, zero_planes, 0)
    for copy in edges:
        copy.wait()

    BR = 64

    def level(c, kk):
        k = c * CHUNK + kk
        level_no = k.astype(F32)
        before = table[0, k]

        def block(i, carry):
            r = pl.multiple_of(i * BR, BR)
            b = pl.multiple_of(8 + i * BR, 8)
            wet = [kmask[0, t, pl.ds(r, BR), :] > level_no for t in range(2)]
            packed = cols[c, pl.ds(b, BR), :]
            for m in range(2):
                j = kk * 2 + m
                u = [buf[0, k, m, t, pl.ds(b, BR), :] for t in range(2)]
                v = [buf[1, k, m, t, pl.ds(b, BR), :] for t in range(2)]
                vs = [buf[1, k, m, t, pl.ds(b - 1, BR), :] for t in range(2)]
                uw = west_pair(*u, halo(packed, j))
                for f, ref in ((2, tt), (3, ts)):
                    q = [buf[f, k, m, t, pl.ds(b, BR), :] for t in range(2)]
                    edge = halo(packed, f * PAIRS + j)
                    qe, qw = east_pair(*q, edge), west_pair(*q, edge)
                    for t in range(2):
                        lane = slice(t * LN, (t + 1) * LN)
                        fy = v[t] * (q[t] + buf[f, k, m, t, pl.ds(b + 1, BR), :])
                        fs = vs[t] * (q[t] + buf[f, k, m, t, pl.ds(b - 1, BR), :])
                        adv = q[t] - 0.5 * ((u[t] * (q[t] + qe[t]) - uw[t] * (q[t] + qw[t])) + (fy - fs))
                        adv = jnp.where(wet[t], adv, 0.0)
                        new = adv + before * ct[f - 2, m, t, pl.ds(r, BR), :]
                        ct[f - 2, m, t, pl.ds(r, BR), :] = new
                        ref[k, m, pl.ds(r, BR), lane] = new
            for t in range(2):
                lane = slice(t * LN, (t + 1) * LN)
                wet_x = kmask[1, t, pl.ds(r, BR), :] > level_no
                wet_y = kmask[2, t, pl.ds(r, BR), :] > level_no
                for m in range(2):
                    su[k, m, pl.ds(r, BR), lane] = jnp.where(wet_x, su[k, m, pl.ds(r, BR), lane] + corr[0, m, t, pl.ds(r, BR), :], 0.0)
                    sv[k, m, pl.ds(r, BR), lane] = jnp.where(wet_y, sv[k, m, pl.ds(r, BR), lane] + corr[1, m, t, pl.ds(r, BR), :], 0.0)
            return carry
        lax.fori_loop(0, ROWS // BR, block, 0)

    def chunk_step(c, carry):
        for copy in loads(c):
            copy.wait()
        for kk in range(CHUNK):
            k = c * CHUNK + kk
            for m in range(2):
                jj = kk * 2 + m
                for f in (1, 2, 3):
                    for t in range(2):
                        buf[f, k, m, t, 7:8, :] = rows[0, c, t, f, jj:jj + 1, :]
                for f in (2, 3):
                    for t in range(2):
                        buf[f, k, m, t, 8 + ROWS:9 + ROWS, :] = rows[1, c, t, f, jj:jj + 1, :]

        def one_level(kk, carry2):
            level(c, kk)
            return carry2
        lax.fori_loop(0, CHUNK, one_level, 0)
        for copy in stores_v(c):
            copy.start()
        return carry
    lax.fori_loop(0, NCH, chunk_step, 0)

    for copy in small_in:
        copy.wait()
    for copy in small_out:
        copy.start()

    def upward(step, carry):
        c = NCH - 1 - step

        def block(i, carry2):
            r = pl.multiple_of(i * UP, UP)
            for t in range(2):
                lane = slice(t * LN, (t + 1) * LN)
                depth = kmask[0, t, pl.ds(r, UP), :]
                below = [[ref[c * CHUNK + CHUNK, m, pl.ds(r, UP), lane] for m in range(2)] for ref in (tt, ts)]
                for kk in range(CHUNK - 1, -1, -1):
                    k = c * CHUNK + kk
                    level_no = k.astype(F32)
                    inv = jnp.where(depth > level_no + 1.0, table[2, k], jnp.where(depth > level_no, table[3, k], 0.0))
                    for f, ref in enumerate((tt, ts)):
                        for m in range(2):
                            below[f][m] = ref[k, m, pl.ds(r, UP), lane] * inv + table[1, k] * below[f][m]
                            ref[k, m, pl.ds(r, UP), lane] = below[f][m]
            return carry2
        lax.fori_loop(0, ROWS // UP, block, 0)
        for copy in stores_t(c):
            copy.start()
        return carry
    lax.fori_loop(0, NCH, upward, 0)

    for copy in small_out:
        copy.wait()

    def drain(c, carry):
        for copy in stores_v(c) + stores_t(c):
            copy.wait()
        return carry
    lax.fori_loop(0, NCH, drain, 0)


def solution(mesh):
    assert mesh.shape["col"] == 2 and mesh.shape["row"] == 4
    any_spec = pl.BlockSpec(memory_space=pl.ANY)
    vmem_spec = pl.BlockSpec(memory_space=pltpu.VMEM)
    smem_spec = pl.BlockSpec(memory_space=pltpu.SMEM)
    shape = lambda *dims: jax.ShapeDtypeStruct(dims, F32)
    dma = lambda *dims: pltpu.SemaphoreType.DMA(dims)
    vm = lambda *dims: pltpu.VMEM(dims, F32)
    visc = solve_table(VISC_NUMBER)
    diff = solve_table(DIFF_NUMBER)
    full = (LEVELS, 2, ROWS, 2 * LN)
    flat = (2, ROWS, 2 * LN)

    momentum = pl.pallas_call(
        momentum_kernel,
        name="momentum",
        out_shape=(shape(*full), shape(*full), shape(*flat), shape(*flat), shape(*flat), shape(2, 2, 2, ROWS, LN),
                   shape(3, 2, ROWS, LN), shape(NCH, PR, LN), shape(2, NCH, 2, 4, PAIRS, LN)),
        in_specs=[any_spec] * 8 + [vmem_spec, smem_spec, smem_spec],
        out_specs=(any_spec, any_spec, vmem_spec, vmem_spec, vmem_spec, vmem_spec, vmem_spec, any_spec, any_spec),
        scratch_shapes=[
            vm(4, LEVELS, 2, 2, PR, LN), vm(LEVELS + 1, 2, 2, ROWS, LN), vm(LEVELS + 1, 2, 2, ROWS, LN),
            vm(2, 2, ROWS, LN), vm(2, 2, ROWS, LN), vm(2, 2, 2, PR, LN), vm(2, 2, PR, LN), vm(2, PR, LN), vm(ROWS, LN),
            vm(2, 2, 2, ROWS, LN), vm(2, 2, 2, ROWS, LN), vm(2, ROWS, LN), vm(2, ROWS, LN),
            vm(NCH, ROWS, LN), vm(NCH, PR, LN), vm(2, NCH, 2, 4, PAIRS, LN), vm(2, NCH, 2, 4, PAIRS, LN),
            vm(8, 3, EXT, LN), vm(4, ROWS, LN), vm(4, EXT, LN), vm(4, 3, EXT, LN), vm(2, ROWS, LN), vm(2, EXT, LN),
            vm(3, EXT, LN), vm(3, EXT, LN), vm(3, EXT, LN), vm(3, EXT, LN), vm(3, EXT, LN), vm(3, EXT, LN), vm(3, EXT, LN),
            vm(2, 3, EXT, LN), vm(2, 3, EXT, LN), vm(2, 3, EXT, LN), vm(2, 3, EXT, LN), vm(2, 2, ROWS + 8, LN), vm(2, 3, ROWS + 8, LN),
            dma(NCH, 8), dma(8), dma(NCH, 5), dma(NCH, 5), dma(5), dma(5), dma(5), dma(5), dma(NCH, 4), dma(2),
        ],
        compiler_params=pltpu.CompilerParams(collective_id=0, has_side_effects=True, vmem_limit_bytes=67043328),
    )

    tracers = pl.pallas_call(
        tracer_kernel,
        name="tracers",
        out_shape=(shape(*flat), shape(*flat), shape(*flat), shape(*full), shape(*full), shape(*full), shape(*full)),
        in_specs=[any_spec] * 13 + [smem_spec],
        out_specs=(any_spec,) * 7,
        scratch_shapes=[
            vm(4, LEVELS, 2, 2, PR, LN), vm(LEVELS + 1, 2, ROWS, 2 * LN), vm(LEVELS + 1, 2, ROWS, 2 * LN), vm(2, 2, 2, ROWS, LN),
            vm(*full), vm(*full), vm(3, 2, ROWS, 2 * LN), vm(2, 2, 2, ROWS, LN), vm(3, 2, ROWS, LN),
            vm(NCH, PR, LN), vm(2, NCH, 2, 4, PAIRS, LN),
            dma(NCH, 10), dma(4), dma(NCH, 4), dma(3), dma(3),
        ],
        compiler_params=pltpu.CompilerParams(vmem_limit_bytes=67043328),
    )

    def local_step(vel_x, vel_y, pot_temp, salinity, surf_eta, trans_x, trans_y, col_depth, wet_levels, avg_weights):
        star_x, star_y, eta, tx, ty, corr, kmask, cols, rows = momentum(
            vel_x, vel_y, pot_temp, salinity, surf_eta, trans_x, trans_y, col_depth, wet_levels, avg_weights, jnp.asarray(visc))
        return tracers(vel_x, vel_y, pot_temp, salinity, star_x, star_y, eta, tx, ty, corr, kmask, cols, rows, jnp.asarray(diff))

    spec_3d = P(None, None, "row", "col")
    spec_2d = P(None, "row", "col")
    spec_map = P("row", "col")
    return jax.shard_map(local_step, mesh=mesh, in_specs=(spec_3d, spec_3d, spec_3d, spec_3d, spec_2d, spec_2d, spec_2d, spec_map, spec_map, P()),
                         out_specs=(spec_2d, spec_2d, spec_2d, spec_3d, spec_3d, spec_3d, spec_3d), check_vma=False)
```

```python
import functools
import numpy as np
import jax
import jax.numpy as jnp
from jax import lax
from jax.experimental import pallas as pl
from jax.experimental.pallas import tpu as pltpu
from jax.sharding import PartitionSpec as P

WAVE_COURANT = 0.4
THERM_EXP = 0.2
HALINE_CON = 0.15
PRESS_SCALE = 0.5
VISC_NUMBER = 1.0
DIFF_NUMBER = 0.5

LEVELS = 20
SUBS = 20
CHUNK = 4
NCH = LEVELS // CHUNK
PAIRS = 2 * CHUNK
ROWS = 128
LN = 128
PR = 144
EXT = 192
F32 = jnp.float32
PK = 64
UP = 32
MESH_ID = pl.DeviceIdType.MESH


def solve_table(strength):
    inner = np.zeros(LEVELS)
    last = np.zeros(LEVELS)
    inner[0] = 1.0 + strength
    last[0] = 1.0
    for k in range(1, LEVELS):
        inner[k] = 1.0 + 2.0 * strength - strength**2 / inner[k - 1]
        last[k] = 1.0 + strength - strength**2 / inner[k - 1]
    ratio = strength / inner
    before = np.concatenate([[0.0], ratio[:-1]])
    return np.stack([before, ratio, 1.0 / inner, 1.0 / last]).astype(np.float32)


def lanes(rows):
    return lax.broadcasted_iota(jnp.int32, (rows, LN), 1)


def east(tile, following):
    return pltpu.roll(jnp.where(lanes(tile.shape[0]) == 0, following, tile), LN - 1, 1)


def west(tile, previous):
    return pltpu.roll(jnp.where(lanes(tile.shape[0]) == LN - 1, previous, tile), 1, 1)


NEXT = (1, 2, 0)
PREV = (2, 0, 1)


def halo(packed, j):
    return pltpu.roll(packed, LN - 1 - 2 * j, 1)


def east_pair(first, second, edge):
    last = lanes(first.shape[0]) == LN - 1
    a, b = pltpu.roll(first, LN - 1, 1), pltpu.roll(second, LN - 1, 1)
    return jnp.where(last, b, a), jnp.where(last, edge, b)


def west_pair(first, second, edge):
    origin = lanes(first.shape[0]) == 0
    a, b = pltpu.roll(first, 1, 1), pltpu.roll(second, 1, 1)
    return jnp.where(origin, edge, a), jnp.where(origin, a, b)


def momentum_kernel(u_hbm, v_hbm, t_hbm, s_hbm, eta_hbm, tx_hbm, ty_hbm, h_hbm, kmt_ref, weights, table,
                    us_hbm, vs_hbm, eta_out, tx_out, ty_out, corr_out, kmask_out, col_out, rows_out,
                    buf, tu, tv, cu, cv, pbuf, pacc, phal, rhoc, gsum, xsum, ku, kv,
                    send_col, recv_col, send_row, recv_row,
                    xb, sp, rp, xf, sf, rf, hux, huy, ae, aw, an, as_, cc, ebufa, ebufb, dbuf, gbuf, eacc, bacc,
                    ld_sem, xl_sem, cs_sem, cr_sem, xs_sem, xr_sem, fs_sem, fr_sem, st_sem, ot_sem):
    me_c = lax.axis_index("col")
    me_r = lax.axis_index("row")
    peer = 1 - me_c
    has_n = me_r < 3
    has_s = me_r > 0
    hbm = (u_hbm, v_hbm, t_hbm, s_hbm)

    def loads(c):
        out = []
        for f in range(4):
            for t in range(2):
                out.append(pltpu.make_async_copy(
                    hbm[f].at[pl.ds(c * CHUNK, CHUNK), :, :, pl.ds(t * LN, LN)],
                    buf.at[f, pl.ds(c * CHUNK, CHUNK), :, t, pl.ds(8, ROWS), :], ld_sem.at[c, f * 2 + t]))
        return out

    def ext_loads():
        out = []
        for t in range(2):
            lane = pl.ds(t * LN, LN)
            out.append(pltpu.make_async_copy(h_hbm.at[:, lane], xb.at[1, t, pl.ds(32, ROWS), :], xl_sem.at[t]))
            for i, ref in enumerate((eta_hbm, tx_hbm, ty_hbm)):
                out.append(pltpu.make_async_copy(ref.at[:, :, lane], xb.at[pl.ds(2 + 2 * i, 2), t, pl.ds(32, ROWS), :], xl_sem.at[2 + 2 * i + t]))
        return out

    for copy in loads(0) + ext_loads() + loads(1):
        copy.start()

    barrier = pltpu.get_barrier_semaphore()

    def greet(col, row):
        pl.semaphore_signal(barrier, inc=1, device_id={"col": col, "row": row}, device_id_type=MESH_ID)

    greet(peer, me_r)

    @pl.when(has_n)
    def _():
        greet(me_c, me_r + 1)
        greet(peer, me_r + 1)

    @pl.when(has_s)
    def _():
        greet(me_c, me_r - 1)
        greet(peer, me_r - 1)

    zrow = jnp.zeros((8, LN), F32)
    for ref, count in ((xb, 8), (xf, 4)):
        for f in range(count):
            for t in range(3):
                ref[f, t, 0:8, :] = zrow
                ref[f, t, EXT - 8:EXT, :] = zrow
    for ref, count in ((rp, 4), (rf, 2)):
        for f in range(count):
            ref[f, 0:8, :] = zrow
            ref[f, EXT - 8:EXT, :] = zrow

    def zero_side(side, lo):
        z24 = jnp.zeros((24, LN), F32)
        for f in range(8):
            for t in range(2):
                xb[f, t, lo:lo + 24, :] = z24
        for f in range(4):
            rp[f, lo:lo + 24, :] = z24
            for t in range(2):
                xf[f, t, lo:lo + 24, :] = z24
        for f in range(2):
            rf[f, lo:lo + 24, :] = z24
        for c in range(NCH):
            recv_col[c, 136 * side:136 * side + 8, :] = zrow
            for f in range(4):
                for t in range(2):
                    recv_row[side, c, t, f, :, :] = zrow

    @pl.when(me_r == 0)
    def _():
        zero_side(0, 8)

    @pl.when(me_r == 3)
    def _():
        zero_side(1, 160)

    def zero_planes(i, carry):
        r = pl.multiple_of(i * 16, 16)
        z = jnp.zeros((16, LN), F32)
        for m in range(2):
            for t in range(2):
                pacc[m, t, pl.ds(r, 16), :] = z
            phal[m, pl.ds(r, 16), :] = z
        return carry
    lax.fori_loop(0, PR // 16, zero_planes, 0)

    def zero_planes2(i, carry):
        r = pl.multiple_of(i * 16, 16)
        z = jnp.zeros((16, LN), F32)
        for m in range(2):
            for t in range(2):
                for f in range(2):
                    gsum[f, m, t, pl.ds(r, 16), :] = z
                    xsum[f, m, t, pl.ds(r, 16), :] = z
                for ref in (cu, cv):
                    ref[m, t, pl.ds(r, 16), :] = z
                for ref in (tu, tv):
                    ref[LEVELS, m, t, pl.ds(r, 16), :] = z
        return carry
    lax.fori_loop(0, ROWS // 16, zero_planes2, 0)

    for t in range(2):
        for r in range(0, ROWS, 32):
            xb[0, t, 32 + r:64 + r, :] = kmt_ref[r:r + 32, t * LN:(t + 1) * LN].astype(F32)
    for copy in ext_loads():
        copy.wait()

    @pl.when((me_r == 0) | (me_r == 3))
    def _():
        pl.semaphore_wait(barrier, 3)

    @pl.when((me_r != 0) & (me_r != 3))
    def _():
        pl.semaphore_wait(barrier, 5)

    def remote(src, dst, ssem, rsem, col, row):
        return pltpu.make_async_remote_copy(src_ref=src, dst_ref=dst, send_sem=ssem, recv_sem=rsem,
                                            device_id={"col": col, "row": row}, device_id_type=MESH_ID)

    def wide_copies(own, packed, landing, ssem, rsem):
        north, south = me_r + 1, me_r - 1
        side = remote(packed, landing.at[:, pl.ds(32, ROWS), :], ssem.at[0], rsem.at[0], peer, me_r)
        up = (remote(own.at[:, pl.ds(0, 2), pl.ds(136, 24), :], own.at[:, pl.ds(0, 2), pl.ds(8, 24), :], ssem.at[1], rsem.at[1], me_c, north),
              remote(packed.at[:, pl.ds(104, 24), :], landing.at[:, pl.ds(8, 24), :], ssem.at[2], rsem.at[2], peer, north))
        down = (remote(own.at[:, pl.ds(0, 2), pl.ds(32, 24), :], own.at[:, pl.ds(0, 2), pl.ds(160, 24), :], ssem.at[3], rsem.at[3], me_c, south),
                remote(packed.at[:, pl.ds(0, 24), :], landing.at[:, pl.ds(160, 24), :], ssem.at[4], rsem.at[4], peer, south))
        return side, up, down

    def edge_copies(c):
        north, south = me_r + 1, me_r - 1
        side = remote(send_col.at[c], recv_col.at[c, pl.ds(8, ROWS), :], cs_sem.at[c, 0], cr_sem.at[c, 0], peer, me_r)
        up = (remote(send_row.at[0, c], recv_row.at[0, c], cs_sem.at[c, 1], cr_sem.at[c, 1], me_c, north),
              remote(send_col.at[c, pl.ds(ROWS - 8, 8), :], recv_col.at[c, pl.ds(0, 8), :], cs_sem.at[c, 2], cr_sem.at[c, 2], peer, north))
        down = (remote(send_row.at[1, c], recv_row.at[1, c], cs_sem.at[c, 3], cr_sem.at[c, 3], me_c, south),
                remote(send_col.at[c, pl.ds(0, 8), :], recv_col.at[c, pl.ds(8 + ROWS, 8), :], cs_sem.at[c, 4], cr_sem.at[c, 4], peer, south))
        return side, up, down

    def start_all(copies):
        side, up, down = copies
        if side is not None:
            side.start()

        @pl.when(has_n)
        def _():
            for copy in up:
                copy.start()

        @pl.when(has_s)
        def _():
            for copy in down:
                copy.start()

    def wait_recv_all(copies):
        side, up, down = copies
        if side is not None:
            side.wait_recv()

        @pl.when(has_s)
        def _():
            for copy in up:
                copy.wait_recv()

        @pl.when(has_n)
        def _():
            for copy in down:
                copy.wait_recv()

    def wait_send_all(copies):
        side, up, down = copies
        side.wait_send()

        @pl.when(has_n)
        def _():
            for copy in up:
                copy.wait_send()

        @pl.when(has_s)
        def _():
            for copy in down:
                copy.wait_send()

    def rows_only(copies):
        return None, copies[1][:1], copies[2][:1]

    def columns_only(copies):
        return copies[0], copies[1][1:], copies[2][1:]

    start_all(rows_only(wide_copies(xb, sp, rp, xs_sem, xr_sem)))

    def pack_and_send(c, with_maps=False):
        for copy in loads(c):
            copy.wait()
        lane = lanes(PK)

        def block(i, carry):
            r = pl.multiple_of(i * PK, PK)
            pairs = [(f, c * CHUNK + kk, m) for f in range(4) for kk in range(CHUNK) for m in range(2)]
            column = [[buf[f, k, m, t, pl.ds(8 + r, PK), :] for f, k, m in pairs] for t in range(2)]
            if with_maps:
                for t in range(2):
                    column[t] += [xb[0, t, pl.ds(32 + r, PK), :], xb[1, t, pl.ds(32 + r, PK), :]]
            packed = jnp.zeros((PK, LN), F32)
            count = len(column[0])
            for i in range(count + 1):
                edge = jnp.where(lane == 0, column[0][min(i, count - 1)], column[1][max(i - 1, 0)])
                edge = pltpu.roll(edge, 2 * i, 1) if i else edge
                packed = jnp.where(lane >= 2 * i - 1, edge, packed) if i else edge
            send_col[c, pl.ds(r, PK), :] = packed
            return carry
        for kk in range(CHUNK):
            for m in range(2):
                jj = kk * 2 + m
                k = c * CHUNK + kk
                for side, row in ((0, 8 + ROWS - 1), (1, 8)):
                    for f in range(4):
                        for t in range(2):
                            send_row[side, c, t, f, jj:jj + 1, :] = buf[f, k, m, t, row:row + 1, :]
        lax.fori_loop(0, ROWS // PK, block, 0)
        start_all(edge_copies(c))

    pack_and_send(0, with_maps=True)
    for copy in loads(2):
        copy.start()
    pack_and_send(1)

    RHO_T = np.float32(-THERM_EXP * PRESS_SCALE / LEVELS / 2)
    RHO_S = np.float32(HALINE_CON * PRESS_SCALE / LEVELS / 2)
    BR = 64
    SB = 16

    def pressure_rows(k, slot, base, rows):
        for m in range(2):
            for t in range(2):
                half = RHO_T * buf[2, k, m, t, pl.ds(base, rows), :] + RHO_S * buf[3, k, m, t, pl.ds(base, rows), :]
                p = pacc[m, t, pl.ds(base, rows), :] + half
                slot[m, t, pl.ds(base, rows), :] = p
                pacc[m, t, pl.ds(base, rows), :] = p + half

    def level(c, kk, now, later):
        k = c * CHUNK + kk
        pressure_rows(k, now, 8 + ROWS, 8)
        level_no = k.astype(F32)
        before = table[0, k]
        following = jnp.minimum(k + 1, LEVELS - 1)

        def block(i, carry):
            for q in range(0, BR, SB):
                piece(pl.multiple_of(i * BR + q, SB), pl.multiple_of(8 + i * BR + q, 8))
            return carry

        def piece(r, b):
            wet_x = [ku[t, pl.ds(r, SB), :] > level_no for t in range(2)]
            wet_y = [kv[t, pl.ds(r, SB), :] > level_no for t in range(2)]
            packed = recv_col[c, pl.ds(b, SB), :]
            packed_w = packed + recv_col[c, pl.ds(b - 1, SB), :]
            packed_z = packed + recv_col[c, pl.ds(b + 1, SB), :]
            packed_r = rhoc[pl.ds(r, SB), :]
            for m in range(2):
                j = kk * 2 + m
                half = halo(packed_r, j)
                p_edge = phal[m, pl.ds(r, SB), :] + half
                phal[m, pl.ds(r, SB), :] = p_edge + half
                u_edge, v_edge = halo(packed, j), halo(packed, PAIRS + j)
                w_edge, z_edge = halo(packed_w, PAIRS + j), halo(packed_z, j)
                u = [buf[0, k, m, t, pl.ds(b, SB), :] for t in range(2)]
                v = [buf[1, k, m, t, pl.ds(b, SB), :] for t in range(2)]
                un = [buf[0, k, m, t, pl.ds(b + 1, SB), :] for t in range(2)]
                vs = [buf[1, k, m, t, pl.ds(b - 1, SB), :] for t in range(2)]
                p = [now[m, t, pl.ds(b, SB), :] for t in range(2)]
                w = [v[t] + vs[t] for t in range(2)]
                z = [u[t] + un[t] for t in range(2)]
                ue, uw = east_pair(*u, u_edge), west_pair(*u, u_edge)
                ve, vw = east_pair(*v, v_edge), west_pair(*v, v_edge)
                pe, we, zw = east_pair(*p, p_edge), east_pair(*w, w_edge), west_pair(*z, z_edge)
                for t in range(2):
                    us = buf[0, k, m, t, pl.ds(b - 1, SB), :]
                    gu = (p[t] - pe[t]) - (0.5 * u[t]) * (ue[t] - uw[t]) - (0.125 * (w[t] + we[t])) * (un[t] - us)
                    gu = jnp.where(wet_x[t], gu, 0.0)
                    gsum[0, m, t, pl.ds(r, SB), :] += gu
                    new = u[t] + gu + before * cu[m, t, pl.ds(r, SB), :]
                    cu[m, t, pl.ds(r, SB), :] = new
                    tu[k, m, t, pl.ds(r, SB), :] = new
                    vn = buf[1, k, m, t, pl.ds(b + 1, SB), :]
                    pn = now[m, t, pl.ds(b + 1, SB), :]
                    gv = (p[t] - pn) - (0.125 * (z[t] + zw[t])) * (ve[t] - vw[t]) - (0.5 * v[t]) * (vn - vs[t])
                    gv = jnp.where(wet_y[t], gv, 0.0)
                    gsum[1, m, t, pl.ds(r, SB), :] += gv
                    new = v[t] + gv + before * cv[m, t, pl.ds(r, SB), :]
                    cv[m, t, pl.ds(r, SB), :] = new
                    tv[k, m, t, pl.ds(r, SB), :] = new
            pressure_rows(following, later, b, SB)
        lax.fori_loop(0, ROWS // BR, block, 0)

    def first_pressure(i, carry):
        pressure_rows(0, pbuf.at[0], pl.multiple_of(8 + i * 64, 8), 64)
        return carry
    lax.fori_loop(0, 2, first_pressure, 0)

    def chunk_step(c, carry):
        @pl.when(c + 3 < NCH)
        def _():
            for copy in loads(c + 3):
                copy.start()

        @pl.when(c + 2 < NCH)
        def _():
            pack_and_send(c + 2)

        @pl.when(c == 2)
        def _():
            pack_wide()

        wait_recv_all(edge_copies(c))

        @pl.when(c == 0)
        def _():
            face_maps()

        for kk in range(CHUNK):
            k = c * CHUNK + kk
            for m in range(2):
                jj = kk * 2 + m
                for side, row in ((0, 7), (1, 8 + ROWS)):
                    for f in range(4):
                        for t in range(2):
                            buf[f, k, m, t, row:row + 1, :] = recv_row[side, c, t, f, jj:jj + 1, :]
        packed = recv_col[c, 8:8 + ROWS, :]
        rhoc[...] = RHO_T * pltpu.roll(packed, LN - 4 * PAIRS, 1) + RHO_S * pltpu.roll(packed, LN - 6 * PAIRS, 1)

        def two_levels(h, carry2):
            level(c, 2 * h, pbuf.at[0], pbuf.at[1])
            level(c, 2 * h + 1, pbuf.at[1], pbuf.at[0])
            return carry2
        lax.fori_loop(0, CHUNK // 2, two_levels, 0)
        return carry

    def pack_wide():
        for pair in range(4):
            pack_pair(lambda t, r, p=pair: xb[2 * p, t, pl.ds(32 + r, 64), :],
                      lambda t, r, p=pair: xb[2 * p + 1, t, pl.ds(32 + r, 64), :], sp, pair, 64)
        start_all(columns_only(wide_copies(xb, sp, rp, xs_sem, xr_sem)))

    def face_maps():
        wait_recv_all(rows_only(wide_copies(xb, sp, rp, xs_sem, xr_sem)))

        def maps(i, carry):
            r = pl.multiple_of(i * 64, 64)
            packed = recv_col[0, pl.ds(8 + r, 64), :]
            kt = [xb[0, t, pl.ds(32 + r, 64), :] for t in range(2)]
            ht = [xb[1, t, pl.ds(32 + r, 64), :] for t in range(2)]
            ke = east_pair(*kt, halo(packed, 4 * PAIRS))
            he = east_pair(*ht, halo(packed, 4 * PAIRS + 1))
            for t in range(2):
                kx = jnp.minimum(kt[t], ke[t])
                ky = jnp.minimum(kt[t], xb[0, t, pl.ds(33 + r, 64), :])
                ku[t, pl.ds(r, 64), :] = kx
                kv[t, pl.ds(r, 64), :] = ky
                kmask_out[0, t, pl.ds(r, 64), :] = kt[t]
                kmask_out[1, t, pl.ds(r, 64), :] = kx
                kmask_out[2, t, pl.ds(r, 64), :] = ky
                hux[t, pl.ds(32 + r, 64), :] = jnp.where(kx > 0.0, 0.5 * (ht[t] + he[t]), 0.0)
                huy[t, pl.ds(32 + r, 64), :] = jnp.where(ky > 0.0, 0.5 * (ht[t] + xb[1, t, pl.ds(33 + r, 64), :]), 0.0)
            return carry
        lax.fori_loop(0, 2, maps, 0)

    def pack_pair(first, second, send, slot, rows):
        lane = lanes(rows)

        def block(i, carry):
            r = pl.multiple_of(i * rows, rows)
            a = jnp.where(lane < 64, first(0, r), first(1, r))
            b = jnp.where(lane < 64, second(0, r), second(1, r))
            outer = (lane < 32) | (lane >= 96)
            send[slot, pl.ds(r, rows), :] = jnp.where(outer, a, pltpu.roll(b, 64, 1))
            return carry
        lax.fori_loop(0, ROWS // rows, block, 0)

    lax.fori_loop(0, NCH, chunk_step, 0)

    packet_copies = [pltpu.make_async_copy(recv_col, col_out, ot_sem.at[0]),
                     pltpu.make_async_copy(recv_row, rows_out, ot_sem.at[1])]
    for copy in packet_copies:
        copy.start()

    def forcing(i, carry):
        r = pl.multiple_of(i * 32, 32)
        for t in range(2):
            nx = jnp.maximum(ku[t, pl.ds(r, 32), :], 1.0)
            ny = jnp.maximum(kv[t, pl.ds(r, 32), :], 1.0)
            fx = hux[t, pl.ds(32 + r, 32), :] / nx / SUBS
            fy = huy[t, pl.ds(32 + r, 32), :] / ny / SUBS
            for m in range(2):
                xf[m, t, pl.ds(32 + r, 32), :] = fx * gsum[0, m, t, pl.ds(r, 32), :]
                xf[2 + m, t, pl.ds(32 + r, 32), :] = fy * gsum[1, m, t, pl.ds(r, 32), :]
        return carry
    lax.fori_loop(0, ROWS // 32, forcing, 0)
    for m in range(2):
        pack_pair(lambda t, r, m=m: xf[m, t, pl.ds(32 + r, 64), :],
                  lambda t, r, m=m: xf[2 + m, t, pl.ds(32 + r, 64), :], sf, m, 64)
    start_all(wide_copies(xf, sf, rf, fs_sem, fr_sem))

    def stores(c):
        out = []
        for f, (ref, dst) in enumerate(((tu, us_hbm), (tv, vs_hbm))):
            for t in range(2):
                out.append(pltpu.make_async_copy(ref.at[pl.ds(c * CHUNK, CHUNK), :, t, :, :],
                                                 dst.at[pl.ds(c * CHUNK, CHUNK), :, :, pl.ds(t * LN, LN)], st_sem.at[c, f * 2 + t]))
        return out

    def upward(step, carry):
        c = NCH - 1 - step

        def block(i, carry2):
            r = pl.multiple_of(i * UP, UP)
            for f, (ref, kp) in enumerate(((tu, ku), (tv, kv))):
                for t in range(2):
                    depth = kp[t, pl.ds(r, UP), :]
                    below = [ref[c * CHUNK + CHUNK, m, t, pl.ds(r, UP), :] for m in range(2)]
                    total = [xsum[f, m, t, pl.ds(r, UP), :] for m in range(2)]
                    for kk in range(CHUNK - 1, -1, -1):
                        k = c * CHUNK + kk
                        level_no = k.astype(F32)
                        inv = jnp.where(depth > level_no + 1.0, table[2, k], jnp.where(depth > level_no, table[3, k], 0.0))
                        for m in range(2):
                            below[m] = ref[k, m, t, pl.ds(r, UP), :] * inv + table[1, k] * below[m]
                            ref[k, m, t, pl.ds(r, UP), :] = below[m]
                            total[m] = total[m] + below[m]
                    for m in range(2):
                        xsum[f, m, t, pl.ds(r, UP), :] = total[m]
            return carry2
        lax.fori_loop(0, ROWS // UP, block, 0)
        for copy in stores(c):
            copy.start()
        return carry
    lax.fori_loop(0, NCH, upward, 0)

    wait_recv_all(columns_only(wide_copies(xb, sp, rp, xs_sem, xr_sem)))

    def unpack_wide(i, carry):
        r = pl.multiple_of(i * 32, 32)
        for pair in range(4):
            tile = rp[pair, pl.ds(r, 32), :]
            xb[2 * pair, 2, pl.ds(r, 32), :] = tile
            xb[2 * pair + 1, 2, pl.ds(r, 32), :] = pltpu.roll(tile, 64, 1)
        return carry
    lax.fori_loop(0, EXT // 32, unpack_wide, 0)

    XR = 88

    def depths(i, carry):
        r = pl.multiple_of(8 + i * XR, 8)
        kt = [xb[0, t, pl.ds(r, XR), :] for t in range(3)]
        ht = [xb[1, t, pl.ds(r, XR), :] for t in range(3)]
        for t in range(3):
            kx = jnp.minimum(kt[t], east(kt[t], kt[NEXT[t]]))
            ky = jnp.minimum(kt[t], xb[0, t, pl.ds(r + 1, XR), :])
            hux[t, pl.ds(r, XR), :] = jnp.where(kx > 0.0, 0.5 * (ht[t] + east(ht[t], ht[NEXT[t]])), 0.0)
            huy[t, pl.ds(r, XR), :] = jnp.where(ky > 0.0, 0.5 * (ht[t] + xb[1, t, pl.ds(r + 1, XR), :]), 0.0)
            cc[t, pl.ds(r, XR), :] = jnp.where(kt[t] > 0.0, WAVE_COURANT, 0.0)
        return carry
    for t in range(3):
        for ref in (hux, huy):
            ref[t, 0:8, :] = zrow
        for ref in (ebufa, ebufb):
            for m in range(2):
                ref[m, t, 0:8, :] = zrow
                ref[m, t, EXT - 8:EXT, :] = zrow
    lax.fori_loop(0, 2, depths, 0)

    def coefficients(i, carry):
        r = pl.multiple_of(8 + i * XR, 8)
        hx = [hux[t, pl.ds(r, XR), :] for t in range(3)]
        for t in range(3):
            c0 = cc[t, pl.ds(r, XR), :]
            cw = WAVE_COURANT * c0
            ae[t, pl.ds(r, XR), :] = cw * hx[t]
            aw[t, pl.ds(r, XR), :] = cw * west(hx[t], hx[PREV[t]])
            an[t, pl.ds(r, XR), :] = cw * huy[t, pl.ds(r, XR), :]
            as_[t, pl.ds(r, XR), :] = cw * huy[t, pl.ds(r - 1, XR), :]
        return carry
    lax.fori_loop(0, 2, coefficients, 0)

    def first_subcycle(m, base, rows):
        tx = [xb[4 + m, t, pl.ds(base, rows), :] for t in range(3)]
        for t in range(3):
            c0 = cc[t, pl.ds(base, rows), :]
            ty = xb[6 + m, t, pl.ds(base, rows), :]
            div = tx[t] - west(tx[t], tx[PREV[t]]) + ty - xb[6 + m, t, pl.ds(base - 1, rows), :]
            change = -c0 * div
            dbuf[m, t, pl.ds(base, rows), :] = change
            eta = jnp.where(c0 > 0.0, xb[2 + m, t, pl.ds(base, rows), :], 0.0) + change
            ebufa[m, t, pl.ds(base, rows), :] = eta

    def first_block(i, carry):
        for m in range(2):
            first_subcycle(m, pl.multiple_of(8 + i * XR, 8), XR)
        return carry
    lax.fori_loop(0, 2, first_block, 0)

    wait_recv_all(wide_copies(xf, sf, rf, fs_sem, fr_sem))

    def unpack_force(i, carry):
        r = pl.multiple_of(i * 32, 32)
        for m in range(2):
            tile = rf[m, pl.ds(r, 32), :]
            xf[m, 2, pl.ds(r, 32), :] = tile
            xf[2 + m, 2, pl.ds(r, 32), :] = pltpu.roll(tile, 64, 1)
        return carry
    lax.fori_loop(0, EXT // 32, unpack_force, 0)

    def forcing_divergence(i, carry):
        r = pl.multiple_of(8 + i * XR, 8)
        for m in range(2):
            fx = [xf[m, t, pl.ds(r, XR), :] for t in range(3)]
            for t in range(3):
                div = fx[t] - west(fx[t], fx[PREV[t]]) + xf[2 + m, t, pl.ds(r, XR), :] - xf[2 + m, t, pl.ds(r - 1, XR), :]
                gbuf[m, t, pl.ds(r, XR), :] = cc[t, pl.ds(r, XR), :] * div
        return carry
    lax.fori_loop(0, 2, forcing_divergence, 0)

    whole = weights[SUBS - 1]
    moment = weights[SUBS - 1]
    for n in range(SUBS - 2, -1, -1):
        whole = whole + weights[n]
        moment = moment + whole

    def first_sums(i, carry):
        r = pl.multiple_of(i * 8, 8)
        for m in range(2):
            for t in range(3):
                eta = ebufa[m, t, pl.ds(32 + r, 8), :]
                bacc[m, t, pl.ds(r, 8), :] = whole * eta
                if t < 2:
                    eacc[m, t, pl.ds(r, 8), :] = weights[0] * eta
        return carry
    lax.fori_loop(0, 17, first_sums, 0)

    def subcycle(n, tail, lo, hi, old, new):
        tail = tail - weights[n - 2]
        weight = weights[n - 1]
        for r, end in ((lo, 96), (96, hi)):
            first = max(r, 32)
            for t in range(3):
                c_e, c_w = ae[t, r:end, :], aw[t, r:end, :]
                c_n, c_s = an[t, r:end, :], as_[t, r:end, :]
                for m in range(2):
                    e = old[m, t, r:end, :]
                    to_e = east(e, old[m, NEXT[t], r:end, :])
                    to_w = west(e, old[m, PREV[t], r:end, :])
                    to_n = old[m, t, r + 1:end + 1, :]
                    to_s = old[m, t, r - 1:end - 1, :]
                    d = dbuf[m, t, r:end, :] - gbuf[m, t, r:end, :]
                    d = d + (c_e * (to_e - e) + c_w * (to_w - e)) + (c_n * (to_n - e) + c_s * (to_s - e))
                    dbuf[m, t, r:end, :] = d
                    e = e + d
                    new[m, t, r:end, :] = e
                    last = min(end, 168)
                    bacc[m, t, first - 32:last - 32, :] += tail * e[first - r:last - r]
                    if t < 2:
                        last = min(end, 160)
                        eacc[m, t, first - 32:last - 32, :] += weight * e[first - r:last - r]
        return tail

    tail = subcycle(2, whole, 8, 184, ebufa, ebufb)
    for first_n, steps, lo, hi in ((3, 1, 8, 184), (5, 4, 16, 176), (13, 4, 24, 168)):
        def two_cycles(h, carry, first_n=first_n, lo=lo, hi=hi):
            n = first_n + 2 * h
            carry = subcycle(n, carry, lo, hi, ebufb, ebufa)
            return subcycle(n + 1, carry, lo, hi, ebufa, ebufb)
        tail = lax.fori_loop(0, steps, two_cycles, tail)

    def averages(i, carry):
        r = pl.multiple_of(i * 16, 16)
        g = pl.multiple_of(32 + i * 16, 16)
        for t in range(2):
            depth_x = hux[t, pl.ds(g, 16), :]
            depth_y = huy[t, pl.ds(g, 16), :]
            kx = ku[t, pl.ds(r, 16), :]
            ky = kv[t, pl.ds(r, 16), :]
            inv_x = 1.0 / (depth_x + jnp.where(kx > 0.0, 0.0, 1.0))
            inv_y = 1.0 / (depth_y + jnp.where(ky > 0.0, 0.0, 1.0))
            mean_x = 1.0 / jnp.maximum(kx, 1.0)
            mean_y = 1.0 / jnp.maximum(ky, 1.0)
            for m in range(2):
                lane = slice(t * LN, (t + 1) * LN)
                acc = bacc[m, t, pl.ds(r, 16), :]
                eta_out[m, pl.ds(r, 16), lane] = eacc[m, t, pl.ds(r, 16), :]
                tx = whole * xb[4 + m, t, pl.ds(g, 16), :] + moment * xf[m, t, pl.ds(g, 16), :] \
                    - WAVE_COURANT * depth_x * (east(acc, bacc[m, NEXT[t], pl.ds(r, 16), :]) - acc)
                ty = whole * xb[6 + m, t, pl.ds(g, 16), :] + moment * xf[2 + m, t, pl.ds(g, 16), :] \
                    - WAVE_COURANT * depth_y * (bacc[m, t, pl.ds(r + 1, 16), :] - acc)
                tx = jnp.where(kx > 0.0, tx, 0.0)
                ty = jnp.where(ky > 0.0, ty, 0.0)
                tx_out[m, pl.ds(r, 16), lane] = tx
                ty_out[m, pl.ds(r, 16), lane] = ty
                corr_out[0, m, t, pl.ds(r, 16), :] = tx * inv_x - xsum[0, m, t, pl.ds(r, 16), :] * mean_x
                corr_out[1, m, t, pl.ds(r, 16), :] = ty * inv_y - xsum[1, m, t, pl.ds(r, 16), :] * mean_y
        return carry
    lax.fori_loop(0, ROWS // 16, averages, 0)

    wait_send_all(wide_copies(xb, sp, rp, xs_sem, xr_sem))
    wait_send_all(wide_copies(xf, sf, rf, fs_sem, fr_sem))
    for copy in packet_copies:
        copy.wait()

    def drain(c, carry):
        wait_send_all(edge_copies(c))
        for copy in stores(c):
            copy.wait()
        return carry
    lax.fori_loop(0, NCH, drain, 0)


def tracer_kernel(u_hbm, v_hbm, t_hbm, s_hbm, us_hbm, vs_hbm, eta_in, tx_in, ty_in, corr_in, kmask_in, col_in, rows_in, table,
                  eta_hbm, tx_hbm, ty_hbm, un_hbm, vn_hbm, tn_hbm, sn_hbm,
                  buf, tt, ts, ct, su, sv, small, corr, kmask, cols, rows, ld_sem, ed_sem, st_sem, in_sem, out_sem):
    hbm = (u_hbm, v_hbm, t_hbm, s_hbm)
    sources = (eta_in, tx_in, ty_in)
    sinks = (eta_hbm, tx_hbm, ty_hbm)

    def loads(c):
        out = []
        for f in range(4):
            for t in range(2):
                out.append(pltpu.make_async_copy(
                    hbm[f].at[pl.ds(c * CHUNK, CHUNK), :, :, pl.ds(t * LN, LN)],
                    buf.at[f, pl.ds(c * CHUNK, CHUNK), :, t, pl.ds(8, ROWS), :], ld_sem.at[c, f * 2 + t]))
        for f, (src, dst) in enumerate(((us_hbm, su), (vs_hbm, sv))):
            out.append(pltpu.make_async_copy(src.at[pl.ds(c * CHUNK, CHUNK)], dst.at[pl.ds(c * CHUNK, CHUNK)], ld_sem.at[c, 8 + f]))
        return out

    def stores_v(c):
        return [pltpu.make_async_copy(src.at[pl.ds(c * CHUNK, CHUNK)], dst.at[pl.ds(c * CHUNK, CHUNK)], st_sem.at[c, f])
                for f, (src, dst) in enumerate(((su, un_hbm), (sv, vn_hbm)))]

    def stores_t(c):
        return [pltpu.make_async_copy(src.at[pl.ds(c * CHUNK, CHUNK)], dst.at[pl.ds(c * CHUNK, CHUNK)], st_sem.at[c, 2 + f])
                for f, (src, dst) in enumerate(((tt, tn_hbm), (ts, sn_hbm)))]

    edges = [pltpu.make_async_copy(src, dst, ed_sem.at[i])
             for i, (src, dst) in enumerate(((col_in, cols), (rows_in, rows), (corr_in, corr), (kmask_in, kmask)))]
    for copy in edges:
        copy.start()
    for c in range(NCH):
        for copy in loads(c):
            copy.start()
    small_in = [pltpu.make_async_copy(sources[i], small.at[i], in_sem.at[i]) for i in range(3)]
    small_out = [pltpu.make_async_copy(small.at[i], sinks[i], out_sem.at[i]) for i in range(3)]
    for copy in small_in:
        copy.start()

    def zero_planes(i, carry):
        r = pl.multiple_of(i * 16, 16)
        z = jnp.zeros((16, 2 * LN), F32)
        for f in range(2):
            for m in range(2):
                for t in range(2):
                    ct[f, m, t, pl.ds(r, 16), :] = z[:, :LN]
        for m in range(2):
            for ref in (tt, ts):
                ref[LEVELS, m, pl.ds(r, 16), :] = z
        return carry
    lax.fori_loop(0, ROWS // 16, zero_planes, 0)
    for copy in edges:
        copy.wait()

    BR = 128
    SB = 16

    def level(c, kk):
        k = c * CHUNK + kk
        level_no = k.astype(F32)
        before = table[0, k]

        def block(i, carry):
            for q in range(0, BR, SB):
                piece(pl.multiple_of(i * BR + q, SB), pl.multiple_of(8 + i * BR + q, 8))
            return carry

        def piece(r, b):
            wet = [kmask[0, t, pl.ds(r, SB), :] > level_no for t in range(2)]
            packed = cols[c, pl.ds(b, SB), :]
            for m in range(2):
                j = kk * 2 + m
                u = [buf[0, k, m, t, pl.ds(b, SB), :] for t in range(2)]
                v = [buf[1, k, m, t, pl.ds(b, SB), :] for t in range(2)]
                vs = [buf[1, k, m, t, pl.ds(b - 1, SB), :] for t in range(2)]
                uw = west_pair(*u, halo(packed, j))
                for f, ref in ((2, tt), (3, ts)):
                    q = [buf[f, k, m, t, pl.ds(b, SB), :] for t in range(2)]
                    edge = halo(packed, f * PAIRS + j)
                    qe, qw = east_pair(*q, edge), west_pair(*q, edge)
                    for t in range(2):
                        lane = slice(t * LN, (t + 1) * LN)
                        fy = v[t] * (q[t] + buf[f, k, m, t, pl.ds(b + 1, SB), :])
                        fs = vs[t] * (q[t] + buf[f, k, m, t, pl.ds(b - 1, SB), :])
                        adv = q[t] - 0.5 * ((u[t] * (q[t] + qe[t]) - uw[t] * (q[t] + qw[t])) + (fy - fs))
                        adv = jnp.where(wet[t], adv, 0.0)
                        new = adv + before * ct[f - 2, m, t, pl.ds(r, SB), :]
                        ct[f - 2, m, t, pl.ds(r, SB), :] = new
                        ref[k, m, pl.ds(r, SB), lane] = new
            for t in range(2):
                lane = slice(t * LN, (t + 1) * LN)
                wet_x = kmask[1, t, pl.ds(r, SB), :] > level_no
                wet_y = kmask[2, t, pl.ds(r, SB), :] > level_no
                for m in range(2):
                    su[k, m, pl.ds(r, SB), lane] = jnp.where(wet_x, su[k, m, pl.ds(r, SB), lane] + corr[0, m, t, pl.ds(r, SB), :], 0.0)
                    sv[k, m, pl.ds(r, SB), lane] = jnp.where(wet_y, sv[k, m, pl.ds(r, SB), lane] + corr[1, m, t, pl.ds(r, SB), :], 0.0)
        lax.fori_loop(0, ROWS // BR, block, 0)

    def chunk_step(c, carry):
        for copy in loads(c):
            copy.wait()
        for kk in range(CHUNK):
            k = c * CHUNK + kk
            for m in range(2):
                jj = kk * 2 + m
                for f in (1, 2, 3):
                    for t in range(2):
                        buf[f, k, m, t, 7:8, :] = rows[0, c, t, f, jj:jj + 1, :]
                for f in (2, 3):
                    for t in range(2):
                        buf[f, k, m, t, 8 + ROWS:9 + ROWS, :] = rows[1, c, t, f, jj:jj + 1, :]

        def one_level(kk, carry2):
            level(c, kk)
            return carry2
        lax.fori_loop(0, CHUNK, one_level, 0)
        for copy in stores_v(c):
            copy.start()
        return carry
    lax.fori_loop(0, NCH, chunk_step, 0)

    for copy in small_in:
        copy.wait()
    for copy in small_out:
        copy.start()

    def upward(step, carry):
        c = NCH - 1 - step

        def block(i, carry2):
            r = pl.multiple_of(i * UP, UP)
            for t in range(2):
                lane = slice(t * LN, (t + 1) * LN)
                depth = kmask[0, t, pl.ds(r, UP), :]
                below = [[ref[c * CHUNK + CHUNK, m, pl.ds(r, UP), lane] for m in range(2)] for ref in (tt, ts)]
                for kk in range(CHUNK - 1, -1, -1):
                    k = c * CHUNK + kk
                    level_no = k.astype(F32)
                    inv = jnp.where(depth > level_no + 1.0, table[2, k], jnp.where(depth > level_no, table[3, k], 0.0))
                    for f, ref in enumerate((tt, ts)):
                        for m in range(2):
                            below[f][m] = ref[k, m, pl.ds(r, UP), lane] * inv + table[1, k] * below[f][m]
                            ref[k, m, pl.ds(r, UP), lane] = below[f][m]
            return carry2
        lax.fori_loop(0, ROWS // UP, block, 0)
        for copy in stores_t(c):
            copy.start()
        return carry
    lax.fori_loop(0, NCH, upward, 0)

    for copy in small_out:
        copy.wait()

    def drain(c, carry):
        for copy in stores_v(c) + stores_t(c):
            copy.wait()
        return carry
    lax.fori_loop(0, NCH, drain, 0)


def solution(mesh):
    assert mesh.shape["col"] == 2 and mesh.shape["row"] == 4
    any_spec = pl.BlockSpec(memory_space=pl.ANY)
    vmem_spec = pl.BlockSpec(memory_space=pltpu.VMEM)
    smem_spec = pl.BlockSpec(memory_space=pltpu.SMEM)
    shape = lambda *dims: jax.ShapeDtypeStruct(dims, F32)
    dma = lambda *dims: pltpu.SemaphoreType.DMA(dims)
    vm = lambda *dims: pltpu.VMEM(dims, F32)
    visc = solve_table(VISC_NUMBER)
    diff = solve_table(DIFF_NUMBER)
    full = (LEVELS, 2, ROWS, 2 * LN)
    flat = (2, ROWS, 2 * LN)

    momentum = pl.pallas_call(
        momentum_kernel,
        name="momentum",
        out_shape=(shape(*full), shape(*full), shape(*flat), shape(*flat), shape(*flat), shape(2, 2, 2, ROWS, LN),
                   shape(3, 2, ROWS, LN), shape(NCH, PR, LN), shape(2, NCH, 2, 4, PAIRS, LN)),
        in_specs=[any_spec] * 8 + [vmem_spec, smem_spec, smem_spec],
        out_specs=(any_spec, any_spec, vmem_spec, vmem_spec, vmem_spec, vmem_spec, vmem_spec, any_spec, any_spec),
        scratch_shapes=[
            vm(4, LEVELS, 2, 2, PR, LN), vm(LEVELS + 1, 2, 2, ROWS, LN), vm(LEVELS + 1, 2, 2, ROWS, LN),
            vm(2, 2, ROWS, LN), vm(2, 2, ROWS, LN), vm(2, 2, 2, PR, LN), vm(2, 2, PR, LN), vm(2, PR, LN), vm(ROWS, LN),
            vm(2, 2, 2, ROWS, LN), vm(2, 2, 2, ROWS, LN), vm(2, ROWS, LN), vm(2, ROWS, LN),
            vm(NCH, ROWS, LN), vm(NCH, PR, LN), vm(2, NCH, 2, 4, PAIRS, LN), vm(2, NCH, 2, 4, PAIRS, LN),
            vm(8, 3, EXT, LN), vm(4, ROWS, LN), vm(4, EXT, LN), vm(4, 3, EXT, LN), vm(2, ROWS, LN), vm(2, EXT, LN),
            vm(3, EXT, LN), vm(3, EXT, LN), vm(3, EXT, LN), vm(3, EXT, LN), vm(3, EXT, LN), vm(3, EXT, LN), vm(3, EXT, LN),
            vm(2, 3, EXT, LN), vm(2, 3, EXT, LN), vm(2, 3, EXT, LN), vm(2, 3, EXT, LN), vm(2, 2, ROWS + 8, LN), vm(2, 3, ROWS + 8, LN),
            dma(NCH, 8), dma(8), dma(NCH, 5), dma(NCH, 5), dma(5), dma(5), dma(5), dma(5), dma(NCH, 4), dma(2),
        ],
        compiler_params=pltpu.CompilerParams(collective_id=0, has_side_effects=True, vmem_limit_bytes=67043328),
    )

    tracers = pl.pallas_call(
        tracer_kernel,
        name="tracers",
        out_shape=(shape(*flat), shape(*flat), shape(*flat), shape(*full), shape(*full), shape(*full), shape(*full)),
        in_specs=[any_spec] * 13 + [smem_spec],
        out_specs=(any_spec,) * 7,
        scratch_shapes=[
            vm(4, LEVELS, 2, 2, PR, LN), vm(LEVELS + 1, 2, ROWS, 2 * LN), vm(LEVELS + 1, 2, ROWS, 2 * LN), vm(2, 2, 2, ROWS, LN),
            vm(*full), vm(*full), vm(3, 2, ROWS, 2 * LN), vm(2, 2, 2, ROWS, LN), vm(3, 2, ROWS, LN),
            vm(NCH, PR, LN), vm(2, NCH, 2, 4, PAIRS, LN),
            dma(NCH, 10), dma(4), dma(NCH, 4), dma(3), dma(3),
        ],
        compiler_params=pltpu.CompilerParams(vmem_limit_bytes=67043328),
    )

    def local_step(vel_x, vel_y, pot_temp, salinity, surf_eta, trans_x, trans_y, col_depth, wet_levels, avg_weights):
        star_x, star_y, eta, tx, ty, corr, kmask, cols, rows = momentum(
            vel_x, vel_y, pot_temp, salinity, surf_eta, trans_x, trans_y, col_depth, wet_levels, avg_weights, jnp.asarray(visc))
        return tracers(vel_x, vel_y, pot_temp, salinity, star_x, star_y, eta, tx, ty, corr, kmask, cols, rows, jnp.asarray(diff))

    spec_3d = P(None, None, "row", "col")
    spec_2d = P(None, "row", "col")
    spec_map = P("row", "col")
    return jax.shard_map(local_step, mesh=mesh, in_specs=(spec_3d, spec_3d, spec_3d, spec_3d, spec_2d, spec_2d, spec_2d, spec_map, spec_map, P()),
                         out_specs=(spec_2d, spec_2d, spec_2d, spec_3d, spec_3d, spec_3d, spec_3d), check_vma=False)
```

```python
import functools
import numpy as np
import jax
import jax.numpy as jnp
from jax import lax
from jax.experimental import pallas as pl
from jax.experimental.pallas import tpu as pltpu
from jax.sharding import PartitionSpec as P

WAVE_COURANT = 0.4
THERM_EXP = 0.2
HALINE_CON = 0.15
PRESS_SCALE = 0.5
VISC_NUMBER = 1.0
DIFF_NUMBER = 0.5

LEVELS = 20
SUBS = 20
CHUNK = 4
NCH = LEVELS // CHUNK
PAIRS = 2 * CHUNK
ROWS = 128
LN = 128
PR = 144
EXT = 192
F32 = jnp.float32
PK = 64
UP = 32
MESH_ID = pl.DeviceIdType.MESH


def solve_table(strength):
    inner = np.zeros(LEVELS)
    last = np.zeros(LEVELS)
    inner[0] = 1.0 + strength
    last[0] = 1.0
    for k in range(1, LEVELS):
        inner[k] = 1.0 + 2.0 * strength - strength**2 / inner[k - 1]
        last[k] = 1.0 + strength - strength**2 / inner[k - 1]
    ratio = strength / inner
    before = np.concatenate([[0.0], ratio[:-1]])
    return np.stack([before, ratio, 1.0 / inner, 1.0 / last]).astype(np.float32)


def lanes(rows):
    return lax.broadcasted_iota(jnp.int32, (rows, LN), 1)


def east(tile, following):
    return pltpu.roll(jnp.where(lanes(tile.shape[0]) == 0, following, tile), LN - 1, 1)


def west(tile, previous):
    return pltpu.roll(jnp.where(lanes(tile.shape[0]) == LN - 1, previous, tile), 1, 1)


NEXT = (1, 2, 0)
PREV = (2, 0, 1)


def halo(packed, j):
    return pltpu.roll(packed, LN - 1 - 2 * j, 1)


def east_pair(first, second, edge):
    last = lanes(first.shape[0]) == LN - 1
    a, b = pltpu.roll(first, LN - 1, 1), pltpu.roll(second, LN - 1, 1)
    return jnp.where(last, b, a), jnp.where(last, edge, b)


def west_pair(first, second, edge):
    origin = lanes(first.shape[0]) == 0
    a, b = pltpu.roll(first, 1, 1), pltpu.roll(second, 1, 1)
    return jnp.where(origin, edge, a), jnp.where(origin, a, b)


def momentum_kernel(u_hbm, v_hbm, t_hbm, s_hbm, eta_hbm, tx_hbm, ty_hbm, h_hbm, kmt_hbm, weights, table,
                    us_hbm, vs_hbm, eta_out, tx_out, ty_out, corr_out, kmask_out, col_out, own_out, rows_out,
                    buf, tu, tv, cu, cv, pbufa, pbufb, pacc, phal, rhoc, gsum, xsum, kmask, kmt, vep, uwp, dup, txb, tyb, corr,
                    send_col, recv_col, send_row, recv_row,
                    xb, sp, rp, xf, sf, rf, hux, huy, ae, aw, an, as_, cc, ebufa, ebufb, dbuf, gbuf, eacc, bacc,
                    ld_sem, xl_sem, cs_sem, cr_sem, xs_sem, xr_sem, fs_sem, fr_sem, st_sem, ot_sem, av_sem):
    ku, kv = kmask.at[1], kmask.at[2]
    me_c = lax.axis_index("col")
    me_r = lax.axis_index("row")
    peer = 1 - me_c
    has_n = me_r < 3
    has_s = me_r > 0
    hbm = (u_hbm, v_hbm, t_hbm, s_hbm)

    def loads(c):
        out = []
        for f in range(4):
            for t in range(2):
                out.append(pltpu.make_async_copy(
                    hbm[f].at[pl.ds(c * CHUNK, CHUNK), :, :, pl.ds(t * LN, LN)],
                    buf.at[f, pl.ds(c * CHUNK, CHUNK), :, t, pl.ds(8, ROWS), :], ld_sem.at[c, f * 2 + t]))
        return out

    def map_loads():
        return [pltpu.make_async_copy(kmt_hbm, kmt, xl_sem.at[8])] + [
            pltpu.make_async_copy(h_hbm.at[:, pl.ds(t * LN, LN)], xb.at[1, t, pl.ds(32, ROWS), :], xl_sem.at[t]) for t in range(2)]

    def flow_loads():
        return [pltpu.make_async_copy(ref.at[:, :, pl.ds(t * LN, LN)], xb.at[pl.ds(2 + 2 * i, 2), t, pl.ds(32, ROWS), :], xl_sem.at[2 + 2 * i + t])
                for t in range(2) for i, ref in enumerate((eta_hbm, tx_hbm, ty_hbm))]

    for copy in map_loads() + loads(0) + loads(1) + loads(2) + flow_loads():
        copy.start()

    barrier = pltpu.get_barrier_semaphore()

    def greet(col, row):
        pl.semaphore_signal(barrier, inc=1, device_id={"col": col, "row": row}, device_id_type=MESH_ID)

    greet(peer, me_r)

    @pl.when(has_n)
    def _():
        greet(me_c, me_r + 1)
        greet(peer, me_r + 1)

    @pl.when(has_s)
    def _():
        greet(me_c, me_r - 1)
        greet(peer, me_r - 1)

    zrow = jnp.zeros((8, LN), F32)
    for ref, count in ((xb, 8), (xf, 4)):
        for f in range(count):
            for t in range(3):
                ref[f, t, 0:8, :] = zrow
                ref[f, t, EXT - 8:EXT, :] = zrow
    for ref, count in ((rp, 4), (rf, 2)):
        for f in range(count):
            ref[f, 0:8, :] = zrow
            ref[f, EXT - 8:EXT, :] = zrow

    def zero_side(side, lo):
        z24 = jnp.zeros((24, LN), F32)
        for f in range(8):
            for t in range(2):
                xb[f, t, lo:lo + 24, :] = z24
        for f in range(4):
            rp[f, lo:lo + 24, :] = z24
            for t in range(2):
                xf[f, t, lo:lo + 24, :] = z24
        for f in range(2):
            rf[f, lo:lo + 24, :] = z24
        for c in range(NCH):
            recv_col[c, 136 * side:136 * side + 8, :] = zrow
            for f in range(4):
                for t in range(2):
                    recv_row[side, c, t, f, :, :] = zrow

    @pl.when(me_r == 0)
    def _():
        zero_side(0, 8)

    @pl.when(me_r == 3)
    def _():
        zero_side(1, 160)

    def zero_planes(i, carry):
        r = pl.multiple_of(i * 16, 16)
        z = jnp.zeros((16, LN), F32)
        for m in range(2):
            for t in range(2):
                pacc[m, t, pl.ds(r, 16), :] = z
            phal[m, pl.ds(r, 16), :] = z
        return carry
    lax.fori_loop(0, PR // 16, zero_planes, 0)

    def zero_planes2(i, carry):
        r = pl.multiple_of(i * 16, 16)
        z = jnp.zeros((16, LN), F32)
        for m in range(2):
            for t in range(2):
                for f in range(2):
                    gsum[f, m, t, pl.ds(r, 16), :] = z
                    xsum[f, m, t, pl.ds(r, 16), :] = z
                for ref in (cu, cv):
                    ref[m, t, pl.ds(r, 16), :] = z
                for ref in (tu, tv):
                    ref[LEVELS, m, t, pl.ds(r, 16), :] = z
        return carry
    lax.fori_loop(0, ROWS // 16, zero_planes2, 0)

    for copy in map_loads():
        copy.wait()
    for t in range(2):
        for r in range(0, ROWS, 64):
            level_count = kmt[r:r + 64, t * LN:(t + 1) * LN].astype(F32)
            xb[0, t, 32 + r:96 + r, :] = level_count
            kmask[0, t, r:r + 64, :] = level_count

    @pl.when((me_r == 0) | (me_r == 3))
    def _():
        pl.semaphore_wait(barrier, 3)

    @pl.when((me_r != 0) & (me_r != 3))
    def _():
        pl.semaphore_wait(barrier, 5)

    def remote(src, dst, ssem, rsem, col, row):
        return pltpu.make_async_remote_copy(src_ref=src, dst_ref=dst, send_sem=ssem, recv_sem=rsem,
                                            device_id={"col": col, "row": row}, device_id_type=MESH_ID)

    def wide_rows(own, first, count, ssem, rsem, slot):
        fields = pl.ds(first, count)
        return ((remote(own.at[fields, pl.ds(0, 2), pl.ds(136, 24), :], own.at[fields, pl.ds(0, 2), pl.ds(8, 24), :],
                        ssem.at[slot], rsem.at[slot], me_c, me_r + 1),),
                (remote(own.at[fields, pl.ds(0, 2), pl.ds(32, 24), :], own.at[fields, pl.ds(0, 2), pl.ds(160, 24), :],
                        ssem.at[slot + 1], rsem.at[slot + 1], me_c, me_r - 1),))

    def wide_copies(own, first, count, packed, landing, ssem, rsem):
        side = remote(packed, landing.at[:, pl.ds(32, ROWS), :], ssem.at[0], rsem.at[0], peer, me_r)
        up, down = wide_rows(own, first, count, ssem, rsem, 1)
        up += (remote(packed.at[:, pl.ds(104, 24), :], landing.at[:, pl.ds(8, 24), :], ssem.at[3], rsem.at[3], peer, me_r + 1),)
        down += (remote(packed.at[:, pl.ds(0, 24), :], landing.at[:, pl.ds(160, 24), :], ssem.at[4], rsem.at[4], peer, me_r - 1),)
        return side, up, down

    def map_copies():
        return (None, *wide_rows(xb, 0, 2, xs_sem, xr_sem, 5))

    def flow_copies():
        return wide_copies(xb, 2, 6, sp, rp, xs_sem, xr_sem)

    def force_copies():
        return wide_copies(xf, 0, 4, sf, rf, fs_sem, fr_sem)

    def edge_copies(c):
        north, south = me_r + 1, me_r - 1
        side = remote(send_col.at[c], recv_col.at[c, pl.ds(8, ROWS), :], cs_sem.at[c, 0], cr_sem.at[c, 0], peer, me_r)
        up = (remote(send_row.at[0, c], recv_row.at[0, c], cs_sem.at[c, 1], cr_sem.at[c, 1], me_c, north),
              remote(send_col.at[c, pl.ds(ROWS - 8, 8), :], recv_col.at[c, pl.ds(0, 8), :], cs_sem.at[c, 2], cr_sem.at[c, 2], peer, north))
        down = (remote(send_row.at[1, c], recv_row.at[1, c], cs_sem.at[c, 3], cr_sem.at[c, 3], me_c, south),
                remote(send_col.at[c, pl.ds(0, 8), :], recv_col.at[c, pl.ds(8 + ROWS, 8), :], cs_sem.at[c, 4], cr_sem.at[c, 4], peer, south))
        return side, up, down

    def start_all(copies):
        side, up, down = copies
        if side is not None:
            side.start()

        @pl.when(has_n)
        def _():
            for copy in up:
                copy.start()

        @pl.when(has_s)
        def _():
            for copy in down:
                copy.start()

    def wait_recv_all(copies):
        side, up, down = copies
        if side is not None:
            side.wait_recv()

        @pl.when(has_s)
        def _():
            for copy in up:
                copy.wait_recv()

        @pl.when(has_n)
        def _():
            for copy in down:
                copy.wait_recv()

    def wait_send_all(copies):
        side, up, down = copies
        if side is not None:
            side.wait_send()

        @pl.when(has_n)
        def _():
            for copy in up:
                copy.wait_send()

        @pl.when(has_s)
        def _():
            for copy in down:
                copy.wait_send()

    start_all(map_copies())

    def pack_and_send(c, with_maps=False):
        for copy in loads(c):
            copy.wait()
        lane = lanes(PK)

        def block(i, carry):
            r = pl.multiple_of(i * PK, PK)
            pairs = [(f, c * CHUNK + kk, m) for f in range(4) for kk in range(CHUNK) for m in range(2)]
            column = [[buf[f, k, m, t, pl.ds(8 + r, PK), :] for f, k, m in pairs] for t in range(2)]
            if with_maps:
                for t in range(2):
                    column[t] += [xb[0, t, pl.ds(32 + r, PK), :], xb[1, t, pl.ds(32 + r, PK), :]]
            packed = jnp.zeros((PK, LN), F32)
            count = len(column[0])
            for i in range(count + 1):
                edge = jnp.where(lane == 0, column[0][min(i, count - 1)], column[1][max(i - 1, 0)])
                edge = pltpu.roll(edge, 2 * i, 1) if i else edge
                packed = jnp.where(lane >= 2 * i - 1, edge, packed) if i else edge
            send_col[c, pl.ds(r, PK), :] = packed
            return carry
        for kk in range(CHUNK):
            for m in range(2):
                jj = kk * 2 + m
                k = c * CHUNK + kk
                for side, row in ((0, 8 + ROWS - 1), (1, 8)):
                    for f in range(4):
                        for t in range(2):
                            send_row[side, c, t, f, jj:jj + 1, :] = buf[f, k, m, t, row:row + 1, :]
        lax.fori_loop(0, ROWS // PK, block, 0)
        start_all(edge_copies(c))

    pack_and_send(0, with_maps=True)
    pack_and_send(1)

    RHO_T = np.float32(-THERM_EXP * PRESS_SCALE / LEVELS / 2)
    RHO_S = np.float32(HALINE_CON * PRESS_SCALE / LEVELS / 2)
    BR = 64
    SB = 16

    def pressure_rows(k, slot, base, rows):
        for m in range(2):
            for t in range(2):
                half = RHO_T * buf[2, k, m, t, pl.ds(base, rows), :] + RHO_S * buf[3, k, m, t, pl.ds(base, rows), :]
                p = pacc[m, t, pl.ds(base, rows), :] + half
                slot[m, t, pl.ds(base, rows), :] = p
                pacc[m, t, pl.ds(base, rows), :] = p + half

    def shift_u(c, kk, m, base, rows):
        u = [buf[0, c * CHUNK + kk, m, t, pl.ds(base, rows), :] for t in range(2)]
        edge = halo(recv_col[c, pl.ds(base, rows), :], kk * 2 + m)
        ue, uw = east_pair(*u, edge), west_pair(*u, edge)
        for t in range(2):
            uwp[m, t, pl.ds(base, rows), :] = uw[t]
            dup[m, t, pl.ds(base, rows), :] = ue[t] - uw[t]

    def level(c, kk, now, later):
        k = c * CHUNK + kk
        pressure_rows(k, now, 8 + ROWS, 8)
        for m in range(2):
            shift_u(c, kk, m, 8, 8)
            ve = east_pair(*(buf[1, k, m, t, 0:8, :] for t in range(2)), halo(recv_col[c, 0:8, :], PAIRS + kk * 2 + m))
            for t in range(2):
                vep[m, t, 0:8, :] = ve[t]
        level_no = k.astype(F32)
        before = table[0, k]
        following = jnp.minimum(k + 1, LEVELS - 1)

        def block(i, carry):
            for q in range(0, BR, SB):
                piece(pl.multiple_of(i * BR + q, SB), pl.multiple_of(8 + i * BR + q, 8))
            return carry

        def piece(r, b):
            wet_x = [ku[t, pl.ds(r, SB), :] > level_no for t in range(2)]
            wet_y = [kv[t, pl.ds(r, SB), :] > level_no for t in range(2)]
            packed = recv_col[c, pl.ds(b, SB), :]
            packed_r = rhoc[pl.ds(r, SB), :]
            for m in range(2):
                j = kk * 2 + m
                shift_u(c, kk, m, pl.multiple_of(b + 8, 8), SB)
                half = halo(packed_r, j)
                p_edge = phal[m, pl.ds(r, SB), :] + half
                phal[m, pl.ds(r, SB), :] = p_edge + half
                v = [buf[1, k, m, t, pl.ds(b, SB), :] for t in range(2)]
                p = [now[m, t, pl.ds(b, SB), :] for t in range(2)]
                v_edge = halo(packed, PAIRS + j)
                ve, vw = east_pair(*v, v_edge), west_pair(*v, v_edge)
                pe = east_pair(*p, p_edge)
                for t in range(2):
                    vep[m, t, pl.ds(b, SB), :] = ve[t]
                    u = buf[0, k, m, t, pl.ds(b, SB), :]
                    un = buf[0, k, m, t, pl.ds(b + 1, SB), :]
                    us = buf[0, k, m, t, pl.ds(b - 1, SB), :]
                    vs = buf[1, k, m, t, pl.ds(b - 1, SB), :]
                    vn = buf[1, k, m, t, pl.ds(b + 1, SB), :]
                    pn = now[m, t, pl.ds(b + 1, SB), :]
                    w = (v[t] + vs) + (ve[t] + vep[m, t, pl.ds(b - 1, SB), :])
                    z = (u + un) + (uwp[m, t, pl.ds(b, SB), :] + uwp[m, t, pl.ds(b + 1, SB), :])
                    gu = (p[t] - pe[t]) - (0.5 * u) * dup[m, t, pl.ds(b, SB), :] - (0.125 * w) * (un - us)
                    gu = jnp.where(wet_x[t], gu, 0.0)
                    gsum[0, m, t, pl.ds(r, SB), :] += gu
                    new = u + gu + before * cu[m, t, pl.ds(r, SB), :]
                    cu[m, t, pl.ds(r, SB), :] = new
                    tu[k, m, t, pl.ds(r, SB), :] = new
                    gv = (p[t] - pn) - (0.125 * z) * (ve[t] - vw[t]) - (0.5 * v[t]) * (vn - vs)
                    gv = jnp.where(wet_y[t], gv, 0.0)
                    gsum[1, m, t, pl.ds(r, SB), :] += gv
                    new = v[t] + gv + before * cv[m, t, pl.ds(r, SB), :]
                    cv[m, t, pl.ds(r, SB), :] = new
                    tv[k, m, t, pl.ds(r, SB), :] = new
            pressure_rows(following, later, b, SB)
        lax.fori_loop(0, ROWS // BR, block, 0)

    def first_pressure(i, carry):
        pressure_rows(0, pbufa, pl.multiple_of(8 + i * 64, 8), 64)
        return carry
    lax.fori_loop(0, 2, first_pressure, 0)

    def chunk_step(c, carry):
        @pl.when(c + 3 < NCH)
        def _():
            for copy in loads(c + 3):
                copy.start()

        @pl.when(c + 2 < NCH)
        def _():
            pack_and_send(c + 2)

        @pl.when(c == 2)
        def _():
            pack_wide()

        wait_recv_all(edge_copies(c))

        @pl.when(c == 0)
        def _():
            face_maps()

        for kk in range(CHUNK):
            k = c * CHUNK + kk
            for m in range(2):
                jj = kk * 2 + m
                for side, row in ((0, 7), (1, 8 + ROWS)):
                    for f in range(4):
                        for t in range(2):
                            buf[f, k, m, t, row:row + 1, :] = recv_row[side, c, t, f, jj:jj + 1, :]
        packed = recv_col[c, 8:8 + ROWS, :]
        rhoc[...] = RHO_T * pltpu.roll(packed, LN - 4 * PAIRS, 1) + RHO_S * pltpu.roll(packed, LN - 6 * PAIRS, 1)

        def two_levels(h, carry2):
            level(c, 2 * h, pbufa, pbufb)
            level(c, 2 * h + 1, pbufb, pbufa)
            return carry2
        lax.fori_loop(0, CHUNK // 2, two_levels, 0)
        return carry

    def pack_wide():
        for copy in flow_loads():
            copy.wait()
        for pair in range(4):
            pack_pair(lambda t, r, p=pair: xb[2 * p, t, pl.ds(32 + r, 64), :],
                      lambda t, r, p=pair: xb[2 * p + 1, t, pl.ds(32 + r, 64), :], sp, pair, 64)
        start_all(flow_copies())

    def face_maps():
        wait_recv_all(map_copies())

        def maps(i, carry):
            r = pl.multiple_of(i * 64, 64)
            packed = recv_col[0, pl.ds(8 + r, 64), :]
            kt = [xb[0, t, pl.ds(32 + r, 64), :] for t in range(2)]
            ht = [xb[1, t, pl.ds(32 + r, 64), :] for t in range(2)]
            ke = east_pair(*kt, halo(packed, 4 * PAIRS))
            he = east_pair(*ht, halo(packed, 4 * PAIRS + 1))
            for t in range(2):
                kx = jnp.minimum(kt[t], ke[t])
                ky = jnp.minimum(kt[t], xb[0, t, pl.ds(33 + r, 64), :])
                ku[t, pl.ds(r, 64), :] = kx
                kv[t, pl.ds(r, 64), :] = ky
                hux[t, pl.ds(32 + r, 64), :] = jnp.where(kx > 0.0, 0.5 * (ht[t] + he[t]), 0.0)
                huy[t, pl.ds(32 + r, 64), :] = jnp.where(ky > 0.0, 0.5 * (ht[t] + xb[1, t, pl.ds(33 + r, 64), :]), 0.0)
            return carry
        lax.fori_loop(0, 2, maps, 0)

    def pack_pair(first, second, send, slot, rows):
        lane = lanes(rows)

        def block(i, carry):
            r = pl.multiple_of(i * rows, rows)
            a = jnp.where(lane < 64, first(0, r), first(1, r))
            b = jnp.where(lane < 64, second(0, r), second(1, r))
            outer = (lane < 32) | (lane >= 96)
            send[slot, pl.ds(r, rows), :] = jnp.where(outer, a, pltpu.roll(b, 64, 1))
            return carry
        lax.fori_loop(0, ROWS // rows, block, 0)

    lax.fori_loop(0, NCH, chunk_step, 0)

    packet_copies = [pltpu.make_async_copy(src, dst, ot_sem.at[i]) for i, (src, dst) in enumerate(
        ((recv_col, col_out), (recv_row, rows_out), (kmask, kmask_out), (send_col, own_out)))]
    for copy in packet_copies:
        copy.start()

    def forcing(i, carry):
        r = pl.multiple_of(i * 32, 32)
        for t in range(2):
            nx = jnp.maximum(ku[t, pl.ds(r, 32), :], 1.0)
            ny = jnp.maximum(kv[t, pl.ds(r, 32), :], 1.0)
            fx = hux[t, pl.ds(32 + r, 32), :] / nx / SUBS
            fy = huy[t, pl.ds(32 + r, 32), :] / ny / SUBS
            for m in range(2):
                xf[m, t, pl.ds(32 + r, 32), :] = fx * gsum[0, m, t, pl.ds(r, 32), :]
                xf[2 + m, t, pl.ds(32 + r, 32), :] = fy * gsum[1, m, t, pl.ds(r, 32), :]
        return carry
    lax.fori_loop(0, ROWS // 32, forcing, 0)
    for m in range(2):
        pack_pair(lambda t, r, m=m: xf[m, t, pl.ds(32 + r, 64), :],
                  lambda t, r, m=m: xf[2 + m, t, pl.ds(32 + r, 64), :], sf, m, 64)
    start_all(force_copies())

    def stores(c):
        out = []
        for f, (ref, dst) in enumerate(((tu, us_hbm), (tv, vs_hbm))):
            for t in range(2):
                out.append(pltpu.make_async_copy(ref.at[pl.ds(c * CHUNK, CHUNK), :, t, :, :],
                                                 dst.at[pl.ds(c * CHUNK, CHUNK), :, :, pl.ds(t * LN, LN)], st_sem.at[c, f * 2 + t]))
        return out

    def upward(step, carry):
        c = NCH - 1 - step

        def block(i, carry2):
            r = pl.multiple_of(i * UP, UP)
            for f, (ref, kp) in enumerate(((tu, ku), (tv, kv))):
                for t in range(2):
                    depth = kp[t, pl.ds(r, UP), :]
                    below = [ref[c * CHUNK + CHUNK, m, t, pl.ds(r, UP), :] for m in range(2)]
                    total = [xsum[f, m, t, pl.ds(r, UP), :] for m in range(2)]
                    for kk in range(CHUNK - 1, -1, -1):
                        k = c * CHUNK + kk
                        level_no = k.astype(F32)
                        inv = jnp.where(depth > level_no + 1.0, table[2, k], jnp.where(depth > level_no, table[3, k], 0.0))
                        for m in range(2):
                            below[m] = ref[k, m, t, pl.ds(r, UP), :] * inv + table[1, k] * below[m]
                            ref[k, m, t, pl.ds(r, UP), :] = below[m]
                            total[m] = total[m] + below[m]
                    for m in range(2):
                        xsum[f, m, t, pl.ds(r, UP), :] = total[m]
            return carry2
        lax.fori_loop(0, ROWS // UP, block, 0)
        for copy in stores(c):
            copy.start()
        return carry
    lax.fori_loop(0, NCH, upward, 0)

    wait_recv_all(flow_copies())

    def unpack_wide(i, carry):
        r = pl.multiple_of(i * 32, 32)
        for pair in range(4):
            tile = rp[pair, pl.ds(r, 32), :]
            xb[2 * pair, 2, pl.ds(r, 32), :] = tile
            xb[2 * pair + 1, 2, pl.ds(r, 32), :] = pltpu.roll(tile, 64, 1)
        return carry
    lax.fori_loop(0, EXT // 32, unpack_wide, 0)

    XR = 88

    def depths(i, carry):
        r = pl.multiple_of(8 + i * XR, 8)
        kt = [xb[0, t, pl.ds(r, XR), :] for t in range(3)]
        ht = [xb[1, t, pl.ds(r, XR), :] for t in range(3)]
        for t in range(3):
            kx = jnp.minimum(kt[t], east(kt[t], kt[NEXT[t]]))
            ky = jnp.minimum(kt[t], xb[0, t, pl.ds(r + 1, XR), :])
            hux[t, pl.ds(r, XR), :] = jnp.where(kx > 0.0, 0.5 * (ht[t] + east(ht[t], ht[NEXT[t]])), 0.0)
            huy[t, pl.ds(r, XR), :] = jnp.where(ky > 0.0, 0.5 * (ht[t] + xb[1, t, pl.ds(r + 1, XR), :]), 0.0)
            cc[t, pl.ds(r, XR), :] = jnp.where(kt[t] > 0.0, WAVE_COURANT, 0.0)
        return carry
    for t in range(3):
        for ref in (hux, huy):
            ref[t, 0:8, :] = zrow
        for ref in (ebufa, ebufb):
            for m in range(2):
                ref[m, t, 0:8, :] = zrow
                ref[m, t, EXT - 8:EXT, :] = zrow
    lax.fori_loop(0, 2, depths, 0)

    def coefficients(i, carry):
        r = pl.multiple_of(8 + i * XR, 8)
        hx = [hux[t, pl.ds(r, XR), :] for t in range(3)]
        for t in range(3):
            c0 = cc[t, pl.ds(r, XR), :]
            cw = WAVE_COURANT * c0
            ae[t, pl.ds(r, XR), :] = cw * hx[t]
            aw[t, pl.ds(r, XR), :] = cw * west(hx[t], hx[PREV[t]])
            an[t, pl.ds(r, XR), :] = cw * huy[t, pl.ds(r, XR), :]
            as_[t, pl.ds(r, XR), :] = cw * huy[t, pl.ds(r - 1, XR), :]
        return carry
    lax.fori_loop(0, 2, coefficients, 0)

    def first_subcycle(m, base, rows):
        tx = [xb[4 + m, t, pl.ds(base, rows), :] for t in range(3)]
        for t in range(3):
            c0 = cc[t, pl.ds(base, rows), :]
            ty = xb[6 + m, t, pl.ds(base, rows), :]
            div = tx[t] - west(tx[t], tx[PREV[t]]) + ty - xb[6 + m, t, pl.ds(base - 1, rows), :]
            change = -c0 * div
            dbuf[m, t, pl.ds(base, rows), :] = change
            eta = jnp.where(c0 > 0.0, xb[2 + m, t, pl.ds(base, rows), :], 0.0) + change
            ebufa[m, t, pl.ds(base, rows), :] = eta

    def first_block(i, carry):
        for m in range(2):
            first_subcycle(m, pl.multiple_of(8 + i * XR, 8), XR)
        return carry
    lax.fori_loop(0, 2, first_block, 0)

    wait_recv_all(force_copies())

    def unpack_force(i, carry):
        r = pl.multiple_of(i * 32, 32)
        for m in range(2):
            tile = rf[m, pl.ds(r, 32), :]
            xf[m, 2, pl.ds(r, 32), :] = tile
            xf[2 + m, 2, pl.ds(r, 32), :] = pltpu.roll(tile, 64, 1)
        return carry
    lax.fori_loop(0, EXT // 32, unpack_force, 0)

    def forcing_divergence(i, carry):
        r = pl.multiple_of(8 + i * XR, 8)
        for m in range(2):
            fx = [xf[m, t, pl.ds(r, XR), :] for t in range(3)]
            for t in range(3):
                div = fx[t] - west(fx[t], fx[PREV[t]]) + xf[2 + m, t, pl.ds(r, XR), :] - xf[2 + m, t, pl.ds(r - 1, XR), :]
                gbuf[m, t, pl.ds(r, XR), :] = cc[t, pl.ds(r, XR), :] * div
        return carry
    lax.fori_loop(0, 2, forcing_divergence, 0)

    whole = weights[SUBS - 1]
    moment = weights[SUBS - 1]
    for n in range(SUBS - 2, -1, -1):
        whole = whole + weights[n]
        moment = moment + whole

    def first_sums(i, carry):
        r = pl.multiple_of(i * 8, 8)
        for m in range(2):
            for t in range(3):
                eta = ebufa[m, t, pl.ds(32 + r, 8), :]
                bacc[m, t, pl.ds(r, 8), :] = whole * eta
                if t < 2:
                    eacc[m, t, pl.ds(r, 8), :] = weights[0] * eta
        return carry
    lax.fori_loop(0, 17, first_sums, 0)

    def subcycle(n, tail, lo, hi, old, new):
        tail = tail - weights[n - 2]
        weight = weights[n - 1]
        for r, end in ((lo, 96), (96, hi)):
            first = max(r, 32)
            for t in range(3):
                c_e, c_w = ae[t, r:end, :], aw[t, r:end, :]
                c_n, c_s = an[t, r:end, :], as_[t, r:end, :]
                for m in range(2):
                    e = old[m, t, r:end, :]
                    to_e = east(e, old[m, NEXT[t], r:end, :])
                    to_w = west(e, old[m, PREV[t], r:end, :])
                    to_n = old[m, t, r + 1:end + 1, :]
                    to_s = old[m, t, r - 1:end - 1, :]
                    d = dbuf[m, t, r:end, :] - gbuf[m, t, r:end, :]
                    d = d + (c_e * (to_e - e) + c_w * (to_w - e)) + (c_n * (to_n - e) + c_s * (to_s - e))
                    dbuf[m, t, r:end, :] = d
                    e = e + d
                    new[m, t, r:end, :] = e
                    last = min(end, 168)
                    bacc[m, t, first - 32:last - 32, :] += tail * e[first - r:last - r]
                    if t < 2:
                        last = min(end, 160)
                        eacc[m, t, first - 32:last - 32, :] += weight * e[first - r:last - r]
        return tail

    tail = subcycle(2, whole, 8, 184, ebufa, ebufb)
    for first_n, steps, lo, hi in ((3, 1, 8, 184), (5, 4, 16, 176), (13, 4, 24, 168)):
        def two_cycles(h, carry, first_n=first_n, lo=lo, hi=hi):
            n = first_n + 2 * h
            carry = subcycle(n, carry, lo, hi, ebufb, ebufa)
            return subcycle(n + 1, carry, lo, hi, ebufa, ebufb)
        tail = lax.fori_loop(0, steps, two_cycles, tail)

    eta_copies = [pltpu.make_async_copy(eacc.at[:, t, pl.ds(0, ROWS), :], eta_out.at[:, :, pl.ds(t * LN, LN)], ot_sem.at[4 + t]) for t in range(2)]
    for copy in eta_copies:
        copy.start()

    AV = 64

    def average_copies(i):
        r = pl.multiple_of(i * AV, AV)
        return [pltpu.make_async_copy(src, dst, av_sem.at[i, n]) for n, (src, dst) in enumerate((
            (txb.at[:, pl.ds(r, AV), :], tx_out.at[:, pl.ds(r, AV), :]), (tyb.at[:, pl.ds(r, AV), :], ty_out.at[:, pl.ds(r, AV), :]),
            (corr.at[:, :, :, pl.ds(r, AV), :], corr_out.at[:, :, :, pl.ds(r, AV), :])))]

    def averages(i, carry):
        for q in range(0, AV, 16):
            r = pl.multiple_of(i * AV + q, 16)
            g = pl.multiple_of(32 + i * AV + q, 16)
            for t in range(2):
                depth_x = hux[t, pl.ds(g, 16), :]
                depth_y = huy[t, pl.ds(g, 16), :]
                kx = ku[t, pl.ds(r, 16), :]
                ky = kv[t, pl.ds(r, 16), :]
                inv_x = 1.0 / (depth_x + jnp.where(kx > 0.0, 0.0, 1.0))
                inv_y = 1.0 / (depth_y + jnp.where(ky > 0.0, 0.0, 1.0))
                mean_x = 1.0 / jnp.maximum(kx, 1.0)
                mean_y = 1.0 / jnp.maximum(ky, 1.0)
                for m in range(2):
                    lane = slice(t * LN, (t + 1) * LN)
                    acc = bacc[m, t, pl.ds(r, 16), :]
                    tx = whole * xb[4 + m, t, pl.ds(g, 16), :] + moment * xf[m, t, pl.ds(g, 16), :] \
                        - WAVE_COURANT * depth_x * (east(acc, bacc[m, NEXT[t], pl.ds(r, 16), :]) - acc)
                    ty = whole * xb[6 + m, t, pl.ds(g, 16), :] + moment * xf[2 + m, t, pl.ds(g, 16), :] \
                        - WAVE_COURANT * depth_y * (bacc[m, t, pl.ds(r + 1, 16), :] - acc)
                    tx = jnp.where(kx > 0.0, tx, 0.0)
                    ty = jnp.where(ky > 0.0, ty, 0.0)
                    txb[m, pl.ds(r, 16), lane] = tx
                    tyb[m, pl.ds(r, 16), lane] = ty
                    corr[0, m, t, pl.ds(r, 16), :] = tx * inv_x - xsum[0, m, t, pl.ds(r, 16), :] * mean_x
                    corr[1, m, t, pl.ds(r, 16), :] = ty * inv_y - xsum[1, m, t, pl.ds(r, 16), :] * mean_y
        for copy in average_copies(i):
            copy.start()
        return carry
    lax.fori_loop(0, ROWS // AV, averages, 0)

    wait_send_all(map_copies())
    wait_send_all(flow_copies())
    wait_send_all(force_copies())
    for copy in packet_copies + eta_copies:
        copy.wait()
    for i in range(ROWS // AV):
        for copy in average_copies(i):
            copy.wait()

    def drain(c, carry):
        wait_send_all(edge_copies(c))
        for copy in stores(c):
            copy.wait()
        return carry
    lax.fori_loop(0, NCH, drain, 0)


def tracer_kernel(u_hbm, v_hbm, t_hbm, s_hbm, us_hbm, vs_hbm, eta_in, tx_in, ty_in, corr_in, kmask_in, col_in, own_in, rows_in, table,
                  eta_hbm, tx_hbm, ty_hbm, un_hbm, vn_hbm, tn_hbm, sn_hbm,
                  buf, tt, ts, ct, su, sv, small, corr, kmask, cols, own, rows, qcol, ld_sem, ed_sem, st_sem, in_sem, out_sem):
    hbm = (u_hbm, v_hbm, t_hbm, s_hbm)
    sources = (eta_in, tx_in, ty_in)
    sinks = (eta_hbm, tx_hbm, ty_hbm)

    def loads(c):
        out = []
        for f in range(4):
            for t in range(2):
                out.append(pltpu.make_async_copy(
                    hbm[f].at[pl.ds(c * CHUNK, CHUNK), :, :, pl.ds(t * LN, LN)],
                    buf.at[f, pl.ds(c * CHUNK, CHUNK), :, t, pl.ds(8, ROWS), :], ld_sem.at[c, f * 2 + t]))
        for f, (src, dst) in enumerate(((us_hbm, su), (vs_hbm, sv))):
            out.append(pltpu.make_async_copy(src.at[pl.ds(c * CHUNK, CHUNK)], dst.at[pl.ds(c * CHUNK, CHUNK)], ld_sem.at[c, 8 + f]))
        return out

    def stores_v(c):
        return [pltpu.make_async_copy(src.at[pl.ds(c * CHUNK, CHUNK)], dst.at[pl.ds(c * CHUNK, CHUNK)], st_sem.at[c, f])
                for f, (src, dst) in enumerate(((su, un_hbm), (sv, vn_hbm)))]

    def stores_t(c):
        return [pltpu.make_async_copy(src.at[pl.ds(c * CHUNK, CHUNK)], dst.at[pl.ds(c * CHUNK, CHUNK)], st_sem.at[c, 2 + f])
                for f, (src, dst) in enumerate(((tt, tn_hbm), (ts, sn_hbm)))]

    edges = [pltpu.make_async_copy(src, dst, ed_sem.at[i])
             for i, (src, dst) in enumerate(((col_in, cols), (rows_in, rows), (corr_in, corr), (kmask_in, kmask), (own_in, own)))]
    for copy in edges:
        copy.start()
    for c in range(NCH):
        for copy in loads(c):
            copy.start()
    small_in = [pltpu.make_async_copy(sources[i], small.at[i], in_sem.at[i]) for i in range(3)]
    small_out = [pltpu.make_async_copy(small.at[i], sinks[i], out_sem.at[i]) for i in range(3)]
    for copy in small_in:
        copy.start()

    def zero_planes(i, carry):
        r = pl.multiple_of(i * 16, 16)
        z = jnp.zeros((16, 2 * LN), F32)
        for f in range(2):
            for m in range(2):
                for t in range(2):
                    ct[f, m, t, pl.ds(r, 16), :] = z[:, :LN]
        for m in range(2):
            for ref in (tt, ts):
                ref[LEVELS, m, pl.ds(r, 16), :] = z
        return carry
    lax.fori_loop(0, ROWS // 16, zero_planes, 0)
    for copy in edges:
        copy.wait()

    BR = 128
    SB = 16

    def level(c, kk):
        k = c * CHUNK + kk
        level_no = k.astype(F32)
        before = table[0, k]

        def block(i, carry):
            for q in range(0, BR, SB):
                piece(pl.multiple_of(i * BR + q, SB), pl.multiple_of(8 + i * BR + q, 8))
            return carry

        def piece(r, b):
            wet = [kmask[0, t, pl.ds(r, SB), :] > level_no for t in range(2)]
            packed = qcol[pl.ds(r, SB), :]
            for m in range(2):
                j = kk * 2 + m
                u = [buf[0, k, m, t, pl.ds(b, SB), :] for t in range(2)]
                v = [buf[1, k, m, t, pl.ds(b, SB), :] for t in range(2)]
                vs = [buf[1, k, m, t, pl.ds(b - 1, SB), :] for t in range(2)]
                for f, ref in ((2, tt), (3, ts)):
                    q = [buf[f, k, m, t, pl.ds(b, SB), :] for t in range(2)]
                    edge = halo(packed, f * PAIRS + j)
                    qe = east_pair(*q, edge)
                    fx = [u[t] * (q[t] + qe[t]) for t in range(2)]
                    fw = west_pair(*fx, edge)
                    for t in range(2):
                        lane = slice(t * LN, (t + 1) * LN)
                        fy = v[t] * (q[t] + buf[f, k, m, t, pl.ds(b + 1, SB), :])
                        fs = vs[t] * (q[t] + buf[f, k, m, t, pl.ds(b - 1, SB), :])
                        adv = q[t] - 0.5 * ((fx[t] - fw[t]) + (fy - fs))
                        adv = jnp.where(wet[t], adv, 0.0)
                        new = adv + before * ct[f - 2, m, t, pl.ds(r, SB), :]
                        ct[f - 2, m, t, pl.ds(r, SB), :] = new
                        ref[k, m, pl.ds(r, SB), lane] = new
            for t in range(2):
                lane = slice(t * LN, (t + 1) * LN)
                wet_x = kmask[1, t, pl.ds(r, SB), :] > level_no
                wet_y = kmask[2, t, pl.ds(r, SB), :] > level_no
                for m in range(2):
                    su[k, m, pl.ds(r, SB), lane] = jnp.where(wet_x, su[k, m, pl.ds(r, SB), lane] + corr[0, m, t, pl.ds(r, SB), :], 0.0)
                    sv[k, m, pl.ds(r, SB), lane] = jnp.where(wet_y, sv[k, m, pl.ds(r, SB), lane] + corr[1, m, t, pl.ds(r, SB), :], 0.0)
        lax.fori_loop(0, ROWS // BR, block, 0)

    def chunk_step(c, carry):
        for copy in loads(c):
            copy.wait()
        for kk in range(CHUNK):
            k = c * CHUNK + kk
            for m in range(2):
                jj = kk * 2 + m
                for f in (1, 2, 3):
                    for t in range(2):
                        buf[f, k, m, t, 7:8, :] = rows[0, c, t, f, jj:jj + 1, :]
                for f in (2, 3):
                    for t in range(2):
                        buf[f, k, m, t, 8 + ROWS:9 + ROWS, :] = rows[1, c, t, f, jj:jj + 1, :]

        packed = cols[c, 8:8 + ROWS, :]
        lane = lanes(ROWS)
        west_u = jnp.where(lane < 6 * PAIRS, pltpu.roll(packed, 4 * PAIRS, 1), pltpu.roll(packed, 6 * PAIRS, 1))
        flux = west_u * (packed + pltpu.roll(own[c], 1, 1))
        qcol[...] = jnp.where(lax.rem(lane, 2) == 1, flux, packed)

        def one_level(kk, carry2):
            level(c, kk)
            return carry2
        lax.fori_loop(0, CHUNK, one_level, 0)
        for copy in stores_v(c):
            copy.start()
        return carry
    lax.fori_loop(0, NCH, chunk_step, 0)

    for copy in small_in:
        copy.wait()
    for copy in small_out:
        copy.start()

    def upward(step, carry):
        c = NCH - 1 - step

        def block(i, carry2):
            r = pl.multiple_of(i * UP, UP)
            for t in range(2):
                lane = slice(t * LN, (t + 1) * LN)
                depth = kmask[0, t, pl.ds(r, UP), :]
                below = [[ref[c * CHUNK + CHUNK, m, pl.ds(r, UP), lane] for m in range(2)] for ref in (tt, ts)]
                for kk in range(CHUNK - 1, -1, -1):
                    k = c * CHUNK + kk
                    level_no = k.astype(F32)
                    inv = jnp.where(depth > level_no + 1.0, table[2, k], jnp.where(depth > level_no, table[3, k], 0.0))
                    for f, ref in enumerate((tt, ts)):
                        for m in range(2):
                            below[f][m] = ref[k, m, pl.ds(r, UP), lane] * inv + table[1, k] * below[f][m]
                            ref[k, m, pl.ds(r, UP), lane] = below[f][m]
            return carry2
        lax.fori_loop(0, ROWS // UP, block, 0)
        for copy in stores_t(c):
            copy.start()
        return carry
    lax.fori_loop(0, NCH, upward, 0)

    for copy in small_out:
        copy.wait()

    def drain(c, carry):
        for copy in stores_v(c) + stores_t(c):
            copy.wait()
        return carry
    lax.fori_loop(0, NCH, drain, 0)


def solution(mesh):
    assert mesh.shape["col"] == 2 and mesh.shape["row"] == 4
    any_spec = pl.BlockSpec(memory_space=pl.ANY)
    vmem_spec = pl.BlockSpec(memory_space=pltpu.VMEM)
    smem_spec = pl.BlockSpec(memory_space=pltpu.SMEM)
    shape = lambda *dims: jax.ShapeDtypeStruct(dims, F32)
    dma = lambda *dims: pltpu.SemaphoreType.DMA(dims)
    vm = lambda *dims: pltpu.VMEM(dims, F32)
    visc = solve_table(VISC_NUMBER)
    diff = solve_table(DIFF_NUMBER)
    full = (LEVELS, 2, ROWS, 2 * LN)
    flat = (2, ROWS, 2 * LN)

    momentum = pl.pallas_call(
        momentum_kernel,
        name="momentum",
        out_shape=(shape(*full), shape(*full), shape(*flat), shape(*flat), shape(*flat), shape(2, 2, 2, ROWS, LN),
                   shape(3, 2, ROWS, LN), shape(NCH, PR, LN), shape(NCH, ROWS, LN), shape(2, NCH, 2, 4, PAIRS, LN)),
        in_specs=[any_spec] * 9 + [smem_spec, smem_spec],
        out_specs=(any_spec,) * 10,
        scratch_shapes=[
            vm(4, LEVELS, 2, 2, PR, LN), vm(LEVELS + 1, 2, 2, ROWS, LN), vm(LEVELS + 1, 2, 2, ROWS, LN),
            vm(2, 2, ROWS, LN), vm(2, 2, ROWS, LN), vm(2, 2, PR, LN), vm(2, 2, PR, LN), vm(2, 2, PR, LN), vm(2, PR, LN), vm(ROWS, LN),
            vm(2, 2, 2, ROWS, LN), vm(2, 2, 2, ROWS, LN), vm(3, 2, ROWS, LN), pltpu.VMEM((ROWS, 2 * LN), jnp.int32),
            vm(2, 2, PR, LN), vm(2, 2, PR, LN), vm(2, 2, PR, LN), vm(*flat), vm(*flat), vm(2, 2, 2, ROWS, LN),
            vm(NCH, ROWS, LN), vm(NCH, PR, LN), vm(2, NCH, 2, 4, PAIRS, LN), vm(2, NCH, 2, 4, PAIRS, LN),
            vm(8, 3, EXT, LN), vm(4, ROWS, LN), vm(4, EXT, LN), vm(4, 3, EXT, LN), vm(2, ROWS, LN), vm(2, EXT, LN),
            vm(3, EXT, LN), vm(3, EXT, LN), vm(3, EXT, LN), vm(3, EXT, LN), vm(3, EXT, LN), vm(3, EXT, LN), vm(3, EXT, LN),
            vm(2, 3, EXT, LN), vm(2, 3, EXT, LN), vm(2, 3, EXT, LN), vm(2, 3, EXT, LN), vm(2, 2, ROWS + 8, LN), vm(2, 3, ROWS + 8, LN),
            dma(NCH, 8), dma(9), dma(NCH, 5), dma(NCH, 5), dma(7), dma(7), dma(5), dma(5), dma(NCH, 4), dma(6), dma(2, 3),
        ],
        compiler_params=pltpu.CompilerParams(collective_id=0, has_side_effects=True, vmem_limit_bytes=67043328),
    )

    tracers = pl.pallas_call(
        tracer_kernel,
        name="tracers",
        out_shape=(shape(*flat), shape(*flat), shape(*flat), shape(*full), shape(*full), shape(*full), shape(*full)),
        in_specs=[any_spec] * 14 + [smem_spec],
        out_specs=(any_spec,) * 7,
        scratch_shapes=[
            vm(4, LEVELS, 2, 2, PR, LN), vm(LEVELS + 1, 2, ROWS, 2 * LN), vm(LEVELS + 1, 2, ROWS, 2 * LN), vm(2, 2, 2, ROWS, LN),
            vm(*full), vm(*full), vm(3, 2, ROWS, 2 * LN), vm(2, 2, 2, ROWS, LN), vm(3, 2, ROWS, LN),
            vm(NCH, PR, LN), vm(NCH, ROWS, LN), vm(2, NCH, 2, 4, PAIRS, LN), vm(ROWS, LN),
            dma(NCH, 10), dma(5), dma(NCH, 4), dma(3), dma(3),
        ],
        compiler_params=pltpu.CompilerParams(vmem_limit_bytes=67043328),
    )

    def local_step(vel_x, vel_y, pot_temp, salinity, surf_eta, trans_x, trans_y, col_depth, wet_levels, avg_weights):
        star_x, star_y, eta, tx, ty, corr, kmask, cols, own, rows = momentum(
            vel_x, vel_y, pot_temp, salinity, surf_eta, trans_x, trans_y, col_depth, wet_levels, avg_weights, jnp.asarray(visc))
        return tracers(vel_x, vel_y, pot_temp, salinity, star_x, star_y, eta, tx, ty, corr, kmask, cols, own, rows, jnp.asarray(diff))

    spec_3d = P(None, None, "row", "col")
    spec_2d = P(None, "row", "col")
    spec_map = P("row", "col")
    return jax.shard_map(local_step, mesh=mesh, in_specs=(spec_3d, spec_3d, spec_3d, spec_3d, spec_2d, spec_2d, spec_2d, spec_map, spec_map, P()),
                         out_specs=(spec_2d, spec_2d, spec_2d, spec_3d, spec_3d, spec_3d, spec_3d), check_vma=False)
```

```python
import functools
import numpy as np
import jax
import jax.numpy as jnp
from jax import lax
from jax.experimental import pallas as pl
from jax.experimental.pallas import tpu as pltpu
from jax.sharding import PartitionSpec as P

WAVE_COURANT = 0.4
THERM_EXP = 0.2
HALINE_CON = 0.15
PRESS_SCALE = 0.5
VISC_NUMBER = 1.0
DIFF_NUMBER = 0.5

LEVELS = 20
SUBS = 20
CHUNK = 4
NCH = LEVELS // CHUNK
PAIRS = 2 * CHUNK
ROWS = 128
LN = 128
PR = 144
EXT = 192
F32 = jnp.float32
PK = 64
UP = 32
MESH_ID = pl.DeviceIdType.MESH


def solve_table(strength):
    inner = np.zeros(LEVELS)
    last = np.zeros(LEVELS)
    inner[0] = 1.0 + strength
    last[0] = 1.0
    for k in range(1, LEVELS):
        inner[k] = 1.0 + 2.0 * strength - strength**2 / inner[k - 1]
        last[k] = 1.0 + strength - strength**2 / inner[k - 1]
    ratio = strength / inner
    before = np.concatenate([[0.0], ratio[:-1]])
    return np.stack([before, ratio, 1.0 / inner, 1.0 / last]).astype(np.float32)


def lanes(rows):
    return lax.broadcasted_iota(jnp.int32, (rows, LN), 1)


def east(tile, following):
    return pltpu.roll(jnp.where(lanes(tile.shape[0]) == 0, following, tile), LN - 1, 1)


def west(tile, previous):
    return pltpu.roll(jnp.where(lanes(tile.shape[0]) == LN - 1, previous, tile), 1, 1)


NEXT = (1, 2, 0)
PREV = (2, 0, 1)


def halo(packed, j):
    return pltpu.roll(packed, LN - 1 - 2 * j, 1)


def east_pair(first, second, edge):
    last = lanes(first.shape[0]) == LN - 1
    a, b = pltpu.roll(first, LN - 1, 1), pltpu.roll(second, LN - 1, 1)
    return jnp.where(last, b, a), jnp.where(last, edge, b)


def west_pair(first, second, edge):
    origin = lanes(first.shape[0]) == 0
    a, b = pltpu.roll(first, 1, 1), pltpu.roll(second, 1, 1)
    return jnp.where(origin, edge, a), jnp.where(origin, a, b)


def momentum_kernel(u_hbm, v_hbm, t_hbm, s_hbm, eta_hbm, tx_hbm, ty_hbm, h_hbm, kmt_hbm, weights, table,
                    us_hbm, vs_hbm, eta_out, tx_out, ty_out, corr_out, kmask_out, col_out, rows_out,
                    buf, tu, tv, cu, cv, pbufa, pbufb, pacc, phal, rhoc, gsum, xsum, kmask, kmt, vep, uwp, dup, txb, tyb, corr,
                    send_col, recv_col, send_row, recv_row,
                    xb, sp, rp, xf, sf, rf, hux, huy, ae, aw, an, as_, cc, ebufa, ebufb, dbuf, gbuf, eacc, bacc,
                    ld_sem, xl_sem, cs_sem, cr_sem, xs_sem, xr_sem, fs_sem, fr_sem, st_sem, ot_sem, av_sem):
    ku, kv = kmask.at[1], kmask.at[2]
    me_c = lax.axis_index("col")
    me_r = lax.axis_index("row")
    peer = 1 - me_c
    has_n = me_r < 3
    has_s = me_r > 0
    hbm = (u_hbm, v_hbm, t_hbm, s_hbm)

    def loads(c):
        out = []
        for f in range(4):
            for t in range(2):
                out.append(pltpu.make_async_copy(
                    hbm[f].at[pl.ds(c * CHUNK, CHUNK), :, :, pl.ds(t * LN, LN)],
                    buf.at[f, pl.ds(c * CHUNK, CHUNK), :, t, pl.ds(8, ROWS), :], ld_sem.at[c, f * 2 + t]))
        return out

    def map_loads():
        return [pltpu.make_async_copy(kmt_hbm, kmt, xl_sem.at[8])] + [
            pltpu.make_async_copy(h_hbm.at[:, pl.ds(t * LN, LN)], xb.at[1, t, pl.ds(32, ROWS), :], xl_sem.at[t]) for t in range(2)]

    def flow_loads():
        return [pltpu.make_async_copy(ref.at[:, :, pl.ds(t * LN, LN)], xb.at[pl.ds(2 + 2 * i, 2), t, pl.ds(32, ROWS), :], xl_sem.at[2 + 2 * i + t])
                for t in range(2) for i, ref in enumerate((eta_hbm, tx_hbm, ty_hbm))]

    for copy in map_loads() + loads(0) + loads(1) + loads(2) + flow_loads():
        copy.start()

    barrier = pltpu.get_barrier_semaphore()

    def greet(col, row):
        pl.semaphore_signal(barrier, inc=1, device_id={"col": col, "row": row}, device_id_type=MESH_ID)

    greet(peer, me_r)

    @pl.when(has_n)
    def _():
        greet(me_c, me_r + 1)
        greet(peer, me_r + 1)

    @pl.when(has_s)
    def _():
        greet(me_c, me_r - 1)
        greet(peer, me_r - 1)

    zrow = jnp.zeros((8, LN), F32)
    for ref, count in ((xb, 8), (xf, 4)):
        for f in range(count):
            for t in range(3):
                ref[f, t, 0:8, :] = zrow
                ref[f, t, EXT - 8:EXT, :] = zrow
    for ref, count in ((rp, 4), (rf, 2)):
        for f in range(count):
            ref[f, 0:8, :] = zrow
            ref[f, EXT - 8:EXT, :] = zrow

    def zero_side(side, lo):
        z24 = jnp.zeros((24, LN), F32)
        for f in range(8):
            for t in range(2):
                xb[f, t, lo:lo + 24, :] = z24
        for f in range(4):
            rp[f, lo:lo + 24, :] = z24
            for t in range(2):
                xf[f, t, lo:lo + 24, :] = z24
        for f in range(2):
            rf[f, lo:lo + 24, :] = z24
        for c in range(NCH):
            recv_col[c, 136 * side:136 * side + 8, :] = zrow
            for f in range(4):
                for t in range(2):
                    recv_row[side, c, t, f, :, :] = zrow

    @pl.when(me_r == 0)
    def _():
        zero_side(0, 8)

    @pl.when(me_r == 3)
    def _():
        zero_side(1, 160)

    def zero_planes(i, carry):
        r = pl.multiple_of(i * 16, 16)
        z = jnp.zeros((16, LN), F32)
        for m in range(2):
            for t in range(2):
                pacc[m, t, pl.ds(r, 16), :] = z
            phal[m, pl.ds(r, 16), :] = z
        return carry
    lax.fori_loop(0, PR // 16, zero_planes, 0)

    def zero_planes2(i, carry):
        r = pl.multiple_of(i * 16, 16)
        z = jnp.zeros((16, LN), F32)
        for m in range(2):
            for t in range(2):
                for f in range(2):
                    gsum[f, m, t, pl.ds(r, 16), :] = z
                    xsum[f, m, t, pl.ds(r, 16), :] = z
                for ref in (cu, cv):
                    ref[m, t, pl.ds(r, 16), :] = z
                for ref in (tu, tv):
                    ref[LEVELS, m, t, pl.ds(r, 16), :] = z
        return carry
    lax.fori_loop(0, ROWS // 16, zero_planes2, 0)

    for copy in map_loads():
        copy.wait()
    for t in range(2):
        for r in range(0, ROWS, 64):
            level_count = kmt[r:r + 64, t * LN:(t + 1) * LN].astype(F32)
            xb[0, t, 32 + r:96 + r, :] = level_count
            kmask[0, t, r:r + 64, :] = level_count

    @pl.when((me_r == 0) | (me_r == 3))
    def _():
        pl.semaphore_wait(barrier, 3)

    @pl.when((me_r != 0) & (me_r != 3))
    def _():
        pl.semaphore_wait(barrier, 5)

    def remote(src, dst, ssem, rsem, col, row):
        return pltpu.make_async_remote_copy(src_ref=src, dst_ref=dst, send_sem=ssem, recv_sem=rsem,
                                            device_id={"col": col, "row": row}, device_id_type=MESH_ID)

    def wide_rows(own, first, count, ssem, rsem, slot):
        fields = pl.ds(first, count)
        return ((remote(own.at[fields, pl.ds(0, 2), pl.ds(136, 24), :], own.at[fields, pl.ds(0, 2), pl.ds(8, 24), :],
                        ssem.at[slot], rsem.at[slot], me_c, me_r + 1),),
                (remote(own.at[fields, pl.ds(0, 2), pl.ds(32, 24), :], own.at[fields, pl.ds(0, 2), pl.ds(160, 24), :],
                        ssem.at[slot + 1], rsem.at[slot + 1], me_c, me_r - 1),))

    def wide_copies(own, first, count, packed, landing, ssem, rsem):
        side = remote(packed, landing.at[:, pl.ds(32, ROWS), :], ssem.at[0], rsem.at[0], peer, me_r)
        up, down = wide_rows(own, first, count, ssem, rsem, 1)
        up += (remote(packed.at[:, pl.ds(104, 24), :], landing.at[:, pl.ds(8, 24), :], ssem.at[3], rsem.at[3], peer, me_r + 1),)
        down += (remote(packed.at[:, pl.ds(0, 24), :], landing.at[:, pl.ds(160, 24), :], ssem.at[4], rsem.at[4], peer, me_r - 1),)
        return side, up, down

    def map_copies():
        return (None, *wide_rows(xb, 0, 2, xs_sem, xr_sem, 5))

    def flow_copies():
        return wide_copies(xb, 2, 6, sp, rp, xs_sem, xr_sem)

    def force_copies():
        return wide_copies(xf, 0, 4, sf, rf, fs_sem, fr_sem)

    def edge_copies(c):
        north, south = me_r + 1, me_r - 1
        side = remote(send_col.at[c], recv_col.at[c, pl.ds(8, ROWS), :], cs_sem.at[c, 0], cr_sem.at[c, 0], peer, me_r)
        up = (remote(send_row.at[0, c], recv_row.at[0, c], cs_sem.at[c, 1], cr_sem.at[c, 1], me_c, north),
              remote(send_col.at[c, pl.ds(ROWS - 8, 8), :], recv_col.at[c, pl.ds(0, 8), :], cs_sem.at[c, 2], cr_sem.at[c, 2], peer, north))
        down = (remote(send_row.at[1, c], recv_row.at[1, c], cs_sem.at[c, 3], cr_sem.at[c, 3], me_c, south),
                remote(send_col.at[c, pl.ds(0, 8), :], recv_col.at[c, pl.ds(8 + ROWS, 8), :], cs_sem.at[c, 4], cr_sem.at[c, 4], peer, south))
        return side, up, down

    def start_all(copies):
        side, up, down = copies
        if side is not None:
            side.start()

        @pl.when(has_n)
        def _():
            for copy in up:
                copy.start()

        @pl.when(has_s)
        def _():
            for copy in down:
                copy.start()

    def wait_recv_all(copies):
        side, up, down = copies
        if side is not None:
            side.wait_recv()

        @pl.when(has_s)
        def _():
            for copy in up:
                copy.wait_recv()

        @pl.when(has_n)
        def _():
            for copy in down:
                copy.wait_recv()

    def wait_send_all(copies):
        side, up, down = copies
        if side is not None:
            side.wait_send()

        @pl.when(has_n)
        def _():
            for copy in up:
                copy.wait_send()

        @pl.when(has_s)
        def _():
            for copy in down:
                copy.wait_send()

    start_all(map_copies())

    def pack_and_send(c, with_maps=False):
        for copy in loads(c):
            copy.wait()
        lane = lanes(PK)

        def block(i, carry):
            r = pl.multiple_of(i * PK, PK)
            pairs = [(f, c * CHUNK + kk, m) for f in range(4) for kk in range(CHUNK) for m in range(2)]
            column = [[buf[f, k, m, t, pl.ds(8 + r, PK), :] for f, k, m in pairs] for t in range(2)]
            if with_maps:
                for t in range(2):
                    column[t] += [xb[0, t, pl.ds(32 + r, PK), :], xb[1, t, pl.ds(32 + r, PK), :]]
            packed = jnp.zeros((PK, LN), F32)
            count = len(column[0])
            for i in range(count + 1):
                edge = jnp.where(lane == 0, column[0][min(i, count - 1)], column[1][max(i - 1, 0)])
                edge = pltpu.roll(edge, 2 * i, 1) if i else edge
                packed = jnp.where(lane >= 2 * i - 1, edge, packed) if i else edge
            send_col[c, pl.ds(r, PK), :] = packed
            return carry
        for kk in range(CHUNK):
            for m in range(2):
                jj = kk * 2 + m
                k = c * CHUNK + kk
                for side, row in ((0, 8 + ROWS - 1), (1, 8)):
                    for f in range(4):
                        for t in range(2):
                            send_row[side, c, t, f, jj:jj + 1, :] = buf[f, k, m, t, row:row + 1, :]
        lax.fori_loop(0, ROWS // PK, block, 0)
        start_all(edge_copies(c))

    pack_and_send(0, with_maps=True)
    pack_and_send(1)

    RHO_T = np.float32(-THERM_EXP * PRESS_SCALE / LEVELS / 2)
    RHO_S = np.float32(HALINE_CON * PRESS_SCALE / LEVELS / 2)
    BR = 128
    SB = 16

    def pressure_rows(k, slot, base, rows):
        for m in range(2):
            for t in range(2):
                half = RHO_T * buf[2, k, m, t, pl.ds(base, rows), :] + RHO_S * buf[3, k, m, t, pl.ds(base, rows), :]
                p = pacc[m, t, pl.ds(base, rows), :] + half
                slot[m, t, pl.ds(base, rows), :] = p
                pacc[m, t, pl.ds(base, rows), :] = p + half

    def shift_u(c, kk, m, base, rows):
        u = [buf[0, c * CHUNK + kk, m, t, pl.ds(base, rows), :] for t in range(2)]
        edge = halo(recv_col[c, pl.ds(base, rows), :], kk * 2 + m)
        ue, uw = east_pair(*u, edge), west_pair(*u, edge)
        for t in range(2):
            uwp[m, t, pl.ds(base, rows), :] = uw[t]
            dup[m, t, pl.ds(base, rows), :] = ue[t] - uw[t]

    def level(c, kk, now, later):
        k = c * CHUNK + kk
        pressure_rows(k, now, 8 + ROWS, 8)
        for m in range(2):
            shift_u(c, kk, m, 8, 8)
            ve = east_pair(*(buf[1, k, m, t, 0:8, :] for t in range(2)), halo(recv_col[c, 0:8, :], PAIRS + kk * 2 + m))
            for t in range(2):
                vep[m, t, 0:8, :] = ve[t]
        level_no = k.astype(F32)
        before = table[0, k]
        following = jnp.minimum(k + 1, LEVELS - 1)

        def block(i, carry):
            for q in range(0, BR, SB):
                piece(pl.multiple_of(i * BR + q, SB), pl.multiple_of(8 + i * BR + q, 8))
            return carry

        def piece(r, b):
            wet_x = [ku[t, pl.ds(r, SB), :] > level_no for t in range(2)]
            wet_y = [kv[t, pl.ds(r, SB), :] > level_no for t in range(2)]
            packed = recv_col[c, pl.ds(b, SB), :]
            packed_r = rhoc[pl.ds(r, SB), :]
            for m in range(2):
                j = kk * 2 + m
                shift_u(c, kk, m, pl.multiple_of(b + 8, 8), SB)
                half = halo(packed_r, j)
                p_edge = phal[m, pl.ds(r, SB), :] + half
                phal[m, pl.ds(r, SB), :] = p_edge + half
                v = [buf[1, k, m, t, pl.ds(b, SB), :] for t in range(2)]
                p = [now[m, t, pl.ds(b, SB), :] for t in range(2)]
                v_edge = halo(packed, PAIRS + j)
                ve, vw = east_pair(*v, v_edge), west_pair(*v, v_edge)
                pe = east_pair(*p, p_edge)
                for t in range(2):
                    vep[m, t, pl.ds(b, SB), :] = ve[t]
                    u = buf[0, k, m, t, pl.ds(b, SB), :]
                    un = buf[0, k, m, t, pl.ds(b + 1, SB), :]
                    us = buf[0, k, m, t, pl.ds(b - 1, SB), :]
                    vs = buf[1, k, m, t, pl.ds(b - 1, SB), :]
                    vn = buf[1, k, m, t, pl.ds(b + 1, SB), :]
                    pn = now[m, t, pl.ds(b + 1, SB), :]
                    w = (v[t] + vs) + (ve[t] + vep[m, t, pl.ds(b - 1, SB), :])
                    z = (u + un) + (uwp[m, t, pl.ds(b, SB), :] + uwp[m, t, pl.ds(b + 1, SB), :])
                    gu = (p[t] - pe[t]) - (0.5 * u) * dup[m, t, pl.ds(b, SB), :] - (0.125 * w) * (un - us)
                    gu = jnp.where(wet_x[t], gu, 0.0)
                    gsum[0, m, t, pl.ds(r, SB), :] += gu
                    new = u + gu + before * cu[m, t, pl.ds(r, SB), :]
                    cu[m, t, pl.ds(r, SB), :] = new
                    tu[k, m, t, pl.ds(r, SB), :] = new
                    gv = (p[t] - pn) - (0.125 * z) * (ve[t] - vw[t]) - (0.5 * v[t]) * (vn - vs)
                    gv = jnp.where(wet_y[t], gv, 0.0)
                    gsum[1, m, t, pl.ds(r, SB), :] += gv
                    new = v[t] + gv + before * cv[m, t, pl.ds(r, SB), :]
                    cv[m, t, pl.ds(r, SB), :] = new
                    tv[k, m, t, pl.ds(r, SB), :] = new
            pressure_rows(following, later, b, SB)
        lax.fori_loop(0, ROWS // BR, block, 0)

    def first_pressure(i, carry):
        pressure_rows(0, pbufa, pl.multiple_of(8 + i * 64, 8), 64)
        return carry
    lax.fori_loop(0, 2, first_pressure, 0)

    def chunk_step(c, carry):
        @pl.when(c + 3 < NCH)
        def _():
            for copy in loads(c + 3):
                copy.start()

        @pl.when(c + 2 < NCH)
        def _():
            pack_and_send(c + 2)

        @pl.when(c == 2)
        def _():
            pack_wide()

        wait_recv_all(edge_copies(c))

        @pl.when(c == 0)
        def _():
            face_maps()

        for kk in range(CHUNK):
            k = c * CHUNK + kk
            for m in range(2):
                jj = kk * 2 + m
                for side, row in ((0, 7), (1, 8 + ROWS)):
                    for f in range(4):
                        for t in range(2):
                            buf[f, k, m, t, row:row + 1, :] = recv_row[side, c, t, f, jj:jj + 1, :]
        packed = recv_col[c, 8:8 + ROWS, :]
        rhoc[...] = RHO_T * pltpu.roll(packed, LN - 4 * PAIRS, 1) + RHO_S * pltpu.roll(packed, LN - 6 * PAIRS, 1)

        def two_levels(h, carry2):
            level(c, 2 * h, pbufa, pbufb)
            level(c, 2 * h + 1, pbufb, pbufa)
            return carry2
        lax.fori_loop(0, CHUNK // 2, two_levels, 0)
        return carry

    def pack_wide():
        for copy in flow_loads():
            copy.wait()
        for pair in range(4):
            pack_pair(lambda t, r, p=pair: xb[2 * p, t, pl.ds(32 + r, 64), :],
                      lambda t, r, p=pair: xb[2 * p + 1, t, pl.ds(32 + r, 64), :], sp, pair, 64)
        start_all(flow_copies())

    def face_maps():
        wait_recv_all(map_copies())

        def maps(i, carry):
            r = pl.multiple_of(i * 64, 64)
            packed = recv_col[0, pl.ds(8 + r, 64), :]
            kt = [xb[0, t, pl.ds(32 + r, 64), :] for t in range(2)]
            ht = [xb[1, t, pl.ds(32 + r, 64), :] for t in range(2)]
            ke = east_pair(*kt, halo(packed, 4 * PAIRS))
            he = east_pair(*ht, halo(packed, 4 * PAIRS + 1))
            for t in range(2):
                kx = jnp.minimum(kt[t], ke[t])
                ky = jnp.minimum(kt[t], xb[0, t, pl.ds(33 + r, 64), :])
                ku[t, pl.ds(r, 64), :] = kx
                kv[t, pl.ds(r, 64), :] = ky
                hux[t, pl.ds(32 + r, 64), :] = jnp.where(kx > 0.0, 0.5 * (ht[t] + he[t]), 0.0)
                huy[t, pl.ds(32 + r, 64), :] = jnp.where(ky > 0.0, 0.5 * (ht[t] + xb[1, t, pl.ds(33 + r, 64), :]), 0.0)
            return carry
        lax.fori_loop(0, 2, maps, 0)

    def pack_pair(first, second, send, slot, rows):
        lane = lanes(rows)

        def block(i, carry):
            r = pl.multiple_of(i * rows, rows)
            a = jnp.where(lane < 64, first(0, r), first(1, r))
            b = jnp.where(lane < 64, second(0, r), second(1, r))
            outer = (lane < 32) | (lane >= 96)
            send[slot, pl.ds(r, rows), :] = jnp.where(outer, a, pltpu.roll(b, 64, 1))
            return carry
        lax.fori_loop(0, ROWS // rows, block, 0)

    lax.fori_loop(0, NCH, chunk_step, 0)

    packet_copies = [pltpu.make_async_copy(src, dst, ot_sem.at[i]) for i, (src, dst) in enumerate(
        ((recv_col, col_out), (recv_row, rows_out), (kmask, kmask_out)))]
    for copy in packet_copies:
        copy.start()

    def forcing(i, carry):
        r = pl.multiple_of(i * 32, 32)
        for t in range(2):
            nx = jnp.maximum(ku[t, pl.ds(r, 32), :], 1.0)
            ny = jnp.maximum(kv[t, pl.ds(r, 32), :], 1.0)
            fx = hux[t, pl.ds(32 + r, 32), :] / nx / SUBS
            fy = huy[t, pl.ds(32 + r, 32), :] / ny / SUBS
            for m in range(2):
                xf[m, t, pl.ds(32 + r, 32), :] = fx * gsum[0, m, t, pl.ds(r, 32), :]
                xf[2 + m, t, pl.ds(32 + r, 32), :] = fy * gsum[1, m, t, pl.ds(r, 32), :]
        return carry
    lax.fori_loop(0, ROWS // 32, forcing, 0)
    for m in range(2):
        pack_pair(lambda t, r, m=m: xf[m, t, pl.ds(32 + r, 64), :],
                  lambda t, r, m=m: xf[2 + m, t, pl.ds(32 + r, 64), :], sf, m, 64)
    start_all(force_copies())

    def stores(c):
        out = []
        for f, (ref, dst) in enumerate(((tu, us_hbm), (tv, vs_hbm))):
            for t in range(2):
                out.append(pltpu.make_async_copy(ref.at[pl.ds(c * CHUNK, CHUNK), :, t, :, :],
                                                 dst.at[pl.ds(c * CHUNK, CHUNK), :, :, pl.ds(t * LN, LN)], st_sem.at[c, f * 2 + t]))
        return out

    def upward(step, carry):
        c = NCH - 1 - step

        def block(i, carry2):
            r = pl.multiple_of(i * UP, UP)
            for f, (ref, kp) in enumerate(((tu, ku), (tv, kv))):
                for t in range(2):
                    depth = kp[t, pl.ds(r, UP), :]
                    below = [ref[c * CHUNK + CHUNK, m, t, pl.ds(r, UP), :] for m in range(2)]
                    total = [xsum[f, m, t, pl.ds(r, UP), :] for m in range(2)]
                    for kk in range(CHUNK - 1, -1, -1):
                        k = c * CHUNK + kk
                        level_no = k.astype(F32)
                        inv = jnp.where(depth > level_no + 1.0, table[2, k], jnp.where(depth > level_no, table[3, k], 0.0))
                        for m in range(2):
                            below[m] = ref[k, m, t, pl.ds(r, UP), :] * inv + table[1, k] * below[m]
                            ref[k, m, t, pl.ds(r, UP), :] = below[m]
                            total[m] = total[m] + below[m]
                    for m in range(2):
                        xsum[f, m, t, pl.ds(r, UP), :] = total[m]
            return carry2
        lax.fori_loop(0, ROWS // UP, block, 0)
        for copy in stores(c):
            copy.start()
        return carry
    lax.fori_loop(0, NCH, upward, 0)

    wait_recv_all(flow_copies())

    def unpack_wide(i, carry):
        r = pl.multiple_of(i * 32, 32)
        for pair in range(4):
            tile = rp[pair, pl.ds(r, 32), :]
            xb[2 * pair, 2, pl.ds(r, 32), :] = tile
            xb[2 * pair + 1, 2, pl.ds(r, 32), :] = pltpu.roll(tile, 64, 1)
        return carry
    lax.fori_loop(0, EXT // 32, unpack_wide, 0)

    XR = 88

    def depths(i, carry):
        r = pl.multiple_of(8 + i * XR, 8)
        kt = [xb[0, t, pl.ds(r, XR), :] for t in range(3)]
        ht = [xb[1, t, pl.ds(r, XR), :] for t in range(3)]
        for t in range(3):
            kx = jnp.minimum(kt[t], east(kt[t], kt[NEXT[t]]))
            ky = jnp.minimum(kt[t], xb[0, t, pl.ds(r + 1, XR), :])
            hux[t, pl.ds(r, XR), :] = jnp.where(kx > 0.0, 0.5 * (ht[t] + east(ht[t], ht[NEXT[t]])), 0.0)
            huy[t, pl.ds(r, XR), :] = jnp.where(ky > 0.0, 0.5 * (ht[t] + xb[1, t, pl.ds(r + 1, XR), :]), 0.0)
            cc[t, pl.ds(r, XR), :] = jnp.where(kt[t] > 0.0, WAVE_COURANT, 0.0)
        return carry
    for t in range(3):
        for ref in (hux, huy):
            ref[t, 0:8, :] = zrow
        for ref in (ebufa, ebufb):
            for m in range(2):
                ref[m, t, 0:8, :] = zrow
                ref[m, t, EXT - 8:EXT, :] = zrow
    lax.fori_loop(0, 2, depths, 0)

    def coefficients(i, carry):
        r = pl.multiple_of(8 + i * XR, 8)
        hx = [hux[t, pl.ds(r, XR), :] for t in range(3)]
        for t in range(3):
            c0 = cc[t, pl.ds(r, XR), :]
            cw = WAVE_COURANT * c0
            ae[t, pl.ds(r, XR), :] = cw * hx[t]
            aw[t, pl.ds(r, XR), :] = cw * west(hx[t], hx[PREV[t]])
            an[t, pl.ds(r, XR), :] = cw * huy[t, pl.ds(r, XR), :]
            as_[t, pl.ds(r, XR), :] = cw * huy[t, pl.ds(r - 1, XR), :]
        return carry
    lax.fori_loop(0, 2, coefficients, 0)

    def first_subcycle(m, base, rows):
        tx = [xb[4 + m, t, pl.ds(base, rows), :] for t in range(3)]
        for t in range(3):
            c0 = cc[t, pl.ds(base, rows), :]
            ty = xb[6 + m, t, pl.ds(base, rows), :]
            div = tx[t] - west(tx[t], tx[PREV[t]]) + ty - xb[6 + m, t, pl.ds(base - 1, rows), :]
            change = -c0 * div
            dbuf[m, t, pl.ds(base, rows), :] = change
            eta = jnp.where(c0 > 0.0, xb[2 + m, t, pl.ds(base, rows), :], 0.0) + change
            ebufa[m, t, pl.ds(base, rows), :] = eta

    def first_block(i, carry):
        for m in range(2):
            first_subcycle(m, pl.multiple_of(8 + i * XR, 8), XR)
        return carry
    lax.fori_loop(0, 2, first_block, 0)

    wait_recv_all(force_copies())

    def unpack_force(i, carry):
        r = pl.multiple_of(i * 32, 32)
        for m in range(2):
            tile = rf[m, pl.ds(r, 32), :]
            xf[m, 2, pl.ds(r, 32), :] = tile
            xf[2 + m, 2, pl.ds(r, 32), :] = pltpu.roll(tile, 64, 1)
        return carry
    lax.fori_loop(0, EXT // 32, unpack_force, 0)

    def forcing_divergence(i, carry):
        r = pl.multiple_of(8 + i * XR, 8)
        for m in range(2):
            fx = [xf[m, t, pl.ds(r, XR), :] for t in range(3)]
            for t in range(3):
                div = fx[t] - west(fx[t], fx[PREV[t]]) + xf[2 + m, t, pl.ds(r, XR), :] - xf[2 + m, t, pl.ds(r - 1, XR), :]
                gbuf[m, t, pl.ds(r, XR), :] = cc[t, pl.ds(r, XR), :] * div
        return carry
    lax.fori_loop(0, 2, forcing_divergence, 0)

    whole = weights[SUBS - 1]
    moment = weights[SUBS - 1]
    for n in range(SUBS - 2, -1, -1):
        whole = whole + weights[n]
        moment = moment + whole

    def first_sums(i, carry):
        r = pl.multiple_of(i * 8, 8)
        for m in range(2):
            for t in range(3):
                eta = ebufa[m, t, pl.ds(32 + r, 8), :]
                bacc[m, t, pl.ds(r, 8), :] = whole * eta
                if t < 2:
                    eacc[m, t, pl.ds(r, 8), :] = weights[0] * eta
        return carry
    lax.fori_loop(0, 17, first_sums, 0)

    def subcycle(n, tail, lo, hi, old, new):
        tail = tail - weights[n - 2]
        weight = weights[n - 1]
        for r, end in ((lo, 96), (96, hi)):
            first = max(r, 32)
            for t in range(3):
                c_e, c_w = ae[t, r:end, :], aw[t, r:end, :]
                c_n, c_s = an[t, r:end, :], as_[t, r:end, :]
                for m in range(2):
                    e = old[m, t, r:end, :]
                    to_e = east(e, old[m, NEXT[t], r:end, :])
                    to_w = west(e, old[m, PREV[t], r:end, :])
                    to_n = old[m, t, r + 1:end + 1, :]
                    to_s = old[m, t, r - 1:end - 1, :]
                    d = dbuf[m, t, r:end, :] - gbuf[m, t, r:end, :]
                    d = d + (c_e * (to_e - e) + c_w * (to_w - e)) + (c_n * (to_n - e) + c_s * (to_s - e))
                    dbuf[m, t, r:end, :] = d
                    e = e + d
                    new[m, t, r:end, :] = e
                    last = min(end, 168)
                    bacc[m, t, first - 32:last - 32, :] += tail * e[first - r:last - r]
                    if t < 2:
                        last = min(end, 160)
                        eacc[m, t, first - 32:last - 32, :] += weight * e[first - r:last - r]
        return tail

    tail = subcycle(2, whole, 8, 184, ebufa, ebufb)
    for first_n, steps, lo, hi in ((3, 1, 8, 184), (5, 4, 16, 176), (13, 4, 24, 168)):
        def two_cycles(h, carry, first_n=first_n, lo=lo, hi=hi):
            n = first_n + 2 * h
            carry = subcycle(n, carry, lo, hi, ebufb, ebufa)
            return subcycle(n + 1, carry, lo, hi, ebufa, ebufb)
        tail = lax.fori_loop(0, steps, two_cycles, tail)

    eta_copies = [pltpu.make_async_copy(eacc.at[:, t, pl.ds(0, ROWS), :], eta_out.at[:, :, pl.ds(t * LN, LN)], ot_sem.at[4 + t]) for t in range(2)]
    for copy in eta_copies:
        copy.start()

    AV = 64

    def average_copies(i):
        r = pl.multiple_of(i * AV, AV)
        return [pltpu.make_async_copy(src, dst, av_sem.at[i, n]) for n, (src, dst) in enumerate((
            (txb.at[:, pl.ds(r, AV), :], tx_out.at[:, pl.ds(r, AV), :]), (tyb.at[:, pl.ds(r, AV), :], ty_out.at[:, pl.ds(r, AV), :]),
            (corr.at[:, :, :, pl.ds(r, AV), :], corr_out.at[:, :, :, pl.ds(r, AV), :])))]

    def averages(i, carry):
        for q in range(0, AV, 16):
            r = pl.multiple_of(i * AV + q, 16)
            g = pl.multiple_of(32 + i * AV + q, 16)
            for t in range(2):
                depth_x = hux[t, pl.ds(g, 16), :]
                depth_y = huy[t, pl.ds(g, 16), :]
                kx = ku[t, pl.ds(r, 16), :]
                ky = kv[t, pl.ds(r, 16), :]
                inv_x = 1.0 / (depth_x + jnp.where(kx > 0.0, 0.0, 1.0))
                inv_y = 1.0 / (depth_y + jnp.where(ky > 0.0, 0.0, 1.0))
                mean_x = 1.0 / jnp.maximum(kx, 1.0)
                mean_y = 1.0 / jnp.maximum(ky, 1.0)
                for m in range(2):
                    lane = slice(t * LN, (t + 1) * LN)
                    acc = bacc[m, t, pl.ds(r, 16), :]
                    tx = whole * xb[4 + m, t, pl.ds(g, 16), :] + moment * xf[m, t, pl.ds(g, 16), :] \
                        - WAVE_COURANT * depth_x * (east(acc, bacc[m, NEXT[t], pl.ds(r, 16), :]) - acc)
                    ty = whole * xb[6 + m, t, pl.ds(g, 16), :] + moment * xf[2 + m, t, pl.ds(g, 16), :] \
                        - WAVE_COURANT * depth_y * (bacc[m, t, pl.ds(r + 1, 16), :] - acc)
                    tx = jnp.where(kx > 0.0, tx, 0.0)
                    ty = jnp.where(ky > 0.0, ty, 0.0)
                    txb[m, pl.ds(r, 16), lane] = tx
                    tyb[m, pl.ds(r, 16), lane] = ty
                    corr[0, m, t, pl.ds(r, 16), :] = tx * inv_x - xsum[0, m, t, pl.ds(r, 16), :] * mean_x
                    corr[1, m, t, pl.ds(r, 16), :] = ty * inv_y - xsum[1, m, t, pl.ds(r, 16), :] * mean_y
        for copy in average_copies(i):
            copy.start()
        return carry
    lax.fori_loop(0, ROWS // AV, averages, 0)

    wait_send_all(map_copies())
    wait_send_all(flow_copies())
    wait_send_all(force_copies())
    for copy in packet_copies + eta_copies:
        copy.wait()
    for i in range(ROWS // AV):
        for copy in average_copies(i):
            copy.wait()

    def drain(c, carry):
        wait_send_all(edge_copies(c))
        for copy in stores(c):
            copy.wait()
        return carry
    lax.fori_loop(0, NCH, drain, 0)


def tracer_kernel(u_hbm, v_hbm, t_hbm, s_hbm, us_hbm, vs_hbm, eta_in, tx_in, ty_in, corr_in, kmask_in, col_in, rows_in, table,
                  eta_hbm, tx_hbm, ty_hbm, un_hbm, vn_hbm, tn_hbm, sn_hbm,
                  buf, tt, ts, ct, su, sv, small, corr, kmask, cols, rows, ld_sem, ed_sem, st_sem, in_sem, out_sem):
    hbm = (u_hbm, v_hbm, t_hbm, s_hbm)
    sources = (eta_in, tx_in, ty_in)
    sinks = (eta_hbm, tx_hbm, ty_hbm)

    def loads(c):
        out = []
        for f in range(4):
            for t in range(2):
                out.append(pltpu.make_async_copy(
                    hbm[f].at[pl.ds(c * CHUNK, CHUNK), :, :, pl.ds(t * LN, LN)],
                    buf.at[f, pl.ds(c * CHUNK, CHUNK), :, t, pl.ds(8, ROWS), :], ld_sem.at[c, f * 2 + t]))
        for f, (src, dst) in enumerate(((us_hbm, su), (vs_hbm, sv))):
            out.append(pltpu.make_async_copy(src.at[pl.ds(c * CHUNK, CHUNK)], dst.at[pl.ds(c * CHUNK, CHUNK)], ld_sem.at[c, 8 + f]))
        return out

    def stores_v(c):
        return [pltpu.make_async_copy(src.at[pl.ds(c * CHUNK, CHUNK)], dst.at[pl.ds(c * CHUNK, CHUNK)], st_sem.at[c, f])
                for f, (src, dst) in enumerate(((su, un_hbm), (sv, vn_hbm)))]

    def stores_t(c):
        return [pltpu.make_async_copy(src.at[pl.ds(c * CHUNK, CHUNK)], dst.at[pl.ds(c * CHUNK, CHUNK)], st_sem.at[c, 2 + f])
                for f, (src, dst) in enumerate(((tt, tn_hbm), (ts, sn_hbm)))]

    edges = [pltpu.make_async_copy(src, dst, ed_sem.at[i])
             for i, (src, dst) in enumerate(((col_in, cols), (rows_in, rows), (corr_in, corr), (kmask_in, kmask)))]
    for copy in edges:
        copy.start()
    for c in range(NCH):
        for copy in loads(c):
            copy.start()
    small_in = [pltpu.make_async_copy(sources[i], small.at[i], in_sem.at[i]) for i in range(3)]
    small_out = [pltpu.make_async_copy(small.at[i], sinks[i], out_sem.at[i]) for i in range(3)]
    for copy in small_in:
        copy.start()

    def zero_planes(i, carry):
        r = pl.multiple_of(i * 16, 16)
        z = jnp.zeros((16, 2 * LN), F32)
        for f in range(2):
            for m in range(2):
                for t in range(2):
                    ct[f, m, t, pl.ds(r, 16), :] = z[:, :LN]
        for m in range(2):
            for ref in (tt, ts):
                ref[LEVELS, m, pl.ds(r, 16), :] = z
        return carry
    lax.fori_loop(0, ROWS // 16, zero_planes, 0)
    for copy in edges:
        copy.wait()

    BR = 128
    SB = 16

    def level(c, kk):
        k = c * CHUNK + kk
        level_no = k.astype(F32)
        before = table[0, k]

        def block(i, carry):
            for q in range(0, BR, SB):
                piece(pl.multiple_of(i * BR + q, SB), pl.multiple_of(8 + i * BR + q, 8))
            return carry

        def piece(r, b):
            wet = [kmask[0, t, pl.ds(r, SB), :] > level_no for t in range(2)]
            packed = cols[c, pl.ds(b, SB), :]
            for m in range(2):
                j = kk * 2 + m
                u = [buf[0, k, m, t, pl.ds(b, SB), :] for t in range(2)]
                v = [buf[1, k, m, t, pl.ds(b, SB), :] for t in range(2)]
                vs = [buf[1, k, m, t, pl.ds(b - 1, SB), :] for t in range(2)]
                uw = west_pair(*u, halo(packed, j))
                for f, ref in ((2, tt), (3, ts)):
                    q = [buf[f, k, m, t, pl.ds(b, SB), :] for t in range(2)]
                    edge = halo(packed, f * PAIRS + j)
                    qe, qw = east_pair(*q, edge), west_pair(*q, edge)
                    for t in range(2):
                        lane = slice(t * LN, (t + 1) * LN)
                        fy = v[t] * (q[t] + buf[f, k, m, t, pl.ds(b + 1, SB), :])
                        fs = vs[t] * (q[t] + buf[f, k, m, t, pl.ds(b - 1, SB), :])
                        adv = q[t] - 0.5 * ((u[t] * (q[t] + qe[t]) - uw[t] * (q[t] + qw[t])) + (fy - fs))
                        adv = jnp.where(wet[t], adv, 0.0)
                        new = adv + before * ct[f - 2, m, t, pl.ds(r, SB), :]
                        ct[f - 2, m, t, pl.ds(r, SB), :] = new
                        ref[k, m, pl.ds(r, SB), lane] = new
            for t in range(2):
                lane = slice(t * LN, (t + 1) * LN)
                wet_x = kmask[1, t, pl.ds(r, SB), :] > level_no
                wet_y = kmask[2, t, pl.ds(r, SB), :] > level_no
                for m in range(2):
                    su[k, m, pl.ds(r, SB), lane] = jnp.where(wet_x, su[k, m, pl.ds(r, SB), lane] + corr[0, m, t, pl.ds(r, SB), :], 0.0)
                    sv[k, m, pl.ds(r, SB), lane] = jnp.where(wet_y, sv[k, m, pl.ds(r, SB), lane] + corr[1, m, t, pl.ds(r, SB), :], 0.0)
        lax.fori_loop(0, ROWS // BR, block, 0)

    def chunk_step(c, carry):
        for copy in loads(c):
            copy.wait()
        for kk in range(CHUNK):
            k = c * CHUNK + kk
            for m in range(2):
                jj = kk * 2 + m
                for f in (1, 2, 3):
                    for t in range(2):
                        buf[f, k, m, t, 7:8, :] = rows[0, c, t, f, jj:jj + 1, :]
                for f in (2, 3):
                    for t in range(2):
                        buf[f, k, m, t, 8 + ROWS:9 + ROWS, :] = rows[1, c, t, f, jj:jj + 1, :]

        def one_level(kk, carry2):
            level(c, kk)
            return carry2
        lax.fori_loop(0, CHUNK, one_level, 0)
        for copy in stores_v(c):
            copy.start()
        return carry
    lax.fori_loop(0, NCH, chunk_step, 0)

    for copy in small_in:
        copy.wait()
    for copy in small_out:
        copy.start()

    def upward(step, carry):
        c = NCH - 1 - step

        def block(i, carry2):
            r = pl.multiple_of(i * UP, UP)
            for t in range(2):
                lane = slice(t * LN, (t + 1) * LN)
                depth = kmask[0, t, pl.ds(r, UP), :]
                below = [[ref[c * CHUNK + CHUNK, m, pl.ds(r, UP), lane] for m in range(2)] for ref in (tt, ts)]
                for kk in range(CHUNK - 1, -1, -1):
                    k = c * CHUNK + kk
                    level_no = k.astype(F32)
                    inv = jnp.where(depth > level_no + 1.0, table[2, k], jnp.where(depth > level_no, table[3, k], 0.0))
                    for f, ref in enumerate((tt, ts)):
                        for m in range(2):
                            below[f][m] = ref[k, m, pl.ds(r, UP), lane] * inv + table[1, k] * below[f][m]
                            ref[k, m, pl.ds(r, UP), lane] = below[f][m]
            return carry2
        lax.fori_loop(0, ROWS // UP, block, 0)
        for copy in stores_t(c):
            copy.start()
        return carry
    lax.fori_loop(0, NCH, upward, 0)

    for copy in small_out:
        copy.wait()

    def drain(c, carry):
        for copy in stores_v(c) + stores_t(c):
            copy.wait()
        return carry
    lax.fori_loop(0, NCH, drain, 0)


def solution(mesh):
    assert mesh.shape["col"] == 2 and mesh.shape["row"] == 4
    any_spec = pl.BlockSpec(memory_space=pl.ANY)
    vmem_spec = pl.BlockSpec(memory_space=pltpu.VMEM)
    smem_spec = pl.BlockSpec(memory_space=pltpu.SMEM)
    shape = lambda *dims: jax.ShapeDtypeStruct(dims, F32)
    dma = lambda *dims: pltpu.SemaphoreType.DMA(dims)
    vm = lambda *dims: pltpu.VMEM(dims, F32)
    visc = solve_table(VISC_NUMBER)
    diff = solve_table(DIFF_NUMBER)
    full = (LEVELS, 2, ROWS, 2 * LN)
    flat = (2, ROWS, 2 * LN)

    momentum = pl.pallas_call(
        momentum_kernel,
        name="momentum",
        out_shape=(shape(*full), shape(*full), shape(*flat), shape(*flat), shape(*flat), shape(2, 2, 2, ROWS, LN),
                   shape(3, 2, ROWS, LN), shape(NCH, PR, LN), shape(2, NCH, 2, 4, PAIRS, LN)),
        in_specs=[any_spec] * 9 + [smem_spec, smem_spec],
        out_specs=(any_spec,) * 9,
        scratch_shapes=[
            vm(4, LEVELS, 2, 2, PR, LN), vm(LEVELS + 1, 2, 2, ROWS, LN), vm(LEVELS + 1, 2, 2, ROWS, LN),
            vm(2, 2, ROWS, LN), vm(2, 2, ROWS, LN), vm(2, 2, PR, LN), vm(2, 2, PR, LN), vm(2, 2, PR, LN), vm(2, PR, LN), vm(ROWS, LN),
            vm(2, 2, 2, ROWS, LN), vm(2, 2, 2, ROWS, LN), vm(3, 2, ROWS, LN), pltpu.VMEM((ROWS, 2 * LN), jnp.int32),
            vm(2, 2, PR, LN), vm(2, 2, PR, LN), vm(2, 2, PR, LN), vm(*flat), vm(*flat), vm(2, 2, 2, ROWS, LN),
            vm(NCH, ROWS, LN), vm(NCH, PR, LN), vm(2, NCH, 2, 4, PAIRS, LN), vm(2, NCH, 2, 4, PAIRS, LN),
            vm(8, 3, EXT, LN), vm(4, ROWS, LN), vm(4, EXT, LN), vm(4, 3, EXT, LN), vm(2, ROWS, LN), vm(2, EXT, LN),
            vm(3, EXT, LN), vm(3, EXT, LN), vm(3, EXT, LN), vm(3, EXT, LN), vm(3, EXT, LN), vm(3, EXT, LN), vm(3, EXT, LN),
            vm(2, 3, EXT, LN), vm(2, 3, EXT, LN), vm(2, 3, EXT, LN), vm(2, 3, EXT, LN), vm(2, 2, ROWS + 8, LN), vm(2, 3, ROWS + 8, LN),
            dma(NCH, 8), dma(9), dma(NCH, 5), dma(NCH, 5), dma(7), dma(7), dma(5), dma(5), dma(NCH, 4), dma(6), dma(2, 3),
        ],
        compiler_params=pltpu.CompilerParams(collective_id=0, has_side_effects=True, vmem_limit_bytes=67043328),
    )

    tracers = pl.pallas_call(
        tracer_kernel,
        name="tracers",
        out_shape=(shape(*flat), shape(*flat), shape(*flat), shape(*full), shape(*full), shape(*full), shape(*full)),
        in_specs=[any_spec] * 13 + [smem_spec],
        out_specs=(any_spec,) * 7,
        scratch_shapes=[
            vm(4, LEVELS, 2, 2, PR, LN), vm(LEVELS + 1, 2, ROWS, 2 * LN), vm(LEVELS + 1, 2, ROWS, 2 * LN), vm(2, 2, 2, ROWS, LN),
            vm(*full), vm(*full), vm(3, 2, ROWS, 2 * LN), vm(2, 2, 2, ROWS, LN), vm(3, 2, ROWS, LN),
            vm(NCH, PR, LN), vm(2, NCH, 2, 4, PAIRS, LN),
            dma(NCH, 10), dma(4), dma(NCH, 4), dma(3), dma(3),
        ],
        compiler_params=pltpu.CompilerParams(vmem_limit_bytes=67043328),
    )

    def local_step(vel_x, vel_y, pot_temp, salinity, surf_eta, trans_x, trans_y, col_depth, wet_levels, avg_weights):
        star_x, star_y, eta, tx, ty, corr, kmask, cols, rows = momentum(
            vel_x, vel_y, pot_temp, salinity, surf_eta, trans_x, trans_y, col_depth, wet_levels, avg_weights, jnp.asarray(visc))
        return tracers(vel_x, vel_y, pot_temp, salinity, star_x, star_y, eta, tx, ty, corr, kmask, cols, rows, jnp.asarray(diff))

    spec_3d = P(None, None, "row", "col")
    spec_2d = P(None, "row", "col")
    spec_map = P("row", "col")
    return jax.shard_map(local_step, mesh=mesh, in_specs=(spec_3d, spec_3d, spec_3d, spec_3d, spec_2d, spec_2d, spec_2d, spec_map, spec_map, P()),
                         out_specs=(spec_2d, spec_2d, spec_2d, spec_3d, spec_3d, spec_3d, spec_3d), check_vma=False)
```

```python
import functools
import numpy as np
import jax
import jax.numpy as jnp
from jax import lax
from jax.experimental import pallas as pl
from jax.experimental.pallas import tpu as pltpu
from jax.sharding import PartitionSpec as P

WAVE_COURANT = 0.4
THERM_EXP = 0.2
HALINE_CON = 0.15
PRESS_SCALE = 0.5
VISC_NUMBER = 1.0
DIFF_NUMBER = 0.5

LEVELS = 20
SUBS = 20
CHUNK = 4
NCH = LEVELS // CHUNK
PAIRS = 2 * CHUNK
ROWS = 128
LN = 128
PR = 144
EXT = 192
F32 = jnp.float32
TC = 2
AHEAD = 4
PK = 64
UP = 32
MESH_ID = pl.DeviceIdType.MESH


def solve_table(strength):
    inner = np.zeros(LEVELS)
    last = np.zeros(LEVELS)
    inner[0] = 1.0 + strength
    last[0] = 1.0
    for k in range(1, LEVELS):
        inner[k] = 1.0 + 2.0 * strength - strength**2 / inner[k - 1]
        last[k] = 1.0 + strength - strength**2 / inner[k - 1]
    ratio = strength / inner
    before = np.concatenate([[0.0], ratio[:-1]])
    return np.stack([before, ratio, 1.0 / inner, 1.0 / last]).astype(np.float32)


def lanes(rows):
    return lax.broadcasted_iota(jnp.int32, (rows, LN), 1)


def east(tile, following):
    return pltpu.roll(jnp.where(lanes(tile.shape[0]) == 0, following, tile), LN - 1, 1)


def west(tile, previous):
    return pltpu.roll(jnp.where(lanes(tile.shape[0]) == LN - 1, previous, tile), 1, 1)


NEXT = (1, 2, 0)
PREV = (2, 0, 1)


def halo(packed, j):
    return pltpu.roll(packed, LN - 1 - 2 * j, 1)


def east_pair(first, second, edge):
    last = lanes(first.shape[0]) == LN - 1
    a, b = pltpu.roll(first, LN - 1, 1), pltpu.roll(second, LN - 1, 1)
    return jnp.where(last, b, a), jnp.where(last, edge, b)


def west_pair(first, second, edge):
    origin = lanes(first.shape[0]) == 0
    a, b = pltpu.roll(first, 1, 1), pltpu.roll(second, 1, 1)
    return jnp.where(origin, edge, a), jnp.where(origin, a, b)


def momentum_kernel(u_hbm, v_hbm, t_hbm, s_hbm, eta_hbm, tx_hbm, ty_hbm, h_hbm, kmt_hbm, weights, table,
                    us_hbm, vs_hbm, eta_out, tx_out, ty_out, corr_out, kmask_out, col_out, rows_out,
                    buf, tu, tv, cu, cv, pbufa, pbufb, pacc, phal, rhoc, gsum, xsum, kmask, kmt, vep, uwp, dup, txb, tyb, corr,
                    send_col, recv_col, send_row, recv_row,
                    xb, sp, rp, xf, sf, rf, hux, huy, ae, aw, an, as_, cc, ebufa, ebufb, dbuf, gbuf, eacc, bacc,
                    ld_sem, xl_sem, cs_sem, cr_sem, xs_sem, xr_sem, fs_sem, fr_sem, st_sem, ot_sem, av_sem):
    ku, kv = kmask.at[1], kmask.at[2]
    me_c = lax.axis_index("col")
    me_r = lax.axis_index("row")
    peer = 1 - me_c
    has_n = me_r < 3
    has_s = me_r > 0
    hbm = (u_hbm, v_hbm, t_hbm, s_hbm)

    def loads(c):
        out = []
        for f in range(4):
            for t in range(2):
                out.append(pltpu.make_async_copy(
                    hbm[f].at[pl.ds(c * CHUNK, CHUNK), :, :, pl.ds(t * LN, LN)],
                    buf.at[f, pl.ds(c * CHUNK, CHUNK), :, t, pl.ds(8, ROWS), :], ld_sem.at[c, f * 2 + t]))
        return out

    def map_loads():
        return [pltpu.make_async_copy(kmt_hbm, kmt, xl_sem.at[8])] + [
            pltpu.make_async_copy(h_hbm.at[:, pl.ds(t * LN, LN)], xb.at[1, t, pl.ds(32, ROWS), :], xl_sem.at[t]) for t in range(2)]

    def flow_loads():
        return [pltpu.make_async_copy(ref.at[:, :, pl.ds(t * LN, LN)], xb.at[pl.ds(2 + 2 * i, 2), t, pl.ds(32, ROWS), :], xl_sem.at[2 + 2 * i + t])
                for t in range(2) for i, ref in enumerate((eta_hbm, tx_hbm, ty_hbm))]

    for copy in map_loads() + loads(0) + loads(1) + loads(2) + flow_loads() + loads(3) + loads(4):
        copy.start()

    barrier = pltpu.get_barrier_semaphore()

    def greet(col, row):
        pl.semaphore_signal(barrier, inc=1, device_id={"col": col, "row": row}, device_id_type=MESH_ID)

    greet(peer, me_r)

    @pl.when(has_n)
    def _():
        greet(me_c, me_r + 1)
        greet(peer, me_r + 1)

    @pl.when(has_s)
    def _():
        greet(me_c, me_r - 1)
        greet(peer, me_r - 1)

    zrow = jnp.zeros((8, LN), F32)
    for ref, count in ((xb, 8), (xf, 4)):
        for f in range(count):
            for t in range(3):
                ref[f, t, 0:8, :] = zrow
                ref[f, t, EXT - 8:EXT, :] = zrow
    for ref, count in ((rp, 4), (rf, 2)):
        for f in range(count):
            ref[f, 0:8, :] = zrow
            ref[f, EXT - 8:EXT, :] = zrow

    def zero_side(side, lo):
        z24 = jnp.zeros((24, LN), F32)
        for f in range(8):
            for t in range(2):
                xb[f, t, lo:lo + 24, :] = z24
        for f in range(4):
            rp[f, lo:lo + 24, :] = z24
            for t in range(2):
                xf[f, t, lo:lo + 24, :] = z24
        for f in range(2):
            rf[f, lo:lo + 24, :] = z24
        for c in range(NCH):
            recv_col[c, 136 * side:136 * side + 8, :] = zrow
            for f in range(4):
                for t in range(2):
                    recv_row[side, c, t, f, :, :] = zrow

    @pl.when(me_r == 0)
    def _():
        zero_side(0, 8)

    @pl.when(me_r == 3)
    def _():
        zero_side(1, 160)

    def zero_planes(i, carry):
        r = pl.multiple_of(i * 16, 16)
        z = jnp.zeros((16, LN), F32)
        for m in range(2):
            for t in range(2):
                pacc[m, t, pl.ds(r, 16), :] = z
            phal[m, pl.ds(r, 16), :] = z
        return carry
    lax.fori_loop(0, PR // 16, zero_planes, 0)

    def zero_planes2(i, carry):
        r = pl.multiple_of(i * 16, 16)
        z = jnp.zeros((16, LN), F32)
        for m in range(2):
            for t in range(2):
                for f in range(2):
                    gsum[f, m, t, pl.ds(r, 16), :] = z
                    xsum[f, m, t, pl.ds(r, 16), :] = z
                for ref in (cu, cv):
                    ref[m, t, pl.ds(r, 16), :] = z
                for ref in (tu, tv):
                    ref[LEVELS, m, t, pl.ds(r, 16), :] = z
        return carry
    lax.fori_loop(0, ROWS // 16, zero_planes2, 0)

    for copy in map_loads():
        copy.wait()
    for t in range(2):
        for r in range(0, ROWS, 64):
            level_count = kmt[r:r + 64, t * LN:(t + 1) * LN].astype(F32)
            xb[0, t, 32 + r:96 + r, :] = level_count
            kmask[0, t, r:r + 64, :] = level_count

    @pl.when((me_r == 0) | (me_r == 3))
    def _():
        pl.semaphore_wait(barrier, 3)

    @pl.when((me_r != 0) & (me_r != 3))
    def _():
        pl.semaphore_wait(barrier, 5)

    def remote(src, dst, ssem, rsem, col, row):
        return pltpu.make_async_remote_copy(src_ref=src, dst_ref=dst, send_sem=ssem, recv_sem=rsem,
                                            device_id={"col": col, "row": row}, device_id_type=MESH_ID)

    def wide_rows(own, first, count, ssem, rsem, slot):
        fields = pl.ds(first, count)
        return ((remote(own.at[fields, pl.ds(0, 2), pl.ds(136, 24), :], own.at[fields, pl.ds(0, 2), pl.ds(8, 24), :],
                        ssem.at[slot], rsem.at[slot], me_c, me_r + 1),),
                (remote(own.at[fields, pl.ds(0, 2), pl.ds(32, 24), :], own.at[fields, pl.ds(0, 2), pl.ds(160, 24), :],
                        ssem.at[slot + 1], rsem.at[slot + 1], me_c, me_r - 1),))

    def wide_copies(own, first, count, packed, landing, ssem, rsem):
        side = remote(packed, landing.at[:, pl.ds(32, ROWS), :], ssem.at[0], rsem.at[0], peer, me_r)
        up, down = wide_rows(own, first, count, ssem, rsem, 1)
        up += (remote(packed.at[:, pl.ds(104, 24), :], landing.at[:, pl.ds(8, 24), :], ssem.at[3], rsem.at[3], peer, me_r + 1),)
        down += (remote(packed.at[:, pl.ds(0, 24), :], landing.at[:, pl.ds(160, 24), :], ssem.at[4], rsem.at[4], peer, me_r - 1),)
        return side, up, down

    def map_copies():
        return (None, *wide_rows(xb, 0, 2, xs_sem, xr_sem, 5))

    def flow_copies():
        return wide_copies(xb, 2, 6, sp, rp, xs_sem, xr_sem)

    def force_copies():
        return wide_copies(xf, 0, 4, sf, rf, fs_sem, fr_sem)

    def edge_copies(c):
        north, south = me_r + 1, me_r - 1
        side = remote(send_col.at[c], recv_col.at[c, pl.ds(8, ROWS), :], cs_sem.at[c, 0], cr_sem.at[c, 0], peer, me_r)
        up = (remote(send_row.at[0, c], recv_row.at[0, c], cs_sem.at[c, 1], cr_sem.at[c, 1], me_c, north),
              remote(send_col.at[c, pl.ds(ROWS - 8, 8), :], recv_col.at[c, pl.ds(0, 8), :], cs_sem.at[c, 2], cr_sem.at[c, 2], peer, north))
        down = (remote(send_row.at[1, c], recv_row.at[1, c], cs_sem.at[c, 3], cr_sem.at[c, 3], me_c, south),
                remote(send_col.at[c, pl.ds(0, 8), :], recv_col.at[c, pl.ds(8 + ROWS, 8), :], cs_sem.at[c, 4], cr_sem.at[c, 4], peer, south))
        return side, up, down

    def start_all(copies):
        side, up, down = copies
        if side is not None:
            side.start()

        @pl.when(has_n)
        def _():
            for copy in up:
                copy.start()

        @pl.when(has_s)
        def _():
            for copy in down:
                copy.start()

    def wait_recv_all(copies):
        side, up, down = copies
        if side is not None:
            side.wait_recv()

        @pl.when(has_s)
        def _():
            for copy in up:
                copy.wait_recv()

        @pl.when(has_n)
        def _():
            for copy in down:
                copy.wait_recv()

    def wait_send_all(copies):
        side, up, down = copies
        if side is not None:
            side.wait_send()

        @pl.when(has_n)
        def _():
            for copy in up:
                copy.wait_send()

        @pl.when(has_s)
        def _():
            for copy in down:
                copy.wait_send()

    start_all(map_copies())

    def pack_and_send(c, with_maps=False):
        for copy in loads(c):
            copy.wait()
        lane = lanes(PK)

        def block(i, carry):
            r = pl.multiple_of(i * PK, PK)
            pairs = [(f, c * CHUNK + kk, m) for f in range(4) for kk in range(CHUNK) for m in range(2)]
            column = [[buf[f, k, m, t, pl.ds(8 + r, PK), :] for f, k, m in pairs] for t in range(2)]
            if with_maps:
                for t in range(2):
                    column[t] += [xb[0, t, pl.ds(32 + r, PK), :], xb[1, t, pl.ds(32 + r, PK), :]]
            packed = jnp.zeros((PK, LN), F32)
            count = len(column[0])
            for i in range(count + 1):
                edge = jnp.where(lane == 0, column[0][min(i, count - 1)], column[1][max(i - 1, 0)])
                edge = pltpu.roll(edge, 2 * i, 1) if i else edge
                packed = jnp.where(lane >= 2 * i - 1, edge, packed) if i else edge
            send_col[c, pl.ds(r, PK), :] = packed
            return carry
        for kk in range(CHUNK):
            for m in range(2):
                jj = kk * 2 + m
                k = c * CHUNK + kk
                for side, row in ((0, 8 + ROWS - 1), (1, 8)):
                    for f in range(4):
                        for t in range(2):
                            send_row[side, c, t, f, jj:jj + 1, :] = buf[f, k, m, t, row:row + 1, :]
        lax.fori_loop(0, ROWS // PK, block, 0)
        start_all(edge_copies(c))

    pack_and_send(0, with_maps=True)

    def pack_pairs(source, firsts, seconds, send):
        lane = lanes(ROWS)
        outer = (lane < 32) | (lane >= 96)
        for slot, (f, g) in enumerate(zip(firsts, seconds)):
            a, b = (jnp.where(lane < 64, source[n, 0, 32:32 + ROWS, :], source[n, 1, 32:32 + ROWS, :]) for n in (f, g))
            send[slot, :, :] = jnp.where(outer, a, pltpu.roll(b, 64, 1))

    def pack_wide():
        for copy in flow_loads():
            copy.wait()
        pack_pairs(xb, (0, 2, 4, 6), (1, 3, 5, 7), sp)
        start_all(flow_copies())

    def pack_rest(c, carry):
        pack_and_send(c)
        return carry
    lax.fori_loop(1, NCH, pack_rest, 0)
    pack_wide()

    RHO_T = np.float32(-THERM_EXP * PRESS_SCALE / LEVELS / 2)
    RHO_S = np.float32(HALINE_CON * PRESS_SCALE / LEVELS / 2)
    BR = 128
    SB = 16

    def pressure_rows(k, slot, base, rows):
        for m in range(2):
            for t in range(2):
                half = RHO_T * buf[2, k, m, t, pl.ds(base, rows), :] + RHO_S * buf[3, k, m, t, pl.ds(base, rows), :]
                p = pacc[m, t, pl.ds(base, rows), :] + half
                slot[m, t, pl.ds(base, rows), :] = p
                pacc[m, t, pl.ds(base, rows), :] = p + half

    def shift_u(c, kk, m, base, rows):
        u = [buf[0, c * CHUNK + kk, m, t, pl.ds(base, rows), :] for t in range(2)]
        edge = halo(recv_col[c, pl.ds(base, rows), :], kk * 2 + m)
        ue, uw = east_pair(*u, edge), west_pair(*u, edge)
        for t in range(2):
            uwp[m, t, pl.ds(base, rows), :] = uw[t]
            dup[m, t, pl.ds(base, rows), :] = ue[t] - uw[t]

    def level(c, kk, now, later):
        k = c * CHUNK + kk
        pressure_rows(k, now, 8 + ROWS, 8)
        for m in range(2):
            shift_u(c, kk, m, 8, 8)
            ve = east_pair(*(buf[1, k, m, t, 0:8, :] for t in range(2)), halo(recv_col[c, 0:8, :], PAIRS + kk * 2 + m))
            for t in range(2):
                vep[m, t, 0:8, :] = ve[t]
        level_no = k.astype(F32)
        before = table[0, k]
        following = jnp.minimum(k + 1, LEVELS - 1)

        def block(i, carry):
            for q in range(0, BR, SB):
                piece(pl.multiple_of(i * BR + q, SB), pl.multiple_of(8 + i * BR + q, 8))
            return carry

        def piece(r, b):
            wet_x = [ku[t, pl.ds(r, SB), :] > level_no for t in range(2)]
            wet_y = [kv[t, pl.ds(r, SB), :] > level_no for t in range(2)]
            packed = recv_col[c, pl.ds(b, SB), :]
            packed_r = rhoc[pl.ds(r, SB), :]
            for m in range(2):
                j = kk * 2 + m
                shift_u(c, kk, m, pl.multiple_of(b + 8, 8), SB)
                half = halo(packed_r, j)
                p_edge = phal[m, pl.ds(r, SB), :] + half
                phal[m, pl.ds(r, SB), :] = p_edge + half
                v = [buf[1, k, m, t, pl.ds(b, SB), :] for t in range(2)]
                p = [now[m, t, pl.ds(b, SB), :] for t in range(2)]
                v_edge = halo(packed, PAIRS + j)
                ve, vw = east_pair(*v, v_edge), west_pair(*v, v_edge)
                pe = east_pair(*p, p_edge)
                for t in range(2):
                    vep[m, t, pl.ds(b, SB), :] = ve[t]
                    u = buf[0, k, m, t, pl.ds(b, SB), :]
                    un = buf[0, k, m, t, pl.ds(b + 1, SB), :]
                    us = buf[0, k, m, t, pl.ds(b - 1, SB), :]
                    vs = buf[1, k, m, t, pl.ds(b - 1, SB), :]
                    vn = buf[1, k, m, t, pl.ds(b + 1, SB), :]
                    pn = now[m, t, pl.ds(b + 1, SB), :]
                    w = (v[t] + vs) + (ve[t] + vep[m, t, pl.ds(b - 1, SB), :])
                    z = (u + un) + (uwp[m, t, pl.ds(b, SB), :] + uwp[m, t, pl.ds(b + 1, SB), :])
                    gu = (p[t] - pe[t]) - (0.5 * u) * dup[m, t, pl.ds(b, SB), :] - (0.125 * w) * (un - us)
                    gu = jnp.where(wet_x[t], gu, 0.0)
                    gsum[0, m, t, pl.ds(r, SB), :] += gu
                    new = u + gu + before * cu[m, t, pl.ds(r, SB), :]
                    cu[m, t, pl.ds(r, SB), :] = new
                    tu[k, m, t, pl.ds(r, SB), :] = new
                    gv = (p[t] - pn) - (0.125 * z) * (ve[t] - vw[t]) - (0.5 * v[t]) * (vn - vs)
                    gv = jnp.where(wet_y[t], gv, 0.0)
                    gsum[1, m, t, pl.ds(r, SB), :] += gv
                    new = v[t] + gv + before * cv[m, t, pl.ds(r, SB), :]
                    cv[m, t, pl.ds(r, SB), :] = new
                    tv[k, m, t, pl.ds(r, SB), :] = new
            pressure_rows(following, later, b, SB)
        lax.fori_loop(0, ROWS // BR, block, 0)

    def first_pressure(i, carry):
        pressure_rows(0, pbufa, pl.multiple_of(8 + i * 64, 8), 64)
        return carry
    lax.fori_loop(0, 2, first_pressure, 0)

    def chunk_step(c, carry):
        wait_recv_all(edge_copies(c))

        @pl.when(c == 0)
        def _():
            face_maps()

        for kk in range(CHUNK):
            k = c * CHUNK + kk
            for m in range(2):
                jj = kk * 2 + m
                for side, row in ((0, 7), (1, 8 + ROWS)):
                    for f in range(4):
                        for t in range(2):
                            buf[f, k, m, t, row:row + 1, :] = recv_row[side, c, t, f, jj:jj + 1, :]
        packed = recv_col[c, 8:8 + ROWS, :]
        rhoc[...] = RHO_T * pltpu.roll(packed, LN - 4 * PAIRS, 1) + RHO_S * pltpu.roll(packed, LN - 6 * PAIRS, 1)

        def two_levels(h, carry2):
            level(c, 2 * h, pbufa, pbufb)
            level(c, 2 * h + 1, pbufb, pbufa)
            return carry2
        lax.fori_loop(0, CHUNK // 2, two_levels, 0)
        return carry

    def face_maps():
        wait_recv_all(map_copies())

        def maps(i, carry):
            r = pl.multiple_of(i * 64, 64)
            packed = recv_col[0, pl.ds(8 + r, 64), :]
            kt = [xb[0, t, pl.ds(32 + r, 64), :] for t in range(2)]
            ht = [xb[1, t, pl.ds(32 + r, 64), :] for t in range(2)]
            ke = east_pair(*kt, halo(packed, 4 * PAIRS))
            he = east_pair(*ht, halo(packed, 4 * PAIRS + 1))
            for t in range(2):
                kx = jnp.minimum(kt[t], ke[t])
                ky = jnp.minimum(kt[t], xb[0, t, pl.ds(33 + r, 64), :])
                ku[t, pl.ds(r, 64), :] = kx
                kv[t, pl.ds(r, 64), :] = ky
                hux[t, pl.ds(32 + r, 64), :] = jnp.where(kx > 0.0, 0.5 * (ht[t] + he[t]), 0.0)
                huy[t, pl.ds(32 + r, 64), :] = jnp.where(ky > 0.0, 0.5 * (ht[t] + xb[1, t, pl.ds(33 + r, 64), :]), 0.0)
            return carry
        lax.fori_loop(0, 2, maps, 0)

    lax.fori_loop(0, NCH, chunk_step, 0)

    packet_copies = [pltpu.make_async_copy(src, dst, ot_sem.at[i]) for i, (src, dst) in enumerate(
        ((recv_col, col_out), (recv_row, rows_out), (kmask, kmask_out)))]
    for copy in packet_copies:
        copy.start()

    def forcing(i, carry):
        r = pl.multiple_of(i * 32, 32)
        for t in range(2):
            nx = jnp.maximum(ku[t, pl.ds(r, 32), :], 1.0)
            ny = jnp.maximum(kv[t, pl.ds(r, 32), :], 1.0)
            fx = hux[t, pl.ds(32 + r, 32), :] / nx / SUBS
            fy = huy[t, pl.ds(32 + r, 32), :] / ny / SUBS
            for m in range(2):
                xf[m, t, pl.ds(32 + r, 32), :] = fx * gsum[0, m, t, pl.ds(r, 32), :]
                xf[2 + m, t, pl.ds(32 + r, 32), :] = fy * gsum[1, m, t, pl.ds(r, 32), :]
        return carry
    lax.fori_loop(0, ROWS // 32, forcing, 0)
    pack_pairs(xf, (0, 1), (2, 3), sf)
    start_all(force_copies())

    def stores(c):
        out = []
        for f, (ref, dst) in enumerate(((tu, us_hbm), (tv, vs_hbm))):
            for t in range(2):
                out.append(pltpu.make_async_copy(ref.at[pl.ds(c * CHUNK, CHUNK), :, t, :, :],
                                                 dst.at[pl.ds(c * CHUNK, CHUNK), :, :, pl.ds(t * LN, LN)], st_sem.at[c, f * 2 + t]))
        return out

    def upward(step, carry):
        c = NCH - 1 - step

        def block(i, carry2):
            r = pl.multiple_of(i * UP, UP)
            for f, (ref, kp) in enumerate(((tu, ku), (tv, kv))):
                for t in range(2):
                    depth = kp[t, pl.ds(r, UP), :]
                    below = [ref[c * CHUNK + CHUNK, m, t, pl.ds(r, UP), :] for m in range(2)]
                    total = [xsum[f, m, t, pl.ds(r, UP), :] for m in range(2)]
                    for kk in range(CHUNK - 1, -1, -1):
                        k = c * CHUNK + kk
                        level_no = k.astype(F32)
                        inv = jnp.where(depth > level_no + 1.0, table[2, k], jnp.where(depth > level_no, table[3, k], 0.0))
                        for m in range(2):
                            below[m] = ref[k, m, t, pl.ds(r, UP), :] * inv + table[1, k] * below[m]
                            ref[k, m, t, pl.ds(r, UP), :] = below[m]
                            total[m] = total[m] + below[m]
                    for m in range(2):
                        xsum[f, m, t, pl.ds(r, UP), :] = total[m]
            return carry2
        lax.fori_loop(0, ROWS // UP, block, 0)
        for copy in stores(c):
            copy.start()
        return carry
    lax.fori_loop(0, NCH, upward, 0)

    wait_recv_all(flow_copies())

    def unpack_wide(i, carry):
        r = pl.multiple_of(i * 96, 32)
        for pair in range(4):
            tile = rp[pair, pl.ds(r, 96), :]
            xb[2 * pair, 2, pl.ds(r, 96), :] = tile
            xb[2 * pair + 1, 2, pl.ds(r, 96), :] = pltpu.roll(tile, 64, 1)
        return carry
    lax.fori_loop(0, EXT // 96, unpack_wide, 0)

    XR = 88

    def depths(i, carry):
        r = pl.multiple_of(8 + i * XR, 8)
        kt = [xb[0, t, pl.ds(r, XR), :] for t in range(3)]
        ht = [xb[1, t, pl.ds(r, XR), :] for t in range(3)]
        for t in range(3):
            kx = jnp.minimum(kt[t], east(kt[t], kt[NEXT[t]]))
            ky = jnp.minimum(kt[t], xb[0, t, pl.ds(r + 1, XR), :])
            hux[t, pl.ds(r, XR), :] = jnp.where(kx > 0.0, 0.5 * (ht[t] + east(ht[t], ht[NEXT[t]])), 0.0)
            huy[t, pl.ds(r, XR), :] = jnp.where(ky > 0.0, 0.5 * (ht[t] + xb[1, t, pl.ds(r + 1, XR), :]), 0.0)
            cc[t, pl.ds(r, XR), :] = jnp.where(kt[t] > 0.0, WAVE_COURANT, 0.0)
        return carry
    for t in range(3):
        for ref in (hux, huy):
            ref[t, 0:8, :] = zrow
        for ref in (ebufa, ebufb):
            for m in range(2):
                ref[m, t, 0:8, :] = zrow
                ref[m, t, EXT - 8:EXT, :] = zrow
    lax.fori_loop(0, 2, depths, 0)

    def coefficients(i, carry):
        r = pl.multiple_of(8 + i * XR, 8)
        hx = [hux[t, pl.ds(r, XR), :] for t in range(3)]
        for t in range(3):
            c0 = cc[t, pl.ds(r, XR), :]
            cw = WAVE_COURANT * c0
            ae[t, pl.ds(r, XR), :] = cw * hx[t]
            aw[t, pl.ds(r, XR), :] = cw * west(hx[t], hx[PREV[t]])
            an[t, pl.ds(r, XR), :] = cw * huy[t, pl.ds(r, XR), :]
            as_[t, pl.ds(r, XR), :] = cw * huy[t, pl.ds(r - 1, XR), :]
        return carry
    lax.fori_loop(0, 2, coefficients, 0)

    def first_subcycle(m, base, rows):
        tx = [xb[4 + m, t, pl.ds(base, rows), :] for t in range(3)]
        for t in range(3):
            c0 = cc[t, pl.ds(base, rows), :]
            ty = xb[6 + m, t, pl.ds(base, rows), :]
            div = tx[t] - west(tx[t], tx[PREV[t]]) + ty - xb[6 + m, t, pl.ds(base - 1, rows), :]
            change = -c0 * div
            dbuf[m, t, pl.ds(base, rows), :] = change
            eta = jnp.where(c0 > 0.0, xb[2 + m, t, pl.ds(base, rows), :], 0.0) + change
            ebufa[m, t, pl.ds(base, rows), :] = eta

    def first_block(i, carry):
        for m in range(2):
            first_subcycle(m, pl.multiple_of(8 + i * XR, 8), XR)
        return carry
    lax.fori_loop(0, 2, first_block, 0)

    whole = weights[SUBS - 1]
    moment = weights[SUBS - 1]
    for n in range(SUBS - 2, -1, -1):
        whole = whole + weights[n]
        moment = moment + whole

    def first_sums(i, carry):
        r = pl.multiple_of(i * 8, 8)
        for m in range(2):
            for t in range(3):
                eta = ebufa[m, t, pl.ds(32 + r, 8), :]
                bacc[m, t, pl.ds(r, 8), :] = whole * eta
                if t < 2:
                    eacc[m, t, pl.ds(r, 8), :] = weights[0] * eta
        return carry
    lax.fori_loop(0, 17, first_sums, 0)

    wait_recv_all(force_copies())

    def unpack_force(i, carry):
        r = pl.multiple_of(i * 96, 32)
        for m in range(2):
            tile = rf[m, pl.ds(r, 96), :]
            xf[m, 2, pl.ds(r, 96), :] = tile
            xf[2 + m, 2, pl.ds(r, 96), :] = pltpu.roll(tile, 64, 1)
        return carry
    lax.fori_loop(0, EXT // 96, unpack_force, 0)

    def forcing_divergence(i, carry):
        r = pl.multiple_of(8 + i * XR, 8)
        for m in range(2):
            fx = [xf[m, t, pl.ds(r, XR), :] for t in range(3)]
            for t in range(3):
                div = fx[t] - west(fx[t], fx[PREV[t]]) + xf[2 + m, t, pl.ds(r, XR), :] - xf[2 + m, t, pl.ds(r - 1, XR), :]
                gbuf[m, t, pl.ds(r, XR), :] = cc[t, pl.ds(r, XR), :] * div
        return carry
    lax.fori_loop(0, 2, forcing_divergence, 0)

    def subcycle(n, tail, lo, hi, old, new):
        tail = tail - weights[n - 2]
        weight = weights[n - 1]
        for r, end in ((lo, 96), (96, hi)):
            first = max(r, 32)
            for t in range(3):
                c_e, c_w = ae[t, r:end, :], aw[t, r:end, :]
                c_n, c_s = an[t, r:end, :], as_[t, r:end, :]
                for m in range(2):
                    e = old[m, t, r:end, :]
                    to_e = east(e, old[m, NEXT[t], r:end, :])
                    to_w = west(e, old[m, PREV[t], r:end, :])
                    to_n = old[m, t, r + 1:end + 1, :]
                    to_s = old[m, t, r - 1:end - 1, :]
                    d = dbuf[m, t, r:end, :] - gbuf[m, t, r:end, :]
                    d = d + (c_e * (to_e - e) + c_w * (to_w - e)) + (c_n * (to_n - e) + c_s * (to_s - e))
                    dbuf[m, t, r:end, :] = d
                    e = e + d
                    new[m, t, r:end, :] = e
                    last = min(end, 168)
                    bacc[m, t, first - 32:last - 32, :] += tail * e[first - r:last - r]
                    if t < 2:
                        last = min(end, 160)
                        eacc[m, t, first - 32:last - 32, :] += weight * e[first - r:last - r]
        return tail

    tail = subcycle(2, whole, 8, 184, ebufa, ebufb)
    for first_n, steps, lo, hi in ((3, 1, 8, 184), (5, 4, 16, 176), (13, 4, 24, 168)):
        def two_cycles(h, carry, first_n=first_n, lo=lo, hi=hi):
            n = first_n + 2 * h
            carry = subcycle(n, carry, lo, hi, ebufb, ebufa)
            return subcycle(n + 1, carry, lo, hi, ebufa, ebufb)
        tail = lax.fori_loop(0, steps, two_cycles, tail)

    eta_copies = [pltpu.make_async_copy(eacc.at[:, t, pl.ds(0, ROWS), :], eta_out.at[:, :, pl.ds(t * LN, LN)], ot_sem.at[4 + t]) for t in range(2)]
    for copy in eta_copies:
        copy.start()

    AV = 64

    def average_copies(i):
        r = pl.multiple_of(i * AV, AV)
        return [pltpu.make_async_copy(src, dst, av_sem.at[i, n]) for n, (src, dst) in enumerate((
            (txb.at[:, pl.ds(r, AV), :], tx_out.at[:, pl.ds(r, AV), :]), (tyb.at[:, pl.ds(r, AV), :], ty_out.at[:, pl.ds(r, AV), :]),
            (corr.at[:, :, :, pl.ds(r, AV), :], corr_out.at[:, :, :, pl.ds(r, AV), :])))]

    def averages(i, carry):
        for q in range(0, AV, 16):
            r = pl.multiple_of(i * AV + q, 16)
            g = pl.multiple_of(32 + i * AV + q, 16)
            for t in range(2):
                depth_x = hux[t, pl.ds(g, 16), :]
                depth_y = huy[t, pl.ds(g, 16), :]
                kx = ku[t, pl.ds(r, 16), :]
                ky = kv[t, pl.ds(r, 16), :]
                inv_x = 1.0 / (depth_x + jnp.where(kx > 0.0, 0.0, 1.0))
                inv_y = 1.0 / (depth_y + jnp.where(ky > 0.0, 0.0, 1.0))
                mean_x = 1.0 / jnp.maximum(kx, 1.0)
                mean_y = 1.0 / jnp.maximum(ky, 1.0)
                for m in range(2):
                    lane = slice(t * LN, (t + 1) * LN)
                    acc = bacc[m, t, pl.ds(r, 16), :]
                    tx = whole * xb[4 + m, t, pl.ds(g, 16), :] + moment * xf[m, t, pl.ds(g, 16), :] \
                        - WAVE_COURANT * depth_x * (east(acc, bacc[m, NEXT[t], pl.ds(r, 16), :]) - acc)
                    ty = whole * xb[6 + m, t, pl.ds(g, 16), :] + moment * xf[2 + m, t, pl.ds(g, 16), :] \
                        - WAVE_COURANT * depth_y * (bacc[m, t, pl.ds(r + 1, 16), :] - acc)
                    tx = jnp.where(kx > 0.0, tx, 0.0)
                    ty = jnp.where(ky > 0.0, ty, 0.0)
                    txb[m, pl.ds(r, 16), lane] = tx
                    tyb[m, pl.ds(r, 16), lane] = ty
                    corr[0, m, t, pl.ds(r, 16), :] = tx * inv_x - xsum[0, m, t, pl.ds(r, 16), :] * mean_x
                    corr[1, m, t, pl.ds(r, 16), :] = ty * inv_y - xsum[1, m, t, pl.ds(r, 16), :] * mean_y
        for copy in average_copies(i):
            copy.start()
        return carry
    lax.fori_loop(0, ROWS // AV, averages, 0)

    wait_send_all(map_copies())
    wait_send_all(flow_copies())
    wait_send_all(force_copies())
    for copy in packet_copies + eta_copies:
        copy.wait()
    for i in range(ROWS // AV):
        for copy in average_copies(i):
            copy.wait()

    def drain(c, carry):
        wait_send_all(edge_copies(c))
        for copy in stores(c):
            copy.wait()
        return carry
    lax.fori_loop(0, NCH, drain, 0)


def tracer_kernel(u_hbm, v_hbm, t_hbm, s_hbm, us_hbm, vs_hbm, eta_in, tx_in, ty_in, corr_in, kmask_in, col_in, rows_in, table,
                  eta_hbm, tx_hbm, ty_hbm, un_hbm, vn_hbm, tn_hbm, sn_hbm,
                  buf, tt, ts, ct, su, sv, small, corr, kmask, cols, rows, ld_sem, ed_sem, st_sem, sv_sem, in_sem, out_sem):
    hbm = (u_hbm, v_hbm, t_hbm, s_hbm)
    sources = (eta_in, tx_in, ty_in)
    sinks = (eta_hbm, tx_hbm, ty_hbm)

    def loads(c):
        out = []
        for f in range(4):
            for t in range(2):
                out.append(pltpu.make_async_copy(
                    hbm[f].at[pl.ds(c * TC, TC), :, :, pl.ds(t * LN, LN)],
                    buf.at[f, pl.ds(c * TC, TC), :, t, pl.ds(8, ROWS), :], ld_sem.at[c, f * 2 + t]))
        for f, (src, dst) in enumerate(((us_hbm, su), (vs_hbm, sv))):
            out.append(pltpu.make_async_copy(src.at[pl.ds(c * TC, TC)], dst.at[pl.ds(c * TC, TC)], ld_sem.at[c, 8 + f]))
        return out

    def stores_v(c):
        return [pltpu.make_async_copy(src.at[pl.ds(c * TC, TC)], dst.at[pl.ds(c * TC, TC)], sv_sem.at[c, f])
                for f, (src, dst) in enumerate(((su, un_hbm), (sv, vn_hbm)))]

    def stores_t(c):
        return [pltpu.make_async_copy(src.at[pl.ds(c * CHUNK, CHUNK)], dst.at[pl.ds(c * CHUNK, CHUNK)], st_sem.at[c, f])
                for f, (src, dst) in enumerate(((tt, tn_hbm), (ts, sn_hbm)))]

    edges = [pltpu.make_async_copy(src, dst, ed_sem.at[i])
             for i, (src, dst) in enumerate(((col_in, cols), (rows_in, rows), (corr_in, corr), (kmask_in, kmask)))]
    for copy in edges:
        copy.start()
    for c in range(AHEAD):
        for copy in loads(c):
            copy.start()
    small_in = [pltpu.make_async_copy(sources[i], small.at[i], in_sem.at[i]) for i in range(3)]
    small_out = [pltpu.make_async_copy(small.at[i], sinks[i], out_sem.at[i]) for i in range(3)]
    for copy in small_in:
        copy.start()

    def zero_planes(i, carry):
        r = pl.multiple_of(i * 16, 16)
        z = jnp.zeros((16, 2 * LN), F32)
        for f in range(2):
            for m in range(2):
                for t in range(2):
                    ct[f, m, t, pl.ds(r, 16), :] = z[:, :LN]
        for m in range(2):
            for ref in (tt, ts):
                ref[LEVELS, m, pl.ds(r, 16), :] = z
        return carry
    lax.fori_loop(0, ROWS // 16, zero_planes, 0)
    for copy in edges:
        copy.wait()

    BR = 128
    SB = 16

    def level(k, c, kk):
        level_no = k.astype(F32)
        before = table[0, k]

        def block(i, carry):
            for q in range(0, BR, SB):
                piece(pl.multiple_of(i * BR + q, SB), pl.multiple_of(8 + i * BR + q, 8))
            return carry

        def piece(r, b):
            wet = [kmask[0, t, pl.ds(r, SB), :] > level_no for t in range(2)]
            packed = cols[c, pl.ds(b, SB), :]
            for m in range(2):
                j = kk * 2 + m
                u = [buf[0, k, m, t, pl.ds(b, SB), :] for t in range(2)]
                v = [buf[1, k, m, t, pl.ds(b, SB), :] for t in range(2)]
                vs = [buf[1, k, m, t, pl.ds(b - 1, SB), :] for t in range(2)]
                uw = west_pair(*u, halo(packed, j))
                for f, ref in ((2, tt), (3, ts)):
                    q = [buf[f, k, m, t, pl.ds(b, SB), :] for t in range(2)]
                    edge = halo(packed, f * PAIRS + j)
                    qe, qw = east_pair(*q, edge), west_pair(*q, edge)
                    for t in range(2):
                        lane = slice(t * LN, (t + 1) * LN)
                        fy = v[t] * (q[t] + buf[f, k, m, t, pl.ds(b + 1, SB), :])
                        fs = vs[t] * (q[t] + buf[f, k, m, t, pl.ds(b - 1, SB), :])
                        adv = q[t] - 0.5 * ((u[t] * (q[t] + qe[t]) - uw[t] * (q[t] + qw[t])) + (fy - fs))
                        adv = jnp.where(wet[t], adv, 0.0)
                        new = adv + before * ct[f - 2, m, t, pl.ds(r, SB), :]
                        ct[f - 2, m, t, pl.ds(r, SB), :] = new
                        ref[k, m, pl.ds(r, SB), lane] = new
            for t in range(2):
                lane = slice(t * LN, (t + 1) * LN)
                wet_x = kmask[1, t, pl.ds(r, SB), :] > level_no
                wet_y = kmask[2, t, pl.ds(r, SB), :] > level_no
                for m in range(2):
                    su[k, m, pl.ds(r, SB), lane] = jnp.where(wet_x, su[k, m, pl.ds(r, SB), lane] + corr[0, m, t, pl.ds(r, SB), :], 0.0)
                    sv[k, m, pl.ds(r, SB), lane] = jnp.where(wet_y, sv[k, m, pl.ds(r, SB), lane] + corr[1, m, t, pl.ds(r, SB), :], 0.0)
        lax.fori_loop(0, ROWS // BR, block, 0)

    def chunk_step(c, carry):
        @pl.when(c + AHEAD < LEVELS // TC)
        def _():
            for copy in loads(c + AHEAD):
                copy.start()

        for copy in loads(c):
            copy.wait()
        packet = c // (CHUNK // TC)
        first = lax.rem(c, CHUNK // TC) * TC
        for kk in range(TC):
            k = c * TC + kk
            for m in range(2):
                jj = (first + kk) * 2 + m
                for f in (1, 2, 3):
                    for t in range(2):
                        buf[f, k, m, t, 7:8, :] = rows[0, packet, t, f, pl.ds(jj, 1), :]
                for f in (2, 3):
                    for t in range(2):
                        buf[f, k, m, t, 8 + ROWS:9 + ROWS, :] = rows[1, packet, t, f, pl.ds(jj, 1), :]

        def one_level(kk, carry2):
            level(c * TC + kk, packet, first + kk)
            return carry2
        lax.fori_loop(0, TC, one_level, 0)
        for copy in stores_v(c):
            copy.start()
        return carry
    lax.fori_loop(0, LEVELS // TC, chunk_step, 0)

    for copy in small_in:
        copy.wait()
    for copy in small_out:
        copy.start()

    def upward(step, carry):
        c = NCH - 1 - step

        def block(i, carry2):
            r = pl.multiple_of(i * UP, UP)
            for t in range(2):
                lane = slice(t * LN, (t + 1) * LN)
                depth = kmask[0, t, pl.ds(r, UP), :]
                below = [[ref[c * CHUNK + CHUNK, m, pl.ds(r, UP), lane] for m in range(2)] for ref in (tt, ts)]
                for kk in range(CHUNK - 1, -1, -1):
                    k = c * CHUNK + kk
                    level_no = k.astype(F32)
                    inv = jnp.where(depth > level_no + 1.0, table[2, k], jnp.where(depth > level_no, table[3, k], 0.0))
                    for f, ref in enumerate((tt, ts)):
                        for m in range(2):
                            below[f][m] = ref[k, m, pl.ds(r, UP), lane] * inv + table[1, k] * below[f][m]
                            ref[k, m, pl.ds(r, UP), lane] = below[f][m]
            return carry2
        lax.fori_loop(0, ROWS // UP, block, 0)
        for copy in stores_t(c):
            copy.start()
        return carry
    lax.fori_loop(0, NCH, upward, 0)

    for copy in small_out:
        copy.wait()

    def drain(c, carry):
        for copy in stores_t(c):
            copy.wait()
        return carry
    lax.fori_loop(0, NCH, drain, 0)

    def drain_v(c, carry):
        for copy in stores_v(c):
            copy.wait()
        return carry
    lax.fori_loop(0, LEVELS // TC, drain_v, 0)


def solution(mesh):
    assert mesh.shape["col"] == 2 and mesh.shape["row"] == 4
    any_spec = pl.BlockSpec(memory_space=pl.ANY)
    vmem_spec = pl.BlockSpec(memory_space=pltpu.VMEM)
    smem_spec = pl.BlockSpec(memory_space=pltpu.SMEM)
    shape = lambda *dims: jax.ShapeDtypeStruct(dims, F32)
    dma = lambda *dims: pltpu.SemaphoreType.DMA(dims)
    vm = lambda *dims: pltpu.VMEM(dims, F32)
    visc = solve_table(VISC_NUMBER)
    diff = solve_table(DIFF_NUMBER)
    full = (LEVELS, 2, ROWS, 2 * LN)
    flat = (2, ROWS, 2 * LN)

    momentum = pl.pallas_call(
        momentum_kernel,
        name="momentum",
        out_shape=(shape(*full), shape(*full), shape(*flat), shape(*flat), shape(*flat), shape(2, 2, 2, ROWS, LN),
                   shape(3, 2, ROWS, LN), shape(NCH, PR, LN), shape(2, NCH, 2, 4, PAIRS, LN)),
        in_specs=[any_spec] * 9 + [smem_spec, smem_spec],
        out_specs=(any_spec,) * 9,
        scratch_shapes=[
            vm(4, LEVELS, 2, 2, PR, LN), vm(LEVELS + 1, 2, 2, ROWS, LN), vm(LEVELS + 1, 2, 2, ROWS, LN),
            vm(2, 2, ROWS, LN), vm(2, 2, ROWS, LN), vm(2, 2, PR, LN), vm(2, 2, PR, LN), vm(2, 2, PR, LN), vm(2, PR, LN), vm(ROWS, LN),
            vm(2, 2, 2, ROWS, LN), vm(2, 2, 2, ROWS, LN), vm(3, 2, ROWS, LN), pltpu.VMEM((ROWS, 2 * LN), jnp.int32),
            vm(2, 2, PR, LN), vm(2, 2, PR, LN), vm(2, 2, PR, LN), vm(*flat), vm(*flat), vm(2, 2, 2, ROWS, LN),
            vm(NCH, ROWS, LN), vm(NCH, PR, LN), vm(2, NCH, 2, 4, PAIRS, LN), vm(2, NCH, 2, 4, PAIRS, LN),
            vm(8, 3, EXT, LN), vm(4, ROWS, LN), vm(4, EXT, LN), vm(4, 3, EXT, LN), vm(2, ROWS, LN), vm(2, EXT, LN),
            vm(3, EXT, LN), vm(3, EXT, LN), vm(3, EXT, LN), vm(3, EXT, LN), vm(3, EXT, LN), vm(3, EXT, LN), vm(3, EXT, LN),
            vm(2, 3, EXT, LN), vm(2, 3, EXT, LN), vm(2, 3, EXT, LN), vm(2, 3, EXT, LN), vm(2, 2, ROWS + 8, LN), vm(2, 3, ROWS + 8, LN),
            dma(NCH, 8), dma(9), dma(NCH, 5), dma(NCH, 5), dma(7), dma(7), dma(5), dma(5), dma(NCH, 4), dma(6), dma(2, 3),
        ],
        compiler_params=pltpu.CompilerParams(collective_id=0, has_side_effects=True, vmem_limit_bytes=67043328),
    )

    tracers = pl.pallas_call(
        tracer_kernel,
        name="tracers",
        out_shape=(shape(*flat), shape(*flat), shape(*flat), shape(*full), shape(*full), shape(*full), shape(*full)),
        in_specs=[any_spec] * 13 + [smem_spec],
        out_specs=(any_spec,) * 7,
        scratch_shapes=[
            vm(4, LEVELS, 2, 2, PR, LN), vm(LEVELS + 1, 2, ROWS, 2 * LN), vm(LEVELS + 1, 2, ROWS, 2 * LN), vm(2, 2, 2, ROWS, LN),
            vm(*full), vm(*full), vm(3, 2, ROWS, 2 * LN), vm(2, 2, 2, ROWS, LN), vm(3, 2, ROWS, LN),
            vm(NCH, PR, LN), vm(2, NCH, 2, 4, PAIRS, LN),
            dma(LEVELS // TC, 10), dma(4), dma(NCH, 2), dma(LEVELS // TC, 2), dma(3), dma(3),
        ],
        compiler_params=pltpu.CompilerParams(vmem_limit_bytes=67043328),
    )

    def local_step(vel_x, vel_y, pot_temp, salinity, surf_eta, trans_x, trans_y, col_depth, wet_levels, avg_weights):
        star_x, star_y, eta, tx, ty, corr, kmask, cols, rows = momentum(
            vel_x, vel_y, pot_temp, salinity, surf_eta, trans_x, trans_y, col_depth, wet_levels, avg_weights, jnp.asarray(visc))
        return tracers(vel_x, vel_y, pot_temp, salinity, star_x, star_y, eta, tx, ty, corr, kmask, cols, rows, jnp.asarray(diff))

    spec_3d = P(None, None, "row", "col")
    spec_2d = P(None, "row", "col")
    spec_map = P("row", "col")
    return jax.shard_map(local_step, mesh=mesh, in_specs=(spec_3d, spec_3d, spec_3d, spec_3d, spec_2d, spec_2d, spec_2d, spec_map, spec_map, P()),
                         out_specs=(spec_2d, spec_2d, spec_2d, spec_3d, spec_3d, spec_3d, spec_3d), check_vma=False)
```

```python
import functools
import numpy as np
import jax
import jax.numpy as jnp
from jax import lax
from jax.experimental import pallas as pl
from jax.experimental.pallas import tpu as pltpu
from jax.sharding import PartitionSpec as P

WAVE_COURANT = 0.4
THERM_EXP = 0.2
HALINE_CON = 0.15
PRESS_SCALE = 0.5
VISC_NUMBER = 1.0
DIFF_NUMBER = 0.5

LEVELS = 20
SUBS = 20
CHUNK = 4
NCH = LEVELS // CHUNK
PAIRS = 2 * CHUNK
ROWS = 128
LN = 128
PR = 144
EXT = 192
F32 = jnp.float32
TC = 2
AHEAD = 4
PK = 64
UP = 32
MESH_ID = pl.DeviceIdType.MESH


def solve_table(strength):
    inner = np.zeros(LEVELS)
    last = np.zeros(LEVELS)
    inner[0] = 1.0 + strength
    last[0] = 1.0
    for k in range(1, LEVELS):
        inner[k] = 1.0 + 2.0 * strength - strength**2 / inner[k - 1]
        last[k] = 1.0 + strength - strength**2 / inner[k - 1]
    ratio = strength / inner
    before = np.concatenate([[0.0], ratio[:-1]])
    return np.stack([before, ratio, 1.0 / inner, 1.0 / last]).astype(np.float32)


def write_table(table, strength):
    values = solve_table(strength)
    for i in range(values.shape[0]):
        for k in range(LEVELS):
            table[i, k] = values[i, k]


def lanes(rows):
    return lax.broadcasted_iota(jnp.int32, (rows, LN), 1)


def east(tile, following):
    return pltpu.roll(jnp.where(lanes(tile.shape[0]) == 0, following, tile), LN - 1, 1)


def west(tile, previous):
    return pltpu.roll(jnp.where(lanes(tile.shape[0]) == LN - 1, previous, tile), 1, 1)


NEXT = (1, 2, 0)
PREV = (2, 0, 1)


def halo(packed, j):
    return pltpu.roll(packed, LN - 1 - 2 * j, 1)


def east_pair(first, second, edge):
    last = lanes(first.shape[0]) == LN - 1
    a, b = pltpu.roll(first, LN - 1, 1), pltpu.roll(second, LN - 1, 1)
    return jnp.where(last, b, a), jnp.where(last, edge, b)


def west_pair(first, second, edge):
    origin = lanes(first.shape[0]) == 0
    a, b = pltpu.roll(first, 1, 1), pltpu.roll(second, 1, 1)
    return jnp.where(origin, edge, a), jnp.where(origin, a, b)


def momentum_kernel(u_hbm, v_hbm, t_hbm, s_hbm, eta_hbm, tx_hbm, ty_hbm, h_hbm, kmt_hbm, weights_hbm,
                    us_hbm, vs_hbm, eta_out, tx_out, ty_out, corr_out, kmask_out, col_out, rows_out,
                    buf, tu, tv, cu, cv, pbufa, pbufb, pacc, phal, rhoc, gsum, xsum, kmask, kmt, vep, uwp, dup, txb, tyb, corr,
                    send_col, recv_col, send_row, recv_row,
                    xb, sp, rp, xf, sf, rf, hux, huy, ae, aw, an, as_, cc, ebufa, ebufb, dbuf, gbuf, eacc, bacc,
                    ld_sem, xl_sem, cs_sem, cr_sem, xs_sem, xr_sem, fs_sem, fr_sem, st_sem, ot_sem, av_sem, weights, table, w_sem):
    weights_load = pltpu.make_async_copy(weights_hbm, weights, w_sem)
    ku, kv = kmask.at[1], kmask.at[2]
    me_c = lax.axis_index("col")
    me_r = lax.axis_index("row")
    peer = 1 - me_c
    has_n = me_r < 3
    has_s = me_r > 0
    hbm = (u_hbm, v_hbm, t_hbm, s_hbm)

    def loads(c):
        out = []
        for f in range(4):
            for t in range(2):
                out.append(pltpu.make_async_copy(
                    hbm[f].at[pl.ds(c * CHUNK, CHUNK), :, :, pl.ds(t * LN, LN)],
                    buf.at[f, pl.ds(c * CHUNK, CHUNK), :, t, pl.ds(8, ROWS), :], ld_sem.at[c, f * 2 + t]))
        return out

    def map_loads():
        return [pltpu.make_async_copy(kmt_hbm, kmt, xl_sem.at[8])] + [
            pltpu.make_async_copy(h_hbm.at[:, pl.ds(t * LN, LN)], xb.at[1, t, pl.ds(32, ROWS), :], xl_sem.at[t]) for t in range(2)]

    def flow_loads():
        return [pltpu.make_async_copy(ref.at[:, :, pl.ds(t * LN, LN)], xb.at[pl.ds(2 + 2 * i, 2), t, pl.ds(32, ROWS), :], xl_sem.at[2 + 2 * i + t])
                for t in range(2) for i, ref in enumerate((eta_hbm, tx_hbm, ty_hbm))]

    write_table(table, VISC_NUMBER)
    for copy in map_loads() + loads(0) + loads(1) + loads(2) + flow_loads() + loads(3) + loads(4) + [weights_load]:
        copy.start()

    barrier = pltpu.get_barrier_semaphore()

    def greet(col, row):
        pl.semaphore_signal(barrier, inc=1, device_id={"col": col, "row": row}, device_id_type=MESH_ID)

    greet(peer, me_r)

    @pl.when(has_n)
    def _():
        greet(me_c, me_r + 1)
        greet(peer, me_r + 1)

    @pl.when(has_s)
    def _():
        greet(me_c, me_r - 1)
        greet(peer, me_r - 1)

    zrow = jnp.zeros((8, LN), F32)
    for ref, count in ((xb, 8), (xf, 4)):
        for f in range(count):
            for t in range(3):
                ref[f, t, 0:8, :] = zrow
                ref[f, t, EXT - 8:EXT, :] = zrow
    for ref, count in ((rp, 4), (rf, 2)):
        for f in range(count):
            ref[f, 0:8, :] = zrow
            ref[f, EXT - 8:EXT, :] = zrow

    def zero_side(side, lo):
        z24 = jnp.zeros((24, LN), F32)
        for f in range(8):
            for t in range(2):
                xb[f, t, lo:lo + 24, :] = z24
        for f in range(4):
            rp[f, lo:lo + 24, :] = z24
            for t in range(2):
                xf[f, t, lo:lo + 24, :] = z24
        for f in range(2):
            rf[f, lo:lo + 24, :] = z24
        for c in range(NCH):
            recv_col[c, 136 * side:136 * side + 8, :] = zrow
            for f in range(4):
                for t in range(2):
                    recv_row[side, c, t, f, :, :] = zrow

    @pl.when(me_r == 0)
    def _():
        zero_side(0, 8)

    @pl.when(me_r == 3)
    def _():
        zero_side(1, 160)

    def zero_planes(i, carry):
        r = pl.multiple_of(i * 16, 16)
        z = jnp.zeros((16, LN), F32)
        for m in range(2):
            for t in range(2):
                pacc[m, t, pl.ds(r, 16), :] = z
            phal[m, pl.ds(r, 16), :] = z
        return carry
    lax.fori_loop(0, PR // 16, zero_planes, 0)

    def zero_planes2(i, carry):
        r = pl.multiple_of(i * 16, 16)
        z = jnp.zeros((16, LN), F32)
        for m in range(2):
            for t in range(2):
                for f in range(2):
                    gsum[f, m, t, pl.ds(r, 16), :] = z
                    xsum[f, m, t, pl.ds(r, 16), :] = z
                for ref in (cu, cv):
                    ref[m, t, pl.ds(r, 16), :] = z
                for ref in (tu, tv):
                    ref[LEVELS, m, t, pl.ds(r, 16), :] = z
        return carry
    lax.fori_loop(0, ROWS // 16, zero_planes2, 0)

    for copy in map_loads():
        copy.wait()
    for t in range(2):
        for r in range(0, ROWS, 64):
            level_count = kmt[r:r + 64, t * LN:(t + 1) * LN].astype(F32)
            xb[0, t, 32 + r:96 + r, :] = level_count
            kmask[0, t, r:r + 64, :] = level_count

    def remote(src, dst, ssem, rsem, col, row):
        return pltpu.make_async_remote_copy(src_ref=src, dst_ref=dst, send_sem=ssem, recv_sem=rsem,
                                            device_id={"col": col, "row": row}, device_id_type=MESH_ID)

    def wide_rows(own, first, count, ssem, rsem, slot):
        fields = pl.ds(first, count)
        return ((remote(own.at[fields, pl.ds(0, 2), pl.ds(136, 24), :], own.at[fields, pl.ds(0, 2), pl.ds(8, 24), :],
                        ssem.at[slot], rsem.at[slot], me_c, me_r + 1),),
                (remote(own.at[fields, pl.ds(0, 2), pl.ds(32, 24), :], own.at[fields, pl.ds(0, 2), pl.ds(160, 24), :],
                        ssem.at[slot + 1], rsem.at[slot + 1], me_c, me_r - 1),))

    def wide_copies(own, first, count, packed, landing, ssem, rsem):
        side = remote(packed, landing.at[:, pl.ds(32, ROWS), :], ssem.at[0], rsem.at[0], peer, me_r)
        up, down = wide_rows(own, first, count, ssem, rsem, 1)
        up += (remote(packed.at[:, pl.ds(104, 24), :], landing.at[:, pl.ds(8, 24), :], ssem.at[3], rsem.at[3], peer, me_r + 1),)
        down += (remote(packed.at[:, pl.ds(0, 24), :], landing.at[:, pl.ds(160, 24), :], ssem.at[4], rsem.at[4], peer, me_r - 1),)
        return side, up, down

    def map_copies():
        return (None, *wide_rows(xb, 0, 2, xs_sem, xr_sem, 5))

    def flow_copies():
        return wide_copies(xb, 2, 6, sp, rp, xs_sem, xr_sem)

    def force_copies():
        return wide_copies(xf, 0, 4, sf, rf, fs_sem, fr_sem)

    def edge_copies(c):
        north, south = me_r + 1, me_r - 1
        side = remote(send_col.at[c], recv_col.at[c, pl.ds(8, ROWS), :], cs_sem.at[c, 0], cr_sem.at[c, 0], peer, me_r)
        up = (remote(send_row.at[0, c], recv_row.at[0, c], cs_sem.at[c, 1], cr_sem.at[c, 1], me_c, north),
              remote(send_col.at[c, pl.ds(ROWS - 8, 8), :], recv_col.at[c, pl.ds(0, 8), :], cs_sem.at[c, 2], cr_sem.at[c, 2], peer, north))
        down = (remote(send_row.at[1, c], recv_row.at[1, c], cs_sem.at[c, 3], cr_sem.at[c, 3], me_c, south),
                remote(send_col.at[c, pl.ds(0, 8), :], recv_col.at[c, pl.ds(8 + ROWS, 8), :], cs_sem.at[c, 4], cr_sem.at[c, 4], peer, south))
        return side, up, down

    def start_all(copies):
        side, up, down = copies
        if side is not None:
            side.start()

        @pl.when(has_n)
        def _():
            for copy in up:
                copy.start()

        @pl.when(has_s)
        def _():
            for copy in down:
                copy.start()

    def wait_recv_all(copies):
        side, up, down = copies
        if side is not None:
            side.wait_recv()

        @pl.when(has_s)
        def _():
            for copy in up:
                copy.wait_recv()

        @pl.when(has_n)
        def _():
            for copy in down:
                copy.wait_recv()

    def wait_send_all(copies):
        side, up, down = copies
        if side is not None:
            side.wait_send()

        @pl.when(has_n)
        def _():
            for copy in up:
                copy.wait_send()

        @pl.when(has_s)
        def _():
            for copy in down:
                copy.wait_send()

    def all_entered():
        @pl.when((me_r == 0) | (me_r == 3))
        def _():
            pl.semaphore_wait(barrier, 3)

        @pl.when((me_r != 0) & (me_r != 3))
        def _():
            pl.semaphore_wait(barrier, 5)

    def pack_and_send(c, with_maps=False):
        for copy in loads(c):
            copy.wait()
        lane = lanes(PK)

        def block(i, carry):
            r = pl.multiple_of(i * PK, PK)
            pairs = [(f, c * CHUNK + kk, m) for f in range(4) for kk in range(CHUNK) for m in range(2)]
            column = [[buf[f, k, m, t, pl.ds(8 + r, PK), :] for f, k, m in pairs] for t in range(2)]
            if with_maps:
                for t in range(2):
                    column[t] += [xb[0, t, pl.ds(32 + r, PK), :], xb[1, t, pl.ds(32 + r, PK), :]]
            packed = jnp.zeros((PK, LN), F32)
            count = len(column[0])
            for i in range(count + 1):
                edge = jnp.where(lane == 0, column[0][min(i, count - 1)], column[1][max(i - 1, 0)])
                edge = pltpu.roll(edge, 2 * i, 1) if i else edge
                packed = jnp.where(lane >= 2 * i - 1, edge, packed) if i else edge
            send_col[c, pl.ds(r, PK), :] = packed
            return carry
        for kk in range(CHUNK):
            for m in range(2):
                jj = kk * 2 + m
                k = c * CHUNK + kk
                for side, row in ((0, 8 + ROWS - 1), (1, 8)):
                    for f in range(4):
                        for t in range(2):
                            send_row[side, c, t, f, jj:jj + 1, :] = buf[f, k, m, t, row:row + 1, :]
        lax.fori_loop(0, ROWS // PK, block, 0)
        if with_maps:
            all_entered()
            start_all(map_copies())
        start_all(edge_copies(c))

    pack_and_send(0, with_maps=True)

    def pack_pairs(source, firsts, seconds, send):
        lane = lanes(ROWS)
        outer = (lane < 32) | (lane >= 96)
        for slot, (f, g) in enumerate(zip(firsts, seconds)):
            a, b = (jnp.where(lane < 64, source[n, 0, 32:32 + ROWS, :], source[n, 1, 32:32 + ROWS, :]) for n in (f, g))
            send[slot, :, :] = jnp.where(outer, a, pltpu.roll(b, 64, 1))

    def pack_wide():
        for copy in flow_loads():
            copy.wait()
        pack_pairs(xb, (0, 2, 4, 6), (1, 3, 5, 7), sp)
        start_all(flow_copies())

    def pack_rest(c, carry):
        pack_and_send(c)
        return carry
    lax.fori_loop(1, NCH - 1, pack_rest, 0)

    RHO_T = np.float32(-THERM_EXP * PRESS_SCALE / LEVELS / 2)
    RHO_S = np.float32(HALINE_CON * PRESS_SCALE / LEVELS / 2)
    BR = 128
    SB = 16

    def pressure_rows(k, slot, base, rows):
        for m in range(2):
            for t in range(2):
                half = RHO_T * buf[2, k, m, t, pl.ds(base, rows), :] + RHO_S * buf[3, k, m, t, pl.ds(base, rows), :]
                p = pacc[m, t, pl.ds(base, rows), :] + half
                slot[m, t, pl.ds(base, rows), :] = p
                pacc[m, t, pl.ds(base, rows), :] = p + half

    def shift_u(c, kk, m, base, rows):
        u = [buf[0, c * CHUNK + kk, m, t, pl.ds(base, rows), :] for t in range(2)]
        edge = halo(recv_col[c, pl.ds(base, rows), :], kk * 2 + m)
        ue, uw = east_pair(*u, edge), west_pair(*u, edge)
        for t in range(2):
            uwp[m, t, pl.ds(base, rows), :] = uw[t]
            dup[m, t, pl.ds(base, rows), :] = ue[t] - uw[t]

    def level(c, kk, now, later):
        k = c * CHUNK + kk
        pressure_rows(k, now, 8 + ROWS, 8)
        for m in range(2):
            shift_u(c, kk, m, 8, 8)
            ve = east_pair(*(buf[1, k, m, t, 0:8, :] for t in range(2)), halo(recv_col[c, 0:8, :], PAIRS + kk * 2 + m))
            for t in range(2):
                vep[m, t, 0:8, :] = ve[t]
        level_no = k.astype(F32)
        before = table[0, k]
        following = jnp.minimum(k + 1, LEVELS - 1)

        def block(i, carry):
            for q in range(0, BR, SB):
                piece(pl.multiple_of(i * BR + q, SB), pl.multiple_of(8 + i * BR + q, 8))
            return carry

        def piece(r, b):
            wet_x = [ku[t, pl.ds(r, SB), :] > level_no for t in range(2)]
            wet_y = [kv[t, pl.ds(r, SB), :] > level_no for t in range(2)]
            packed = recv_col[c, pl.ds(b, SB), :]
            packed_r = rhoc[pl.ds(r, SB), :]
            for m in range(2):
                j = kk * 2 + m
                shift_u(c, kk, m, pl.multiple_of(b + 8, 8), SB)
                half = halo(packed_r, j)
                p_edge = phal[m, pl.ds(r, SB), :] + half
                phal[m, pl.ds(r, SB), :] = p_edge + half
                v = [buf[1, k, m, t, pl.ds(b, SB), :] for t in range(2)]
                p = [now[m, t, pl.ds(b, SB), :] for t in range(2)]
                v_edge = halo(packed, PAIRS + j)
                ve, vw = east_pair(*v, v_edge), west_pair(*v, v_edge)
                pe = east_pair(*p, p_edge)
                for t in range(2):
                    vep[m, t, pl.ds(b, SB), :] = ve[t]
                    u = buf[0, k, m, t, pl.ds(b, SB), :]
                    un = buf[0, k, m, t, pl.ds(b + 1, SB), :]
                    us = buf[0, k, m, t, pl.ds(b - 1, SB), :]
                    vs = buf[1, k, m, t, pl.ds(b - 1, SB), :]
                    vn = buf[1, k, m, t, pl.ds(b + 1, SB), :]
                    pn = now[m, t, pl.ds(b + 1, SB), :]
                    w = (v[t] + vs) + (ve[t] + vep[m, t, pl.ds(b - 1, SB), :])
                    z = (u + un) + (uwp[m, t, pl.ds(b, SB), :] + uwp[m, t, pl.ds(b + 1, SB), :])
                    gu = (p[t] - pe[t]) - (0.5 * u) * dup[m, t, pl.ds(b, SB), :] - (0.125 * w) * (un - us)
                    gu = jnp.where(wet_x[t], gu, 0.0)
                    gsum[0, m, t, pl.ds(r, SB), :] += gu
                    new = u + gu + before * cu[m, t, pl.ds(r, SB), :]
                    cu[m, t, pl.ds(r, SB), :] = new
                    tu[k, m, t, pl.ds(r, SB), :] = new
                    gv = (p[t] - pn) - (0.125 * z) * (ve[t] - vw[t]) - (0.5 * v[t]) * (vn - vs)
                    gv = jnp.where(wet_y[t], gv, 0.0)
                    gsum[1, m, t, pl.ds(r, SB), :] += gv
                    new = v[t] + gv + before * cv[m, t, pl.ds(r, SB), :]
                    cv[m, t, pl.ds(r, SB), :] = new
                    tv[k, m, t, pl.ds(r, SB), :] = new
            pressure_rows(following, later, b, SB)
        lax.fori_loop(0, ROWS // BR, block, 0)

    def first_pressure(i, carry):
        pressure_rows(0, pbufa, pl.multiple_of(8 + i * 64, 8), 64)
        return carry
    lax.fori_loop(0, 2, first_pressure, 0)

    def chunk_step(c, carry):
        @pl.when(c == 1)
        def _():
            pack_and_send(NCH - 1)

        @pl.when(c == 2)
        def _():
            pack_wide()

        wait_recv_all(edge_copies(c))

        @pl.when(c == 0)
        def _():
            face_maps()

        for kk in range(CHUNK):
            k = c * CHUNK + kk
            for m in range(2):
                jj = kk * 2 + m
                for side, row in ((0, 7), (1, 8 + ROWS)):
                    for f in range(4):
                        for t in range(2):
                            buf[f, k, m, t, row:row + 1, :] = recv_row[side, c, t, f, jj:jj + 1, :]
        packed = recv_col[c, 8:8 + ROWS, :]
        rhoc[...] = RHO_T * pltpu.roll(packed, LN - 4 * PAIRS, 1) + RHO_S * pltpu.roll(packed, LN - 6 * PAIRS, 1)

        def two_levels(h, carry2):
            level(c, 2 * h, pbufa, pbufb)
            level(c, 2 * h + 1, pbufb, pbufa)
            return carry2
        lax.fori_loop(0, CHUNK // 2, two_levels, 0)
        return carry

    def face_maps():
        wait_recv_all(map_copies())

        def maps(i, carry):
            r = pl.multiple_of(i * 64, 64)
            packed = recv_col[0, pl.ds(8 + r, 64), :]
            kt = [xb[0, t, pl.ds(32 + r, 64), :] for t in range(2)]
            ht = [xb[1, t, pl.ds(32 + r, 64), :] for t in range(2)]
            ke = east_pair(*kt, halo(packed, 4 * PAIRS))
            he = east_pair(*ht, halo(packed, 4 * PAIRS + 1))
            for t in range(2):
                kx = jnp.minimum(kt[t], ke[t])
                ky = jnp.minimum(kt[t], xb[0, t, pl.ds(33 + r, 64), :])
                ku[t, pl.ds(r, 64), :] = kx
                kv[t, pl.ds(r, 64), :] = ky
                hux[t, pl.ds(32 + r, 64), :] = jnp.where(kx > 0.0, 0.5 * (ht[t] + he[t]), 0.0)
                huy[t, pl.ds(32 + r, 64), :] = jnp.where(ky > 0.0, 0.5 * (ht[t] + xb[1, t, pl.ds(33 + r, 64), :]), 0.0)
            return carry
        lax.fori_loop(0, 2, maps, 0)

    lax.fori_loop(0, NCH, chunk_step, 0)

    packet_copies = [pltpu.make_async_copy(src, dst, ot_sem.at[i]) for i, (src, dst) in enumerate(
        ((recv_col, col_out), (recv_row, rows_out), (kmask, kmask_out)))]
    for copy in packet_copies:
        copy.start()

    def forcing(i, carry):
        r = pl.multiple_of(i * 32, 32)
        for t in range(2):
            nx = jnp.maximum(ku[t, pl.ds(r, 32), :], 1.0)
            ny = jnp.maximum(kv[t, pl.ds(r, 32), :], 1.0)
            fx = hux[t, pl.ds(32 + r, 32), :] / nx / SUBS
            fy = huy[t, pl.ds(32 + r, 32), :] / ny / SUBS
            for m in range(2):
                xf[m, t, pl.ds(32 + r, 32), :] = fx * gsum[0, m, t, pl.ds(r, 32), :]
                xf[2 + m, t, pl.ds(32 + r, 32), :] = fy * gsum[1, m, t, pl.ds(r, 32), :]
        return carry
    lax.fori_loop(0, ROWS // 32, forcing, 0)
    pack_pairs(xf, (0, 1), (2, 3), sf)
    start_all(force_copies())

    def stores(c):
        out = []
        for f, (ref, dst) in enumerate(((tu, us_hbm), (tv, vs_hbm))):
            for t in range(2):
                out.append(pltpu.make_async_copy(ref.at[pl.ds(c * CHUNK, CHUNK), :, t, :, :],
                                                 dst.at[pl.ds(c * CHUNK, CHUNK), :, :, pl.ds(t * LN, LN)], st_sem.at[c, f * 2 + t]))
        return out

    def upward(step, carry):
        c = NCH - 1 - step

        def block(i, carry2):
            r = pl.multiple_of(i * UP, UP)
            for f, (ref, kp) in enumerate(((tu, ku), (tv, kv))):
                for t in range(2):
                    depth = kp[t, pl.ds(r, UP), :]
                    below = [ref[c * CHUNK + CHUNK, m, t, pl.ds(r, UP), :] for m in range(2)]
                    total = [xsum[f, m, t, pl.ds(r, UP), :] for m in range(2)]
                    for kk in range(CHUNK - 1, -1, -1):
                        k = c * CHUNK + kk
                        level_no = k.astype(F32)
                        inv = jnp.where(depth > level_no + 1.0, table[2, k], jnp.where(depth > level_no, table[3, k], 0.0))
                        for m in range(2):
                            below[m] = ref[k, m, t, pl.ds(r, UP), :] * inv + table[1, k] * below[m]
                            ref[k, m, t, pl.ds(r, UP), :] = below[m]
                            total[m] = total[m] + below[m]
                    for m in range(2):
                        xsum[f, m, t, pl.ds(r, UP), :] = total[m]
            return carry2
        lax.fori_loop(0, ROWS // UP, block, 0)
        for copy in stores(c):
            copy.start()
        return carry
    lax.fori_loop(0, NCH, upward, 0)

    wait_recv_all(flow_copies())

    def unpack_wide(i, carry):
        r = pl.multiple_of(i * 96, 32)
        for pair in range(4):
            tile = rp[pair, pl.ds(r, 96), :]
            xb[2 * pair, 2, pl.ds(r, 96), :] = tile
            xb[2 * pair + 1, 2, pl.ds(r, 96), :] = pltpu.roll(tile, 64, 1)
        return carry
    lax.fori_loop(0, EXT // 96, unpack_wide, 0)

    XR = 88

    def depths(i, carry):
        r = pl.multiple_of(8 + i * XR, 8)
        kt = [xb[0, t, pl.ds(r, XR), :] for t in range(3)]
        ht = [xb[1, t, pl.ds(r, XR), :] for t in range(3)]
        for t in range(3):
            kx = jnp.minimum(kt[t], east(kt[t], kt[NEXT[t]]))
            ky = jnp.minimum(kt[t], xb[0, t, pl.ds(r + 1, XR), :])
            hux[t, pl.ds(r, XR), :] = jnp.where(kx > 0.0, 0.5 * (ht[t] + east(ht[t], ht[NEXT[t]])), 0.0)
            huy[t, pl.ds(r, XR), :] = jnp.where(ky > 0.0, 0.5 * (ht[t] + xb[1, t, pl.ds(r + 1, XR), :]), 0.0)
            cc[t, pl.ds(r, XR), :] = jnp.where(kt[t] > 0.0, WAVE_COURANT, 0.0)
        return carry
    for t in range(3):
        for ref in (hux, huy):
            ref[t, 0:8, :] = zrow
        for ref in (ebufa, ebufb):
            for m in range(2):
                ref[m, t, 0:8, :] = zrow
                ref[m, t, EXT - 8:EXT, :] = zrow
    lax.fori_loop(0, 2, depths, 0)

    def coefficients(i, carry):
        r = pl.multiple_of(8 + i * XR, 8)
        hx = [hux[t, pl.ds(r, XR), :] for t in range(3)]
        for t in range(3):
            c0 = cc[t, pl.ds(r, XR), :]
            cw = WAVE_COURANT * c0
            ae[t, pl.ds(r, XR), :] = cw * hx[t]
            aw[t, pl.ds(r, XR), :] = cw * west(hx[t], hx[PREV[t]])
            an[t, pl.ds(r, XR), :] = cw * huy[t, pl.ds(r, XR), :]
            as_[t, pl.ds(r, XR), :] = cw * huy[t, pl.ds(r - 1, XR), :]
        return carry
    lax.fori_loop(0, 2, coefficients, 0)

    def first_subcycle(m, base, rows):
        tx = [xb[4 + m, t, pl.ds(base, rows), :] for t in range(3)]
        for t in range(3):
            c0 = cc[t, pl.ds(base, rows), :]
            ty = xb[6 + m, t, pl.ds(base, rows), :]
            div = tx[t] - west(tx[t], tx[PREV[t]]) + ty - xb[6 + m, t, pl.ds(base - 1, rows), :]
            change = -c0 * div
            dbuf[m, t, pl.ds(base, rows), :] = change
            eta = jnp.where(c0 > 0.0, xb[2 + m, t, pl.ds(base, rows), :], 0.0) + change
            ebufa[m, t, pl.ds(base, rows), :] = eta

    def first_block(i, carry):
        for m in range(2):
            first_subcycle(m, pl.multiple_of(8 + i * XR, 8), XR)
        return carry
    lax.fori_loop(0, 2, first_block, 0)

    weights_load.wait()
    whole = weights[SUBS - 1]
    moment = weights[SUBS - 1]
    for n in range(SUBS - 2, -1, -1):
        whole = whole + weights[n]
        moment = moment + whole

    def first_sums(i, carry):
        r = pl.multiple_of(i * 8, 8)
        for m in range(2):
            for t in range(3):
                eta = ebufa[m, t, pl.ds(32 + r, 8), :]
                bacc[m, t, pl.ds(r, 8), :] = whole * eta
                if t < 2:
                    eacc[m, t, pl.ds(r, 8), :] = weights[0] * eta
        return carry
    lax.fori_loop(0, 17, first_sums, 0)

    wait_recv_all(force_copies())

    def unpack_force(i, carry):
        r = pl.multiple_of(i * 96, 32)
        for m in range(2):
            tile = rf[m, pl.ds(r, 96), :]
            xf[m, 2, pl.ds(r, 96), :] = tile
            xf[2 + m, 2, pl.ds(r, 96), :] = pltpu.roll(tile, 64, 1)
        return carry
    lax.fori_loop(0, EXT // 96, unpack_force, 0)

    def forcing_divergence(i, carry):
        r = pl.multiple_of(8 + i * XR, 8)
        for m in range(2):
            fx = [xf[m, t, pl.ds(r, XR), :] for t in range(3)]
            for t in range(3):
                div = fx[t] - west(fx[t], fx[PREV[t]]) + xf[2 + m, t, pl.ds(r, XR), :] - xf[2 + m, t, pl.ds(r - 1, XR), :]
                gbuf[m, t, pl.ds(r, XR), :] = cc[t, pl.ds(r, XR), :] * div
        return carry
    lax.fori_loop(0, 2, forcing_divergence, 0)

    def subcycle(n, tail, lo, hi, old, new):
        tail = tail - weights[n - 2]
        weight = weights[n - 1]
        for r, end in ((lo, 96), (96, hi)):
            first = max(r, 32)
            for t in range(3):
                c_e, c_w = ae[t, r:end, :], aw[t, r:end, :]
                c_n, c_s = an[t, r:end, :], as_[t, r:end, :]
                for m in range(2):
                    e = old[m, t, r:end, :]
                    to_e = east(e, old[m, NEXT[t], r:end, :])
                    to_w = west(e, old[m, PREV[t], r:end, :])
                    to_n = old[m, t, r + 1:end + 1, :]
                    to_s = old[m, t, r - 1:end - 1, :]
                    d = dbuf[m, t, r:end, :] - gbuf[m, t, r:end, :]
                    d = d + (c_e * (to_e - e) + c_w * (to_w - e)) + (c_n * (to_n - e) + c_s * (to_s - e))
                    dbuf[m, t, r:end, :] = d
                    e = e + d
                    new[m, t, r:end, :] = e
                    last = min(end, 168)
                    bacc[m, t, first - 32:last - 32, :] += tail * e[first - r:last - r]
                    if t < 2:
                        last = min(end, 160)
                        eacc[m, t, first - 32:last - 32, :] += weight * e[first - r:last - r]
        return tail

    tail = subcycle(2, whole, 8, 184, ebufa, ebufb)
    for first_n, steps, lo, hi in ((3, 1, 8, 184), (5, 4, 16, 176), (13, 4, 24, 168)):
        def two_cycles(h, carry, first_n=first_n, lo=lo, hi=hi):
            n = first_n + 2 * h
            carry = subcycle(n, carry, lo, hi, ebufb, ebufa)
            return subcycle(n + 1, carry, lo, hi, ebufa, ebufb)
        tail = lax.fori_loop(0, steps, two_cycles, tail)

    eta_copies = [pltpu.make_async_copy(eacc.at[:, t, pl.ds(0, ROWS), :], eta_out.at[:, :, pl.ds(t * LN, LN)], ot_sem.at[4 + t]) for t in range(2)]
    for copy in eta_copies:
        copy.start()

    AV = 64

    def average_copies(i):
        r = pl.multiple_of(i * AV, AV)
        return [pltpu.make_async_copy(src, dst, av_sem.at[i, n]) for n, (src, dst) in enumerate((
            (txb.at[:, pl.ds(r, AV), :], tx_out.at[:, pl.ds(r, AV), :]), (tyb.at[:, pl.ds(r, AV), :], ty_out.at[:, pl.ds(r, AV), :]),
            (corr.at[:, :, :, pl.ds(r, AV), :], corr_out.at[:, :, :, pl.ds(r, AV), :])))]

    def averages(i, carry):
        for q in range(0, AV, 16):
            r = pl.multiple_of(i * AV + q, 16)
            g = pl.multiple_of(32 + i * AV + q, 16)
            for t in range(2):
                depth_x = hux[t, pl.ds(g, 16), :]
                depth_y = huy[t, pl.ds(g, 16), :]
                kx = ku[t, pl.ds(r, 16), :]
                ky = kv[t, pl.ds(r, 16), :]
                inv_x = 1.0 / (depth_x + jnp.where(kx > 0.0, 0.0, 1.0))
                inv_y = 1.0 / (depth_y + jnp.where(ky > 0.0, 0.0, 1.0))
                mean_x = 1.0 / jnp.maximum(kx, 1.0)
                mean_y = 1.0 / jnp.maximum(ky, 1.0)
                for m in range(2):
                    lane = slice(t * LN, (t + 1) * LN)
                    acc = bacc[m, t, pl.ds(r, 16), :]
                    tx = whole * xb[4 + m, t, pl.ds(g, 16), :] + moment * xf[m, t, pl.ds(g, 16), :] \
                        - WAVE_COURANT * depth_x * (east(acc, bacc[m, NEXT[t], pl.ds(r, 16), :]) - acc)
                    ty = whole * xb[6 + m, t, pl.ds(g, 16), :] + moment * xf[2 + m, t, pl.ds(g, 16), :] \
                        - WAVE_COURANT * depth_y * (bacc[m, t, pl.ds(r + 1, 16), :] - acc)
                    tx = jnp.where(kx > 0.0, tx, 0.0)
                    ty = jnp.where(ky > 0.0, ty, 0.0)
                    txb[m, pl.ds(r, 16), lane] = tx
                    tyb[m, pl.ds(r, 16), lane] = ty
                    corr[0, m, t, pl.ds(r, 16), :] = tx * inv_x - xsum[0, m, t, pl.ds(r, 16), :] * mean_x
                    corr[1, m, t, pl.ds(r, 16), :] = ty * inv_y - xsum[1, m, t, pl.ds(r, 16), :] * mean_y
        for copy in average_copies(i):
            copy.start()
        return carry
    lax.fori_loop(0, ROWS // AV, averages, 0)

    wait_send_all(map_copies())
    wait_send_all(flow_copies())
    wait_send_all(force_copies())
    for copy in packet_copies + eta_copies:
        copy.wait()
    for i in range(ROWS // AV):
        for copy in average_copies(i):
            copy.wait()

    def drain(c, carry):
        wait_send_all(edge_copies(c))
        for copy in stores(c):
            copy.wait()
        return carry
    lax.fori_loop(0, NCH, drain, 0)


def tracer_kernel(u_hbm, v_hbm, t_hbm, s_hbm, us_hbm, vs_hbm, eta_in, tx_in, ty_in, corr_in, kmask_in, col_in, rows_in,
                  eta_hbm, tx_hbm, ty_hbm, un_hbm, vn_hbm, tn_hbm, sn_hbm,
                  buf, tt, ts, ct, su, sv, small, corr, kmask, cols, rows, ld_sem, ed_sem, st_sem, sv_sem, in_sem, out_sem, table):
    hbm = (u_hbm, v_hbm, t_hbm, s_hbm)
    sources = (eta_in, tx_in, ty_in)
    sinks = (eta_hbm, tx_hbm, ty_hbm)

    def loads(c):
        out = []
        for f in range(4):
            for t in range(2):
                out.append(pltpu.make_async_copy(
                    hbm[f].at[pl.ds(c * TC, TC), :, :, pl.ds(t * LN, LN)],
                    buf.at[f, pl.ds(c * TC, TC), :, t, pl.ds(8, ROWS), :], ld_sem.at[c, f * 2 + t]))
        for f, (src, dst) in enumerate(((us_hbm, su), (vs_hbm, sv))):
            out.append(pltpu.make_async_copy(src.at[pl.ds(c * TC, TC)], dst.at[pl.ds(c * TC, TC)], ld_sem.at[c, 8 + f]))
        return out

    def stores_v(c):
        return [pltpu.make_async_copy(src.at[pl.ds(c * TC, TC)], dst.at[pl.ds(c * TC, TC)], sv_sem.at[c, f])
                for f, (src, dst) in enumerate(((su, un_hbm), (sv, vn_hbm)))]

    def stores_t(c):
        return [pltpu.make_async_copy(src.at[pl.ds(c * CHUNK, CHUNK)], dst.at[pl.ds(c * CHUNK, CHUNK)], st_sem.at[c, f])
                for f, (src, dst) in enumerate(((tt, tn_hbm), (ts, sn_hbm)))]

    edges = [pltpu.make_async_copy(src, dst, ed_sem.at[i])
             for i, (src, dst) in enumerate(((col_in, cols), (rows_in, rows), (corr_in, corr), (kmask_in, kmask)))]
    for copy in edges:
        copy.start()
    for c in range(AHEAD):
        for copy in loads(c):
            copy.start()
    write_table(table, DIFF_NUMBER)
    small_in = [pltpu.make_async_copy(sources[i], small.at[i], in_sem.at[i]) for i in range(3)]
    small_out = [pltpu.make_async_copy(small.at[i], sinks[i], out_sem.at[i]) for i in range(3)]
    for copy in small_in:
        copy.start()

    def zero_planes(i, carry):
        r = pl.multiple_of(i * 16, 16)
        z = jnp.zeros((16, 2 * LN), F32)
        for f in range(2):
            for m in range(2):
                for t in range(2):
                    ct[f, m, t, pl.ds(r, 16), :] = z[:, :LN]
        for m in range(2):
            for ref in (tt, ts):
                ref[LEVELS, m, pl.ds(r, 16), :] = z
        return carry
    lax.fori_loop(0, ROWS // 16, zero_planes, 0)
    for copy in edges:
        copy.wait()

    BR = 128
    SB = 16

    def level(k, c, kk):
        level_no = k.astype(F32)
        before = table[0, k]

        def block(i, carry):
            for q in range(0, BR, SB):
                piece(pl.multiple_of(i * BR + q, SB), pl.multiple_of(8 + i * BR + q, 8))
            return carry

        def piece(r, b):
            wet = [kmask[0, t, pl.ds(r, SB), :] > level_no for t in range(2)]
            packed = cols[c, pl.ds(b, SB), :]
            for m in range(2):
                j = kk * 2 + m
                u = [buf[0, k, m, t, pl.ds(b, SB), :] for t in range(2)]
                v = [buf[1, k, m, t, pl.ds(b, SB), :] for t in range(2)]
                vs = [buf[1, k, m, t, pl.ds(b - 1, SB), :] for t in range(2)]
                uw = west_pair(*u, halo(packed, j))
                for f, ref in ((2, tt), (3, ts)):
                    q = [buf[f, k, m, t, pl.ds(b, SB), :] for t in range(2)]
                    edge = halo(packed, f * PAIRS + j)
                    qe, qw = east_pair(*q, edge), west_pair(*q, edge)
                    for t in range(2):
                        lane = slice(t * LN, (t + 1) * LN)
                        fy = v[t] * (q[t] + buf[f, k, m, t, pl.ds(b + 1, SB), :])
                        fs = vs[t] * (q[t] + buf[f, k, m, t, pl.ds(b - 1, SB), :])
                        adv = q[t] - 0.5 * ((u[t] * (q[t] + qe[t]) - uw[t] * (q[t] + qw[t])) + (fy - fs))
                        adv = jnp.where(wet[t], adv, 0.0)
                        new = adv + before * ct[f - 2, m, t, pl.ds(r, SB), :]
                        ct[f - 2, m, t, pl.ds(r, SB), :] = new
                        ref[k, m, pl.ds(r, SB), lane] = new
            for t in range(2):
                lane = slice(t * LN, (t + 1) * LN)
                wet_x = kmask[1, t, pl.ds(r, SB), :] > level_no
                wet_y = kmask[2, t, pl.ds(r, SB), :] > level_no
                for m in range(2):
                    su[k, m, pl.ds(r, SB), lane] = jnp.where(wet_x, su[k, m, pl.ds(r, SB), lane] + corr[0, m, t, pl.ds(r, SB), :], 0.0)
                    sv[k, m, pl.ds(r, SB), lane] = jnp.where(wet_y, sv[k, m, pl.ds(r, SB), lane] + corr[1, m, t, pl.ds(r, SB), :], 0.0)
        lax.fori_loop(0, ROWS // BR, block, 0)

    def chunk_step(c, carry):
        @pl.when(c + AHEAD < LEVELS // TC)
        def _():
            for copy in loads(c + AHEAD):
                copy.start()

        for copy in loads(c):
            copy.wait()
        packet = c // (CHUNK // TC)
        first = lax.rem(c, CHUNK // TC) * TC
        for kk in range(TC):
            k = c * TC + kk
            for m in range(2):
                jj = (first + kk) * 2 + m
                for f in (1, 2, 3):
                    for t in range(2):
                        buf[f, k, m, t, 7:8, :] = rows[0, packet, t, f, pl.ds(jj, 1), :]
                for f in (2, 3):
                    for t in range(2):
                        buf[f, k, m, t, 8 + ROWS:9 + ROWS, :] = rows[1, packet, t, f, pl.ds(jj, 1), :]

        def one_level(kk, carry2):
            level(c * TC + kk, packet, first + kk)
            return carry2
        lax.fori_loop(0, TC, one_level, 0)
        for copy in stores_v(c):
            copy.start()
        return carry
    lax.fori_loop(0, LEVELS // TC, chunk_step, 0)

    for copy in small_in:
        copy.wait()
    for copy in small_out:
        copy.start()

    def upward(step, carry):
        c = NCH - 1 - step

        def block(i, carry2):
            r = pl.multiple_of(i * UP, UP)
            for t in range(2):
                lane = slice(t * LN, (t + 1) * LN)
                depth = kmask[0, t, pl.ds(r, UP), :]
                below = [[ref[c * CHUNK + CHUNK, m, pl.ds(r, UP), lane] for m in range(2)] for ref in (tt, ts)]
                for kk in range(CHUNK - 1, -1, -1):
                    k = c * CHUNK + kk
                    level_no = k.astype(F32)
                    inv = jnp.where(depth > level_no + 1.0, table[2, k], jnp.where(depth > level_no, table[3, k], 0.0))
                    for f, ref in enumerate((tt, ts)):
                        for m in range(2):
                            below[f][m] = ref[k, m, pl.ds(r, UP), lane] * inv + table[1, k] * below[f][m]
                            ref[k, m, pl.ds(r, UP), lane] = below[f][m]
            return carry2
        lax.fori_loop(0, ROWS // UP, block, 0)
        for copy in stores_t(c):
            copy.start()
        return carry
    lax.fori_loop(0, NCH, upward, 0)

    for copy in small_out:
        copy.wait()

    def drain(c, carry):
        for copy in stores_t(c):
            copy.wait()
        return carry
    lax.fori_loop(0, NCH, drain, 0)

    def drain_v(c, carry):
        for copy in stores_v(c):
            copy.wait()
        return carry
    lax.fori_loop(0, LEVELS // TC, drain_v, 0)


def solution(mesh):
    assert mesh.shape["col"] == 2 and mesh.shape["row"] == 4
    any_spec = pl.BlockSpec(memory_space=pl.ANY)
    shape = lambda *dims: jax.ShapeDtypeStruct(dims, F32)
    dma = lambda *dims: pltpu.SemaphoreType.DMA(dims)
    vm = lambda *dims: pltpu.VMEM(dims, F32)
    full = (LEVELS, 2, ROWS, 2 * LN)
    flat = (2, ROWS, 2 * LN)

    momentum = pl.pallas_call(
        momentum_kernel,
        name="momentum",
        out_shape=(shape(*full), shape(*full), shape(*flat), shape(*flat), shape(*flat), shape(2, 2, 2, ROWS, LN),
                   shape(3, 2, ROWS, LN), shape(NCH, PR, LN), shape(2, NCH, 2, 4, PAIRS, LN)),
        in_specs=[any_spec] * 10,
        out_specs=(any_spec,) * 9,
        scratch_shapes=[
            vm(4, LEVELS, 2, 2, PR, LN), vm(LEVELS + 1, 2, 2, ROWS, LN), vm(LEVELS + 1, 2, 2, ROWS, LN),
            vm(2, 2, ROWS, LN), vm(2, 2, ROWS, LN), vm(2, 2, PR, LN), vm(2, 2, PR, LN), vm(2, 2, PR, LN), vm(2, PR, LN), vm(ROWS, LN),
            vm(2, 2, 2, ROWS, LN), vm(2, 2, 2, ROWS, LN), vm(3, 2, ROWS, LN), pltpu.VMEM((ROWS, 2 * LN), jnp.int32),
            vm(2, 2, PR, LN), vm(2, 2, PR, LN), vm(2, 2, PR, LN), vm(*flat), vm(*flat), vm(2, 2, 2, ROWS, LN),
            vm(NCH, ROWS, LN), vm(NCH, PR, LN), vm(2, NCH, 2, 4, PAIRS, LN), vm(2, NCH, 2, 4, PAIRS, LN),
            vm(8, 3, EXT, LN), vm(4, ROWS, LN), vm(4, EXT, LN), vm(4, 3, EXT, LN), vm(2, ROWS, LN), vm(2, EXT, LN),
            vm(3, EXT, LN), vm(3, EXT, LN), vm(3, EXT, LN), vm(3, EXT, LN), vm(3, EXT, LN), vm(3, EXT, LN), vm(3, EXT, LN),
            vm(2, 3, EXT, LN), vm(2, 3, EXT, LN), vm(2, 3, EXT, LN), vm(2, 3, EXT, LN), vm(2, 2, ROWS + 8, LN), vm(2, 3, ROWS + 8, LN),
            dma(NCH, 8), dma(9), dma(NCH, 5), dma(NCH, 5), dma(7), dma(7), dma(5), dma(5), dma(NCH, 4), dma(6), dma(2, 3),
            pltpu.SMEM((SUBS,), F32), pltpu.SMEM((4, LEVELS), F32), pltpu.SemaphoreType.DMA,
        ],
        compiler_params=pltpu.CompilerParams(collective_id=0, has_side_effects=True, vmem_limit_bytes=67043328),
    )

    tracers = pl.pallas_call(
        tracer_kernel,
        name="tracers",
        out_shape=(shape(*flat), shape(*flat), shape(*flat), shape(*full), shape(*full), shape(*full), shape(*full)),
        in_specs=[any_spec] * 13,
        out_specs=(any_spec,) * 7,
        scratch_shapes=[
            vm(4, LEVELS, 2, 2, PR, LN), vm(LEVELS + 1, 2, ROWS, 2 * LN), vm(LEVELS + 1, 2, ROWS, 2 * LN), vm(2, 2, 2, ROWS, LN),
            vm(*full), vm(*full), vm(3, 2, ROWS, 2 * LN), vm(2, 2, 2, ROWS, LN), vm(3, 2, ROWS, LN),
            vm(NCH, PR, LN), vm(2, NCH, 2, 4, PAIRS, LN),
            dma(LEVELS // TC, 10), dma(4), dma(NCH, 2), dma(LEVELS // TC, 2), dma(3), dma(3), pltpu.SMEM((4, LEVELS), F32),
        ],
        compiler_params=pltpu.CompilerParams(vmem_limit_bytes=67043328),
    )

    def local_step(vel_x, vel_y, pot_temp, salinity, surf_eta, trans_x, trans_y, col_depth, wet_levels, avg_weights):
        star_x, star_y, eta, tx, ty, corr, kmask, cols, rows = momentum(
            vel_x, vel_y, pot_temp, salinity, surf_eta, trans_x, trans_y, col_depth, wet_levels, avg_weights)
        return tracers(vel_x, vel_y, pot_temp, salinity, star_x, star_y, eta, tx, ty, corr, kmask, cols, rows)

    spec_3d = P(None, None, "row", "col")
    spec_2d = P(None, "row", "col")
    spec_map = P("row", "col")
    return jax.shard_map(local_step, mesh=mesh, in_specs=(spec_3d, spec_3d, spec_3d, spec_3d, spec_2d, spec_2d, spec_2d, spec_map, spec_map, P()),
                         out_specs=(spec_2d, spec_2d, spec_2d, spec_3d, spec_3d, spec_3d, spec_3d), check_vma=False)
```

```python
import functools
import numpy as np
import jax
import jax.numpy as jnp
from jax import lax
from jax.experimental import pallas as pl
from jax.experimental.pallas import tpu as pltpu
from jax.sharding import PartitionSpec as P

WAVE_COURANT = 0.4
THERM_EXP = 0.2
HALINE_CON = 0.15
PRESS_SCALE = 0.5
VISC_NUMBER = 1.0
DIFF_NUMBER = 0.5

LEVELS = 20
SUBS = 20
CHUNK = 4
NCH = LEVELS // CHUNK
PAIRS = 2 * CHUNK
ROWS = 128
LN = 128
PR = 144
EXT = 192
F32 = jnp.float32
TC = 2
AHEAD = 6
PK = 64
UP = 32
MESH_ID = pl.DeviceIdType.MESH


def solve_table(strength):
    inner = np.zeros(LEVELS)
    last = np.zeros(LEVELS)
    inner[0] = 1.0 + strength
    last[0] = 1.0
    for k in range(1, LEVELS):
        inner[k] = 1.0 + 2.0 * strength - strength**2 / inner[k - 1]
        last[k] = 1.0 + strength - strength**2 / inner[k - 1]
    ratio = strength / inner
    before = np.concatenate([[0.0], ratio[:-1]])
    return np.stack([before, ratio, 1.0 / inner, 1.0 / last]).astype(np.float32)


def write_table(table, strength):
    values = solve_table(strength)
    for i in range(values.shape[0]):
        for k in range(LEVELS):
            table[i, k] = values[i, k]


def lanes(rows):
    return lax.broadcasted_iota(jnp.int32, (rows, LN), 1)


def east(tile, following):
    return pltpu.roll(jnp.where(lanes(tile.shape[0]) == 0, following, tile), LN - 1, 1)


def west(tile, previous):
    return pltpu.roll(jnp.where(lanes(tile.shape[0]) == LN - 1, previous, tile), 1, 1)


NEXT = (1, 2, 0)
PREV = (2, 0, 1)


def halo(packed, j):
    return pltpu.roll(packed, LN - 1 - 2 * j, 1)


def east_pair(first, second, edge):
    last = lanes(first.shape[0]) == LN - 1
    a, b = pltpu.roll(first, LN - 1, 1), pltpu.roll(second, LN - 1, 1)
    return jnp.where(last, b, a), jnp.where(last, edge, b)


def west_pair(first, second, edge):
    origin = lanes(first.shape[0]) == 0
    a, b = pltpu.roll(first, 1, 1), pltpu.roll(second, 1, 1)
    return jnp.where(origin, edge, a), jnp.where(origin, a, b)


def momentum_kernel(u_hbm, v_hbm, t_hbm, s_hbm, eta_hbm, tx_hbm, ty_hbm, h_hbm, kmt_hbm, weights_hbm,
                    us_hbm, vs_hbm, eta_out, tx_out, ty_out, corr_out, kmask_out, col_out, rows_out,
                    buf, tu, tv, cu, cv, pbufa, pbufb, pacc, phal, rhoc, gsum, xsum, kmask, kmt, vep, uwp, dup, txb, tyb, corr,
                    send_col, recv_col, send_row, recv_row,
                    xb, sp, rp, xf, sf, rf, hux, huy, ae, aw, an, as_, cc, ebufa, ebufb, dbuf, gbuf, eacc, bacc,
                    ld_sem, xl_sem, cs_sem, cr_sem, xs_sem, xr_sem, fs_sem, fr_sem, st_sem, ot_sem, av_sem, weights, table, w_sem):
    weights_load = pltpu.make_async_copy(weights_hbm, weights, w_sem)
    ku, kv = kmask.at[1], kmask.at[2]
    me_c = lax.axis_index("col")
    me_r = lax.axis_index("row")
    peer = 1 - me_c
    has_n = me_r < 3
    has_s = me_r > 0
    hbm = (u_hbm, v_hbm, t_hbm, s_hbm)

    def loads(c):
        out = []
        for f in range(4):
            for t in range(2):
                out.append(pltpu.make_async_copy(
                    hbm[f].at[pl.ds(c * CHUNK, CHUNK), :, :, pl.ds(t * LN, LN)],
                    buf.at[f, pl.ds(c * CHUNK, CHUNK), :, t, pl.ds(8, ROWS), :], ld_sem.at[c, f * 2 + t]))
        return out

    def map_loads():
        return [pltpu.make_async_copy(kmt_hbm, kmt, xl_sem.at[8])] + [
            pltpu.make_async_copy(h_hbm.at[:, pl.ds(t * LN, LN)], xb.at[1, t, pl.ds(32, ROWS), :], xl_sem.at[t]) for t in range(2)]

    def flow_loads():
        return [pltpu.make_async_copy(ref.at[:, :, pl.ds(t * LN, LN)], xb.at[pl.ds(2 + 2 * i, 2), t, pl.ds(32, ROWS), :], xl_sem.at[2 + 2 * i + t])
                for t in range(2) for i, ref in enumerate((eta_hbm, tx_hbm, ty_hbm))]

    write_table(table, VISC_NUMBER)
    for copy in map_loads() + loads(0) + loads(1) + loads(2) + flow_loads() + loads(3) + loads(4) + [weights_load]:
        copy.start()

    barrier = pltpu.get_barrier_semaphore()

    def greet(col, row):
        pl.semaphore_signal(barrier, inc=1, device_id={"col": col, "row": row}, device_id_type=MESH_ID)

    greet(peer, me_r)

    @pl.when(has_n)
    def _():
        greet(me_c, me_r + 1)
        greet(peer, me_r + 1)

    @pl.when(has_s)
    def _():
        greet(me_c, me_r - 1)
        greet(peer, me_r - 1)

    zrow = jnp.zeros((8, LN), F32)
    for ref, count in ((xb, 8), (xf, 4)):
        for f in range(count):
            for t in range(3):
                ref[f, t, 0:8, :] = zrow
                ref[f, t, EXT - 8:EXT, :] = zrow
    for ref, count in ((rp, 4), (rf, 2)):
        for f in range(count):
            ref[f, 0:8, :] = zrow
            ref[f, EXT - 8:EXT, :] = zrow

    def zero_side(side, lo):
        z24 = jnp.zeros((24, LN), F32)
        for f in range(8):
            for t in range(2):
                xb[f, t, lo:lo + 24, :] = z24
        for f in range(4):
            rp[f, lo:lo + 24, :] = z24
            for t in range(2):
                xf[f, t, lo:lo + 24, :] = z24
        for f in range(2):
            rf[f, lo:lo + 24, :] = z24
        for c in range(NCH):
            recv_col[c, 136 * side:136 * side + 8, :] = zrow
            for f in range(4):
                for t in range(2):
                    recv_row[side, c, t, f, :, :] = zrow

    @pl.when(me_r == 0)
    def _():
        zero_side(0, 8)

    @pl.when(me_r == 3)
    def _():
        zero_side(1, 160)

    def zero_planes(i, carry):
        r = pl.multiple_of(i * 16, 16)
        z = jnp.zeros((16, LN), F32)
        for m in range(2):
            for t in range(2):
                pacc[m, t, pl.ds(r, 16), :] = z
            phal[m, pl.ds(r, 16), :] = z
        return carry
    lax.fori_loop(0, PR // 16, zero_planes, 0)

    def zero_planes2(i, carry):
        r = pl.multiple_of(i * 16, 16)
        z = jnp.zeros((16, LN), F32)
        for m in range(2):
            for t in range(2):
                for f in range(2):
                    gsum[f, m, t, pl.ds(r, 16), :] = z
                    xsum[f, m, t, pl.ds(r, 16), :] = z
                for ref in (cu, cv):
                    ref[m, t, pl.ds(r, 16), :] = z
                for ref in (tu, tv):
                    ref[LEVELS, m, t, pl.ds(r, 16), :] = z
        return carry
    lax.fori_loop(0, ROWS // 16, zero_planes2, 0)

    for copy in map_loads():
        copy.wait()
    for t in range(2):
        for r in range(0, ROWS, 64):
            level_count = kmt[r:r + 64, t * LN:(t + 1) * LN].astype(F32)
            xb[0, t, 32 + r:96 + r, :] = level_count
            kmask[0, t, r:r + 64, :] = level_count

    def remote(src, dst, ssem, rsem, col, row):
        return pltpu.make_async_remote_copy(src_ref=src, dst_ref=dst, send_sem=ssem, recv_sem=rsem,
                                            device_id={"col": col, "row": row}, device_id_type=MESH_ID)

    def wide_rows(own, first, count, ssem, rsem, slot):
        fields = pl.ds(first, count)
        return ((remote(own.at[fields, pl.ds(0, 2), pl.ds(136, 24), :], own.at[fields, pl.ds(0, 2), pl.ds(8, 24), :],
                        ssem.at[slot], rsem.at[slot], me_c, me_r + 1),),
                (remote(own.at[fields, pl.ds(0, 2), pl.ds(32, 24), :], own.at[fields, pl.ds(0, 2), pl.ds(160, 24), :],
                        ssem.at[slot + 1], rsem.at[slot + 1], me_c, me_r - 1),))

    def wide_copies(own, first, count, packed, landing, ssem, rsem):
        side = remote(packed, landing.at[:, pl.ds(32, ROWS), :], ssem.at[0], rsem.at[0], peer, me_r)
        up, down = wide_rows(own, first, count, ssem, rsem, 1)
        up += (remote(packed.at[:, pl.ds(104, 24), :], landing.at[:, pl.ds(8, 24), :], ssem.at[3], rsem.at[3], peer, me_r + 1),)
        down += (remote(packed.at[:, pl.ds(0, 24), :], landing.at[:, pl.ds(160, 24), :], ssem.at[4], rsem.at[4], peer, me_r - 1),)
        return side, up, down

    def map_copies():
        return (None, *wide_rows(xb, 0, 2, xs_sem, xr_sem, 5))

    def flow_copies():
        return wide_copies(xb, 2, 6, sp, rp, xs_sem, xr_sem)

    def force_copies():
        return wide_copies(xf, 0, 4, sf, rf, fs_sem, fr_sem)

    def edge_copies(c):
        north, south = me_r + 1, me_r - 1
        side = remote(send_col.at[c], recv_col.at[c, pl.ds(8, ROWS), :], cs_sem.at[c, 0], cr_sem.at[c, 0], peer, me_r)
        up = (remote(send_row.at[0, c], recv_row.at[0, c], cs_sem.at[c, 1], cr_sem.at[c, 1], me_c, north),
              remote(send_col.at[c, pl.ds(ROWS - 8, 8), :], recv_col.at[c, pl.ds(0, 8), :], cs_sem.at[c, 2], cr_sem.at[c, 2], peer, north))
        down = (remote(send_row.at[1, c], recv_row.at[1, c], cs_sem.at[c, 3], cr_sem.at[c, 3], me_c, south),
                remote(send_col.at[c, pl.ds(0, 8), :], recv_col.at[c, pl.ds(8 + ROWS, 8), :], cs_sem.at[c, 4], cr_sem.at[c, 4], peer, south))
        return side, up, down

    def start_all(copies):
        side, up, down = copies
        if side is not None:
            side.start()

        @pl.when(has_n)
        def _():
            for copy in up:
                copy.start()

        @pl.when(has_s)
        def _():
            for copy in down:
                copy.start()

    def wait_recv_all(copies):
        side, up, down = copies
        if side is not None:
            side.wait_recv()

        @pl.when(has_s)
        def _():
            for copy in up:
                copy.wait_recv()

        @pl.when(has_n)
        def _():
            for copy in down:
                copy.wait_recv()

    def wait_send_all(copies):
        side, up, down = copies
        if side is not None:
            side.wait_send()

        @pl.when(has_n)
        def _():
            for copy in up:
                copy.wait_send()

        @pl.when(has_s)
        def _():
            for copy in down:
                copy.wait_send()

    def all_entered():
        @pl.when((me_r == 0) | (me_r == 3))
        def _():
            pl.semaphore_wait(barrier, 3)

        @pl.when((me_r != 0) & (me_r != 3))
        def _():
            pl.semaphore_wait(barrier, 5)

    def pack_and_send(c, with_maps=False):
        for copy in loads(c):
            copy.wait()
        lane = lanes(PK)

        def block(i, carry):
            r = pl.multiple_of(i * PK, PK)
            pairs = [(f, c * CHUNK + kk, m) for f in range(4) for kk in range(CHUNK) for m in range(2)]
            column = [[buf[f, k, m, t, pl.ds(8 + r, PK), :] for f, k, m in pairs] for t in range(2)]
            if with_maps:
                for t in range(2):
                    column[t] += [xb[0, t, pl.ds(32 + r, PK), :], xb[1, t, pl.ds(32 + r, PK), :]]
            packed = jnp.zeros((PK, LN), F32)
            count = len(column[0])
            for i in range(count + 1):
                edge = jnp.where(lane == 0, column[0][min(i, count - 1)], column[1][max(i - 1, 0)])
                edge = pltpu.roll(edge, 2 * i, 1) if i else edge
                packed = jnp.where(lane >= 2 * i - 1, edge, packed) if i else edge
            send_col[c, pl.ds(r, PK), :] = packed
            return carry
        for kk in range(CHUNK):
            for m in range(2):
                jj = kk * 2 + m
                k = c * CHUNK + kk
                for side, row in ((0, 8 + ROWS - 1), (1, 8)):
                    for f in range(4):
                        for t in range(2):
                            send_row[side, c, t, f, jj:jj + 1, :] = buf[f, k, m, t, row:row + 1, :]
        lax.fori_loop(0, ROWS // PK, block, 0)
        if with_maps:
            all_entered()
            start_all(map_copies())
        start_all(edge_copies(c))

    pack_and_send(0, with_maps=True)

    def pack_pairs(source, firsts, seconds, send):
        lane = lanes(ROWS)
        outer = (lane < 32) | (lane >= 96)
        for slot, (f, g) in enumerate(zip(firsts, seconds)):
            a, b = (jnp.where(lane < 64, source[n, 0, 32:32 + ROWS, :], source[n, 1, 32:32 + ROWS, :]) for n in (f, g))
            send[slot, :, :] = jnp.where(outer, a, pltpu.roll(b, 64, 1))

    def pack_wide():
        for copy in flow_loads():
            copy.wait()
        pack_pairs(xb, (0, 2, 4, 6), (1, 3, 5, 7), sp)
        start_all(flow_copies())

    def pack_rest(c, carry):
        pack_and_send(c)
        return carry
    lax.fori_loop(1, NCH - 1, pack_rest, 0)

    RHO_T = np.float32(-THERM_EXP * PRESS_SCALE / LEVELS / 2)
    RHO_S = np.float32(HALINE_CON * PRESS_SCALE / LEVELS / 2)
    BR = 128
    SB = 16

    def pressure_rows(k, slot, base, rows):
        for m in range(2):
            for t in range(2):
                half = RHO_T * buf[2, k, m, t, pl.ds(base, rows), :] + RHO_S * buf[3, k, m, t, pl.ds(base, rows), :]
                p = pacc[m, t, pl.ds(base, rows), :] + half
                slot[m, t, pl.ds(base, rows), :] = p
                pacc[m, t, pl.ds(base, rows), :] = p + half

    def shift_u(c, kk, m, base, rows):
        u = [buf[0, c * CHUNK + kk, m, t, pl.ds(base, rows), :] for t in range(2)]
        edge = halo(recv_col[c, pl.ds(base, rows), :], kk * 2 + m)
        ue, uw = east_pair(*u, edge), west_pair(*u, edge)
        for t in range(2):
            uwp[m, t, pl.ds(base, rows), :] = uw[t]
            dup[m, t, pl.ds(base, rows), :] = ue[t] - uw[t]

    def level(c, kk, now, later):
        k = c * CHUNK + kk
        pressure_rows(k, now, 8 + ROWS, 8)
        for m in range(2):
            shift_u(c, kk, m, 8, 8)
            ve = east_pair(*(buf[1, k, m, t, 0:8, :] for t in range(2)), halo(recv_col[c, 0:8, :], PAIRS + kk * 2 + m))
            for t in range(2):
                vep[m, t, 0:8, :] = ve[t]
        level_no = k.astype(F32)
        before = table[0, k]
        following = jnp.minimum(k + 1, LEVELS - 1)

        def block(i, carry):
            for q in range(0, BR, SB):
                piece(pl.multiple_of(i * BR + q, SB), pl.multiple_of(8 + i * BR + q, 8))
            return carry

        def piece(r, b):
            wet_x = [ku[t, pl.ds(r, SB), :] > level_no for t in range(2)]
            wet_y = [kv[t, pl.ds(r, SB), :] > level_no for t in range(2)]
            packed = recv_col[c, pl.ds(b, SB), :]
            packed_r = rhoc[pl.ds(r, SB), :]
            for m in range(2):
                j = kk * 2 + m
                shift_u(c, kk, m, pl.multiple_of(b + 8, 8), SB)
                half = halo(packed_r, j)
                p_edge = phal[m, pl.ds(r, SB), :] + half
                phal[m, pl.ds(r, SB), :] = p_edge + half
                v = [buf[1, k, m, t, pl.ds(b, SB), :] for t in range(2)]
                p = [now[m, t, pl.ds(b, SB), :] for t in range(2)]
                v_edge = halo(packed, PAIRS + j)
                ve, vw = east_pair(*v, v_edge), west_pair(*v, v_edge)
                pe = east_pair(*p, p_edge)
                for t in range(2):
                    vep[m, t, pl.ds(b, SB), :] = ve[t]
                    u = buf[0, k, m, t, pl.ds(b, SB), :]
                    un = buf[0, k, m, t, pl.ds(b + 1, SB), :]
                    us = buf[0, k, m, t, pl.ds(b - 1, SB), :]
                    vs = buf[1, k, m, t, pl.ds(b - 1, SB), :]
                    vn = buf[1, k, m, t, pl.ds(b + 1, SB), :]
                    pn = now[m, t, pl.ds(b + 1, SB), :]
                    w = (v[t] + vs) + (ve[t] + vep[m, t, pl.ds(b - 1, SB), :])
                    z = (u + un) + (uwp[m, t, pl.ds(b, SB), :] + uwp[m, t, pl.ds(b + 1, SB), :])
                    gu = (p[t] - pe[t]) - (0.5 * u) * dup[m, t, pl.ds(b, SB), :] - (0.125 * w) * (un - us)
                    gu = jnp.where(wet_x[t], gu, 0.0)
                    gsum[0, m, t, pl.ds(r, SB), :] += gu
                    new = u + gu + before * cu[m, t, pl.ds(r, SB), :]
                    cu[m, t, pl.ds(r, SB), :] = new
                    tu[k, m, t, pl.ds(r, SB), :] = new
                    gv = (p[t] - pn) - (0.125 * z) * (ve[t] - vw[t]) - (0.5 * v[t]) * (vn - vs)
                    gv = jnp.where(wet_y[t], gv, 0.0)
                    gsum[1, m, t, pl.ds(r, SB), :] += gv
                    new = v[t] + gv + before * cv[m, t, pl.ds(r, SB), :]
                    cv[m, t, pl.ds(r, SB), :] = new
                    tv[k, m, t, pl.ds(r, SB), :] = new
            pressure_rows(following, later, b, SB)
        lax.fori_loop(0, ROWS // BR, block, 0)

    def first_pressure(i, carry):
        pressure_rows(0, pbufa, pl.multiple_of(8 + i * 64, 8), 64)
        return carry
    lax.fori_loop(0, 2, first_pressure, 0)

    def chunk_step(c, carry):
        @pl.when(c == 1)
        def _():
            pack_and_send(NCH - 1)

        @pl.when(c == 2)
        def _():
            pack_wide()

        wait_recv_all(edge_copies(c))

        @pl.when(c == 0)
        def _():
            face_maps()

        for kk in range(CHUNK):
            k = c * CHUNK + kk
            for m in range(2):
                jj = kk * 2 + m
                for side, row in ((0, 7), (1, 8 + ROWS)):
                    for f in range(4):
                        for t in range(2):
                            buf[f, k, m, t, row:row + 1, :] = recv_row[side, c, t, f, jj:jj + 1, :]
        packed = recv_col[c, 8:8 + ROWS, :]
        rhoc[...] = RHO_T * pltpu.roll(packed, LN - 4 * PAIRS, 1) + RHO_S * pltpu.roll(packed, LN - 6 * PAIRS, 1)

        def two_levels(h, carry2):
            level(c, 2 * h, pbufa, pbufb)
            level(c, 2 * h + 1, pbufb, pbufa)
            return carry2
        lax.fori_loop(0, CHUNK // 2, two_levels, 0)
        return carry

    def face_maps():
        wait_recv_all(map_copies())

        def maps(i, carry):
            r = pl.multiple_of(i * 64, 64)
            packed = recv_col[0, pl.ds(8 + r, 64), :]
            kt = [xb[0, t, pl.ds(32 + r, 64), :] for t in range(2)]
            ht = [xb[1, t, pl.ds(32 + r, 64), :] for t in range(2)]
            ke = east_pair(*kt, halo(packed, 4 * PAIRS))
            he = east_pair(*ht, halo(packed, 4 * PAIRS + 1))
            for t in range(2):
                kx = jnp.minimum(kt[t], ke[t])
                ky = jnp.minimum(kt[t], xb[0, t, pl.ds(33 + r, 64), :])
                ku[t, pl.ds(r, 64), :] = kx
                kv[t, pl.ds(r, 64), :] = ky
                hux[t, pl.ds(32 + r, 64), :] = jnp.where(kx > 0.0, 0.5 * (ht[t] + he[t]), 0.0)
                huy[t, pl.ds(32 + r, 64), :] = jnp.where(ky > 0.0, 0.5 * (ht[t] + xb[1, t, pl.ds(33 + r, 64), :]), 0.0)
            return carry
        lax.fori_loop(0, 2, maps, 0)

    lax.fori_loop(0, NCH, chunk_step, 0)

    packet_copies = [pltpu.make_async_copy(src, dst, ot_sem.at[i]) for i, (src, dst) in enumerate(
        ((recv_col, col_out), (recv_row, rows_out), (kmask, kmask_out)))]
    for copy in packet_copies:
        copy.start()

    def forcing(i, carry):
        r = pl.multiple_of(i * 32, 32)
        for t in range(2):
            nx = jnp.maximum(ku[t, pl.ds(r, 32), :], 1.0)
            ny = jnp.maximum(kv[t, pl.ds(r, 32), :], 1.0)
            fx = hux[t, pl.ds(32 + r, 32), :] / nx / SUBS
            fy = huy[t, pl.ds(32 + r, 32), :] / ny / SUBS
            for m in range(2):
                xf[m, t, pl.ds(32 + r, 32), :] = fx * gsum[0, m, t, pl.ds(r, 32), :]
                xf[2 + m, t, pl.ds(32 + r, 32), :] = fy * gsum[1, m, t, pl.ds(r, 32), :]
        return carry
    lax.fori_loop(0, ROWS // 32, forcing, 0)
    pack_pairs(xf, (0, 1), (2, 3), sf)
    start_all(force_copies())

    def stores(c):
        out = []
        for f, (ref, dst) in enumerate(((tu, us_hbm), (tv, vs_hbm))):
            for t in range(2):
                out.append(pltpu.make_async_copy(ref.at[pl.ds(c * CHUNK, CHUNK), :, t, :, :],
                                                 dst.at[pl.ds(c * CHUNK, CHUNK), :, :, pl.ds(t * LN, LN)], st_sem.at[c, f * 2 + t]))
        return out

    def upward(step, carry):
        c = NCH - 1 - step

        def block(i, carry2):
            r = pl.multiple_of(i * UP, UP)
            for f, (ref, kp) in enumerate(((tu, ku), (tv, kv))):
                for t in range(2):
                    depth = kp[t, pl.ds(r, UP), :]
                    below = [ref[c * CHUNK + CHUNK, m, t, pl.ds(r, UP), :] for m in range(2)]
                    total = [xsum[f, m, t, pl.ds(r, UP), :] for m in range(2)]
                    for kk in range(CHUNK - 1, -1, -1):
                        k = c * CHUNK + kk
                        level_no = k.astype(F32)
                        inv = jnp.where(depth > level_no + 1.0, table[2, k], jnp.where(depth > level_no, table[3, k], 0.0))
                        for m in range(2):
                            below[m] = ref[k, m, t, pl.ds(r, UP), :] * inv + table[1, k] * below[m]
                            ref[k, m, t, pl.ds(r, UP), :] = below[m]
                            total[m] = total[m] + below[m]
                    for m in range(2):
                        xsum[f, m, t, pl.ds(r, UP), :] = total[m]
            return carry2
        lax.fori_loop(0, ROWS // UP, block, 0)
        for copy in stores(c):
            copy.start()
        return carry
    lax.fori_loop(0, NCH, upward, 0)

    wait_recv_all(flow_copies())

    def unpack_wide(i, carry):
        r = pl.multiple_of(i * 96, 32)
        for pair in range(4):
            tile = rp[pair, pl.ds(r, 96), :]
            xb[2 * pair, 2, pl.ds(r, 96), :] = tile
            xb[2 * pair + 1, 2, pl.ds(r, 96), :] = pltpu.roll(tile, 64, 1)
        return carry
    lax.fori_loop(0, EXT // 96, unpack_wide, 0)

    XR = 88

    def depths(i, carry):
        r = pl.multiple_of(8 + i * XR, 8)
        kt = [xb[0, t, pl.ds(r, XR), :] for t in range(3)]
        ht = [xb[1, t, pl.ds(r, XR), :] for t in range(3)]
        for t in range(3):
            kx = jnp.minimum(kt[t], east(kt[t], kt[NEXT[t]]))
            ky = jnp.minimum(kt[t], xb[0, t, pl.ds(r + 1, XR), :])
            hux[t, pl.ds(r, XR), :] = jnp.where(kx > 0.0, 0.5 * (ht[t] + east(ht[t], ht[NEXT[t]])), 0.0)
            huy[t, pl.ds(r, XR), :] = jnp.where(ky > 0.0, 0.5 * (ht[t] + xb[1, t, pl.ds(r + 1, XR), :]), 0.0)
            cc[t, pl.ds(r, XR), :] = jnp.where(kt[t] > 0.0, WAVE_COURANT, 0.0)
        return carry
    for t in range(3):
        for ref in (hux, huy):
            ref[t, 0:8, :] = zrow
        for ref in (ebufa, ebufb):
            for m in range(2):
                ref[m, t, 0:8, :] = zrow
                ref[m, t, EXT - 8:EXT, :] = zrow
    lax.fori_loop(0, 2, depths, 0)

    def coefficients(i, carry):
        r = pl.multiple_of(8 + i * XR, 8)
        hx = [hux[t, pl.ds(r, XR), :] for t in range(3)]
        for t in range(3):
            c0 = cc[t, pl.ds(r, XR), :]
            cw = WAVE_COURANT * c0
            ae[t, pl.ds(r, XR), :] = cw * hx[t]
            aw[t, pl.ds(r, XR), :] = cw * west(hx[t], hx[PREV[t]])
            an[t, pl.ds(r, XR), :] = cw * huy[t, pl.ds(r, XR), :]
            as_[t, pl.ds(r, XR), :] = cw * huy[t, pl.ds(r - 1, XR), :]
        return carry
    lax.fori_loop(0, 2, coefficients, 0)

    def first_subcycle(m, base, rows):
        tx = [xb[4 + m, t, pl.ds(base, rows), :] for t in range(3)]
        for t in range(3):
            c0 = cc[t, pl.ds(base, rows), :]
            ty = xb[6 + m, t, pl.ds(base, rows), :]
            div = tx[t] - west(tx[t], tx[PREV[t]]) + ty - xb[6 + m, t, pl.ds(base - 1, rows), :]
            change = -c0 * div
            dbuf[m, t, pl.ds(base, rows), :] = change
            eta = jnp.where(c0 > 0.0, xb[2 + m, t, pl.ds(base, rows), :], 0.0) + change
            ebufa[m, t, pl.ds(base, rows), :] = eta

    def first_block(i, carry):
        for m in range(2):
            first_subcycle(m, pl.multiple_of(8 + i * XR, 8), XR)
        return carry
    lax.fori_loop(0, 2, first_block, 0)

    weights_load.wait()
    whole = weights[SUBS - 1]
    moment = weights[SUBS - 1]
    for n in range(SUBS - 2, -1, -1):
        whole = whole + weights[n]
        moment = moment + whole

    def first_sums(i, carry):
        r = pl.multiple_of(i * 8, 8)
        for m in range(2):
            for t in range(3):
                eta = ebufa[m, t, pl.ds(32 + r, 8), :]
                bacc[m, t, pl.ds(r, 8), :] = whole * eta
                if t < 2:
                    eacc[m, t, pl.ds(r, 8), :] = weights[0] * eta
        return carry
    lax.fori_loop(0, 17, first_sums, 0)

    wait_recv_all(force_copies())

    def unpack_force(i, carry):
        r = pl.multiple_of(i * 96, 32)
        for m in range(2):
            tile = rf[m, pl.ds(r, 96), :]
            xf[m, 2, pl.ds(r, 96), :] = tile
            xf[2 + m, 2, pl.ds(r, 96), :] = pltpu.roll(tile, 64, 1)
        return carry
    lax.fori_loop(0, EXT // 96, unpack_force, 0)

    def forcing_divergence(i, carry):
        r = pl.multiple_of(8 + i * XR, 8)
        for m in range(2):
            fx = [xf[m, t, pl.ds(r, XR), :] for t in range(3)]
            for t in range(3):
                div = fx[t] - west(fx[t], fx[PREV[t]]) + xf[2 + m, t, pl.ds(r, XR), :] - xf[2 + m, t, pl.ds(r - 1, XR), :]
                gbuf[m, t, pl.ds(r, XR), :] = cc[t, pl.ds(r, XR), :] * div
        return carry
    lax.fori_loop(0, 2, forcing_divergence, 0)

    def subcycle(n, tail, lo, hi, old, new):
        tail = tail - weights[n - 2]
        weight = weights[n - 1]
        for r, end in ((lo, 96), (96, hi)):
            first = max(r, 32)
            for t in range(3):
                c_e, c_w = ae[t, r:end, :], aw[t, r:end, :]
                c_n, c_s = an[t, r:end, :], as_[t, r:end, :]
                for m in range(2):
                    e = old[m, t, r:end, :]
                    to_e = east(e, old[m, NEXT[t], r:end, :])
                    to_w = west(e, old[m, PREV[t], r:end, :])
                    to_n = old[m, t, r + 1:end + 1, :]
                    to_s = old[m, t, r - 1:end - 1, :]
                    d = dbuf[m, t, r:end, :] - gbuf[m, t, r:end, :]
                    d = d + (c_e * (to_e - e) + c_w * (to_w - e)) + (c_n * (to_n - e) + c_s * (to_s - e))
                    dbuf[m, t, r:end, :] = d
                    e = e + d
                    new[m, t, r:end, :] = e
                    last = min(end, 168)
                    bacc[m, t, first - 32:last - 32, :] += tail * e[first - r:last - r]
                    if t < 2:
                        last = min(end, 160)
                        eacc[m, t, first - 32:last - 32, :] += weight * e[first - r:last - r]
        return tail

    tail = subcycle(2, whole, 8, 184, ebufa, ebufb)
    for first_n, steps, lo, hi in ((3, 1, 8, 184), (5, 4, 16, 176), (13, 4, 24, 168)):
        def two_cycles(h, carry, first_n=first_n, lo=lo, hi=hi):
            n = first_n + 2 * h
            carry = subcycle(n, carry, lo, hi, ebufb, ebufa)
            return subcycle(n + 1, carry, lo, hi, ebufa, ebufb)
        tail = lax.fori_loop(0, steps, two_cycles, tail)

    eta_copies = [pltpu.make_async_copy(eacc.at[:, t, pl.ds(0, ROWS), :], eta_out.at[:, :, pl.ds(t * LN, LN)], ot_sem.at[4 + t]) for t in range(2)]
    for copy in eta_copies:
        copy.start()

    AV = 64

    def average_copies(i):
        r = pl.multiple_of(i * AV, AV)
        return [pltpu.make_async_copy(src, dst, av_sem.at[i, n]) for n, (src, dst) in enumerate((
            (txb.at[:, pl.ds(r, AV), :], tx_out.at[:, pl.ds(r, AV), :]), (tyb.at[:, pl.ds(r, AV), :], ty_out.at[:, pl.ds(r, AV), :]),
            (corr.at[:, :, :, pl.ds(r, AV), :], corr_out.at[:, :, :, pl.ds(r, AV), :])))]

    def averages(i, carry):
        for q in range(0, AV, 16):
            r = pl.multiple_of(i * AV + q, 16)
            g = pl.multiple_of(32 + i * AV + q, 16)
            for t in range(2):
                depth_x = hux[t, pl.ds(g, 16), :]
                depth_y = huy[t, pl.ds(g, 16), :]
                kx = ku[t, pl.ds(r, 16), :]
                ky = kv[t, pl.ds(r, 16), :]
                inv_x = 1.0 / (depth_x + jnp.where(kx > 0.0, 0.0, 1.0))
                inv_y = 1.0 / (depth_y + jnp.where(ky > 0.0, 0.0, 1.0))
                mean_x = 1.0 / jnp.maximum(kx, 1.0)
                mean_y = 1.0 / jnp.maximum(ky, 1.0)
                for m in range(2):
                    lane = slice(t * LN, (t + 1) * LN)
                    acc = bacc[m, t, pl.ds(r, 16), :]
                    tx = whole * xb[4 + m, t, pl.ds(g, 16), :] + moment * xf[m, t, pl.ds(g, 16), :] \
                        - WAVE_COURANT * depth_x * (east(acc, bacc[m, NEXT[t], pl.ds(r, 16), :]) - acc)
                    ty = whole * xb[6 + m, t, pl.ds(g, 16), :] + moment * xf[2 + m, t, pl.ds(g, 16), :] \
                        - WAVE_COURANT * depth_y * (bacc[m, t, pl.ds(r + 1, 16), :] - acc)
                    tx = jnp.where(kx > 0.0, tx, 0.0)
                    ty = jnp.where(ky > 0.0, ty, 0.0)
                    txb[m, pl.ds(r, 16), lane] = tx
                    tyb[m, pl.ds(r, 16), lane] = ty
                    corr[0, m, t, pl.ds(r, 16), :] = tx * inv_x - xsum[0, m, t, pl.ds(r, 16), :] * mean_x
                    corr[1, m, t, pl.ds(r, 16), :] = ty * inv_y - xsum[1, m, t, pl.ds(r, 16), :] * mean_y
        for copy in average_copies(i):
            copy.start()
        return carry
    lax.fori_loop(0, ROWS // AV, averages, 0)

    wait_send_all(map_copies())
    wait_send_all(flow_copies())
    wait_send_all(force_copies())
    for copy in packet_copies + eta_copies:
        copy.wait()
    for i in range(ROWS // AV):
        for copy in average_copies(i):
            copy.wait()

    def drain(c, carry):
        wait_send_all(edge_copies(c))
        for copy in stores(c):
            copy.wait()
        return carry
    lax.fori_loop(0, NCH, drain, 0)


def tracer_kernel(u_hbm, v_hbm, t_hbm, s_hbm, us_hbm, vs_hbm, eta_in, tx_in, ty_in, corr_in, kmask_in, col_in, rows_in,
                  eta_hbm, tx_hbm, ty_hbm, un_hbm, vn_hbm, tn_hbm, sn_hbm,
                  buf, tt, ts, ct, su, sv, small, corr, kmask, cols, rows, ld_sem, ed_sem, st_sem, sv_sem, in_sem, out_sem, table):
    hbm = (u_hbm, v_hbm, t_hbm, s_hbm)
    sources = (eta_in, tx_in, ty_in)
    sinks = (eta_hbm, tx_hbm, ty_hbm)

    def loads(c):
        out = []
        for f in range(4):
            for t in range(2):
                out.append(pltpu.make_async_copy(
                    hbm[f].at[pl.ds(c * TC, TC), :, :, pl.ds(t * LN, LN)],
                    buf.at[f, pl.ds(c * TC, TC), :, t, pl.ds(8, ROWS), :], ld_sem.at[c, f * 2 + t]))
        for f, (src, dst) in enumerate(((us_hbm, su), (vs_hbm, sv))):
            out.append(pltpu.make_async_copy(src.at[pl.ds(c * TC, TC)], dst.at[pl.ds(c * TC, TC)], ld_sem.at[c, 8 + f]))
        return out

    def stores_v(c):
        return [pltpu.make_async_copy(src.at[pl.ds(c * TC, TC)], dst.at[pl.ds(c * TC, TC)], sv_sem.at[c, f])
                for f, (src, dst) in enumerate(((su, un_hbm), (sv, vn_hbm)))]

    def stores_t(c):
        return [pltpu.make_async_copy(src.at[pl.ds(c * TC, TC)], dst.at[pl.ds(c * TC, TC)], st_sem.at[c, f])
                for f, (src, dst) in enumerate(((tt, tn_hbm), (ts, sn_hbm)))]

    edges = [pltpu.make_async_copy(src, dst, ed_sem.at[i])
             for i, (src, dst) in enumerate(((col_in, cols), (rows_in, rows), (corr_in, corr), (kmask_in, kmask)))]
    for copy in edges:
        copy.start()
    for c in range(AHEAD):
        for copy in loads(c):
            copy.start()
    write_table(table, DIFF_NUMBER)
    small_in = [pltpu.make_async_copy(sources[i], small.at[i], in_sem.at[i]) for i in range(3)]
    small_out = [pltpu.make_async_copy(small.at[i], sinks[i], out_sem.at[i]) for i in range(3)]
    for copy in small_in:
        copy.start()

    def zero_planes(i, carry):
        r = pl.multiple_of(i * 16, 16)
        z = jnp.zeros((16, 2 * LN), F32)
        for f in range(2):
            for m in range(2):
                for t in range(2):
                    ct[f, m, t, pl.ds(r, 16), :] = z[:, :LN]
        for m in range(2):
            for ref in (tt, ts):
                ref[LEVELS, m, pl.ds(r, 16), :] = z
        return carry
    lax.fori_loop(0, ROWS // 16, zero_planes, 0)
    for copy in edges:
        copy.wait()

    BR = 128
    SB = 16

    def level(k, c, kk):
        level_no = k.astype(F32)
        before = table[0, k]

        def block(i, carry):
            for q in range(0, BR, SB):
                piece(pl.multiple_of(i * BR + q, SB), pl.multiple_of(8 + i * BR + q, 8))
            return carry

        def piece(r, b):
            wet = [kmask[0, t, pl.ds(r, SB), :] > level_no for t in range(2)]
            packed = cols[c, pl.ds(b, SB), :]
            for m in range(2):
                j = kk * 2 + m
                u = [buf[0, k, m, t, pl.ds(b, SB), :] for t in range(2)]
                v = [buf[1, k, m, t, pl.ds(b, SB), :] for t in range(2)]
                vs = [buf[1, k, m, t, pl.ds(b - 1, SB), :] for t in range(2)]
                uw = west_pair(*u, halo(packed, j))
                for f, ref in ((2, tt), (3, ts)):
                    q = [buf[f, k, m, t, pl.ds(b, SB), :] for t in range(2)]
                    edge = halo(packed, f * PAIRS + j)
                    qe, qw = east_pair(*q, edge), west_pair(*q, edge)
                    for t in range(2):
                        lane = slice(t * LN, (t + 1) * LN)
                        fy = v[t] * (q[t] + buf[f, k, m, t, pl.ds(b + 1, SB), :])
                        fs = vs[t] * (q[t] + buf[f, k, m, t, pl.ds(b - 1, SB), :])
                        adv = q[t] - 0.5 * ((u[t] * (q[t] + qe[t]) - uw[t] * (q[t] + qw[t])) + (fy - fs))
                        adv = jnp.where(wet[t], adv, 0.0)
                        new = adv + before * ct[f - 2, m, t, pl.ds(r, SB), :]
                        ct[f - 2, m, t, pl.ds(r, SB), :] = new
                        ref[k, m, pl.ds(r, SB), lane] = new
            for t in range(2):
                lane = slice(t * LN, (t + 1) * LN)
                wet_x = kmask[1, t, pl.ds(r, SB), :] > level_no
                wet_y = kmask[2, t, pl.ds(r, SB), :] > level_no
                for m in range(2):
                    su[k, m, pl.ds(r, SB), lane] = jnp.where(wet_x, su[k, m, pl.ds(r, SB), lane] + corr[0, m, t, pl.ds(r, SB), :], 0.0)
                    sv[k, m, pl.ds(r, SB), lane] = jnp.where(wet_y, sv[k, m, pl.ds(r, SB), lane] + corr[1, m, t, pl.ds(r, SB), :], 0.0)
        lax.fori_loop(0, ROWS // BR, block, 0)

    def chunk_step(c, carry):
        @pl.when(c + AHEAD < LEVELS // TC)
        def _():
            for copy in loads(c + AHEAD):
                copy.start()

        for copy in loads(c):
            copy.wait()
        packet = c // (CHUNK // TC)
        first = lax.rem(c, CHUNK // TC) * TC
        for kk in range(TC):
            k = c * TC + kk
            for m in range(2):
                jj = (first + kk) * 2 + m
                for f in (1, 2, 3):
                    for t in range(2):
                        buf[f, k, m, t, 7:8, :] = rows[0, packet, t, f, pl.ds(jj, 1), :]
                for f in (2, 3):
                    for t in range(2):
                        buf[f, k, m, t, 8 + ROWS:9 + ROWS, :] = rows[1, packet, t, f, pl.ds(jj, 1), :]

        def one_level(kk, carry2):
            level(c * TC + kk, packet, first + kk)
            return carry2
        lax.fori_loop(0, TC, one_level, 0)
        for copy in stores_v(c):
            copy.start()
        return carry
    lax.fori_loop(0, LEVELS // TC, chunk_step, 0)

    for copy in small_in:
        copy.wait()
    for copy in small_out:
        copy.start()

    def upward(step, carry):
        c = LEVELS // TC - 1 - step

        def block(i, carry2):
            r = pl.multiple_of(i * UP, UP)
            for t in range(2):
                lane = slice(t * LN, (t + 1) * LN)
                depth = kmask[0, t, pl.ds(r, UP), :]
                below = [[ref[c * TC + TC, m, pl.ds(r, UP), lane] for m in range(2)] for ref in (tt, ts)]
                for kk in range(TC - 1, -1, -1):
                    k = c * TC + kk
                    level_no = k.astype(F32)
                    inv = jnp.where(depth > level_no + 1.0, table[2, k], jnp.where(depth > level_no, table[3, k], 0.0))
                    for f, ref in enumerate((tt, ts)):
                        for m in range(2):
                            below[f][m] = ref[k, m, pl.ds(r, UP), lane] * inv + table[1, k] * below[f][m]
                            ref[k, m, pl.ds(r, UP), lane] = below[f][m]
            return carry2
        lax.fori_loop(0, ROWS // UP, block, 0)
        for copy in stores_t(c):
            copy.start()
        return carry
    lax.fori_loop(0, LEVELS // TC, upward, 0)

    for copy in small_out:
        copy.wait()

    def drain(c, carry):
        for copy in stores_v(c) + stores_t(c):
            copy.wait()
        return carry
    lax.fori_loop(0, LEVELS // TC, drain, 0)


def solution(mesh):
    assert mesh.shape["col"] == 2 and mesh.shape["row"] == 4
    any_spec = pl.BlockSpec(memory_space=pl.ANY)
    shape = lambda *dims: jax.ShapeDtypeStruct(dims, F32)
    dma = lambda *dims: pltpu.SemaphoreType.DMA(dims)
    vm = lambda *dims: pltpu.VMEM(dims, F32)
    full = (LEVELS, 2, ROWS, 2 * LN)
    flat = (2, ROWS, 2 * LN)

    momentum = pl.pallas_call(
        momentum_kernel,
        name="momentum",
        out_shape=(shape(*full), shape(*full), shape(*flat), shape(*flat), shape(*flat), shape(2, 2, 2, ROWS, LN),
                   shape(3, 2, ROWS, LN), shape(NCH, PR, LN), shape(2, NCH, 2, 4, PAIRS, LN)),
        in_specs=[any_spec] * 10,
        out_specs=(any_spec,) * 9,
        scratch_shapes=[
            vm(4, LEVELS, 2, 2, PR, LN), vm(LEVELS + 1, 2, 2, ROWS, LN), vm(LEVELS + 1, 2, 2, ROWS, LN),
            vm(2, 2, ROWS, LN), vm(2, 2, ROWS, LN), vm(2, 2, PR, LN), vm(2, 2, PR, LN), vm(2, 2, PR, LN), vm(2, PR, LN), vm(ROWS, LN),
            vm(2, 2, 2, ROWS, LN), vm(2, 2, 2, ROWS, LN), vm(3, 2, ROWS, LN), pltpu.VMEM((ROWS, 2 * LN), jnp.int32),
            vm(2, 2, PR, LN), vm(2, 2, PR, LN), vm(2, 2, PR, LN), vm(*flat), vm(*flat), vm(2, 2, 2, ROWS, LN),
            vm(NCH, ROWS, LN), vm(NCH, PR, LN), vm(2, NCH, 2, 4, PAIRS, LN), vm(2, NCH, 2, 4, PAIRS, LN),
            vm(8, 3, EXT, LN), vm(4, ROWS, LN), vm(4, EXT, LN), vm(4, 3, EXT, LN), vm(2, ROWS, LN), vm(2, EXT, LN),
            vm(3, EXT, LN), vm(3, EXT, LN), vm(3, EXT, LN), vm(3, EXT, LN), vm(3, EXT, LN), vm(3, EXT, LN), vm(3, EXT, LN),
            vm(2, 3, EXT, LN), vm(2, 3, EXT, LN), vm(2, 3, EXT, LN), vm(2, 3, EXT, LN), vm(2, 2, ROWS + 8, LN), vm(2, 3, ROWS + 8, LN),
            dma(NCH, 8), dma(9), dma(NCH, 5), dma(NCH, 5), dma(7), dma(7), dma(5), dma(5), dma(NCH, 4), dma(6), dma(2, 3),
            pltpu.SMEM((SUBS,), F32), pltpu.SMEM((4, LEVELS), F32), pltpu.SemaphoreType.DMA,
        ],
        compiler_params=pltpu.CompilerParams(collective_id=0, has_side_effects=True, vmem_limit_bytes=67043328),
    )

    tracers = pl.pallas_call(
        tracer_kernel,
        name="tracers",
        out_shape=(shape(*flat), shape(*flat), shape(*flat), shape(*full), shape(*full), shape(*full), shape(*full)),
        in_specs=[any_spec] * 13,
        out_specs=(any_spec,) * 7,
        scratch_shapes=[
            vm(4, LEVELS, 2, 2, PR, LN), vm(LEVELS + 1, 2, ROWS, 2 * LN), vm(LEVELS + 1, 2, ROWS, 2 * LN), vm(2, 2, 2, ROWS, LN),
            vm(*full), vm(*full), vm(3, 2, ROWS, 2 * LN), vm(2, 2, 2, ROWS, LN), vm(3, 2, ROWS, LN),
            vm(NCH, PR, LN), vm(2, NCH, 2, 4, PAIRS, LN),
            dma(LEVELS // TC, 10), dma(4), dma(LEVELS // TC, 2), dma(LEVELS // TC, 2), dma(3), dma(3), pltpu.SMEM((4, LEVELS), F32),
        ],
        compiler_params=pltpu.CompilerParams(vmem_limit_bytes=67043328),
    )

    def local_step(vel_x, vel_y, pot_temp, salinity, surf_eta, trans_x, trans_y, col_depth, wet_levels, avg_weights):
        star_x, star_y, eta, tx, ty, corr, kmask, cols, rows = momentum(
            vel_x, vel_y, pot_temp, salinity, surf_eta, trans_x, trans_y, col_depth, wet_levels, avg_weights)
        return tracers(vel_x, vel_y, pot_temp, salinity, star_x, star_y, eta, tx, ty, corr, kmask, cols, rows)

    spec_3d = P(None, None, "row", "col")
    spec_2d = P(None, "row", "col")
    spec_map = P("row", "col")
    return jax.shard_map(local_step, mesh=mesh, in_specs=(spec_3d, spec_3d, spec_3d, spec_3d, spec_2d, spec_2d, spec_2d, spec_map, spec_map, P()),
                         out_specs=(spec_2d, spec_2d, spec_2d, spec_3d, spec_3d, spec_3d, spec_3d), check_vma=False)
```

```python
import functools
import numpy as np
import jax
import jax.numpy as jnp
from jax import lax
from jax.experimental import pallas as pl
from jax.experimental.pallas import tpu as pltpu
from jax.sharding import PartitionSpec as P

WAVE_COURANT = 0.4
THERM_EXP = 0.2
HALINE_CON = 0.15
PRESS_SCALE = 0.5
VISC_NUMBER = 1.0
DIFF_NUMBER = 0.5

LEVELS = 20
SUBS = 20
CHUNK = 4
NCH = LEVELS // CHUNK
PAIRS = 2 * CHUNK
ROWS = 128
LN = 128
PR = 144
EXT = 192
F32 = jnp.float32
TC = 2
AHEAD = 6
PK = 64
UP = 32
MESH_ID = pl.DeviceIdType.MESH


def solve_table(strength):
    inner = np.zeros(LEVELS)
    last = np.zeros(LEVELS)
    inner[0] = 1.0 + strength
    last[0] = 1.0
    for k in range(1, LEVELS):
        inner[k] = 1.0 + 2.0 * strength - strength**2 / inner[k - 1]
        last[k] = 1.0 + strength - strength**2 / inner[k - 1]
    ratio = strength / inner
    before = np.concatenate([[0.0], ratio[:-1]])
    return np.stack([before, ratio, 1.0 / inner, 1.0 / last]).astype(np.float32)


def write_table(table, strength):
    values = solve_table(strength)
    for i in range(values.shape[0]):
        for k in range(LEVELS):
            table[i, k] = values[i, k]


def lanes(rows):
    return lax.broadcasted_iota(jnp.int32, (rows, LN), 1)


def east(tile, following):
    return pltpu.roll(jnp.where(lanes(tile.shape[0]) == 0, following, tile), LN - 1, 1)


def west(tile, previous):
    return pltpu.roll(jnp.where(lanes(tile.shape[0]) == LN - 1, previous, tile), 1, 1)


NEXT = (1, 2, 0)
PREV = (2, 0, 1)


def halo(packed, j):
    return pltpu.roll(packed, LN - 1 - 2 * j, 1)


def east_pair(first, second, edge):
    last = lanes(first.shape[0]) == LN - 1
    a, b = pltpu.roll(first, LN - 1, 1), pltpu.roll(second, LN - 1, 1)
    return jnp.where(last, b, a), jnp.where(last, edge, b)


def west_pair(first, second, edge):
    origin = lanes(first.shape[0]) == 0
    a, b = pltpu.roll(first, 1, 1), pltpu.roll(second, 1, 1)
    return jnp.where(origin, edge, a), jnp.where(origin, a, b)


def momentum_kernel(u_hbm, v_hbm, t_hbm, s_hbm, eta_hbm, tx_hbm, ty_hbm, h_hbm, kmt_hbm, weights_hbm,
                    us_hbm, vs_hbm, eta_out, tx_out, ty_out, corr_out, kmask_out, col_out, rows_out,
                    buf, tu, tv, cu, cv, pbufa, pbufb, pacc, phal, rhoc, gsum, xsum, kmask, kmt, vep, uwp, dup, txb, tyb, corr,
                    send_col, recv_col, send_row, recv_row,
                    xb, sp, rp, xf, sf, rf, hux, huy, ae, aw, an, as_, cc, ebufa, ebufb, dbuf, gbuf, eacc, bacc,
                    ld_sem, xl_sem, cs_sem, cr_sem, xs_sem, xr_sem, fs_sem, fr_sem, st_sem, ot_sem, av_sem, weights, table, w_sem):
    weights_load = pltpu.make_async_copy(weights_hbm, weights, w_sem)
    ku, kv = kmask.at[1], kmask.at[2]
    me_c = lax.axis_index("col")
    me_r = lax.axis_index("row")
    peer = 1 - me_c
    has_n = me_r < 3
    has_s = me_r > 0
    hbm = (u_hbm, v_hbm, t_hbm, s_hbm)

    def loads(c):
        out = []
        for f in range(4):
            for t in range(2):
                out.append(pltpu.make_async_copy(
                    hbm[f].at[pl.ds(c * CHUNK, CHUNK), :, :, pl.ds(t * LN, LN)],
                    buf.at[f, pl.ds(c * CHUNK, CHUNK), :, t, pl.ds(8, ROWS), :], ld_sem.at[c, f * 2 + t]))
        return out

    def map_loads():
        return [pltpu.make_async_copy(kmt_hbm, kmt, xl_sem.at[8])] + [
            pltpu.make_async_copy(h_hbm.at[:, pl.ds(t * LN, LN)], xb.at[1, t, pl.ds(32, ROWS), :], xl_sem.at[t]) for t in range(2)]

    def flow_loads():
        return [pltpu.make_async_copy(ref.at[:, :, pl.ds(t * LN, LN)], xb.at[pl.ds(2 + 2 * i, 2), t, pl.ds(32, ROWS), :], xl_sem.at[2 + 2 * i + t])
                for t in range(2) for i, ref in enumerate((eta_hbm, tx_hbm, ty_hbm))]

    write_table(table, VISC_NUMBER)
    for copy in map_loads() + loads(0) + loads(1) + loads(2) + flow_loads() + loads(3) + loads(4) + [weights_load]:
        copy.start()

    barrier = pltpu.get_barrier_semaphore()

    def greet(col, row):
        pl.semaphore_signal(barrier, inc=1, device_id={"col": col, "row": row}, device_id_type=MESH_ID)

    greet(peer, me_r)

    @pl.when(has_n)
    def _():
        greet(me_c, me_r + 1)
        greet(peer, me_r + 1)

    @pl.when(has_s)
    def _():
        greet(me_c, me_r - 1)
        greet(peer, me_r - 1)

    zrow = jnp.zeros((8, LN), F32)
    for ref, count in ((xb, 8), (xf, 4)):
        for f in range(count):
            for t in range(3):
                ref[f, t, 0:8, :] = zrow
                ref[f, t, EXT - 8:EXT, :] = zrow
    for ref, count in ((rp, 4), (rf, 2)):
        for f in range(count):
            ref[f, 0:8, :] = zrow
            ref[f, EXT - 8:EXT, :] = zrow

    def zero_side(side, lo):
        z24 = jnp.zeros((24, LN), F32)
        for f in range(8):
            for t in range(2):
                xb[f, t, lo:lo + 24, :] = z24
        for f in range(4):
            rp[f, lo:lo + 24, :] = z24
            for t in range(2):
                xf[f, t, lo:lo + 24, :] = z24
        for f in range(2):
            rf[f, lo:lo + 24, :] = z24
        for c in range(NCH):
            recv_col[c, 136 * side:136 * side + 8, :] = zrow
            for f in range(4):
                for t in range(2):
                    recv_row[side, c, t, f, :, :] = zrow

    @pl.when(me_r == 0)
    def _():
        zero_side(0, 8)

    @pl.when(me_r == 3)
    def _():
        zero_side(1, 160)

    def zero_planes(i, carry):
        r = pl.multiple_of(i * 16, 16)
        z = jnp.zeros((16, LN), F32)
        for m in range(2):
            for t in range(2):
                pacc[m, t, pl.ds(r, 16), :] = z
            phal[m, pl.ds(r, 16), :] = z
        return carry
    lax.fori_loop(0, PR // 16, zero_planes, 0)

    def zero_planes2(i, carry):
        r = pl.multiple_of(i * 16, 16)
        z = jnp.zeros((16, LN), F32)
        for m in range(2):
            for t in range(2):
                for f in range(2):
                    gsum[f, m, t, pl.ds(r, 16), :] = z
                    xsum[f, m, t, pl.ds(r, 16), :] = z
                for ref in (cu, cv):
                    ref[m, t, pl.ds(r, 16), :] = z
                for ref in (tu, tv):
                    ref[LEVELS, m, t, pl.ds(r, 16), :] = z
        return carry
    lax.fori_loop(0, ROWS // 16, zero_planes2, 0)

    for copy in map_loads():
        copy.wait()
    for t in range(2):
        for r in range(0, ROWS, 64):
            level_count = kmt[r:r + 64, t * LN:(t + 1) * LN].astype(F32)
            xb[0, t, 32 + r:96 + r, :] = level_count
            kmask[0, t, r:r + 64, :] = level_count

    def remote(src, dst, ssem, rsem, col, row):
        return pltpu.make_async_remote_copy(src_ref=src, dst_ref=dst, send_sem=ssem, recv_sem=rsem,
                                            device_id={"col": col, "row": row}, device_id_type=MESH_ID)

    def wide_rows(own, first, count, ssem, rsem, slot):
        fields = pl.ds(first, count)
        return ((remote(own.at[fields, pl.ds(0, 2), pl.ds(136, 24), :], own.at[fields, pl.ds(0, 2), pl.ds(8, 24), :],
                        ssem.at[slot], rsem.at[slot], me_c, me_r + 1),),
                (remote(own.at[fields, pl.ds(0, 2), pl.ds(32, 24), :], own.at[fields, pl.ds(0, 2), pl.ds(160, 24), :],
                        ssem.at[slot + 1], rsem.at[slot + 1], me_c, me_r - 1),))

    def wide_copies(own, first, count, packed, landing, ssem, rsem):
        side = remote(packed, landing.at[:, pl.ds(32, ROWS), :], ssem.at[0], rsem.at[0], peer, me_r)
        up, down = wide_rows(own, first, count, ssem, rsem, 1)
        up += (remote(packed.at[:, pl.ds(104, 24), :], landing.at[:, pl.ds(8, 24), :], ssem.at[3], rsem.at[3], peer, me_r + 1),)
        down += (remote(packed.at[:, pl.ds(0, 24), :], landing.at[:, pl.ds(160, 24), :], ssem.at[4], rsem.at[4], peer, me_r - 1),)
        return side, up, down

    def map_copies():
        return (None, *wide_rows(xb, 0, 2, xs_sem, xr_sem, 5))

    def flow_copies():
        return wide_copies(xb, 2, 6, sp, rp, xs_sem, xr_sem)

    def force_copies():
        return wide_copies(xf, 0, 4, sf, rf, fs_sem, fr_sem)

    def edge_copies(c):
        north, south = me_r + 1, me_r - 1
        side = remote(send_col.at[c], recv_col.at[c, pl.ds(8, ROWS), :], cs_sem.at[c, 0], cr_sem.at[c, 0], peer, me_r)
        up = (remote(send_row.at[0, c], recv_row.at[0, c], cs_sem.at[c, 1], cr_sem.at[c, 1], me_c, north),
              remote(send_col.at[c, pl.ds(ROWS - 8, 8), :], recv_col.at[c, pl.ds(0, 8), :], cs_sem.at[c, 2], cr_sem.at[c, 2], peer, north))
        down = (remote(send_row.at[1, c], recv_row.at[1, c], cs_sem.at[c, 3], cr_sem.at[c, 3], me_c, south),
                remote(send_col.at[c, pl.ds(0, 8), :], recv_col.at[c, pl.ds(8 + ROWS, 8), :], cs_sem.at[c, 4], cr_sem.at[c, 4], peer, south))
        return side, up, down

    def start_all(copies):
        side, up, down = copies
        if side is not None:
            side.start()

        @pl.when(has_n)
        def _():
            for copy in up:
                copy.start()

        @pl.when(has_s)
        def _():
            for copy in down:
                copy.start()

    def wait_recv_all(copies):
        side, up, down = copies
        if side is not None:
            side.wait_recv()

        @pl.when(has_s)
        def _():
            for copy in up:
                copy.wait_recv()

        @pl.when(has_n)
        def _():
            for copy in down:
                copy.wait_recv()

    def wait_send_all(copies):
        side, up, down = copies
        if side is not None:
            side.wait_send()

        @pl.when(has_n)
        def _():
            for copy in up:
                copy.wait_send()

        @pl.when(has_s)
        def _():
            for copy in down:
                copy.wait_send()

    def all_entered():
        @pl.when((me_r == 0) | (me_r == 3))
        def _():
            pl.semaphore_wait(barrier, 3)

        @pl.when((me_r != 0) & (me_r != 3))
        def _():
            pl.semaphore_wait(barrier, 5)

    def pack_and_send(c, with_maps=False):
        for copy in loads(c):
            copy.wait()
        lane = lanes(PK)

        def block(i, carry):
            r = pl.multiple_of(i * PK, PK)
            pairs = [(f, c * CHUNK + kk, m) for f in range(4) for kk in range(CHUNK) for m in range(2)]
            column = [[buf[f, k, m, t, pl.ds(8 + r, PK), :] for f, k, m in pairs] for t in range(2)]
            if with_maps:
                for t in range(2):
                    column[t] += [xb[0, t, pl.ds(32 + r, PK), :], xb[1, t, pl.ds(32 + r, PK), :]]
            packed = jnp.zeros((PK, LN), F32)
            count = len(column[0])
            for i in range(count + 1):
                edge = jnp.where(lane == 0, column[0][min(i, count - 1)], column[1][max(i - 1, 0)])
                edge = pltpu.roll(edge, 2 * i, 1) if i else edge
                packed = jnp.where(lane >= 2 * i - 1, edge, packed) if i else edge
            send_col[c, pl.ds(r, PK), :] = packed
            return carry
        for kk in range(CHUNK):
            for m in range(2):
                jj = kk * 2 + m
                k = c * CHUNK + kk
                for side, row in ((0, 8 + ROWS - 1), (1, 8)):
                    for f in range(4):
                        for t in range(2):
                            send_row[side, c, t, f, jj:jj + 1, :] = buf[f, k, m, t, row:row + 1, :]
        lax.fori_loop(0, ROWS // PK, block, 0)
        if with_maps:
            all_entered()
            start_all(map_copies())
        start_all(edge_copies(c))

    pack_and_send(0, with_maps=True)

    def pack_pairs(source, firsts, seconds, send):
        lane = lanes(ROWS)
        outer = (lane < 32) | (lane >= 96)
        for slot, (f, g) in enumerate(zip(firsts, seconds)):
            a, b = (jnp.where(lane < 64, source[n, 0, 32:32 + ROWS, :], source[n, 1, 32:32 + ROWS, :]) for n in (f, g))
            send[slot, :, :] = jnp.where(outer, a, pltpu.roll(b, 64, 1))

    def pack_wide():
        for copy in flow_loads():
            copy.wait()
        pack_pairs(xb, (0, 2, 4, 6), (1, 3, 5, 7), sp)
        start_all(flow_copies())

    def pack_rest(c, carry):
        pack_and_send(c)
        return carry
    lax.fori_loop(1, NCH - 2, pack_rest, 0)
    pack_wide()
    lax.fori_loop(NCH - 2, NCH - 1, pack_rest, 0)

    RHO_T = np.float32(-THERM_EXP * PRESS_SCALE / LEVELS / 2)
    RHO_S = np.float32(HALINE_CON * PRESS_SCALE / LEVELS / 2)
    BR = 128
    SB = 16

    def pressure_rows(k, slot, base, rows):
        for m in range(2):
            for t in range(2):
                half = RHO_T * buf[2, k, m, t, pl.ds(base, rows), :] + RHO_S * buf[3, k, m, t, pl.ds(base, rows), :]
                p = pacc[m, t, pl.ds(base, rows), :] + half
                slot[m, t, pl.ds(base, rows), :] = p
                pacc[m, t, pl.ds(base, rows), :] = p + half

    def shift_u(c, kk, m, base, rows):
        u = [buf[0, c * CHUNK + kk, m, t, pl.ds(base, rows), :] for t in range(2)]
        edge = halo(recv_col[c, pl.ds(base, rows), :], kk * 2 + m)
        ue, uw = east_pair(*u, edge), west_pair(*u, edge)
        for t in range(2):
            uwp[m, t, pl.ds(base, rows), :] = uw[t]
            dup[m, t, pl.ds(base, rows), :] = ue[t] - uw[t]

    def level(c, kk, now, later):
        k = c * CHUNK + kk
        pressure_rows(k, now, 8 + ROWS, 8)
        for m in range(2):
            shift_u(c, kk, m, 8, 8)
            ve = east_pair(*(buf[1, k, m, t, 0:8, :] for t in range(2)), halo(recv_col[c, 0:8, :], PAIRS + kk * 2 + m))
            for t in range(2):
                vep[m, t, 0:8, :] = ve[t]
        level_no = k.astype(F32)
        before = table[0, k]
        following = jnp.minimum(k + 1, LEVELS - 1)

        def block(i, carry):
            for q in range(0, BR, SB):
                piece(pl.multiple_of(i * BR + q, SB), pl.multiple_of(8 + i * BR + q, 8))
            return carry

        def piece(r, b):
            wet_x = [ku[t, pl.ds(r, SB), :] > level_no for t in range(2)]
            wet_y = [kv[t, pl.ds(r, SB), :] > level_no for t in range(2)]
            packed = recv_col[c, pl.ds(b, SB), :]
            packed_r = rhoc[pl.ds(r, SB), :]
            for m in range(2):
                j = kk * 2 + m
                shift_u(c, kk, m, pl.multiple_of(b + 8, 8), SB)
                half = halo(packed_r, j)
                p_edge = phal[m, pl.ds(r, SB), :] + half
                phal[m, pl.ds(r, SB), :] = p_edge + half
                v = [buf[1, k, m, t, pl.ds(b, SB), :] for t in range(2)]
                p = [now[m, t, pl.ds(b, SB), :] for t in range(2)]
                v_edge = halo(packed, PAIRS + j)
                ve, vw = east_pair(*v, v_edge), west_pair(*v, v_edge)
                pe = east_pair(*p, p_edge)
                for t in range(2):
                    vep[m, t, pl.ds(b, SB), :] = ve[t]
                    u = buf[0, k, m, t, pl.ds(b, SB), :]
                    un = buf[0, k, m, t, pl.ds(b + 1, SB), :]
                    us = buf[0, k, m, t, pl.ds(b - 1, SB), :]
                    vs = buf[1, k, m, t, pl.ds(b - 1, SB), :]
                    vn = buf[1, k, m, t, pl.ds(b + 1, SB), :]
                    pn = now[m, t, pl.ds(b + 1, SB), :]
                    w = (v[t] + vs) + (ve[t] + vep[m, t, pl.ds(b - 1, SB), :])
                    z = (u + un) + (uwp[m, t, pl.ds(b, SB), :] + uwp[m, t, pl.ds(b + 1, SB), :])
                    gu = (p[t] - pe[t]) - (0.5 * u) * dup[m, t, pl.ds(b, SB), :] - (0.125 * w) * (un - us)
                    gu = jnp.where(wet_x[t], gu, 0.0)
                    gsum[0, m, t, pl.ds(r, SB), :] += gu
                    new = u + gu + before * cu[m, t, pl.ds(r, SB), :]
                    cu[m, t, pl.ds(r, SB), :] = new
                    tu[k, m, t, pl.ds(r, SB), :] = new
                    gv = (p[t] - pn) - (0.125 * z) * (ve[t] - vw[t]) - (0.5 * v[t]) * (vn - vs)
                    gv = jnp.where(wet_y[t], gv, 0.0)
                    gsum[1, m, t, pl.ds(r, SB), :] += gv
                    new = v[t] + gv + before * cv[m, t, pl.ds(r, SB), :]
                    cv[m, t, pl.ds(r, SB), :] = new
                    tv[k, m, t, pl.ds(r, SB), :] = new
            pressure_rows(following, later, b, SB)
        lax.fori_loop(0, ROWS // BR, block, 0)

    def first_pressure(i, carry):
        pressure_rows(0, pbufa, pl.multiple_of(8 + i * 64, 8), 64)
        return carry
    lax.fori_loop(0, 2, first_pressure, 0)

    def chunk_step(c, carry):
        @pl.when(c == 1)
        def _():
            pack_and_send(NCH - 1)

        wait_recv_all(edge_copies(c))

        @pl.when(c == 0)
        def _():
            face_maps()

        for kk in range(CHUNK):
            k = c * CHUNK + kk
            for m in range(2):
                jj = kk * 2 + m
                for side, row in ((0, 7), (1, 8 + ROWS)):
                    for f in range(4):
                        for t in range(2):
                            buf[f, k, m, t, row:row + 1, :] = recv_row[side, c, t, f, jj:jj + 1, :]
        packed = recv_col[c, 8:8 + ROWS, :]
        rhoc[...] = RHO_T * pltpu.roll(packed, LN - 4 * PAIRS, 1) + RHO_S * pltpu.roll(packed, LN - 6 * PAIRS, 1)

        def two_levels(h, carry2):
            level(c, 2 * h, pbufa, pbufb)
            level(c, 2 * h + 1, pbufb, pbufa)
            return carry2
        lax.fori_loop(0, CHUNK // 2, two_levels, 0)
        return carry

    def face_maps():
        wait_recv_all(map_copies())

        def maps(i, carry):
            r = pl.multiple_of(i * 64, 64)
            packed = recv_col[0, pl.ds(8 + r, 64), :]
            kt = [xb[0, t, pl.ds(32 + r, 64), :] for t in range(2)]
            ht = [xb[1, t, pl.ds(32 + r, 64), :] for t in range(2)]
            ke = east_pair(*kt, halo(packed, 4 * PAIRS))
            he = east_pair(*ht, halo(packed, 4 * PAIRS + 1))
            for t in range(2):
                kx = jnp.minimum(kt[t], ke[t])
                ky = jnp.minimum(kt[t], xb[0, t, pl.ds(33 + r, 64), :])
                ku[t, pl.ds(r, 64), :] = kx
                kv[t, pl.ds(r, 64), :] = ky
                hux[t, pl.ds(32 + r, 64), :] = jnp.where(kx > 0.0, 0.5 * (ht[t] + he[t]), 0.0)
                huy[t, pl.ds(32 + r, 64), :] = jnp.where(ky > 0.0, 0.5 * (ht[t] + xb[1, t, pl.ds(33 + r, 64), :]), 0.0)
            return carry
        lax.fori_loop(0, 2, maps, 0)

    lax.fori_loop(0, NCH, chunk_step, 0)

    packet_copies = [pltpu.make_async_copy(src, dst, ot_sem.at[i]) for i, (src, dst) in enumerate(
        ((recv_col, col_out), (recv_row, rows_out), (kmask, kmask_out)))]
    for copy in packet_copies:
        copy.start()

    def forcing(i, carry):
        r = pl.multiple_of(i * 32, 32)
        for t in range(2):
            nx = jnp.maximum(ku[t, pl.ds(r, 32), :], 1.0)
            ny = jnp.maximum(kv[t, pl.ds(r, 32), :], 1.0)
            fx = hux[t, pl.ds(32 + r, 32), :] / nx / SUBS
            fy = huy[t, pl.ds(32 + r, 32), :] / ny / SUBS
            for m in range(2):
                xf[m, t, pl.ds(32 + r, 32), :] = fx * gsum[0, m, t, pl.ds(r, 32), :]
                xf[2 + m, t, pl.ds(32 + r, 32), :] = fy * gsum[1, m, t, pl.ds(r, 32), :]
        return carry
    lax.fori_loop(0, ROWS // 32, forcing, 0)
    pack_pairs(xf, (0, 1), (2, 3), sf)
    start_all(force_copies())

    def stores(c):
        out = []
        for f, (ref, dst) in enumerate(((tu, us_hbm), (tv, vs_hbm))):
            for t in range(2):
                out.append(pltpu.make_async_copy(ref.at[pl.ds(c * CHUNK, CHUNK), :, t, :, :],
                                                 dst.at[pl.ds(c * CHUNK, CHUNK), :, :, pl.ds(t * LN, LN)], st_sem.at[c, f * 2 + t]))
        return out

    def upward(step, carry):
        c = NCH - 1 - step

        def block(i, carry2):
            r = pl.multiple_of(i * UP, UP)
            for f, (ref, kp) in enumerate(((tu, ku), (tv, kv))):
                for t in range(2):
                    depth = kp[t, pl.ds(r, UP), :]
                    below = [ref[c * CHUNK + CHUNK, m, t, pl.ds(r, UP), :] for m in range(2)]
                    total = [xsum[f, m, t, pl.ds(r, UP), :] for m in range(2)]
                    for kk in range(CHUNK - 1, -1, -1):
                        k = c * CHUNK + kk
                        level_no = k.astype(F32)
                        inv = jnp.where(depth > level_no + 1.0, table[2, k], jnp.where(depth > level_no, table[3, k], 0.0))
                        for m in range(2):
                            below[m] = ref[k, m, t, pl.ds(r, UP), :] * inv + table[1, k] * below[m]
                            ref[k, m, t, pl.ds(r, UP), :] = below[m]
                            total[m] = total[m] + below[m]
                    for m in range(2):
                        xsum[f, m, t, pl.ds(r, UP), :] = total[m]
            return carry2
        lax.fori_loop(0, ROWS // UP, block, 0)
        for copy in stores(c):
            copy.start()
        return carry
    lax.fori_loop(0, NCH, upward, 0)

    wait_recv_all(flow_copies())

    def unpack_wide(i, carry):
        r = pl.multiple_of(i * 96, 32)
        for pair in range(4):
            tile = rp[pair, pl.ds(r, 96), :]
            xb[2 * pair, 2, pl.ds(r, 96), :] = tile
            xb[2 * pair + 1, 2, pl.ds(r, 96), :] = pltpu.roll(tile, 64, 1)
        return carry
    lax.fori_loop(0, EXT // 96, unpack_wide, 0)

    XR = 88

    def depths(i, carry):
        r = pl.multiple_of(8 + i * XR, 8)
        kt = [xb[0, t, pl.ds(r, XR), :] for t in range(3)]
        ht = [xb[1, t, pl.ds(r, XR), :] for t in range(3)]
        for t in range(3):
            kx = jnp.minimum(kt[t], east(kt[t], kt[NEXT[t]]))
            ky = jnp.minimum(kt[t], xb[0, t, pl.ds(r + 1, XR), :])
            hux[t, pl.ds(r, XR), :] = jnp.where(kx > 0.0, 0.5 * (ht[t] + east(ht[t], ht[NEXT[t]])), 0.0)
            huy[t, pl.ds(r, XR), :] = jnp.where(ky > 0.0, 0.5 * (ht[t] + xb[1, t, pl.ds(r + 1, XR), :]), 0.0)
            cc[t, pl.ds(r, XR), :] = jnp.where(kt[t] > 0.0, WAVE_COURANT, 0.0)
        return carry
    for t in range(3):
        for ref in (hux, huy):
            ref[t, 0:8, :] = zrow
        for ref in (ebufa, ebufb):
            for m in range(2):
                ref[m, t, 0:8, :] = zrow
                ref[m, t, EXT - 8:EXT, :] = zrow
    lax.fori_loop(0, 2, depths, 0)

    def coefficients(i, carry):
        r = pl.multiple_of(8 + i * XR, 8)
        hx = [hux[t, pl.ds(r, XR), :] for t in range(3)]
        for t in range(3):
            c0 = cc[t, pl.ds(r, XR), :]
            cw = WAVE_COURANT * c0
            ae[t, pl.ds(r, XR), :] = cw * hx[t]
            aw[t, pl.ds(r, XR), :] = cw * west(hx[t], hx[PREV[t]])
            an[t, pl.ds(r, XR), :] = cw * huy[t, pl.ds(r, XR), :]
            as_[t, pl.ds(r, XR), :] = cw * huy[t, pl.ds(r - 1, XR), :]
        return carry
    lax.fori_loop(0, 2, coefficients, 0)

    def first_subcycle(m, base, rows):
        tx = [xb[4 + m, t, pl.ds(base, rows), :] for t in range(3)]
        for t in range(3):
            c0 = cc[t, pl.ds(base, rows), :]
            ty = xb[6 + m, t, pl.ds(base, rows), :]
            div = tx[t] - west(tx[t], tx[PREV[t]]) + ty - xb[6 + m, t, pl.ds(base - 1, rows), :]
            change = -c0 * div
            dbuf[m, t, pl.ds(base, rows), :] = change
            eta = jnp.where(c0 > 0.0, xb[2 + m, t, pl.ds(base, rows), :], 0.0) + change
            ebufa[m, t, pl.ds(base, rows), :] = eta

    def first_block(i, carry):
        for m in range(2):
            first_subcycle(m, pl.multiple_of(8 + i * XR, 8), XR)
        return carry
    lax.fori_loop(0, 2, first_block, 0)

    weights_load.wait()
    whole = weights[SUBS - 1]
    moment = weights[SUBS - 1]
    for n in range(SUBS - 2, -1, -1):
        whole = whole + weights[n]
        moment = moment + whole

    def first_sums(i, carry):
        r = pl.multiple_of(i * 8, 8)
        for m in range(2):
            for t in range(3):
                eta = ebufa[m, t, pl.ds(32 + r, 8), :]
                bacc[m, t, pl.ds(r, 8), :] = whole * eta
                if t < 2:
                    eacc[m, t, pl.ds(r, 8), :] = weights[0] * eta
        return carry
    lax.fori_loop(0, 17, first_sums, 0)

    wait_recv_all(force_copies())

    def unpack_force(i, carry):
        r = pl.multiple_of(i * 96, 32)
        for m in range(2):
            tile = rf[m, pl.ds(r, 96), :]
            xf[m, 2, pl.ds(r, 96), :] = tile
            xf[2 + m, 2, pl.ds(r, 96), :] = pltpu.roll(tile, 64, 1)
        return carry
    lax.fori_loop(0, EXT // 96, unpack_force, 0)

    def forcing_divergence(i, carry):
        r = pl.multiple_of(8 + i * XR, 8)
        for m in range(2):
            fx = [xf[m, t, pl.ds(r, XR), :] for t in range(3)]
            for t in range(3):
                div = fx[t] - west(fx[t], fx[PREV[t]]) + xf[2 + m, t, pl.ds(r, XR), :] - xf[2 + m, t, pl.ds(r - 1, XR), :]
                gbuf[m, t, pl.ds(r, XR), :] = cc[t, pl.ds(r, XR), :] * div
        return carry
    lax.fori_loop(0, 2, forcing_divergence, 0)

    def subcycle(n, tail, lo, hi, old, new):
        tail = tail - weights[n - 2]
        weight = weights[n - 1]
        for r, end in ((lo, 96), (96, hi)):
            first = max(r, 32)
            for t in range(3):
                c_e, c_w = ae[t, r:end, :], aw[t, r:end, :]
                c_n, c_s = an[t, r:end, :], as_[t, r:end, :]
                for m in range(2):
                    e = old[m, t, r:end, :]
                    to_e = east(e, old[m, NEXT[t], r:end, :])
                    to_w = west(e, old[m, PREV[t], r:end, :])
                    to_n = old[m, t, r + 1:end + 1, :]
                    to_s = old[m, t, r - 1:end - 1, :]
                    d = dbuf[m, t, r:end, :] - gbuf[m, t, r:end, :]
                    d = d + (c_e * (to_e - e) + c_w * (to_w - e)) + (c_n * (to_n - e) + c_s * (to_s - e))
                    dbuf[m, t, r:end, :] = d
                    e = e + d
                    new[m, t, r:end, :] = e
                    last = min(end, 168)
                    bacc[m, t, first - 32:last - 32, :] += tail * e[first - r:last - r]
                    if t < 2:
                        last = min(end, 160)
                        eacc[m, t, first - 32:last - 32, :] += weight * e[first - r:last - r]
        return tail

    tail = subcycle(2, whole, 8, 184, ebufa, ebufb)
    for first_n, steps, lo, hi in ((3, 1, 8, 184), (5, 4, 16, 176), (13, 4, 24, 168)):
        def two_cycles(h, carry, first_n=first_n, lo=lo, hi=hi):
            n = first_n + 2 * h
            carry = subcycle(n, carry, lo, hi, ebufb, ebufa)
            return subcycle(n + 1, carry, lo, hi, ebufa, ebufb)
        tail = lax.fori_loop(0, steps, two_cycles, tail)

    eta_copies = [pltpu.make_async_copy(eacc.at[:, t, pl.ds(0, ROWS), :], eta_out.at[:, :, pl.ds(t * LN, LN)], ot_sem.at[4 + t]) for t in range(2)]
    for copy in eta_copies:
        copy.start()

    AV = 64

    def average_copies(i):
        r = pl.multiple_of(i * AV, AV)
        return [pltpu.make_async_copy(src, dst, av_sem.at[i, n]) for n, (src, dst) in enumerate((
            (txb.at[:, pl.ds(r, AV), :], tx_out.at[:, pl.ds(r, AV), :]), (tyb.at[:, pl.ds(r, AV), :], ty_out.at[:, pl.ds(r, AV), :]),
            (corr.at[:, :, :, pl.ds(r, AV), :], corr_out.at[:, :, :, pl.ds(r, AV), :])))]

    def averages(i, carry):
        for q in range(0, AV, 16):
            r = pl.multiple_of(i * AV + q, 16)
            g = pl.multiple_of(32 + i * AV + q, 16)
            for t in range(2):
                depth_x = hux[t, pl.ds(g, 16), :]
                depth_y = huy[t, pl.ds(g, 16), :]
                kx = ku[t, pl.ds(r, 16), :]
                ky = kv[t, pl.ds(r, 16), :]
                inv_x = 1.0 / (depth_x + jnp.where(kx > 0.0, 0.0, 1.0))
                inv_y = 1.0 / (depth_y + jnp.where(ky > 0.0, 0.0, 1.0))
                mean_x = 1.0 / jnp.maximum(kx, 1.0)
                mean_y = 1.0 / jnp.maximum(ky, 1.0)
                for m in range(2):
                    lane = slice(t * LN, (t + 1) * LN)
                    acc = bacc[m, t, pl.ds(r, 16), :]
                    tx = whole * xb[4 + m, t, pl.ds(g, 16), :] + moment * xf[m, t, pl.ds(g, 16), :] \
                        - WAVE_COURANT * depth_x * (east(acc, bacc[m, NEXT[t], pl.ds(r, 16), :]) - acc)
                    ty = whole * xb[6 + m, t, pl.ds(g, 16), :] + moment * xf[2 + m, t, pl.ds(g, 16), :] \
                        - WAVE_COURANT * depth_y * (bacc[m, t, pl.ds(r + 1, 16), :] - acc)
                    tx = jnp.where(kx > 0.0, tx, 0.0)
                    ty = jnp.where(ky > 0.0, ty, 0.0)
                    txb[m, pl.ds(r, 16), lane] = tx
                    tyb[m, pl.ds(r, 16), lane] = ty
                    corr[0, m, t, pl.ds(r, 16), :] = tx * inv_x - xsum[0, m, t, pl.ds(r, 16), :] * mean_x
                    corr[1, m, t, pl.ds(r, 16), :] = ty * inv_y - xsum[1, m, t, pl.ds(r, 16), :] * mean_y
        for copy in average_copies(i):
            copy.start()
        return carry
    lax.fori_loop(0, ROWS // AV, averages, 0)

    wait_send_all(map_copies())
    wait_send_all(flow_copies())
    wait_send_all(force_copies())
    for copy in packet_copies + eta_copies:
        copy.wait()
    for i in range(ROWS // AV):
        for copy in average_copies(i):
            copy.wait()

    def drain(c, carry):
        wait_send_all(edge_copies(c))
        for copy in stores(c):
            copy.wait()
        return carry
    lax.fori_loop(0, NCH, drain, 0)


def tracer_kernel(u_hbm, v_hbm, t_hbm, s_hbm, us_hbm, vs_hbm, eta_in, tx_in, ty_in, corr_in, kmask_in, col_in, rows_in,
                  eta_hbm, tx_hbm, ty_hbm, un_hbm, vn_hbm, tn_hbm, sn_hbm,
                  buf, tt, ts, ct, su, sv, small, corr, kmask, cols, rows, ld_sem, ed_sem, st_sem, sv_sem, in_sem, out_sem, table):
    hbm = (u_hbm, v_hbm, t_hbm, s_hbm)
    sources = (eta_in, tx_in, ty_in)
    sinks = (eta_hbm, tx_hbm, ty_hbm)

    def loads(c):
        out = []
        for f in range(4):
            for t in range(2):
                out.append(pltpu.make_async_copy(
                    hbm[f].at[pl.ds(c * TC, TC), :, :, pl.ds(t * LN, LN)],
                    buf.at[f, pl.ds(c * TC, TC), :, t, pl.ds(8, ROWS), :], ld_sem.at[c, f * 2 + t]))
        for f, (src, dst) in enumerate(((us_hbm, su), (vs_hbm, sv))):
            out.append(pltpu.make_async_copy(src.at[pl.ds(c * TC, TC)], dst.at[pl.ds(c * TC, TC)], ld_sem.at[c, 8 + f]))
        return out

    def stores_v(c):
        return [pltpu.make_async_copy(src.at[pl.ds(c * TC, TC)], dst.at[pl.ds(c * TC, TC)], sv_sem.at[c, f])
                for f, (src, dst) in enumerate(((su, un_hbm), (sv, vn_hbm)))]

    def stores_t(c):
        return [pltpu.make_async_copy(src.at[pl.ds(c * TC, TC)], dst.at[pl.ds(c * TC, TC)], st_sem.at[c, f])
                for f, (src, dst) in enumerate(((tt, tn_hbm), (ts, sn_hbm)))]

    edges = [pltpu.make_async_copy(src, dst, ed_sem.at[i])
             for i, (src, dst) in enumerate(((col_in, cols), (rows_in, rows), (corr_in, corr), (kmask_in, kmask)))]
    for copy in edges:
        copy.start()
    for c in range(AHEAD):
        for copy in loads(c):
            copy.start()
    write_table(table, DIFF_NUMBER)
    small_in = [pltpu.make_async_copy(sources[i], small.at[i], in_sem.at[i]) for i in range(3)]
    small_out = [pltpu.make_async_copy(small.at[i], sinks[i], out_sem.at[i]) for i in range(3)]
    for copy in small_in:
        copy.start()

    def zero_planes(i, carry):
        r = pl.multiple_of(i * 16, 16)
        z = jnp.zeros((16, 2 * LN), F32)
        for f in range(2):
            for m in range(2):
                for t in range(2):
                    ct[f, m, t, pl.ds(r, 16), :] = z[:, :LN]
        for m in range(2):
            for ref in (tt, ts):
                ref[LEVELS, m, pl.ds(r, 16), :] = z
        return carry
    lax.fori_loop(0, ROWS // 16, zero_planes, 0)
    for copy in edges:
        copy.wait()

    BR = 128
    SB = 16

    def level(k, c, kk):
        level_no = k.astype(F32)
        before = table[0, k]

        def block(i, carry):
            for q in range(0, BR, SB):
                piece(pl.multiple_of(i * BR + q, SB), pl.multiple_of(8 + i * BR + q, 8))
            return carry

        def piece(r, b):
            wet = [kmask[0, t, pl.ds(r, SB), :] > level_no for t in range(2)]
            packed = cols[c, pl.ds(b, SB), :]
            for m in range(2):
                j = kk * 2 + m
                u = [buf[0, k, m, t, pl.ds(b, SB), :] for t in range(2)]
                v = [buf[1, k, m, t, pl.ds(b, SB), :] for t in range(2)]
                vs = [buf[1, k, m, t, pl.ds(b - 1, SB), :] for t in range(2)]
                uw = west_pair(*u, halo(packed, j))
                for f, ref in ((2, tt), (3, ts)):
                    q = [buf[f, k, m, t, pl.ds(b, SB), :] for t in range(2)]
                    edge = halo(packed, f * PAIRS + j)
                    qe, qw = east_pair(*q, edge), west_pair(*q, edge)
                    for t in range(2):
                        lane = slice(t * LN, (t + 1) * LN)
                        fy = v[t] * (q[t] + buf[f, k, m, t, pl.ds(b + 1, SB), :])
                        fs = vs[t] * (q[t] + buf[f, k, m, t, pl.ds(b - 1, SB), :])
                        adv = q[t] - 0.5 * ((u[t] * (q[t] + qe[t]) - uw[t] * (q[t] + qw[t])) + (fy - fs))
                        adv = jnp.where(wet[t], adv, 0.0)
                        new = adv + before * ct[f - 2, m, t, pl.ds(r, SB), :]
                        ct[f - 2, m, t, pl.ds(r, SB), :] = new
                        ref[k, m, pl.ds(r, SB), lane] = new
            for t in range(2):
                lane = slice(t * LN, (t + 1) * LN)
                wet_x = kmask[1, t, pl.ds(r, SB), :] > level_no
                wet_y = kmask[2, t, pl.ds(r, SB), :] > level_no
                for m in range(2):
                    su[k, m, pl.ds(r, SB), lane] = jnp.where(wet_x, su[k, m, pl.ds(r, SB), lane] + corr[0, m, t, pl.ds(r, SB), :], 0.0)
                    sv[k, m, pl.ds(r, SB), lane] = jnp.where(wet_y, sv[k, m, pl.ds(r, SB), lane] + corr[1, m, t, pl.ds(r, SB), :], 0.0)
        lax.fori_loop(0, ROWS // BR, block, 0)

    def chunk_step(c, carry):
        @pl.when(c + AHEAD < LEVELS // TC)
        def _():
            for copy in loads(c + AHEAD):
                copy.start()

        for copy in loads(c):
            copy.wait()
        packet = c // (CHUNK // TC)
        first = lax.rem(c, CHUNK // TC) * TC
        for kk in range(TC):
            k = c * TC + kk
            for m in range(2):
                jj = (first + kk) * 2 + m
                for f in (1, 2, 3):
                    for t in range(2):
                        buf[f, k, m, t, 7:8, :] = rows[0, packet, t, f, pl.ds(jj, 1), :]
                for f in (2, 3):
                    for t in range(2):
                        buf[f, k, m, t, 8 + ROWS:9 + ROWS, :] = rows[1, packet, t, f, pl.ds(jj, 1), :]

        def one_level(kk, carry2):
            level(c * TC + kk, packet, first + kk)
            return carry2
        lax.fori_loop(0, TC, one_level, 0)
        for copy in stores_v(c):
            copy.start()
        return carry
    lax.fori_loop(0, LEVELS // TC, chunk_step, 0)

    for copy in small_in:
        copy.wait()
    for copy in small_out:
        copy.start()

    def upward(step, carry):
        c = LEVELS // TC - 1 - step

        def block(i, carry2):
            r = pl.multiple_of(i * UP, UP)
            for t in range(2):
                lane = slice(t * LN, (t + 1) * LN)
                depth = kmask[0, t, pl.ds(r, UP), :]
                below = [[ref[c * TC + TC, m, pl.ds(r, UP), lane] for m in range(2)] for ref in (tt, ts)]
                for kk in range(TC - 1, -1, -1):
                    k = c * TC + kk
                    level_no = k.astype(F32)
                    inv = jnp.where(depth > level_no + 1.0, table[2, k], jnp.where(depth > level_no, table[3, k], 0.0))
                    for f, ref in enumerate((tt, ts)):
                        for m in range(2):
                            below[f][m] = ref[k, m, pl.ds(r, UP), lane] * inv + table[1, k] * below[f][m]
                            ref[k, m, pl.ds(r, UP), lane] = below[f][m]
            return carry2
        lax.fori_loop(0, ROWS // UP, block, 0)
        for copy in stores_t(c):
            copy.start()
        return carry
    lax.fori_loop(0, LEVELS // TC, upward, 0)

    for copy in small_out:
        copy.wait()

    def drain(c, carry):
        for copy in stores_v(c) + stores_t(c):
            copy.wait()
        return carry
    lax.fori_loop(0, LEVELS // TC, drain, 0)


def solution(mesh):
    assert mesh.shape["col"] == 2 and mesh.shape["row"] == 4
    any_spec = pl.BlockSpec(memory_space=pl.ANY)
    shape = lambda *dims: jax.ShapeDtypeStruct(dims, F32)
    dma = lambda *dims: pltpu.SemaphoreType.DMA(dims)
    vm = lambda *dims: pltpu.VMEM(dims, F32)
    full = (LEVELS, 2, ROWS, 2 * LN)
    flat = (2, ROWS, 2 * LN)

    momentum = pl.pallas_call(
        momentum_kernel,
        name="momentum",
        out_shape=(shape(*full), shape(*full), shape(*flat), shape(*flat), shape(*flat), shape(2, 2, 2, ROWS, LN),
                   shape(3, 2, ROWS, LN), shape(NCH, PR, LN), shape(2, NCH, 2, 4, PAIRS, LN)),
        in_specs=[any_spec] * 10,
        out_specs=(any_spec,) * 9,
        scratch_shapes=[
            vm(4, LEVELS, 2, 2, PR, LN), vm(LEVELS + 1, 2, 2, ROWS, LN), vm(LEVELS + 1, 2, 2, ROWS, LN),
            vm(2, 2, ROWS, LN), vm(2, 2, ROWS, LN), vm(2, 2, PR, LN), vm(2, 2, PR, LN), vm(2, 2, PR, LN), vm(2, PR, LN), vm(ROWS, LN),
            vm(2, 2, 2, ROWS, LN), vm(2, 2, 2, ROWS, LN), vm(3, 2, ROWS, LN), pltpu.VMEM((ROWS, 2 * LN), jnp.int32),
            vm(2, 2, PR, LN), vm(2, 2, PR, LN), vm(2, 2, PR, LN), vm(*flat), vm(*flat), vm(2, 2, 2, ROWS, LN),
            vm(NCH, ROWS, LN), vm(NCH, PR, LN), vm(2, NCH, 2, 4, PAIRS, LN), vm(2, NCH, 2, 4, PAIRS, LN),
            vm(8, 3, EXT, LN), vm(4, ROWS, LN), vm(4, EXT, LN), vm(4, 3, EXT, LN), vm(2, ROWS, LN), vm(2, EXT, LN),
            vm(3, EXT, LN), vm(3, EXT, LN), vm(3, EXT, LN), vm(3, EXT, LN), vm(3, EXT, LN), vm(3, EXT, LN), vm(3, EXT, LN),
            vm(2, 3, EXT, LN), vm(2, 3, EXT, LN), vm(2, 3, EXT, LN), vm(2, 3, EXT, LN), vm(2, 2, ROWS + 8, LN), vm(2, 3, ROWS + 8, LN),
            dma(NCH, 8), dma(9), dma(NCH, 5), dma(NCH, 5), dma(7), dma(7), dma(5), dma(5), dma(NCH, 4), dma(6), dma(2, 3),
            pltpu.SMEM((SUBS,), F32), pltpu.SMEM((4, LEVELS), F32), pltpu.SemaphoreType.DMA,
        ],
        compiler_params=pltpu.CompilerParams(collective_id=0, has_side_effects=True, vmem_limit_bytes=67043328),
    )

    tracers = pl.pallas_call(
        tracer_kernel,
        name="tracers",
        out_shape=(shape(*flat), shape(*flat), shape(*flat), shape(*full), shape(*full), shape(*full), shape(*full)),
        in_specs=[any_spec] * 13,
        out_specs=(any_spec,) * 7,
        scratch_shapes=[
            vm(4, LEVELS, 2, 2, PR, LN), vm(LEVELS + 1, 2, ROWS, 2 * LN), vm(LEVELS + 1, 2, ROWS, 2 * LN), vm(2, 2, 2, ROWS, LN),
            vm(*full), vm(*full), vm(3, 2, ROWS, 2 * LN), vm(2, 2, 2, ROWS, LN), vm(3, 2, ROWS, LN),
            vm(NCH, PR, LN), vm(2, NCH, 2, 4, PAIRS, LN),
            dma(LEVELS // TC, 10), dma(4), dma(LEVELS // TC, 2), dma(LEVELS // TC, 2), dma(3), dma(3), pltpu.SMEM((4, LEVELS), F32),
        ],
        compiler_params=pltpu.CompilerParams(vmem_limit_bytes=67043328),
    )

    def local_step(vel_x, vel_y, pot_temp, salinity, surf_eta, trans_x, trans_y, col_depth, wet_levels, avg_weights):
        star_x, star_y, eta, tx, ty, corr, kmask, cols, rows = momentum(
            vel_x, vel_y, pot_temp, salinity, surf_eta, trans_x, trans_y, col_depth, wet_levels, avg_weights)
        return tracers(vel_x, vel_y, pot_temp, salinity, star_x, star_y, eta, tx, ty, corr, kmask, cols, rows)

    spec_3d = P(None, None, "row", "col")
    spec_2d = P(None, "row", "col")
    spec_map = P("row", "col")
    return jax.shard_map(local_step, mesh=mesh, in_specs=(spec_3d, spec_3d, spec_3d, spec_3d, spec_2d, spec_2d, spec_2d, spec_map, spec_map, P()),
                         out_specs=(spec_2d, spec_2d, spec_2d, spec_3d, spec_3d, spec_3d, spec_3d), check_vma=False)
```

```python
import functools
import numpy as np
import jax
import jax.numpy as jnp
from jax import lax
from jax.experimental import pallas as pl
from jax.experimental.pallas import tpu as pltpu
from jax.sharding import PartitionSpec as P

WAVE_COURANT = 0.4
THERM_EXP = 0.2
HALINE_CON = 0.15
PRESS_SCALE = 0.5
VISC_NUMBER = 1.0
DIFF_NUMBER = 0.5

LEVELS = 20
SUBS = 20
CHUNK = 4
NCH = LEVELS // CHUNK
PAIRS = 2 * CHUNK
ROWS = 128
LN = 128
PR = 144
EXT = 192
F32 = jnp.float32
TC = 2
AHEAD = 6
PK = 64
UP = 32
MESH_ID = pl.DeviceIdType.MESH


def solve_table(strength):
    inner = np.zeros(LEVELS)
    last = np.zeros(LEVELS)
    inner[0] = 1.0 + strength
    last[0] = 1.0
    for k in range(1, LEVELS):
        inner[k] = 1.0 + 2.0 * strength - strength**2 / inner[k - 1]
        last[k] = 1.0 + strength - strength**2 / inner[k - 1]
    ratio = strength / inner
    before = np.concatenate([[0.0], ratio[:-1]])
    return np.stack([before, ratio, 1.0 / inner, 1.0 / last]).astype(np.float32)


def write_table(table, strength):
    values = solve_table(strength)
    for i in range(values.shape[0]):
        for k in range(LEVELS):
            table[i, k] = values[i, k]


def lanes(rows):
    return lax.broadcasted_iota(jnp.int32, (rows, LN), 1)


def east(tile, following):
    return pltpu.roll(jnp.where(lanes(tile.shape[0]) == 0, following, tile), LN - 1, 1)


def west(tile, previous):
    return pltpu.roll(jnp.where(lanes(tile.shape[0]) == LN - 1, previous, tile), 1, 1)


NEXT = (1, 2, 0)
PREV = (2, 0, 1)


def halo(packed, j):
    return pltpu.roll(packed, LN - 1 - 2 * j, 1)


def east_pair(first, second, edge):
    last = lanes(first.shape[0]) == LN - 1
    a, b = pltpu.roll(first, LN - 1, 1), pltpu.roll(second, LN - 1, 1)
    return jnp.where(last, b, a), jnp.where(last, edge, b)


def west_pair(first, second, edge):
    origin = lanes(first.shape[0]) == 0
    a, b = pltpu.roll(first, 1, 1), pltpu.roll(second, 1, 1)
    return jnp.where(origin, edge, a), jnp.where(origin, a, b)


def momentum_kernel(u_hbm, v_hbm, t_hbm, s_hbm, eta_hbm, tx_hbm, ty_hbm, h_hbm, kmt_hbm, weights_hbm,
                    us_hbm, vs_hbm, eta_out, tx_out, ty_out, corr_out, kmask_out, col_out, rows_out,
                    buf, tu, tv, cu, cv, pbufa, pbufb, pacc, phal, rhoc, gsum, xsum, kmask, kmt, vep, uwp, dup, txb, tyb, corr,
                    send_col, recv_col, send_row, recv_row,
                    xb, sp, rp, xf, sf, rf, hux, huy, ae, aw, an, as_, cc, ebufa, ebufb, dbuf, gbuf, eacc, bacc,
                    ld_sem, xl_sem, cs_sem, cr_sem, xs_sem, xr_sem, fs_sem, fr_sem, st_sem, ot_sem, av_sem, weights, table, w_sem):
    weights_load = pltpu.make_async_copy(weights_hbm, weights, w_sem)
    ku, kv = kmask.at[1], kmask.at[2]
    me_c = lax.axis_index("col")
    me_r = lax.axis_index("row")
    peer = 1 - me_c
    has_n = me_r < 3
    has_s = me_r > 0
    hbm = (u_hbm, v_hbm, t_hbm, s_hbm)

    def loads(c):
        out = []
        for f in range(4):
            for t in range(2):
                out.append(pltpu.make_async_copy(
                    hbm[f].at[pl.ds(c * CHUNK, CHUNK), :, :, pl.ds(t * LN, LN)],
                    buf.at[f, pl.ds(c * CHUNK, CHUNK), :, t, pl.ds(8, ROWS), :], ld_sem.at[c, f * 2 + t]))
        return out

    def map_loads():
        return [pltpu.make_async_copy(kmt_hbm, kmt, xl_sem.at[8])] + [
            pltpu.make_async_copy(h_hbm.at[:, pl.ds(t * LN, LN)], xb.at[1, t, pl.ds(32, ROWS), :], xl_sem.at[t]) for t in range(2)]

    def flow_loads():
        return [pltpu.make_async_copy(ref.at[:, :, pl.ds(t * LN, LN)], xb.at[pl.ds(2 + 2 * i, 2), t, pl.ds(32, ROWS), :], xl_sem.at[2 + 2 * i + t])
                for t in range(2) for i, ref in enumerate((eta_hbm, tx_hbm, ty_hbm))]

    write_table(table, VISC_NUMBER)
    for copy in map_loads() + loads(0) + loads(1) + loads(2) + flow_loads() + loads(3) + loads(4) + [weights_load]:
        copy.start()

    barrier = pltpu.get_barrier_semaphore()

    def greet(col, row):
        pl.semaphore_signal(barrier, inc=1, device_id={"col": col, "row": row}, device_id_type=MESH_ID)

    greet(peer, me_r)

    @pl.when(has_n)
    def _():
        greet(me_c, me_r + 1)
        greet(peer, me_r + 1)

    @pl.when(has_s)
    def _():
        greet(me_c, me_r - 1)
        greet(peer, me_r - 1)

    zrow = jnp.zeros((8, LN), F32)
    for ref, count in ((xb, 8), (xf, 4)):
        for f in range(count):
            for t in range(3):
                ref[f, t, 0:8, :] = zrow
                ref[f, t, EXT - 8:EXT, :] = zrow
    for ref, count in ((rp, 4), (rf, 2)):
        for f in range(count):
            ref[f, 0:8, :] = zrow
            ref[f, EXT - 8:EXT, :] = zrow

    def zero_side(side, lo):
        z24 = jnp.zeros((24, LN), F32)
        for f in range(8):
            for t in range(2):
                xb[f, t, lo:lo + 24, :] = z24
        for f in range(4):
            rp[f, lo:lo + 24, :] = z24
            for t in range(2):
                xf[f, t, lo:lo + 24, :] = z24
        for f in range(2):
            rf[f, lo:lo + 24, :] = z24
        for c in range(NCH):
            recv_col[c, 136 * side:136 * side + 8, :] = zrow
            for f in range(4):
                for t in range(2):
                    recv_row[side, c, t, f, :, :] = zrow

    @pl.when(me_r == 0)
    def _():
        zero_side(0, 8)

    @pl.when(me_r == 3)
    def _():
        zero_side(1, 160)

    def zero_planes(i, carry):
        r = pl.multiple_of(i * 16, 16)
        z = jnp.zeros((16, LN), F32)
        for m in range(2):
            for t in range(2):
                pacc[m, t, pl.ds(r, 16), :] = z
            phal[m, pl.ds(r, 16), :] = z
        return carry
    lax.fori_loop(0, PR // 16, zero_planes, 0)

    def zero_planes2(i, carry):
        r = pl.multiple_of(i * 16, 16)
        z = jnp.zeros((16, LN), F32)
        for m in range(2):
            for t in range(2):
                for f in range(2):
                    gsum[f, m, t, pl.ds(r, 16), :] = z
                    xsum[f, m, t, pl.ds(r, 16), :] = z
                for ref in (cu, cv):
                    ref[m, t, pl.ds(r, 16), :] = z
                for ref in (tu, tv):
                    ref[LEVELS, m, t, pl.ds(r, 16), :] = z
        return carry
    lax.fori_loop(0, ROWS // 16, zero_planes2, 0)

    for copy in map_loads():
        copy.wait()
    for t in range(2):
        for r in range(0, ROWS, 64):
            level_count = kmt[r:r + 64, t * LN:(t + 1) * LN].astype(F32)
            xb[0, t, 32 + r:96 + r, :] = level_count
            kmask[0, t, r:r + 64, :] = level_count

    def remote(src, dst, ssem, rsem, col, row):
        return pltpu.make_async_remote_copy(src_ref=src, dst_ref=dst, send_sem=ssem, recv_sem=rsem,
                                            device_id={"col": col, "row": row}, device_id_type=MESH_ID)

    def wide_rows(own, first, count, ssem, rsem, slot):
        fields = pl.ds(first, count)
        return ((remote(own.at[fields, pl.ds(0, 2), pl.ds(136, 24), :], own.at[fields, pl.ds(0, 2), pl.ds(8, 24), :],
                        ssem.at[slot], rsem.at[slot], me_c, me_r + 1),),
                (remote(own.at[fields, pl.ds(0, 2), pl.ds(32, 24), :], own.at[fields, pl.ds(0, 2), pl.ds(160, 24), :],
                        ssem.at[slot + 1], rsem.at[slot + 1], me_c, me_r - 1),))

    def wide_copies(own, first, count, packed, landing, ssem, rsem):
        side = remote(packed, landing.at[:, pl.ds(32, ROWS), :], ssem.at[0], rsem.at[0], peer, me_r)
        up, down = wide_rows(own, first, count, ssem, rsem, 1)
        up += (remote(packed.at[:, pl.ds(104, 24), :], landing.at[:, pl.ds(8, 24), :], ssem.at[3], rsem.at[3], peer, me_r + 1),)
        down += (remote(packed.at[:, pl.ds(0, 24), :], landing.at[:, pl.ds(160, 24), :], ssem.at[4], rsem.at[4], peer, me_r - 1),)
        return side, up, down

    def map_copies():
        return (None, *wide_rows(xb, 0, 2, xs_sem, xr_sem, 5))

    def flow_copies():
        return wide_copies(xb, 2, 6, sp, rp, xs_sem, xr_sem)

    def force_copies():
        return wide_copies(xf, 0, 4, sf, rf, fs_sem, fr_sem)

    def edge_copies(c):
        north, south = me_r + 1, me_r - 1
        side = remote(send_col.at[c], recv_col.at[c, pl.ds(8, ROWS), :], cs_sem.at[c, 0], cr_sem.at[c, 0], peer, me_r)
        up = (remote(send_row.at[0, c], recv_row.at[0, c], cs_sem.at[c, 1], cr_sem.at[c, 1], me_c, north),
              remote(send_col.at[c, pl.ds(ROWS - 8, 8), :], recv_col.at[c, pl.ds(0, 8), :], cs_sem.at[c, 2], cr_sem.at[c, 2], peer, north))
        down = (remote(send_row.at[1, c], recv_row.at[1, c], cs_sem.at[c, 3], cr_sem.at[c, 3], me_c, south),
                remote(send_col.at[c, pl.ds(0, 8), :], recv_col.at[c, pl.ds(8 + ROWS, 8), :], cs_sem.at[c, 4], cr_sem.at[c, 4], peer, south))
        return side, up, down

    def start_all(copies):
        side, up, down = copies
        if side is not None:
            side.start()

        @pl.when(has_n)
        def _():
            for copy in up:
                copy.start()

        @pl.when(has_s)
        def _():
            for copy in down:
                copy.start()

    def wait_recv_all(copies):
        side, up, down = copies
        if side is not None:
            side.wait_recv()

        @pl.when(has_s)
        def _():
            for copy in up:
                copy.wait_recv()

        @pl.when(has_n)
        def _():
            for copy in down:
                copy.wait_recv()

    def wait_send_all(copies):
        side, up, down = copies
        if side is not None:
            side.wait_send()

        @pl.when(has_n)
        def _():
            for copy in up:
                copy.wait_send()

        @pl.when(has_s)
        def _():
            for copy in down:
                copy.wait_send()

    def all_entered():
        @pl.when((me_r == 0) | (me_r == 3))
        def _():
            pl.semaphore_wait(barrier, 3)

        @pl.when((me_r != 0) & (me_r != 3))
        def _():
            pl.semaphore_wait(barrier, 5)

    def pack_and_send(c, with_maps=False):
        for copy in loads(c):
            copy.wait()
        lane = lanes(PK)

        def block(i, carry):
            r = pl.multiple_of(i * PK, PK)
            pairs = [(f, c * CHUNK + kk, m) for f in range(4) for kk in range(CHUNK) for m in range(2)]
            column = [[buf[f, k, m, t, pl.ds(8 + r, PK), :] for f, k, m in pairs] for t in range(2)]
            if with_maps:
                for t in range(2):
                    column[t] += [xb[0, t, pl.ds(32 + r, PK), :], xb[1, t, pl.ds(32 + r, PK), :]]
            packed = jnp.zeros((PK, LN), F32)
            count = len(column[0])
            for i in range(count + 1):
                edge = jnp.where(lane == 0, column[0][min(i, count - 1)], column[1][max(i - 1, 0)])
                edge = pltpu.roll(edge, 2 * i, 1) if i else edge
                packed = jnp.where(lane >= 2 * i - 1, edge, packed) if i else edge
            send_col[c, pl.ds(r, PK), :] = packed
            return carry
        for kk in range(CHUNK):
            for m in range(2):
                jj = kk * 2 + m
                k = c * CHUNK + kk
                for side, row in ((0, 8 + ROWS - 1), (1, 8)):
                    for f in range(4):
                        for t in range(2):
                            send_row[side, c, t, f, jj:jj + 1, :] = buf[f, k, m, t, row:row + 1, :]
        lax.fori_loop(0, ROWS // PK, block, 0)
        if with_maps:
            all_entered()
            start_all(map_copies())
        start_all(edge_copies(c))

    pack_and_send(0, with_maps=True)

    def pack_pairs(source, firsts, seconds, send):
        lane = lanes(ROWS)
        outer = (lane < 32) | (lane >= 96)
        for slot, (f, g) in enumerate(zip(firsts, seconds)):
            a, b = (jnp.where(lane < 64, source[n, 0, 32:32 + ROWS, :], source[n, 1, 32:32 + ROWS, :]) for n in (f, g))
            send[slot, :, :] = jnp.where(outer, a, pltpu.roll(b, 64, 1))

    def pack_wide():
        for copy in flow_loads():
            copy.wait()
        pack_pairs(xb, (0, 2, 4, 6), (1, 3, 5, 7), sp)

    def pack_rest(c, carry):
        pack_and_send(c)
        return carry
    lax.fori_loop(1, NCH - 2, pack_rest, 0)
    pack_wide()
    lax.fori_loop(NCH - 2, NCH - 1, pack_rest, 0)

    RHO_T = np.float32(-THERM_EXP * PRESS_SCALE / LEVELS / 2)
    RHO_S = np.float32(HALINE_CON * PRESS_SCALE / LEVELS / 2)
    BR = 128
    SB = 16

    def pressure_rows(k, slot, base, rows):
        for m in range(2):
            for t in range(2):
                half = RHO_T * buf[2, k, m, t, pl.ds(base, rows), :] + RHO_S * buf[3, k, m, t, pl.ds(base, rows), :]
                p = pacc[m, t, pl.ds(base, rows), :] + half
                slot[m, t, pl.ds(base, rows), :] = p
                pacc[m, t, pl.ds(base, rows), :] = p + half

    def shift_u(c, kk, m, base, rows):
        u = [buf[0, c * CHUNK + kk, m, t, pl.ds(base, rows), :] for t in range(2)]
        edge = halo(recv_col[c, pl.ds(base, rows), :], kk * 2 + m)
        ue, uw = east_pair(*u, edge), west_pair(*u, edge)
        for t in range(2):
            uwp[m, t, pl.ds(base, rows), :] = uw[t]
            dup[m, t, pl.ds(base, rows), :] = ue[t] - uw[t]

    def level(c, kk, now, later):
        k = c * CHUNK + kk
        pressure_rows(k, now, 8 + ROWS, 8)
        for m in range(2):
            shift_u(c, kk, m, 8, 8)
            ve = east_pair(*(buf[1, k, m, t, 0:8, :] for t in range(2)), halo(recv_col[c, 0:8, :], PAIRS + kk * 2 + m))
            for t in range(2):
                vep[m, t, 0:8, :] = ve[t]
        level_no = k.astype(F32)
        before = table[0, k]
        following = jnp.minimum(k + 1, LEVELS - 1)

        def block(i, carry):
            for q in range(0, BR, SB):
                piece(pl.multiple_of(i * BR + q, SB), pl.multiple_of(8 + i * BR + q, 8))
            return carry

        def piece(r, b):
            wet_x = [ku[t, pl.ds(r, SB), :] > level_no for t in range(2)]
            wet_y = [kv[t, pl.ds(r, SB), :] > level_no for t in range(2)]
            packed = recv_col[c, pl.ds(b, SB), :]
            packed_r = rhoc[pl.ds(r, SB), :]
            for m in range(2):
                j = kk * 2 + m
                shift_u(c, kk, m, pl.multiple_of(b + 8, 8), SB)
                half = halo(packed_r, j)
                p_edge = phal[m, pl.ds(r, SB), :] + half
                phal[m, pl.ds(r, SB), :] = p_edge + half
                v = [buf[1, k, m, t, pl.ds(b, SB), :] for t in range(2)]
                p = [now[m, t, pl.ds(b, SB), :] for t in range(2)]
                v_edge = halo(packed, PAIRS + j)
                ve, vw = east_pair(*v, v_edge), west_pair(*v, v_edge)
                pe = east_pair(*p, p_edge)
                for t in range(2):
                    vep[m, t, pl.ds(b, SB), :] = ve[t]
                    u = buf[0, k, m, t, pl.ds(b, SB), :]
                    un = buf[0, k, m, t, pl.ds(b + 1, SB), :]
                    us = buf[0, k, m, t, pl.ds(b - 1, SB), :]
                    vs = buf[1, k, m, t, pl.ds(b - 1, SB), :]
                    vn = buf[1, k, m, t, pl.ds(b + 1, SB), :]
                    pn = now[m, t, pl.ds(b + 1, SB), :]
                    w = (v[t] + vs) + (ve[t] + vep[m, t, pl.ds(b - 1, SB), :])
                    z = (u + un) + (uwp[m, t, pl.ds(b, SB), :] + uwp[m, t, pl.ds(b + 1, SB), :])
                    gu = (p[t] - pe[t]) - (0.5 * u) * dup[m, t, pl.ds(b, SB), :] - (0.125 * w) * (un - us)
                    gu = jnp.where(wet_x[t], gu, 0.0)
                    gsum[0, m, t, pl.ds(r, SB), :] += gu
                    new = u + gu + before * cu[m, t, pl.ds(r, SB), :]
                    cu[m, t, pl.ds(r, SB), :] = new
                    tu[k, m, t, pl.ds(r, SB), :] = new
                    gv = (p[t] - pn) - (0.125 * z) * (ve[t] - vw[t]) - (0.5 * v[t]) * (vn - vs)
                    gv = jnp.where(wet_y[t], gv, 0.0)
                    gsum[1, m, t, pl.ds(r, SB), :] += gv
                    new = v[t] + gv + before * cv[m, t, pl.ds(r, SB), :]
                    cv[m, t, pl.ds(r, SB), :] = new
                    tv[k, m, t, pl.ds(r, SB), :] = new
            pressure_rows(following, later, b, SB)
        lax.fori_loop(0, ROWS // BR, block, 0)

    def first_pressure(i, carry):
        pressure_rows(0, pbufa, pl.multiple_of(8 + i * 64, 8), 64)
        return carry
    lax.fori_loop(0, 2, first_pressure, 0)

    def chunk_step(c, carry):
        @pl.when(c == 1)
        def _():
            pack_and_send(NCH - 1)
            start_all(flow_copies())

        wait_recv_all(edge_copies(c))

        @pl.when(c == 0)
        def _():
            face_maps()

        for kk in range(CHUNK):
            k = c * CHUNK + kk
            for m in range(2):
                jj = kk * 2 + m
                for side, row in ((0, 7), (1, 8 + ROWS)):
                    for f in range(4):
                        for t in range(2):
                            buf[f, k, m, t, row:row + 1, :] = recv_row[side, c, t, f, jj:jj + 1, :]
        packed = recv_col[c, 8:8 + ROWS, :]
        rhoc[...] = RHO_T * pltpu.roll(packed, LN - 4 * PAIRS, 1) + RHO_S * pltpu.roll(packed, LN - 6 * PAIRS, 1)

        def two_levels(h, carry2):
            level(c, 2 * h, pbufa, pbufb)
            level(c, 2 * h + 1, pbufb, pbufa)
            return carry2
        lax.fori_loop(0, CHUNK // 2, two_levels, 0)
        return carry

    def face_maps():
        wait_recv_all(map_copies())

        def maps(i, carry):
            r = pl.multiple_of(i * 64, 64)
            packed = recv_col[0, pl.ds(8 + r, 64), :]
            kt = [xb[0, t, pl.ds(32 + r, 64), :] for t in range(2)]
            ht = [xb[1, t, pl.ds(32 + r, 64), :] for t in range(2)]
            ke = east_pair(*kt, halo(packed, 4 * PAIRS))
            he = east_pair(*ht, halo(packed, 4 * PAIRS + 1))
            for t in range(2):
                kx = jnp.minimum(kt[t], ke[t])
                ky = jnp.minimum(kt[t], xb[0, t, pl.ds(33 + r, 64), :])
                ku[t, pl.ds(r, 64), :] = kx
                kv[t, pl.ds(r, 64), :] = ky
                hux[t, pl.ds(32 + r, 64), :] = jnp.where(kx > 0.0, 0.5 * (ht[t] + he[t]), 0.0)
                huy[t, pl.ds(32 + r, 64), :] = jnp.where(ky > 0.0, 0.5 * (ht[t] + xb[1, t, pl.ds(33 + r, 64), :]), 0.0)
            return carry
        lax.fori_loop(0, 2, maps, 0)

    lax.fori_loop(0, NCH, chunk_step, 0)

    packet_copies = [pltpu.make_async_copy(src, dst, ot_sem.at[i]) for i, (src, dst) in enumerate(
        ((recv_col, col_out), (recv_row, rows_out), (kmask, kmask_out)))]
    for copy in packet_copies:
        copy.start()

    def forcing(i, carry):
        r = pl.multiple_of(i * 32, 32)
        for t in range(2):
            nx = jnp.maximum(ku[t, pl.ds(r, 32), :], 1.0)
            ny = jnp.maximum(kv[t, pl.ds(r, 32), :], 1.0)
            fx = hux[t, pl.ds(32 + r, 32), :] / nx / SUBS
            fy = huy[t, pl.ds(32 + r, 32), :] / ny / SUBS
            for m in range(2):
                xf[m, t, pl.ds(32 + r, 32), :] = fx * gsum[0, m, t, pl.ds(r, 32), :]
                xf[2 + m, t, pl.ds(32 + r, 32), :] = fy * gsum[1, m, t, pl.ds(r, 32), :]
        return carry
    lax.fori_loop(0, ROWS // 32, forcing, 0)
    pack_pairs(xf, (0, 1), (2, 3), sf)
    start_all(force_copies())

    def stores(c):
        out = []
        for f, (ref, dst) in enumerate(((tu, us_hbm), (tv, vs_hbm))):
            for t in range(2):
                out.append(pltpu.make_async_copy(ref.at[pl.ds(c * CHUNK, CHUNK), :, t, :, :],
                                                 dst.at[pl.ds(c * CHUNK, CHUNK), :, :, pl.ds(t * LN, LN)], st_sem.at[c, f * 2 + t]))
        return out

    def upward(step, carry):
        c = NCH - 1 - step

        def block(i, carry2):
            r = pl.multiple_of(i * UP, UP)
            for f, (ref, kp) in enumerate(((tu, ku), (tv, kv))):
                for t in range(2):
                    depth = kp[t, pl.ds(r, UP), :]
                    below = [ref[c * CHUNK + CHUNK, m, t, pl.ds(r, UP), :] for m in range(2)]
                    total = [xsum[f, m, t, pl.ds(r, UP), :] for m in range(2)]
                    for kk in range(CHUNK - 1, -1, -1):
                        k = c * CHUNK + kk
                        level_no = k.astype(F32)
                        inv = jnp.where(depth > level_no + 1.0, table[2, k], jnp.where(depth > level_no, table[3, k], 0.0))
                        for m in range(2):
                            below[m] = ref[k, m, t, pl.ds(r, UP), :] * inv + table[1, k] * below[m]
                            ref[k, m, t, pl.ds(r, UP), :] = below[m]
                            total[m] = total[m] + below[m]
                    for m in range(2):
                        xsum[f, m, t, pl.ds(r, UP), :] = total[m]
            return carry2
        lax.fori_loop(0, ROWS // UP, block, 0)
        for copy in stores(c):
            copy.start()
        return carry
    lax.fori_loop(0, NCH, upward, 0)

    wait_recv_all(flow_copies())

    def unpack_wide(i, carry):
        r = pl.multiple_of(i * 96, 32)
        for pair in range(4):
            tile = rp[pair, pl.ds(r, 96), :]
            xb[2 * pair, 2, pl.ds(r, 96), :] = tile
            xb[2 * pair + 1, 2, pl.ds(r, 96), :] = pltpu.roll(tile, 64, 1)
        return carry
    lax.fori_loop(0, EXT // 96, unpack_wide, 0)

    XR = 88

    def depths(i, carry):
        r = pl.multiple_of(8 + i * XR, 8)
        kt = [xb[0, t, pl.ds(r, XR), :] for t in range(3)]
        ht = [xb[1, t, pl.ds(r, XR), :] for t in range(3)]
        for t in range(3):
            kx = jnp.minimum(kt[t], east(kt[t], kt[NEXT[t]]))
            ky = jnp.minimum(kt[t], xb[0, t, pl.ds(r + 1, XR), :])
            hux[t, pl.ds(r, XR), :] = jnp.where(kx > 0.0, 0.5 * (ht[t] + east(ht[t], ht[NEXT[t]])), 0.0)
            huy[t, pl.ds(r, XR), :] = jnp.where(ky > 0.0, 0.5 * (ht[t] + xb[1, t, pl.ds(r + 1, XR), :]), 0.0)
            cc[t, pl.ds(r, XR), :] = jnp.where(kt[t] > 0.0, WAVE_COURANT, 0.0)
        return carry
    for t in range(3):
        for ref in (hux, huy):
            ref[t, 0:8, :] = zrow
        for ref in (ebufa, ebufb):
            for m in range(2):
                ref[m, t, 0:8, :] = zrow
                ref[m, t, EXT - 8:EXT, :] = zrow
    lax.fori_loop(0, 2, depths, 0)

    def coefficients(i, carry):
        r = pl.multiple_of(8 + i * XR, 8)
        hx = [hux[t, pl.ds(r, XR), :] for t in range(3)]
        for t in range(3):
            c0 = cc[t, pl.ds(r, XR), :]
            cw = WAVE_COURANT * c0
            ae[t, pl.ds(r, XR), :] = cw * hx[t]
            aw[t, pl.ds(r, XR), :] = cw * west(hx[t], hx[PREV[t]])
            an[t, pl.ds(r, XR), :] = cw * huy[t, pl.ds(r, XR), :]
            as_[t, pl.ds(r, XR), :] = cw * huy[t, pl.ds(r - 1, XR), :]
        return carry
    lax.fori_loop(0, 2, coefficients, 0)

    def first_subcycle(m, base, rows):
        tx = [xb[4 + m, t, pl.ds(base, rows), :] for t in range(3)]
        for t in range(3):
            c0 = cc[t, pl.ds(base, rows), :]
            ty = xb[6 + m, t, pl.ds(base, rows), :]
            div = tx[t] - west(tx[t], tx[PREV[t]]) + ty - xb[6 + m, t, pl.ds(base - 1, rows), :]
            change = -c0 * div
            dbuf[m, t, pl.ds(base, rows), :] = change
            eta = jnp.where(c0 > 0.0, xb[2 + m, t, pl.ds(base, rows), :], 0.0) + change
            ebufa[m, t, pl.ds(base, rows), :] = eta

    def first_block(i, carry):
        for m in range(2):
            first_subcycle(m, pl.multiple_of(8 + i * XR, 8), XR)
        return carry
    lax.fori_loop(0, 2, first_block, 0)

    weights_load.wait()
    whole = weights[SUBS - 1]
    moment = weights[SUBS - 1]
    for n in range(SUBS - 2, -1, -1):
        whole = whole + weights[n]
        moment = moment + whole

    def first_sums(i, carry):
        r = pl.multiple_of(i * 8, 8)
        for m in range(2):
            for t in range(3):
                eta = ebufa[m, t, pl.ds(32 + r, 8), :]
                bacc[m, t, pl.ds(r, 8), :] = whole * eta
                if t < 2:
                    eacc[m, t, pl.ds(r, 8), :] = weights[0] * eta
        return carry
    lax.fori_loop(0, 17, first_sums, 0)

    wait_recv_all(force_copies())

    def unpack_force(i, carry):
        r = pl.multiple_of(i * 96, 32)
        for m in range(2):
            tile = rf[m, pl.ds(r, 96), :]
            xf[m, 2, pl.ds(r, 96), :] = tile
            xf[2 + m, 2, pl.ds(r, 96), :] = pltpu.roll(tile, 64, 1)
        return carry
    lax.fori_loop(0, EXT // 96, unpack_force, 0)

    def forcing_divergence(i, carry):
        r = pl.multiple_of(8 + i * XR, 8)
        for m in range(2):
            fx = [xf[m, t, pl.ds(r, XR), :] for t in range(3)]
            for t in range(3):
                div = fx[t] - west(fx[t], fx[PREV[t]]) + xf[2 + m, t, pl.ds(r, XR), :] - xf[2 + m, t, pl.ds(r - 1, XR), :]
                gbuf[m, t, pl.ds(r, XR), :] = cc[t, pl.ds(r, XR), :] * div
        return carry
    lax.fori_loop(0, 2, forcing_divergence, 0)

    def subcycle(n, tail, lo, hi, old, new):
        tail = tail - weights[n - 2]
        weight = weights[n - 1]
        for r, end in ((lo, 96), (96, hi)):
            first = max(r, 32)
            for t in range(3):
                c_e, c_w = ae[t, r:end, :], aw[t, r:end, :]
                c_n, c_s = an[t, r:end, :], as_[t, r:end, :]
                for m in range(2):
                    e = old[m, t, r:end, :]
                    to_e = east(e, old[m, NEXT[t], r:end, :])
                    to_w = west(e, old[m, PREV[t], r:end, :])
                    to_n = old[m, t, r + 1:end + 1, :]
                    to_s = old[m, t, r - 1:end - 1, :]
                    d = dbuf[m, t, r:end, :] - gbuf[m, t, r:end, :]
                    d = d + (c_e * (to_e - e) + c_w * (to_w - e)) + (c_n * (to_n - e) + c_s * (to_s - e))
                    dbuf[m, t, r:end, :] = d
                    e = e + d
                    new[m, t, r:end, :] = e
                    last = min(end, 168)
                    bacc[m, t, first - 32:last - 32, :] += tail * e[first - r:last - r]
                    if t < 2:
                        last = min(end, 160)
                        eacc[m, t, first - 32:last - 32, :] += weight * e[first - r:last - r]
        return tail

    tail = subcycle(2, whole, 8, 184, ebufa, ebufb)
    for first_n, steps, lo, hi in ((3, 1, 8, 184), (5, 4, 16, 176), (13, 4, 24, 168)):
        def two_cycles(h, carry, first_n=first_n, lo=lo, hi=hi):
            n = first_n + 2 * h
            carry = subcycle(n, carry, lo, hi, ebufb, ebufa)
            return subcycle(n + 1, carry, lo, hi, ebufa, ebufb)
        tail = lax.fori_loop(0, steps, two_cycles, tail)

    eta_copies = [pltpu.make_async_copy(eacc.at[:, t, pl.ds(0, ROWS), :], eta_out.at[:, :, pl.ds(t * LN, LN)], ot_sem.at[4 + t]) for t in range(2)]
    for copy in eta_copies:
        copy.start()

    AV = 64

    def average_copies(i):
        r = pl.multiple_of(i * AV, AV)
        return [pltpu.make_async_copy(src, dst, av_sem.at[i, n]) for n, (src, dst) in enumerate((
            (txb.at[:, pl.ds(r, AV), :], tx_out.at[:, pl.ds(r, AV), :]), (tyb.at[:, pl.ds(r, AV), :], ty_out.at[:, pl.ds(r, AV), :]),
            (corr.at[:, :, :, pl.ds(r, AV), :], corr_out.at[:, :, :, pl.ds(r, AV), :])))]

    def averages(i, carry):
        for q in range(0, AV, 16):
            r = pl.multiple_of(i * AV + q, 16)
            g = pl.multiple_of(32 + i * AV + q, 16)
            for t in range(2):
                depth_x = hux[t, pl.ds(g, 16), :]
                depth_y = huy[t, pl.ds(g, 16), :]
                kx = ku[t, pl.ds(r, 16), :]
                ky = kv[t, pl.ds(r, 16), :]
                inv_x = 1.0 / (depth_x + jnp.where(kx > 0.0, 0.0, 1.0))
                inv_y = 1.0 / (depth_y + jnp.where(ky > 0.0, 0.0, 1.0))
                mean_x = 1.0 / jnp.maximum(kx, 1.0)
                mean_y = 1.0 / jnp.maximum(ky, 1.0)
                for m in range(2):
                    lane = slice(t * LN, (t + 1) * LN)
                    acc = bacc[m, t, pl.ds(r, 16), :]
                    tx = whole * xb[4 + m, t, pl.ds(g, 16), :] + moment * xf[m, t, pl.ds(g, 16), :] \
                        - WAVE_COURANT * depth_x * (east(acc, bacc[m, NEXT[t], pl.ds(r, 16), :]) - acc)
                    ty = whole * xb[6 + m, t, pl.ds(g, 16), :] + moment * xf[2 + m, t, pl.ds(g, 16), :] \
                        - WAVE_COURANT * depth_y * (bacc[m, t, pl.ds(r + 1, 16), :] - acc)
                    tx = jnp.where(kx > 0.0, tx, 0.0)
                    ty = jnp.where(ky > 0.0, ty, 0.0)
                    txb[m, pl.ds(r, 16), lane] = tx
                    tyb[m, pl.ds(r, 16), lane] = ty
                    corr[0, m, t, pl.ds(r, 16), :] = tx * inv_x - xsum[0, m, t, pl.ds(r, 16), :] * mean_x
                    corr[1, m, t, pl.ds(r, 16), :] = ty * inv_y - xsum[1, m, t, pl.ds(r, 16), :] * mean_y
        for copy in average_copies(i):
            copy.start()
        return carry
    lax.fori_loop(0, ROWS // AV, averages, 0)

    wait_send_all(map_copies())
    wait_send_all(flow_copies())
    wait_send_all(force_copies())
    for copy in packet_copies + eta_copies:
        copy.wait()
    for i in range(ROWS // AV):
        for copy in average_copies(i):
            copy.wait()

    def drain(c, carry):
        wait_send_all(edge_copies(c))
        for copy in stores(c):
            copy.wait()
        return carry
    lax.fori_loop(0, NCH, drain, 0)


def tracer_kernel(u_hbm, v_hbm, t_hbm, s_hbm, us_hbm, vs_hbm, eta_in, tx_in, ty_in, corr_in, kmask_in, col_in, rows_in,
                  eta_hbm, tx_hbm, ty_hbm, un_hbm, vn_hbm, tn_hbm, sn_hbm,
                  buf, tt, ts, ct, su, sv, small, corr, kmask, cols, rows, ld_sem, ed_sem, st_sem, sv_sem, in_sem, out_sem, table):
    hbm = (u_hbm, v_hbm, t_hbm, s_hbm)
    sources = (eta_in, tx_in, ty_in)
    sinks = (eta_hbm, tx_hbm, ty_hbm)

    def loads(c):
        out = []
        for f in range(4):
            for t in range(2):
                out.append(pltpu.make_async_copy(
                    hbm[f].at[pl.ds(c * TC, TC), :, :, pl.ds(t * LN, LN)],
                    buf.at[f, pl.ds(c * TC, TC), :, t, pl.ds(8, ROWS), :], ld_sem.at[c, f * 2 + t]))
        for f, (src, dst) in enumerate(((us_hbm, su), (vs_hbm, sv))):
            out.append(pltpu.make_async_copy(src.at[pl.ds(c * TC, TC)], dst.at[pl.ds(c * TC, TC)], ld_sem.at[c, 8 + f]))
        return out

    def stores_v(c):
        return [pltpu.make_async_copy(src.at[pl.ds(c * TC, TC)], dst.at[pl.ds(c * TC, TC)], sv_sem.at[c, f])
                for f, (src, dst) in enumerate(((su, un_hbm), (sv, vn_hbm)))]

    def stores_t(c):
        return [pltpu.make_async_copy(src.at[pl.ds(c * TC, TC)], dst.at[pl.ds(c * TC, TC)], st_sem.at[c, f])
                for f, (src, dst) in enumerate(((tt, tn_hbm), (ts, sn_hbm)))]

    edges = [pltpu.make_async_copy(src, dst, ed_sem.at[i])
             for i, (src, dst) in enumerate(((col_in, cols), (rows_in, rows), (corr_in, corr), (kmask_in, kmask)))]
    for copy in edges:
        copy.start()
    for c in range(AHEAD):
        for copy in loads(c):
            copy.start()
    write_table(table, DIFF_NUMBER)
    small_in = [pltpu.make_async_copy(sources[i], small.at[i], in_sem.at[i]) for i in range(3)]
    small_out = [pltpu.make_async_copy(small.at[i], sinks[i], out_sem.at[i]) for i in range(3)]
    for copy in small_in:
        copy.start()

    def zero_planes(i, carry):
        r = pl.multiple_of(i * 16, 16)
        z = jnp.zeros((16, 2 * LN), F32)
        for f in range(2):
            for m in range(2):
                for t in range(2):
                    ct[f, m, t, pl.ds(r, 16), :] = z[:, :LN]
        for m in range(2):
            for ref in (tt, ts):
                ref[LEVELS, m, pl.ds(r, 16), :] = z
        return carry
    lax.fori_loop(0, ROWS // 16, zero_planes, 0)
    for copy in edges:
        copy.wait()

    BR = 128
    SB = 16

    def level(k, c, kk):
        level_no = k.astype(F32)
        before = table[0, k]

        def block(i, carry):
            for q in range(0, BR, SB):
                piece(pl.multiple_of(i * BR + q, SB), pl.multiple_of(8 + i * BR + q, 8))
            return carry

        def piece(r, b):
            wet = [kmask[0, t, pl.ds(r, SB), :] > level_no for t in range(2)]
            packed = cols[c, pl.ds(b, SB), :]
            for m in range(2):
                j = kk * 2 + m
                u = [buf[0, k, m, t, pl.ds(b, SB), :] for t in range(2)]
                v = [buf[1, k, m, t, pl.ds(b, SB), :] for t in range(2)]
                vs = [buf[1, k, m, t, pl.ds(b - 1, SB), :] for t in range(2)]
                uw = west_pair(*u, halo(packed, j))
                for f, ref in ((2, tt), (3, ts)):
                    q = [buf[f, k, m, t, pl.ds(b, SB), :] for t in range(2)]
                    edge = halo(packed, f * PAIRS + j)
                    qe, qw = east_pair(*q, edge), west_pair(*q, edge)
                    for t in range(2):
                        lane = slice(t * LN, (t + 1) * LN)
                        fy = v[t] * (q[t] + buf[f, k, m, t, pl.ds(b + 1, SB), :])
                        fs = vs[t] * (q[t] + buf[f, k, m, t, pl.ds(b - 1, SB), :])
                        adv = q[t] - 0.5 * ((u[t] * (q[t] + qe[t]) - uw[t] * (q[t] + qw[t])) + (fy - fs))
                        adv = jnp.where(wet[t], adv, 0.0)
                        new = adv + before * ct[f - 2, m, t, pl.ds(r, SB), :]
                        ct[f - 2, m, t, pl.ds(r, SB), :] = new
                        ref[k, m, pl.ds(r, SB), lane] = new
            for t in range(2):
                lane = slice(t * LN, (t + 1) * LN)
                wet_x = kmask[1, t, pl.ds(r, SB), :] > level_no
                wet_y = kmask[2, t, pl.ds(r, SB), :] > level_no
                for m in range(2):
                    su[k, m, pl.ds(r, SB), lane] = jnp.where(wet_x, su[k, m, pl.ds(r, SB), lane] + corr[0, m, t, pl.ds(r, SB), :], 0.0)
                    sv[k, m, pl.ds(r, SB), lane] = jnp.where(wet_y, sv[k, m, pl.ds(r, SB), lane] + corr[1, m, t, pl.ds(r, SB), :], 0.0)
        lax.fori_loop(0, ROWS // BR, block, 0)

    def chunk_step(c, carry):
        @pl.when(c + AHEAD < LEVELS // TC)
        def _():
            for copy in loads(c + AHEAD):
                copy.start()

        for copy in loads(c):
            copy.wait()
        packet = c // (CHUNK // TC)
        first = lax.rem(c, CHUNK // TC) * TC
        for kk in range(TC):
            k = c * TC + kk
            for m in range(2):
                jj = (first + kk) * 2 + m
                for f in (1, 2, 3):
                    for t in range(2):
                        buf[f, k, m, t, 7:8, :] = rows[0, packet, t, f, pl.ds(jj, 1), :]
                for f in (2, 3):
                    for t in range(2):
                        buf[f, k, m, t, 8 + ROWS:9 + ROWS, :] = rows[1, packet, t, f, pl.ds(jj, 1), :]

        def one_level(kk, carry2):
            level(c * TC + kk, packet, first + kk)
            return carry2
        lax.fori_loop(0, TC, one_level, 0)
        for copy in stores_v(c):
            copy.start()
        return carry
    lax.fori_loop(0, LEVELS // TC, chunk_step, 0)

    for copy in small_in:
        copy.wait()
    for copy in small_out:
        copy.start()

    def upward(step, carry):
        c = LEVELS // TC - 1 - step

        def block(i, carry2):
            r = pl.multiple_of(i * UP, UP)
            for t in range(2):
                lane = slice(t * LN, (t + 1) * LN)
                depth = kmask[0, t, pl.ds(r, UP), :]
                below = [[ref[c * TC + TC, m, pl.ds(r, UP), lane] for m in range(2)] for ref in (tt, ts)]
                for kk in range(TC - 1, -1, -1):
                    k = c * TC + kk
                    level_no = k.astype(F32)
                    inv = jnp.where(depth > level_no + 1.0, table[2, k], jnp.where(depth > level_no, table[3, k], 0.0))
                    for f, ref in enumerate((tt, ts)):
                        for m in range(2):
                            below[f][m] = ref[k, m, pl.ds(r, UP), lane] * inv + table[1, k] * below[f][m]
                            ref[k, m, pl.ds(r, UP), lane] = below[f][m]
            return carry2
        lax.fori_loop(0, ROWS // UP, block, 0)
        for copy in stores_t(c):
            copy.start()
        return carry
    lax.fori_loop(0, LEVELS // TC, upward, 0)

    for copy in small_out:
        copy.wait()

    def drain(c, carry):
        for copy in stores_v(c) + stores_t(c):
            copy.wait()
        return carry
    lax.fori_loop(0, LEVELS // TC, drain, 0)


def solution(mesh):
    assert mesh.shape["col"] == 2 and mesh.shape["row"] == 4
    any_spec = pl.BlockSpec(memory_space=pl.ANY)
    shape = lambda *dims: jax.ShapeDtypeStruct(dims, F32)
    dma = lambda *dims: pltpu.SemaphoreType.DMA(dims)
    vm = lambda *dims: pltpu.VMEM(dims, F32)
    full = (LEVELS, 2, ROWS, 2 * LN)
    flat = (2, ROWS, 2 * LN)

    momentum = pl.pallas_call(
        momentum_kernel,
        name="momentum",
        out_shape=(shape(*full), shape(*full), shape(*flat), shape(*flat), shape(*flat), shape(2, 2, 2, ROWS, LN),
                   shape(3, 2, ROWS, LN), shape(NCH, PR, LN), shape(2, NCH, 2, 4, PAIRS, LN)),
        in_specs=[any_spec] * 10,
        out_specs=(any_spec,) * 9,
        scratch_shapes=[
            vm(4, LEVELS, 2, 2, PR, LN), vm(LEVELS + 1, 2, 2, ROWS, LN), vm(LEVELS + 1, 2, 2, ROWS, LN),
            vm(2, 2, ROWS, LN), vm(2, 2, ROWS, LN), vm(2, 2, PR, LN), vm(2, 2, PR, LN), vm(2, 2, PR, LN), vm(2, PR, LN), vm(ROWS, LN),
            vm(2, 2, 2, ROWS, LN), vm(2, 2, 2, ROWS, LN), vm(3, 2, ROWS, LN), pltpu.VMEM((ROWS, 2 * LN), jnp.int32),
            vm(2, 2, PR, LN), vm(2, 2, PR, LN), vm(2, 2, PR, LN), vm(*flat), vm(*flat), vm(2, 2, 2, ROWS, LN),
            vm(NCH, ROWS, LN), vm(NCH, PR, LN), vm(2, NCH, 2, 4, PAIRS, LN), vm(2, NCH, 2, 4, PAIRS, LN),
            vm(8, 3, EXT, LN), vm(4, ROWS, LN), vm(4, EXT, LN), vm(4, 3, EXT, LN), vm(2, ROWS, LN), vm(2, EXT, LN),
            vm(3, EXT, LN), vm(3, EXT, LN), vm(3, EXT, LN), vm(3, EXT, LN), vm(3, EXT, LN), vm(3, EXT, LN), vm(3, EXT, LN),
            vm(2, 3, EXT, LN), vm(2, 3, EXT, LN), vm(2, 3, EXT, LN), vm(2, 3, EXT, LN), vm(2, 2, ROWS + 8, LN), vm(2, 3, ROWS + 8, LN),
            dma(NCH, 8), dma(9), dma(NCH, 5), dma(NCH, 5), dma(7), dma(7), dma(5), dma(5), dma(NCH, 4), dma(6), dma(2, 3),
            pltpu.SMEM((SUBS,), F32), pltpu.SMEM((4, LEVELS), F32), pltpu.SemaphoreType.DMA,
        ],
        compiler_params=pltpu.CompilerParams(collective_id=0, has_side_effects=True, vmem_limit_bytes=67043328),
    )

    tracers = pl.pallas_call(
        tracer_kernel,
        name="tracers",
        out_shape=(shape(*flat), shape(*flat), shape(*flat), shape(*full), shape(*full), shape(*full), shape(*full)),
        in_specs=[any_spec] * 13,
        out_specs=(any_spec,) * 7,
        scratch_shapes=[
            vm(4, LEVELS, 2, 2, PR, LN), vm(LEVELS + 1, 2, ROWS, 2 * LN), vm(LEVELS + 1, 2, ROWS, 2 * LN), vm(2, 2, 2, ROWS, LN),
            vm(*full), vm(*full), vm(3, 2, ROWS, 2 * LN), vm(2, 2, 2, ROWS, LN), vm(3, 2, ROWS, LN),
            vm(NCH, PR, LN), vm(2, NCH, 2, 4, PAIRS, LN),
            dma(LEVELS // TC, 10), dma(4), dma(LEVELS // TC, 2), dma(LEVELS // TC, 2), dma(3), dma(3), pltpu.SMEM((4, LEVELS), F32),
        ],
        compiler_params=pltpu.CompilerParams(vmem_limit_bytes=67043328),
    )

    def local_step(vel_x, vel_y, pot_temp, salinity, surf_eta, trans_x, trans_y, col_depth, wet_levels, avg_weights):
        star_x, star_y, eta, tx, ty, corr, kmask, cols, rows = momentum(
            vel_x, vel_y, pot_temp, salinity, surf_eta, trans_x, trans_y, col_depth, wet_levels, avg_weights)
        return tracers(vel_x, vel_y, pot_temp, salinity, star_x, star_y, eta, tx, ty, corr, kmask, cols, rows)

    spec_3d = P(None, None, "row", "col")
    spec_2d = P(None, "row", "col")
    spec_map = P("row", "col")
    return jax.shard_map(local_step, mesh=mesh, in_specs=(spec_3d, spec_3d, spec_3d, spec_3d, spec_2d, spec_2d, spec_2d, spec_map, spec_map, P()),
                         out_specs=(spec_2d, spec_2d, spec_2d, spec_3d, spec_3d, spec_3d, spec_3d), check_vma=False)
```
